32 devices in a mesh: data: 2 (over x), model: 4 (over z), stage: 4 (over y, core).
Axes of the slice: x: 2, y: 2, z: 4, core: 2. Of those that a mesh axis runs over, the one named last changes fastest.
Arguments:
- x_in: bfloat16 [6, 512, 1536], P('data'), parts along dimension 0
- y_target: bfloat16 [6, 512, 1536], P('data'), parts along dimension 0
- w_qkv: bfloat16 [4, 1536, 3, 12, 128], P('stage', None, None, 'model')
- w_out: bfloat16 [4, 12, 128, 1536], P('stage', 'model')
- w_up: bfloat16 [4, 1536, 6144], P('stage', None, 'model')
- w_down: bfloat16 [4, 6144, 1536], P('stage', 'model')
- norm_gain: bfloat16 [4, 2, 1536], P('stage')
Outputs:
- output 1: float32 [2], P('data'), parts along dimension 0
- output 2: float32 [8, 1536, 3, 12, 128], P(('data', 'stage'), None, None, 'model'), parts along dimension 0
- output 3: float32 [8, 12, 128, 1536], P(('data', 'stage'), 'model'), parts along dimension 0
- output 4: float32 [8, 1536, 6144], P(('data', 'stage'), None, 'model'), parts along dimension 0
- output 5: float32 [8, 6144, 1536], P(('data', 'stage'), 'model'), parts along dimension 0
- output 6: float32 [8, 2, 1536], P(('data', 'stage')), parts along dimension 0
There are 2 independent parts. The reference program is written for one: setup_inputs(seed, part) draws one part's arguments, and reference() takes and returns one part's arrays. A program takes and returns all parts, laid end to end along the dimension named above; an argument that names none is the same for every part.
All inputs are finite; a program needn't handle non-finite values.
Results may differ from the reference program's by a relative error of at most 0.00722361.
Values are sent between devices in bfloat16 or wider.
A program may use at most 1 GiB of HBM per device.

```python
import jax
import jax.numpy as jnp
from jax import lax

BATCH = 3
SEQ = 512
D = 1536
HEADS = 12
LAYERS = 4

HEAD = D // HEADS
FF = 4 * D
QUERY_BLOCK = min(SEQ, 256)
NORM_EPS = 1e-6
NEG_BIG = -1e30


def setup_inputs(seed: int = 0, part: int = 0) -> dict:
    part_key = jax.random.fold_in(jax.random.key(seed), part)
    key_x, key_y = jax.random.split(part_key, 2)
    key_qkv, key_out, key_up, key_down, key_gain = jax.random.split(jax.random.key(seed + 1), 5)
    x_in = jax.random.normal(key_x, (BATCH, SEQ, D), jnp.float32)
    y_target = jax.random.normal(key_y, (BATCH, SEQ, D), jnp.float32)
    w_qkv = jax.random.normal(key_qkv, (LAYERS, D, 3, HEADS, HEAD), jnp.float32) * D ** -0.5
    w_out = jax.random.normal(key_out, (LAYERS, HEADS, HEAD, D), jnp.float32) * D ** -0.5
    w_up = jax.random.normal(key_up, (LAYERS, D, FF), jnp.float32) * D ** -0.5
    w_down = jax.random.normal(key_down, (LAYERS, FF, D), jnp.float32) * FF ** -0.5
    norm_gain = 1.0 + 0.3 * jax.random.normal(key_gain, (LAYERS, 2, D), jnp.float32)
    return {
        "x_in": x_in.astype(jnp.bfloat16),
        "y_target": y_target.astype(jnp.bfloat16),
        "w_qkv": w_qkv.astype(jnp.bfloat16),
        "w_out": w_out.astype(jnp.bfloat16),
        "w_up": w_up.astype(jnp.bfloat16),
        "w_down": w_down.astype(jnp.bfloat16),
        "norm_gain": norm_gain.astype(jnp.bfloat16),
    }


def rms_scale(hid32, gain32):
    inv_rms = lax.rsqrt(jnp.mean(hid32 * hid32, axis=-1, keepdims=True) + NORM_EPS)
    return (hid32 * inv_rms * gain32).astype(jnp.bfloat16)


def attend_sequence(qkv_seq):
    q_seq = qkv_seq[:, 0].astype(jnp.float32)
    k_seq = qkv_seq[:, 1].astype(jnp.float32)
    v_seq = qkv_seq[:, 2].astype(jnp.float32)
    key_pos = jnp.arange(SEQ)

    def query_block(block_start):
        q_blk = lax.dynamic_slice_in_dim(q_seq, block_start, QUERY_BLOCK, 0)
        scores = jnp.einsum("qhe,khe->hqk", q_blk, k_seq) * HEAD ** -0.5
        q_pos = block_start + jnp.arange(QUERY_BLOCK)
        scores = jnp.where(key_pos[None, None, :] <= q_pos[None, :, None], scores, NEG_BIG)
        attn_probs = jax.nn.softmax(scores, axis=-1).astype(jnp.bfloat16)
        return jnp.einsum("hqk,khe->qhe", attn_probs.astype(jnp.float32), v_seq).astype(jnp.bfloat16)

    blocks = lax.map(jax.checkpoint(query_block), jnp.arange(SEQ // QUERY_BLOCK) * QUERY_BLOCK)
    return blocks.reshape(SEQ, HEADS, HEAD)


def layer_forward(hid, layer_w):
    w_qkv_l, w_out_l, w_up_l, w_down_l, gain_l = layer_w
    hid32 = hid.reshape(BATCH * SEQ, D).astype(jnp.float32)
    norm_a = rms_scale(hid32, gain_l[0])
    qkv_act = jnp.dot(norm_a, w_qkv_l.reshape(D, 3 * D), preferred_element_type=jnp.float32).astype(jnp.bfloat16)
    attn_act = lax.map(attend_sequence, qkv_act.reshape(BATCH, SEQ, 3, HEADS, HEAD))
    mid_hid = hid32 + jnp.dot(attn_act.reshape(BATCH * SEQ, D), w_out_l.reshape(D, D), preferred_element_type=jnp.float32)
    norm_b = rms_scale(mid_hid, gain_l[1])
    up_act = jnp.dot(norm_b, w_up_l, preferred_element_type=jnp.float32)
    gelu_act = jax.nn.gelu(up_act, approximate=True).astype(jnp.bfloat16)
    new_hid = mid_hid + jnp.dot(gelu_act, w_down_l, preferred_element_type=jnp.float32)
    return new_hid.astype(jnp.bfloat16).reshape(BATCH, SEQ, D)


def total_loss(weights, x_in, y_target):
    def layer_step(hid, layer_w):
        return jax.checkpoint(layer_forward)(hid, layer_w), None

    final_hid = lax.scan(layer_step, x_in, weights)[0]
    loss_diff = final_hid.astype(jnp.float32) - y_target.astype(jnp.float32)
    return 0.5 * jnp.mean(loss_diff * loss_diff)


def reference(x_in, y_target, w_qkv, w_out, w_up, w_down, norm_gain):
    weights = (w_qkv, w_out, w_up, w_down, norm_gain.astype(jnp.float32))
    loss_val, grads = jax.value_and_grad(total_loss)(weights, x_in, y_target)
    return (
        loss_val.reshape(1),
        grads[0].astype(jnp.float32),
        grads[1].astype(jnp.float32),
        grads[2].astype(jnp.float32),
        grads[3].astype(jnp.float32),
        grads[4].astype(jnp.float32),
    )
```

```python
import jax
import jax.numpy as jnp
from jax import lax
from jax.experimental import pallas as pl
from jax.experimental.pallas import tpu as pltpu
from jax.sharding import PartitionSpec as P

NORM_EPS = 1e-6
NEG_BIG = -1e30
MESH = pl.DeviceIdType.MESH
GELU_K = 0.7978845608028654
GELU_C = 0.044715
F32 = jnp.float32
BF16 = jnp.bfloat16


def dot_nn(a, b):
    return lax.dot_general(a, b, (((1,), (0,)), ((), ())), preferred_element_type=F32)


def dot_nt(a, b):
    return lax.dot_general(a, b, (((1,), (1,)), ((), ())), preferred_element_type=F32)


def dot_tn(a, b):
    return lax.dot_general(a, b, (((0,), (0,)), ((), ())), preferred_element_type=F32)


def rms_inverse(v32):
    return lax.rsqrt(jnp.mean(v32 * v32, axis=-1, keepdims=True) + NORM_EPS)


def layer_step(dims, x_in, y_target, w_qkv, w_out, w_up, w_down, gain):
    nz, ns = dims["model"], dims["stage"]
    n_seq, seq_len, d_model = x_in.shape
    qkv_w = w_qkv.shape[1]
    att_w = w_out.shape[0]
    ff_w = w_up.shape[1]
    head_dim = 128
    n_head = att_w // head_dim
    tok = 128
    row = tok // nz
    per_seq = seq_len // tok
    n_unit = n_seq * per_seq
    n_chunk = n_unit // 2
    scale = head_dim ** -0.5
    inv_count = 1.0 / (n_seq * seq_len * d_model)
    last_z, last_s = nz - 1, ns - 1
    sub_rows = 16

    def kernel(x_ref, y_ref, wqkv_h, wout_h, wup_h, wdown_h, gain_ref,
               a_out, b_out, d_out, dm_out, dqkv_out, o_out, z_out, du_out, red_out,
               wqkv, wout, wup, wdown, hslot, yslot, dslot, abuf, bbuf, dbuf, dmbuf,
               qkv_all, u_all, m_all, ost, zst, dust, dqkvst, dattst, part,
               recv_r, recv_l, send_r, send_l, accq, hout, dmid, dkacc, dvacc,
               lossacc, ga8, gb8, gx,
               w_sem, hsem, ysem, dsem, hs_sem, save_sem,
               ag_rs, ag_sr, ag_sl, rs_rr, rs_rl, rs_sr, rs_sl, loss_sem, gx_s, gx_r):
        z = lax.axis_index("model")
        st = lax.axis_index("stage")
        is_first = st == 0
        is_last = st == last_s

        def rdma(src, dst, ssem, rsem, dev):
            return pltpu.make_async_remote_copy(src_ref=src, dst_ref=dst, send_sem=ssem, recv_sem=rsem,
                                                device_id=dev, device_id_type=MESH)

        def rows_of(k):
            return pl.ds(pl.multiple_of(k * row, row), row)

        w_copies = [pltpu.make_async_copy(src, dst, w_sem.at[i])
                    for i, (src, dst) in enumerate(((wqkv_h, wqkv), (wout_h, wout), (wup_h, wup), (wdown_h, wdown)))]

        def unit_rows(u):
            return lax.div(u, per_seq), pl.ds(pl.multiple_of(lax.rem(u, per_seq) * tok + z * row, row), row)

        def x_copy(u):
            q, rs = unit_rows(u)
            return pltpu.make_async_copy(x_ref.at[q, rs, :], hslot.at[u], hsem.at[u])

        def y_copy(u):
            q, rs = unit_rows(u)
            return pltpu.make_async_copy(y_ref.at[q, rs, :], yslot.at[u], ysem.at[u])

        @pl.when(is_first)
        def _():
            @pl.loop(0, n_unit)
            def _(u):
                x_copy(u).start()

        for cp in w_copies:
            cp.start()

        @pl.when(is_last)
        def _():
            @pl.loop(0, n_unit)
            def _(u):
                y_copy(u).start()

        barrier = pltpu.get_barrier_semaphore()
        for dz in range(1, nz):
            pl.semaphore_signal(barrier, inc=1, device_id={"model": lax.rem(z + dz, nz)}, device_id_type=MESH)

        @pl.when(st < last_s)
        def _():
            pl.semaphore_signal(barrier, inc=1, device_id={"stage": st + 1}, device_id_type=MESH)

        @pl.when(st > 0)
        def _():
            pl.semaphore_signal(barrier, inc=1, device_id={"stage": st - 1}, device_id_type=MESH)

        qkv_all[...] = jnp.zeros_like(qkv_all)
        lossacc[...] = jnp.zeros_like(lossacc)
        ga8[...] = jnp.zeros_like(ga8)
        gb8[...] = jnp.zeros_like(gb8)
        @pl.when((st == 0) | (st == last_s))
        def _():
            pl.semaphore_wait(barrier, nz)

        @pl.when((st > 0) & (st < last_s))
        def _():
            pl.semaphore_wait(barrier, nz + 1)

        def h_in_copy(u):
            return rdma(hout.at[0], hslot.at[u], hs_sem.at[0], hsem.at[u], {"stage": st})

        def h_send(s, u):
            return rdma(hout.at[s], hslot.at[u], hs_sem.at[s], hsem.at[u], {"stage": st + 1})

        def d_send(s, u):
            return rdma(hout.at[s], dslot.at[u], hs_sem.at[s], dsem.at[u], {"stage": st - 1})

        def ag_right(buf, kind, s, j):
            blk = buf.at[s, rows_of(j), :]
            return rdma(blk, blk, ag_sr.at[kind, s, j], ag_rs.at[kind, s, j], {"model": z + 1})

        def ag_left(buf, kind, s, j):
            blk = buf.at[s, rows_of(j), :]
            return rdma(blk, blk, ag_sl.at[kind, s, j], ag_rs.at[kind, s, j], {"model": z - 1})

        def ag_start(buf, kind, s):
            @pl.when(z < last_z)
            def _():
                ag_right(buf, kind, s, z).start()

            @pl.when(z > 0)
            def _():
                ag_left(buf, kind, s, z).start()

        def ag_step(buf, kind, s, t):
            @pl.when(z >= t)
            def _():
                ag_right(buf, kind, s, z - t).wait_recv()

                @pl.when(z < last_z)
                def _():
                    ag_right(buf, kind, s, z - t).start()

            @pl.when(z + t <= last_z)
            def _():
                ag_left(buf, kind, s, z + t).wait_recv()

                @pl.when(z > 0)
                def _():
                    ag_left(buf, kind, s, z + t).start()

        def ag_drain(buf, kind, s):
            for j in range(nz):
                @pl.when((z >= j) & (z < last_z))
                def _():
                    ag_right(buf, kind, s, j).wait_send()

                @pl.when((z <= j) & (z > 0))
                def _():
                    ag_left(buf, kind, s, j).wait_send()

        def rs_right(s, k):
            return rdma(send_r.at[s, k], recv_r.at[s, k], rs_sr.at[s, k], rs_rr.at[s, k], {"model": z + 1})

        def rs_left(s, k):
            return rdma(send_l.at[s, k], recv_l.at[s, k], rs_sl.at[s, k], rs_rl.at[s, k], {"model": z - 1})

        def rs_step(s, t):
            kr = last_z - t + z
            kl = t - last_z + z

            @pl.when(z == 0)
            def _():
                send_r[s, kr] = part[s, rows_of(kr), :].astype(BF16)
                rs_right(s, kr).start()

            @pl.when((z > 0) & (z <= t))
            def _():
                rs_right(s, kr).wait_recv()
                send_r[s, kr] = (part[s, rows_of(kr), :] + recv_r[s, kr].astype(F32)).astype(BF16)
                rs_right(s, kr).start()

            @pl.when(z == last_z)
            def _():
                send_l[s, kl] = part[s, rows_of(kl), :].astype(BF16)
                rs_left(s, kl).start()

            @pl.when((z < last_z) & (last_z - z <= t))
            def _():
                rs_left(s, kl).wait_recv()
                send_l[s, kl] = (part[s, rows_of(kl), :] + recv_l[s, kl].astype(F32)).astype(BF16)
                rs_left(s, kl).start()

        def rs_final(s):
            accq[s] = part[s, rows_of(z), :]

            @pl.when(z > 0)
            def _():
                rs_right(s, z).wait_recv()
                accq[s] += recv_r[s, z].astype(F32)

            @pl.when(z < last_z)
            def _():
                rs_left(s, z).wait_recv()
                accq[s] += recv_l[s, z].astype(F32)

        def rs_drain(s):
            for k in range(1, nz):
                @pl.when(z < k)
                def _():
                    rs_right(s, k).wait_send()

            for k in range(nz - 1):
                @pl.when(z > k)
                def _():
                    rs_left(s, k).wait_send()

        def save(kind, src, dst, s, u):
            return pltpu.make_async_copy(src.at[s], dst.at[u], save_sem.at[kind, s])

        def softmax_of(u, p, i):
            first = u - p
            cols = pl.ds(i * head_dim, head_dim)
            q = qkv_all[u, :, cols]
            k = qkv_all[pl.ds(first, per_seq), :, pl.ds(att_w + i * head_dim, head_dim)].reshape(seq_len, head_dim)
            v = qkv_all[pl.ds(first, per_seq), :, pl.ds(2 * att_w + i * head_dim, head_dim)].reshape(seq_len, head_dim)
            sc = dot_nt(q, k) * scale
            q_pos = p * tok + lax.broadcasted_iota(jnp.int32, sc.shape, 0)
            k_pos = lax.broadcasted_iota(jnp.int32, sc.shape, 1)
            sc = jnp.where(k_pos <= q_pos, sc, NEG_BIG)
            e = jnp.exp(sc - jnp.max(sc, axis=-1, keepdims=True))
            pr = e * (1.0 / jnp.sum(e, axis=-1, keepdims=True))
            return q, k, v, pr

        gain_a = gain_ref[0:1, :]
        gain_b = gain_ref[1:2, :]

        def fwd_chunk(c, carry):
            for s in range(2):
                u = 2 * c + s

                @pl.when(is_first)
                def _():
                    x_copy(u).wait()

                @pl.when(st > 0)
                def _():
                    h_in_copy(u).wait_recv()

                h32 = hslot[u].astype(F32)
                abuf[s, rows_of(z), :] = (h32 * rms_inverse(h32) * gain_a).astype(BF16)
                ag_start(abuf, 0, s)
            for t in range(1, nz):
                for s in range(2):
                    ag_step(abuf, 0, s, t)

            @pl.when(c == 0)
            def _():
                w_copies[0].wait()
                w_copies[1].wait()

            def attention_part(s, carry):
                u = 2 * c + s
                p = lax.rem(u, per_seq)
                save(0, abuf, a_out, s, u).start()
                qkv_all[u] = dot_nn(abuf[s], wqkv[...]).astype(BF16)
                for i in range(n_head):
                    _, _, v, pr = softmax_of(u, p, i)
                    ost[s, :, pl.ds(i * head_dim, head_dim)] = dot_nn(pr.astype(BF16), v).astype(BF16)
                save(1, ost, o_out, s, u).start()
                part[s] = dot_nn(ost[s], wout[...])
                rs_step(s, 0)
                return carry

            lax.fori_loop(0, 2, attention_part, 0)
            for t in range(1, nz - 1):
                for s in range(2):
                    rs_step(s, t)
            for s in range(2):
                u = 2 * c + s
                rs_final(s)
                m = hslot[u].astype(F32) + accq[s]
                m_all[u] = m
                bbuf[s, rows_of(z), :] = (m * rms_inverse(m) * gain_b).astype(BF16)
                ag_start(bbuf, 1, s)
            for s in range(2):
                rs_drain(s)
                ag_drain(abuf, 0, s)
            for t in range(1, nz):
                for s in range(2):
                    ag_step(bbuf, 1, s, t)

            @pl.when(c == 0)
            def _():
                w_copies[2].wait()
                w_copies[3].wait()

            def mlp_part(s, carry):
                u = 2 * c + s
                save(0, abuf, a_out, s, u).wait()
                save(2, bbuf, b_out, s, u).start()
                u_all[u] = dot_nn(bbuf[s], wup[...])

                def act(r, carry):
                    rr = pl.ds(pl.multiple_of(r * sub_rows, sub_rows), sub_rows)
                    v = u_all[u, rr, :]
                    th = jnp.tanh(GELU_K * (v + GELU_C * (v * v * v)))
                    zst[s, rr, :] = (0.5 * v * (1.0 + th)).astype(BF16)
                    return carry

                lax.fori_loop(0, tok // sub_rows, act, 0)
                save(3, zst, z_out, s, u).start()
                part[s] = dot_nn(zst[s], wdown[...])
                rs_step(s, 0)
                return carry

            lax.fori_loop(0, 2, mlp_part, 0)
            for t in range(1, nz - 1):
                for s in range(2):
                    rs_step(s, t)
            for s in range(2):
                u = 2 * c + s
                rs_final(s)
                h_new = (m_all[u] + accq[s]).astype(BF16)

                @pl.when(st < last_s)
                def _():
                    hout[s] = h_new
                    h_send(s, u).start()

                @pl.when(is_last)
                def _():
                    y_copy(u).wait()
                    diff = h_new.astype(F32) - yslot[u].astype(F32)
                    dslot[u] = (diff * inv_count).astype(BF16)
                    lossacc[...] += jnp.sum((diff * diff).reshape(row // 8, 8, d_model), axis=0)
            for s in range(2):
                u = 2 * c + s
                rs_drain(s)
                ag_drain(bbuf, 1, s)

                @pl.when(st < last_s)
                def _():
                    h_send(s, u).wait_send()

                save(1, ost, o_out, s, u).wait()
                save(2, bbuf, b_out, s, u).wait()
                save(3, zst, z_out, s, u).wait()
            return carry

        lax.fori_loop(0, n_chunk, fwd_chunk, 0)

        def loss_send():
            return rdma(lossacc, lossacc, loss_sem.at[0], loss_sem.at[1], {"stage": st - 1})

        @pl.when(is_last)
        def _():
            loss_send().start()

        def bwd_chunk(step, carry):
            c = n_chunk - 1 - step
            for s in (1, 0):
                u = 2 * c + s

                @pl.when(st < last_s)
                def _():
                    d_send(0, u).wait_recv()

                dbuf[s, rows_of(z), :] = dslot[u]
                ag_start(dbuf, 2, s)
            for t in range(1, nz):
                for s in (1, 0):
                    ag_step(dbuf, 2, s, t)

            def mlp_back(i, carry):
                s = 1 - i
                u = 2 * c + s
                save(4, dbuf, d_out, s, u).start()
                part[s] = dot_nt(dbuf[s], wdown[...])

                def act(r, carry):
                    rr = pl.ds(pl.multiple_of(r * sub_rows, sub_rows), sub_rows)
                    v = u_all[u, rr, :]
                    v2 = v * v
                    th = jnp.tanh(GELU_K * (v + GELU_C * (v2 * v)))
                    slope = 0.5 * (1.0 + th) + 0.5 * v * (1.0 - th * th) * (GELU_K * (1.0 + 3.0 * GELU_C * v2))
                    dust[s, rr, :] = (part[s, rr, :] * slope).astype(BF16)
                    return carry

                lax.fori_loop(0, tok // sub_rows, act, 0)
                save(5, dust, du_out, s, u).start()
                part[s] = dot_nt(dust[s], wup[...])
                rs_step(s, 0)
                return carry

            lax.fori_loop(0, 2, mlp_back, 0)
            for t in range(1, nz - 1):
                for s in (1, 0):
                    rs_step(s, t)
            for s in (1, 0):
                u = 2 * c + s
                rs_final(s)
                m = m_all[u]
                inv = rms_inverse(m)
                normed = m * inv
                dn = accq[s]
                gb8[...] += jnp.sum((dn * normed).reshape(row // 8, 8, d_model), axis=0)
                dn = dn * gain_b
                dm = dslot[u].astype(F32) + inv * (dn - normed * jnp.mean(dn * normed, axis=-1, keepdims=True))
                dmid[s] = dm
                dmbuf[s, rows_of(z), :] = dm.astype(BF16)
                ag_start(dmbuf, 3, s)
            for s in (1, 0):
                rs_drain(s)
                ag_drain(dbuf, 2, s)
            for t in range(1, nz):
                for s in (1, 0):
                    ag_step(dmbuf, 3, s, t)

            def attention_back(i, carry):
                s = 1 - i
                u = 2 * c + s
                p = lax.rem(u, per_seq)
                save(4, dbuf, d_out, s, u).wait()
                save(6, dmbuf, dm_out, s, u).start()

                @pl.when(p == per_seq - 1)
                def _():
                    dkacc[...] = jnp.zeros_like(dkacc)
                    dvacc[...] = jnp.zeros_like(dvacc)

                dattst[s] = dot_nt(dmbuf[s], wout[...]).astype(BF16)
                p_rows = pl.ds(pl.multiple_of(p * tok, tok), tok)
                for h in range(n_head):
                    cols = pl.ds(h * head_dim, head_dim)
                    q, k, v, pr = softmax_of(u, p, h)
                    da = dattst[s, :, cols]
                    dp = dot_nt(da, v)
                    ds = (pr * (dp - jnp.sum(pr * dp, axis=-1, keepdims=True)) * scale).astype(BF16)
                    dvacc[:, cols] += dot_tn(pr.astype(BF16), da)
                    dkacc[:, cols] += dot_tn(ds, q)
                    dqkvst[s, :, cols] = dot_nn(ds, k).astype(BF16)
                dqkvst[s, :, pl.ds(att_w, att_w)] = dkacc[p_rows, :].astype(BF16)
                dqkvst[s, :, pl.ds(2 * att_w, att_w)] = dvacc[p_rows, :].astype(BF16)
                save(7, dqkvst, dqkv_out, s, u).start()
                part[s] = dot_nt(dqkvst[s], wqkv[...])
                rs_step(s, 0)
                return carry

            lax.fori_loop(0, 2, attention_back, 0)
            for t in range(1, nz - 1):
                for s in (1, 0):
                    rs_step(s, t)
            for s in (1, 0):
                u = 2 * c + s
                rs_final(s)
                h32 = hslot[u].astype(F32)
                inv = rms_inverse(h32)
                normed = h32 * inv
                dn = accq[s]
                ga8[...] += jnp.sum((dn * normed).reshape(row // 8, 8, d_model), axis=0)

                @pl.when(st > 0)
                def _():
                    dg = dn * gain_a
                    hout[s] = (dmid[s] + inv * (dg - normed * jnp.mean(dg * normed, axis=-1, keepdims=True))).astype(BF16)
                    d_send(s, u).start()
            for s in (1, 0):
                u = 2 * c + s
                rs_drain(s)
                ag_drain(dmbuf, 3, s)

                @pl.when(st > 0)
                def _():
                    d_send(s, u).wait_send()

                save(5, dust, du_out, s, u).wait()
                save(6, dmbuf, dm_out, s, u).wait()
                save(7, dqkvst, dqkv_out, s, u).wait()
            return carry

        lax.fori_loop(0, n_chunk, bwd_chunk, 0)

        @pl.when(is_last)
        def _():
            loss_send().wait_send()

        @pl.when(st < last_s)
        def _():
            loss_send().wait_recv()

            @pl.when(st > 0)
            def _():
                loss_send().start()
                loss_send().wait_send()

        loss_row = jnp.sum(jnp.sum(lossacc[...], axis=0, keepdims=True), axis=1, keepdims=True)
        gx[z, 0:1, :] = jnp.sum(ga8[...], axis=0, keepdims=True)
        gx[z, 1:2, :] = jnp.sum(gb8[...], axis=0, keepdims=True)
        gx[z, 2:8, :] = jnp.broadcast_to(loss_row, (6, d_model))

        def gx_send(dz):
            return rdma(gx.at[z], gx.at[z], gx_s.at[dz], gx_r.at[z], {"model": lax.rem(z + dz, nz)})

        def gx_recv(dz):
            j = lax.rem(z + dz, nz)
            return rdma(gx.at[j], gx.at[j], gx_s.at[dz], gx_r.at[j], {"model": j})

        for dz in range(1, nz):
            gx_send(dz).start()
        for dz in range(1, nz):
            gx_recv(dz).wait_recv()
        red_out[...] = gx[0] + gx[1] + gx[2] + gx[3]
        for dz in range(1, nz):
            gx_send(dz).wait_send()

    any_spec = pl.BlockSpec(memory_space=pl.ANY)
    vmem_spec = pl.BlockSpec(memory_space=pltpu.VMEM)

    def out(width):
        return jax.ShapeDtypeStruct((n_unit, tok, width), BF16)

    dma = pltpu.SemaphoreType.DMA
    return pl.pallas_call(
        kernel,
        out_shape=(out(d_model), out(d_model), out(d_model), out(d_model), out(qkv_w), out(att_w), out(ff_w), out(ff_w),
                   jax.ShapeDtypeStruct((8, d_model), F32)),
        in_specs=[any_spec] * 6 + [vmem_spec],
        out_specs=(any_spec,) * 8 + (vmem_spec,),
        scratch_shapes=[
            pltpu.VMEM((d_model, qkv_w), BF16), pltpu.VMEM((att_w, d_model), BF16),
            pltpu.VMEM((d_model, ff_w), BF16), pltpu.VMEM((ff_w, d_model), BF16),
            pltpu.VMEM((n_unit, row, d_model), BF16), pltpu.VMEM((n_unit, row, d_model), BF16),
            pltpu.VMEM((n_unit, row, d_model), BF16),
            pltpu.VMEM((2, tok, d_model), BF16), pltpu.VMEM((2, tok, d_model), BF16),
            pltpu.VMEM((2, tok, d_model), BF16), pltpu.VMEM((2, tok, d_model), BF16),
            pltpu.VMEM((n_unit, tok, qkv_w), BF16), pltpu.VMEM((n_unit, tok, ff_w), F32),
            pltpu.VMEM((n_unit, row, d_model), F32),
            pltpu.VMEM((2, tok, att_w), BF16), pltpu.VMEM((2, tok, ff_w), BF16), pltpu.VMEM((2, tok, ff_w), BF16),
            pltpu.VMEM((2, tok, qkv_w), BF16), pltpu.VMEM((2, tok, att_w), BF16), pltpu.VMEM((2, tok, d_model), F32),
            pltpu.VMEM((2, nz, row, d_model), BF16), pltpu.VMEM((2, nz, row, d_model), BF16),
            pltpu.VMEM((2, nz, row, d_model), BF16), pltpu.VMEM((2, nz, row, d_model), BF16),
            pltpu.VMEM((2, row, d_model), F32), pltpu.VMEM((2, row, d_model), BF16), pltpu.VMEM((2, row, d_model), F32),
            pltpu.VMEM((seq_len, att_w), F32), pltpu.VMEM((seq_len, att_w), F32),
            pltpu.VMEM((8, d_model), F32), pltpu.VMEM((8, d_model), F32), pltpu.VMEM((8, d_model), F32),
            pltpu.VMEM((nz, 8, d_model), F32),
            dma((4,)), dma((n_unit,)), dma((n_unit,)), dma((n_unit,)), dma((2,)), dma((8, 2)),
            dma((4, 2, nz)), dma((4, 2, nz)), dma((4, 2, nz)),
            dma((2, nz)), dma((2, nz)), dma((2, nz)), dma((2, nz)), dma((2,)), dma((nz,)), dma((nz,)),
        ],
        compiler_params=pltpu.CompilerParams(collective_id=0, has_side_effects=True, vmem_limit_bytes=66_000_000),
        name="layer_step",
    )(x_in, y_target, w_qkv, w_out, w_up, w_down, gain)


def weight_grad(act, grad):
    return lax.dot_general(act, grad, (((0, 1), (0, 1)), ((), ())), preferred_element_type=F32)


def solution(mesh):
    dims = dict(mesh.shape)

    def device_fn(x_in, y_target, w_qkv, w_out, w_up, w_down, norm_gain):
        n_batch, seq_len, d_model = x_in.shape
        heads, head_dim = w_qkv.shape[3], w_qkv.shape[4]
        a, b, d, dm, dqkv, o, zz, du, red = layer_step(
            dims, x_in, y_target,
            w_qkv[0].reshape(d_model, 3 * heads * head_dim), w_out[0].reshape(heads * head_dim, d_model),
            w_up[0], w_down[0], norm_gain[0].astype(F32))
        grad_qkv = weight_grad(a, dqkv).reshape(1, d_model, 3, heads, head_dim)
        grad_out = weight_grad(o, dm).reshape(1, heads, head_dim, d_model)
        grad_up = weight_grad(b, du)[None]
        grad_down = weight_grad(zz, d)[None]
        loss = 0.5 * red[2, 0:1] / (n_batch * seq_len * d_model)
        return loss, grad_qkv, grad_out, grad_up, grad_down, red[None, 0:2]

    act_spec = P("data", None, None)
    weight_specs = (
        P("stage", None, None, "model", None),
        P("stage", "model", None, None),
        P("stage", None, "model"),
        P("stage", "model", None),
        P("stage", None, None),
    )
    grad_specs = (
        P(("data", "stage"), None, None, "model", None),
        P(("data", "stage"), "model", None, None),
        P(("data", "stage"), None, "model"),
        P(("data", "stage"), "model", None),
        P(("data", "stage"), None, None),
    )
    return jax.shard_map(
        device_fn,
        mesh=mesh,
        in_specs=(act_spec, act_spec) + weight_specs,
        out_specs=(P("data"),) + grad_specs,
        check_vma=False,
    )
```

```python
import jax
import jax.numpy as jnp
from jax import lax
from jax.experimental import pallas as pl
from jax.experimental.pallas import tpu as pltpu
from jax.sharding import PartitionSpec as P

NORM_EPS = 1e-6
NEG_BIG = -1e30
MESH = pl.DeviceIdType.MESH
GELU_K = 0.7978845608028654
GELU_C = 0.044715
F32 = jnp.float32
BF16 = jnp.bfloat16


def dot_nn(a, b):
    return lax.dot_general(a, b, (((1,), (0,)), ((), ())), preferred_element_type=F32)


def dot_nt(a, b):
    return lax.dot_general(a, b, (((1,), (1,)), ((), ())), preferred_element_type=F32)


def dot_tn(a, b):
    return lax.dot_general(a, b, (((0,), (0,)), ((), ())), preferred_element_type=F32)


def rms_inverse(v32):
    return lax.rsqrt(jnp.mean(v32 * v32, axis=-1, keepdims=True) + NORM_EPS)


FWD_ORDER = (0, 1, 7, 5, 10, 13, 11, 2, 8, 6, 14, 12, 3, 4, 9)
BWD_ORDER = (10, 5, 0, 11, 2, 8, 12, 6, 3, 4, 13, 9, 7, 1, 14)


def lags(order):
    place = {phase: i for i, phase in enumerate(order)}
    lag = [0]
    for phase in range(1, len(order)):
        lag.append(lag[-1] + (1 if place[phase] < place[phase - 1] else 0))
    return lag


def layer_step(dims, x_in, y_target, w_qkv, w_out, w_up, w_down, gain):
    nz, ns = dims["model"], dims["stage"]
    n_seq, seq_len, d_model = x_in.shape
    n_slab, _, head_dim = w_qkv.shape
    qkv_w = n_slab * head_dim
    att_w = w_out.shape[0]
    ff_w = w_up.shape[1]
    n_head = att_w // head_dim
    tok = 128
    row = tok // nz
    per_seq = seq_len // tok
    n_unit = n_seq * per_seq
    scale = head_dim ** -0.5
    inv_count = 1.0 / (n_seq * seq_len * d_model)
    last_z, last_s = nz - 1, ns - 1
    sub_rows = 16
    n_send, n_recv, n_gath = 2, 3, 4

    def kernel(x_ref, y_ref, wqkv_h, wout_h, wup_h, wdown_h, gain_ref,
               a_out, b_out, d_out, dm_out, dqkv_out, o_out, z_out, du_out, red_out,
               wqkv, wout, wup, wdown, hslot, yslot, a_all, d_all, bbuf, dmbuf, xtmp,
               qkv_all, u_all, m_all, ost, zst, dust, dqkvst, datt, part,
               recv_r, recv_l, send_r, send_l, accq, hout, aout, dkacc, dvacc,
               gains, gain_next, lossacc, ga8, gb8, gx,
               w_sem, hsem, ysem, x_sem, gain_sem, hand_sem, save_sem,
               a_rs, d_rs, g1_sr, g1_sl, b_rs, dm_rs, g2_sr, g2_sl,
               rs_rr, rs_rl, rs_sr, rs_sl, loss_sem, gx_s, gx_r):
        z = lax.axis_index("model")
        st = lax.axis_index("stage")
        is_first = st == 0
        is_last = st == last_s

        def rdma(src, dst, ssem, rsem, **dev):
            return pltpu.make_async_remote_copy(src_ref=src, dst_ref=dst, send_sem=ssem, recv_sem=rsem,
                                                device_id=dev, device_id_type=MESH)

        def rows_of(k):
            return pl.ds(pl.multiple_of(k * row, row), row)

        qkv_copies = [pltpu.make_async_copy(wqkv_h.at[i], wqkv.at[:, pl.ds(i * head_dim, head_dim)], w_sem.at[i])
                      for i in range(n_slab)]
        w_copies = [pltpu.make_async_copy(src, dst, w_sem.at[n_slab + i])
                    for i, (src, dst) in enumerate(((wout_h, wout), (wup_h, wup), (wdown_h, wdown)))]

        def tokens_of(u):
            return lax.div(u, per_seq), pl.multiple_of(lax.rem(u, per_seq) * tok, tok)

        def x_copy(u):
            q, first = tokens_of(u)
            return pltpu.make_async_copy(x_ref.at[q, pl.ds(first, tok), :], a_all.at[u], hsem.at[u])

        def x_again(u):
            q, first = tokens_of(u)
            slot = lax.rem(u, n_send)
            return pltpu.make_async_copy(x_ref.at[q, pl.ds(first, tok), :], xtmp.at[slot], x_sem.at[slot])

        def y_copy(u):
            q, first = tokens_of(u)
            rs = pl.ds(pl.multiple_of(first + z * row, row), row)
            return pltpu.make_async_copy(y_ref.at[q, rs, :], yslot.at[u], ysem.at[u])

        @pl.when(is_first)
        def _():
            @pl.loop(0, n_unit)
            def _(u):
                x_copy(u).start()

        for cp in qkv_copies + w_copies:
            cp.start()

        @pl.when(is_last)
        def _():
            @pl.loop(0, n_unit)
            def _(u):
                y_copy(u).start()

        barrier = pltpu.get_barrier_semaphore()
        for i in range(1, nz * ns):
            dz, dst = i % nz, i // nz
            pl.semaphore_signal(barrier, inc=1, device_id_type=MESH,
                                device_id={"model": lax.rem(z + dz, nz), "stage": lax.rem(st + dst, ns)})
        qkv_all[...] = jnp.zeros_like(qkv_all)
        lossacc[...] = jnp.zeros_like(lossacc)
        ga8[...] = jnp.zeros_like(ga8)
        gb8[...] = jnp.zeros_like(gb8)
        gains[...] = gain_ref[...].astype(F32)
        pl.semaphore_wait(barrier, nz * ns - 1)

        def gain_send():
            return rdma(gains, gain_next, gain_sem.at[0], gain_sem.at[1], stage=st - 1)

        @pl.when(st > 0)
        def _():
            gain_send().start()

        class Gather:
            def __init__(self, buf, slot, rsem, sr, sl, sslot):
                self.buf, self.slot, self.rsem, self.sr, self.sl, self.sslot = buf, slot, rsem, sr, sl, sslot

            def block(self, j):
                return self.buf.at[self.slot, rows_of(j), :]

            def right(self, j):
                return rdma(self.block(j), self.block(j), self.sr.at[self.sslot, j], self.rsem.at[self.slot, j], model=z + 1)

            def left(self, j):
                return rdma(self.block(j), self.block(j), self.sl.at[self.sslot, j], self.rsem.at[self.slot, j], model=z - 1)

            def start(self):
                @pl.when(z < last_z)
                def _():
                    self.right(z).start()

                @pl.when(z > 0)
                def _():
                    self.left(z).start()

            def step(self, t):
                @pl.when(z >= t)
                def _():
                    self.right(z - t).wait_recv()

                    @pl.when(z < last_z)
                    def _():
                        self.right(z - t).start()

                @pl.when(z + t <= last_z)
                def _():
                    self.left(z + t).wait_recv()

                    @pl.when(z > 0)
                    def _():
                        self.left(z + t).start()

            def own(self):
                self.right(z).wait_recv()

            def drain(self):
                for j in range(nz):
                    @pl.when((z > j) & (z < last_z))
                    def _():
                        self.right(j).wait_send()

                    @pl.when((z < j) & (z > 0))
                    def _():
                        self.left(j).wait_send()

            def drain_own(self):
                @pl.when(z < last_z)
                def _():
                    self.right(z).wait_send()

                @pl.when(z > 0)
                def _():
                    self.left(z).wait_send()

        def gather_a(u):
            return Gather(a_all, u, a_rs, g1_sr, g1_sl, lax.rem(u, n_gath))

        def gather_d(u):
            return Gather(d_all, u, d_rs, g1_sr, g1_sl, lax.rem(u, n_gath))

        def gather_b(u):
            return Gather(bbuf, lax.rem(u, n_gath), b_rs, g2_sr, g2_sl, lax.rem(u, n_gath))

        def gather_dm(u):
            return Gather(dmbuf, lax.rem(u, n_gath), dm_rs, g2_sr, g2_sl, lax.rem(u, n_gath))

        class Scatter:
            def __init__(self, op, u):
                self.op, self.ss, self.rs = op, lax.rem(u, n_send), lax.rem(u, n_recv)

            def right(self, k):
                return rdma(send_r.at[self.op, self.ss, k - 1], recv_r.at[self.op, self.rs, k - 1],
                            rs_sr.at[self.op, self.ss, k - 1], rs_rr.at[self.op, self.rs, k - 1], model=z + 1)

            def left(self, k):
                return rdma(send_l.at[self.op, self.ss, k], recv_l.at[self.op, self.rs, k],
                            rs_sl.at[self.op, self.ss, k], rs_rl.at[self.op, self.rs, k], model=z - 1)

            def mine(self, k):
                return part[self.op, self.ss, rows_of(k), :]

            def step(self, t):
                op, ss, rs = self.op, self.ss, self.rs
                kr = last_z - t + z
                kl = t - last_z + z

                @pl.when(z == 0)
                def _():
                    send_r[op, ss, kr - 1] = self.mine(kr).astype(BF16)
                    self.right(kr).start()

                @pl.when(z == last_z)
                def _():
                    send_l[op, ss, kl] = self.mine(kl).astype(BF16)
                    self.left(kl).start()

                if t > 0:
                    @pl.when((z > 0) & (z <= t))
                    def _():
                        self.right(kr).wait_recv()
                        send_r[op, ss, kr - 1] = (self.mine(kr) + recv_r[op, rs, kr - 1].astype(F32)).astype(BF16)
                        self.right(kr).start()

                    @pl.when((z < last_z) & (last_z - z <= t))
                    def _():
                        self.left(kl).wait_recv()
                        send_l[op, ss, kl] = (self.mine(kl) + recv_l[op, rs, kl].astype(F32)).astype(BF16)
                        self.left(kl).start()

            def final(self):
                accq[...] = self.mine(z)

                @pl.when(z > 0)
                def _():
                    self.right(z).wait_recv()
                    accq[...] += recv_r[self.op, self.rs, z - 1].astype(F32)

                @pl.when(z < last_z)
                def _():
                    self.left(z).wait_recv()
                    accq[...] += recv_l[self.op, self.rs, z].astype(F32)

            def drain(self):
                for k in range(1, nz):
                    @pl.when(z < k)
                    def _():
                        self.right(k).wait_send()

                for k in range(nz - 1):
                    @pl.when(z > k)
                    def _():
                        self.left(k).wait_send()

        def save(kind, src, src_slot, dst, u):
            return pltpu.make_async_copy(src.at[src_slot], dst.at[u], save_sem.at[kind, lax.rem(u, n_gath)])

        def two(u):
            return lax.rem(u, n_send)

        def four(u):
            return lax.rem(u, n_gath)

        def save_a(u):
            return save(0, a_all, u, a_out, u)

        def save_o(u):
            return save(1, ost, two(u), o_out, u)

        def save_b(u):
            return save(2, bbuf, four(u), b_out, u)

        def save_z(u):
            return save(3, zst, two(u), z_out, u)

        def save_d(u):
            return save(4, d_all, u, d_out, u)

        def save_du(u):
            return save(5, dust, two(u), du_out, u)

        def save_dm(u):
            return save(6, dmbuf, four(u), dm_out, u)

        def save_dqkv(u):
            return save(7, dqkvst, two(u), dqkv_out, u)

        gain_a = gains[0:1, :]
        gain_b = gains[1:2, :]

        def hand_h(u, j):
            s = two(j)
            return rdma(hout.at[s], hslot.at[u], hand_sem.at[s, 3], hsem.at[u], stage=st + 1)

        def hand_block(buf, sems, u, j, dz, next_stage):
            s = two(j)
            return rdma(aout.at[s], buf.at[u, rows_of(z), :], hand_sem.at[s, dz + 1], sems.at[u, z],
                        model=z + dz, stage=next_stage)

        def hand_all(buf, sems, u, j, next_stage, act):
            act(hand_block(buf, sems, u, j, 0, next_stage))

            @pl.when(z < last_z)
            def _():
                act(hand_block(buf, sems, u, j, 1, next_stage))

            @pl.when(z > 0)
            def _():
                act(hand_block(buf, sems, u, j, -1, next_stage))

        def begin(cp):
            cp.start()

        def sent(cp):
            cp.wait_send()

        def softmax_of(u, p, i):
            first = u - p
            cols = pl.ds(i * head_dim, head_dim)
            q = qkv_all[u, :, cols]
            k = qkv_all[pl.ds(first, per_seq), :, pl.ds(att_w + i * head_dim, head_dim)].reshape(seq_len, head_dim)
            v = qkv_all[pl.ds(first, per_seq), :, pl.ds(2 * att_w + i * head_dim, head_dim)].reshape(seq_len, head_dim)
            sc = dot_nt(q, k) * scale
            q_pos = p * tok + lax.broadcasted_iota(jnp.int32, sc.shape, 0)
            k_pos = lax.broadcasted_iota(jnp.int32, sc.shape, 1)
            sc = jnp.where(k_pos <= q_pos, sc, NEG_BIG)
            e = jnp.exp(sc - jnp.max(sc, axis=-1, keepdims=True))
            pr = e * (1.0 / jnp.sum(e, axis=-1, keepdims=True))
            return q, k, v, pr

        def fold(v):
            return jnp.sum(v.reshape(v.shape[0] // 8, 8, d_model), axis=0)

        def f_enter(j, u):
            @pl.when(is_first)
            def _():
                x_copy(u).wait()
                hslot[u] = a_all[u, rows_of(z), :]
                for k in range(nz):
                    rs = pl.ds(k * row, row)
                    h32 = a_all[u, rs, :].astype(F32)
                    a_all[u, rs, :] = (h32 * rms_inverse(h32) * gain_a).astype(BF16)

        def f_gather_a(t):
            def run(j, u):
                @pl.when(st > 0)
                def _():
                    gather_a(u).step(t)
                    if t == last_z:
                        gather_a(u).own()
            return run

        def f_attention(j, u):
            @pl.when(j == 0)
            def _():
                for cp in qkv_copies:
                    cp.wait()
                w_copies[0].wait()

            s = two(u)
            p = lax.rem(u, per_seq)
            save_a(u).start()
            qkv_all[u] = dot_nn(a_all[u], wqkv[...]).astype(BF16)
            for i in range(n_head):
                _, _, v, pr = softmax_of(u, p, i)
                ost[s, :, pl.ds(i * head_dim, head_dim)] = dot_nn(pr.astype(BF16), v).astype(BF16)
            save_o(u).start()
            part[0, s] = dot_nn(ost[s], wout[...])
            Scatter(0, u).step(0)

        def scatter_step(op, t):
            def run(j, u):
                Scatter(op, u).step(t)
            return run

        def f_middle(j, u):
            sc = Scatter(0, u)
            sc.final()

            @pl.when(st > 0)
            def _():
                rdma(hout.at[0], hslot.at[u], hand_sem.at[0, 3], hsem.at[u], stage=st).wait_recv()

            m = hslot[u].astype(F32) + accq[...]
            m_all[u] = m
            bbuf[four(u), rows_of(z), :] = (m * rms_inverse(m) * gain_b).astype(BF16)
            gather_b(u).start()
            sc.drain()
            save_o(u).wait()

            @pl.when(st > 0)
            def _():
                gather_a(u).drain()

        def f_gather_b(t):
            def run(j, u):
                gather_b(u).step(t)
            return run

        def f_mlp(j, u):
            @pl.when(j == 0)
            def _():
                w_copies[1].wait()
                w_copies[2].wait()

            s = two(u)
            save_a(u).wait()
            save_b(u).start()
            u_all[u] = dot_nn(bbuf[four(u)], wup[...])

            def act(r, carry):
                rr = pl.ds(pl.multiple_of(r * sub_rows, sub_rows), sub_rows)
                v = u_all[u, rr, :]
                th = jnp.tanh(GELU_K * (v + GELU_C * (v * v * v)))
                zst[s, rr, :] = (0.5 * v * (1.0 + th)).astype(BF16)
                return carry

            lax.fori_loop(0, tok // sub_rows, act, 0)
            save_z(u).start()
            part[1, s] = dot_nn(zst[s], wdown[...])
            Scatter(1, u).step(0)

        def f_leave(j, u):
            sc = Scatter(1, u)
            sc.final()
            s = two(j)
            h_new = (m_all[u] + accq[...]).astype(BF16)

            @pl.when(st < last_s)
            def _():
                @pl.when(j == 0)
                def _():
                    gain_send().wait_recv()

                @pl.when(j >= n_send)
                def _():
                    hand_all(a_all, a_rs, u, j, st + 1, sent)
                    hand_h(u, j).wait_send()

                h32 = h_new.astype(F32)
                aout[s] = (h32 * rms_inverse(h32) * gain_next[0:1, :]).astype(BF16)
                hand_all(a_all, a_rs, u, j, st + 1, begin)
                hout[s] = h_new
                hand_h(u, j).start()

            @pl.when(is_last)
            def _():
                y_copy(u).wait()
                diff = h_new.astype(F32) - yslot[u].astype(F32)
                d_all[u, rows_of(z), :] = (diff * inv_count).astype(BF16)
                lossacc[...] += fold(diff * diff)

            sc.drain()
            gather_b(u).drain()
            gather_b(u).drain_own()
            save_b(u).wait()
            save_z(u).wait()

        def run_phases(order, phases, back):
            lag = lags(order)

            def body(i, carry):
                for phase in order:
                    j = i - lag[phase]

                    @pl.when((j >= 0) & (j < n_unit))
                    def _():
                        phases[phase](j, (n_unit - 1 - j) if back else j)
                return carry

            lax.fori_loop(0, n_unit + lag[-1], body, 0)

        def hand_finish(buf, sems, next_stage, with_h):
            for j in range(n_unit - n_send, n_unit):
                hand_all(buf, sems, j, j, next_stage, sent)
                if with_h:
                    hand_h(j, j).wait_send()

        run_phases(FWD_ORDER, (
            f_enter, f_gather_a(1), f_gather_a(2), f_gather_a(3), f_attention, scatter_step(0, 1), scatter_step(0, 2),
            f_middle, f_gather_b(1), f_gather_b(2), f_gather_b(3), f_mlp, scatter_step(1, 1), scatter_step(1, 2),
            f_leave), False)

        def loss_send():
            return rdma(lossacc, lossacc, loss_sem.at[0], loss_sem.at[1], stage=st - 1)

        @pl.when(is_last)
        def _():
            loss_send().start()

        @pl.when(st < last_s)
        def _():
            hand_finish(a_all, a_rs, st + 1, True)

        def b_enter(j, u):
            @pl.when(is_last)
            def _():
                gather_d(u).start()

        def b_gather_d(t):
            def run(j, u):
                gather_d(u).step(t)
                if t == last_z:
                    @pl.when(st < last_s)
                    def _():
                        gather_d(u).own()
            return run

        def b_mlp(j, u):
            s = two(u)
            save_d(u).start()
            part[0, s] = dot_nt(d_all[u], wdown[...])

            def act(r, carry):
                rr = pl.ds(pl.multiple_of(r * sub_rows, sub_rows), sub_rows)
                v = u_all[u, rr, :]
                v2 = v * v
                th = jnp.tanh(GELU_K * (v + GELU_C * (v2 * v)))
                slope = 0.5 * (1.0 + th) + 0.5 * v * (1.0 - th * th) * (GELU_K * (1.0 + 3.0 * GELU_C * v2))
                dust[s, rr, :] = (part[0, s, rr, :] * slope).astype(BF16)
                return carry

            lax.fori_loop(0, tok // sub_rows, act, 0)
            save_du(u).start()
            part[0, s] = dot_nt(dust[s], wup[...])
            Scatter(0, u).step(0)

        def b_middle(j, u):
            sc = Scatter(0, u)
            sc.final()
            m = m_all[u]
            inv = rms_inverse(m)
            normed = m * inv
            dn = accq[...]
            gb8[...] += fold(dn * normed)
            dn = dn * gain_b
            dm = d_all[u, rows_of(z), :].astype(F32) + inv * (
                dn - normed * jnp.mean(dn * normed, axis=-1, keepdims=True))
            m_all[u] = dm
            dmbuf[four(u), rows_of(z), :] = dm.astype(BF16)
            gather_dm(u).start()
            sc.drain()
            gather_d(u).drain()

            @pl.when(is_last)
            def _():
                gather_d(u).drain_own()

            save_du(u).wait()

        def b_gather_dm(t):
            def run(j, u):
                gather_dm(u).step(t)
            return run

        def b_attention(j, u):
            s = two(u)
            p = lax.rem(u, per_seq)
            save_d(u).wait()
            save_dm(u).start()

            @pl.when(is_first)
            def _():
                x_again(u).start()

            @pl.when(p == per_seq - 1)
            def _():
                dkacc[...] = jnp.zeros_like(dkacc)
                dvacc[...] = jnp.zeros_like(dvacc)

            datt[...] = dot_nt(dmbuf[four(u)], wout[...]).astype(BF16)
            p_rows = pl.ds(pl.multiple_of(p * tok, tok), tok)
            for h in range(n_head):
                cols = pl.ds(h * head_dim, head_dim)
                q, k, v, pr = softmax_of(u, p, h)
                da = datt[:, cols]
                dp = dot_nt(da, v)
                ds = (pr * (dp - jnp.sum(pr * dp, axis=-1, keepdims=True)) * scale).astype(BF16)
                dvacc[:, cols] += dot_tn(pr.astype(BF16), da)
                dkacc[:, cols] += dot_tn(ds, q)
                dqkvst[s, :, cols] = dot_nn(ds, k).astype(BF16)
            dqkvst[s, :, pl.ds(att_w, att_w)] = dkacc[p_rows, :].astype(BF16)
            dqkvst[s, :, pl.ds(2 * att_w, att_w)] = dvacc[p_rows, :].astype(BF16)
            save_dqkv(u).start()
            part[1, s] = dot_nt(dqkvst[s], wqkv[...])

            @pl.when(st > 0)
            def _():
                Scatter(1, u).step(0)

        def b_scatter(t):
            def run(j, u):
                @pl.when(st > 0)
                def _():
                    Scatter(1, u).step(t)
            return run

        def b_leave(j, u):
            s = two(j)

            @pl.when(st > 0)
            def _():
                sc = Scatter(1, u)
                sc.final()
                h32 = hslot[u].astype(F32)
                inv = rms_inverse(h32)
                normed = h32 * inv
                dn = accq[...]
                ga8[...] += fold(dn * normed)

                @pl.when(j >= n_send)
                def _():
                    hand_all(d_all, d_rs, u, j, st - 1, sent)

                dg = dn * gain_a
                aout[s] = (m_all[u] + inv * (
                    dg - normed * jnp.mean(dg * normed, axis=-1, keepdims=True))).astype(BF16)
                hand_all(d_all, d_rs, u, j, st - 1, begin)
                sc.drain()

            @pl.when(is_first)
            def _():
                x_again(u).wait()
                for k in range(nz):
                    rs = pl.ds(k * row, row)
                    h32 = xtmp[two(u), rs, :].astype(F32)
                    ga8[...] += fold(part[1, two(u), rs, :] * (h32 * rms_inverse(h32)))

            gather_dm(u).drain()
            gather_dm(u).drain_own()
            save_dm(u).wait()
            save_dqkv(u).wait()

        run_phases(BWD_ORDER, (
            b_enter, b_gather_d(1), b_gather_d(2), b_gather_d(3), b_mlp, scatter_step(0, 1), scatter_step(0, 2),
            b_middle, b_gather_dm(1), b_gather_dm(2), b_gather_dm(3), b_attention, b_scatter(1), b_scatter(2),
            b_leave), True)

        @pl.when(st > 0)
        def _():
            hand_finish(d_all, d_rs, st - 1, False)
            gain_send().wait_send()

        @pl.when(is_last)
        def _():
            loss_send().wait_send()

        @pl.when(st < last_s)
        def _():
            loss_send().wait_recv()

            @pl.when(st > 0)
            def _():
                loss_send().start()
                loss_send().wait_send()

        loss_row = jnp.sum(jnp.sum(lossacc[...], axis=0, keepdims=True), axis=1, keepdims=True)
        gx[z, 0:1, :] = jnp.sum(ga8[...], axis=0, keepdims=True)
        gx[z, 1:2, :] = jnp.sum(gb8[...], axis=0, keepdims=True)
        gx[z, 2:8, :] = jnp.broadcast_to(loss_row, (6, d_model))

        def gx_send(dz):
            return rdma(gx.at[z], gx.at[z], gx_s.at[dz], gx_r.at[z], model=lax.rem(z + dz, nz))

        def gx_recv(dz):
            k = lax.rem(z + dz, nz)
            return rdma(gx.at[k], gx.at[k], gx_s.at[dz], gx_r.at[k], model=k)

        for dz in range(1, nz):
            gx_send(dz).start()
        for dz in range(1, nz):
            gx_recv(dz).wait_recv()
        red_out[...] = gx[0] + gx[1] + gx[2] + gx[3]
        for dz in range(1, nz):
            gx_send(dz).wait_send()

    any_spec = pl.BlockSpec(memory_space=pl.ANY)
    vmem_spec = pl.BlockSpec(memory_space=pltpu.VMEM)

    def out(width):
        return jax.ShapeDtypeStruct((n_unit, tok, width), BF16)

    dma = pltpu.SemaphoreType.DMA
    vmem = pltpu.VMEM
    return pl.pallas_call(
        kernel,
        out_shape=(out(d_model), out(d_model), out(d_model), out(d_model), out(qkv_w), out(att_w), out(ff_w), out(ff_w),
                   jax.ShapeDtypeStruct((8, d_model), F32)),
        in_specs=[any_spec] * 6 + [vmem_spec],
        out_specs=(any_spec,) * 8 + (vmem_spec,),
        scratch_shapes=[
            vmem((d_model, qkv_w), BF16), vmem((att_w, d_model), BF16), vmem((d_model, ff_w), BF16), vmem((ff_w, d_model), BF16),
            vmem((n_unit, row, d_model), BF16), vmem((n_unit, row, d_model), BF16),
            vmem((n_unit, tok, d_model), BF16), vmem((n_unit, tok, d_model), BF16),
            vmem((n_gath, tok, d_model), BF16), vmem((n_gath, tok, d_model), BF16), vmem((n_send, tok, d_model), BF16),
            vmem((n_unit, tok, qkv_w), BF16), vmem((n_unit, tok, ff_w), F32), vmem((n_unit, row, d_model), F32),
            vmem((n_send, tok, att_w), BF16), vmem((n_send, tok, ff_w), BF16), vmem((n_send, tok, ff_w), BF16),
            vmem((n_send, tok, qkv_w), BF16), vmem((tok, att_w), BF16), vmem((2, n_send, tok, d_model), F32),
            vmem((2, n_recv, nz - 1, row, d_model), BF16), vmem((2, n_recv, nz - 1, row, d_model), BF16),
            vmem((2, n_send, nz - 1, row, d_model), BF16), vmem((2, n_send, nz - 1, row, d_model), BF16),
            vmem((row, d_model), F32), vmem((n_send, row, d_model), BF16), vmem((n_send, row, d_model), BF16),
            vmem((seq_len, att_w), F32), vmem((seq_len, att_w), F32),
            vmem((2, d_model), F32), vmem((2, d_model), F32),
            vmem((8, d_model), F32), vmem((8, d_model), F32), vmem((8, d_model), F32), vmem((nz, 8, d_model), F32),
            dma((n_slab + 3,)), dma((n_unit,)), dma((n_unit,)), dma((n_send,)), dma((2,)), dma((n_send, 4)), dma((8, n_gath)),
            dma((n_unit, nz)), dma((n_unit, nz)), dma((n_gath, nz)), dma((n_gath, nz)),
            dma((n_gath, nz)), dma((n_gath, nz)), dma((n_gath, nz)), dma((n_gath, nz)),
            dma((2, n_recv, nz - 1)), dma((2, n_recv, nz - 1)), dma((2, n_send, nz - 1)), dma((2, n_send, nz - 1)),
            dma((2,)), dma((nz,)), dma((nz,)),
        ],
        compiler_params=pltpu.CompilerParams(collective_id=0, has_side_effects=True, vmem_limit_bytes=67_043_328),
        name="layer_step",
    )(x_in, y_target, w_qkv, w_out, w_up, w_down, gain)


def weight_grad(act, grad):
    return lax.dot_general(act, grad, (((0, 1), (0, 1)), ((), ())), preferred_element_type=F32)


def solution(mesh):
    dims = dict(mesh.shape)

    def device_fn(x_in, y_target, w_qkv, w_out, w_up, w_down, norm_gain):
        n_batch, seq_len, d_model = x_in.shape
        heads, head_dim = w_qkv.shape[3], w_qkv.shape[4]
        a, b, d, dm, dqkv, o, zz, du, red = layer_step(
            dims, x_in, y_target,
            w_qkv[0].transpose(1, 2, 0, 3).reshape(3 * heads, d_model, head_dim),
            w_out[0].reshape(heads * head_dim, d_model), w_up[0], w_down[0], norm_gain[0])
        grad_qkv = weight_grad(a, dqkv).reshape(1, d_model, 3, heads, head_dim)
        grad_out = weight_grad(o, dm).reshape(1, heads, head_dim, d_model)
        grad_up = weight_grad(b, du)[None]
        grad_down = weight_grad(zz, d)[None]
        loss = 0.5 * red[2, 0:1] / (n_batch * seq_len * d_model)
        return loss, grad_qkv, grad_out, grad_up, grad_down, red[None, 0:2]

    act_spec = P("data", None, None)
    weight_specs = (
        P("stage", None, None, "model", None),
        P("stage", "model", None, None),
        P("stage", None, "model"),
        P("stage", "model", None),
        P("stage", None, None),
    )
    grad_specs = (
        P(("data", "stage"), None, None, "model", None),
        P(("data", "stage"), "model", None, None),
        P(("data", "stage"), None, "model"),
        P(("data", "stage"), "model", None),
        P(("data", "stage"), None, None),
    )
    return jax.shard_map(
        device_fn,
        mesh=mesh,
        in_specs=(act_spec, act_spec) + weight_specs,
        out_specs=(P("data"),) + grad_specs,
        check_vma=False,
    )
```

```python
import jax
import jax.numpy as jnp
from jax import lax
from jax.experimental import pallas as pl
from jax.experimental.pallas import tpu as pltpu
from jax.sharding import PartitionSpec as P

NORM_EPS = 1e-6
NEG_BIG = -1e30
MESH = pl.DeviceIdType.MESH
GELU_K = 0.7978845608028654
GELU_C = 0.044715
F32 = jnp.float32
BF16 = jnp.bfloat16


def dot_nn(a, b):
    return lax.dot_general(a, b, (((1,), (0,)), ((), ())), preferred_element_type=F32)


def dot_nt(a, b):
    return lax.dot_general(a, b, (((1,), (1,)), ((), ())), preferred_element_type=F32)


def dot_tn(a, b):
    return lax.dot_general(a, b, (((0,), (0,)), ((), ())), preferred_element_type=F32)


def rms_inverse(v32):
    return lax.rsqrt(jnp.mean(v32 * v32, axis=-1, keepdims=True) + NORM_EPS)


FWD_ORDER = (4, 10, 0, 1, 7, 8, 5, 2, 9, 6, 3)
BWD_ORDER = (9, 3, 6, 4, 1, 10, 0, 5, 7, 8, 2)


def lags(order):
    place = {phase: i for i, phase in enumerate(order)}
    lag = [0]
    for phase in range(1, len(order)):
        lag.append(lag[-1] + (1 if place[phase] < place[phase - 1] else 0))
    return lag


def layer_step(dims, x_in, y_target, w_qkv, w_out, w_up, w_down, gain):
    nz, ns = dims["model"], dims["stage"]
    n_seq, seq_len, d_model = x_in.shape
    n_slab, _, head_dim = w_qkv.shape
    qkv_w = n_slab * head_dim
    att_w = w_out.shape[0]
    ff_w = w_up.shape[1]
    n_head = att_w // head_dim
    tok = 128
    row = tok // nz
    per_seq = seq_len // tok
    n_unit = n_seq * per_seq
    scale = head_dim ** -0.5
    inv_count = 1.0 / (n_seq * seq_len * d_model)
    last_z, last_s = nz - 1, ns - 1
    sub_rows = 16
    half = tok // 2
    n_send, n_recv, n_gath, n_hand = 1, 2, 3, 2
    quarters = range(2)

    def kernel(x_ref, y_ref, wqkv_h, wout_h, wup_h, wdown_h, gain_ref,
               a_out, b_out, d_out, dm_out, dqkv_out, o_out, z_out, du_out, red_out,
               wqkv, wout, wup, wdown, hslot, yslot, a_all, d_all, bbuf, dmbuf, xtmp,
               qkv_all, u_all, m_all, ost, zst, dust, dqkvst, datt, part,
               recv_o, recv_i, send_p, hout, aout, dkacc, dvacc,
               gains, gain_next, lossacc, ga8, gb8, gx,
               w_sem, hsem, ysem, x_sem, gain_sem, hand_sem, save_sem,
               a_rs, d_rs, g1_si, g1_so, b_rs, dm_rs, g2_si, g2_so,
               rs_ro, rs_ri, rs_s, loss_sem, gx_s, gx_r):
        z = lax.axis_index("model")
        st = lax.axis_index("stage")
        is_first = st == 0
        is_last = st == last_s
        inner = (z > 0) & (z < last_z)
        outer = (z == 0) | (z == last_z)
        side = lax.div(z, 2)
        near = 2 * side
        far = 2 - near
        inner_peer = 1 + lax.rem(z, 2)
        outer_peer = last_z * side
        my_half = pl.ds(pl.multiple_of(side * half, half), half)

        def rdma(src, dst, ssem, rsem, **dev):
            return pltpu.make_async_remote_copy(src_ref=src, dst_ref=dst, send_sem=ssem, recv_sem=rsem,
                                                device_id=dev, device_id_type=MESH)

        def rows_of(k):
            return pl.ds(pl.multiple_of(k * row, row), row)

        qkv_copies = [pltpu.make_async_copy(wqkv_h.at[i], wqkv.at[:, pl.ds(i * head_dim, head_dim)], w_sem.at[i])
                      for i in range(n_slab)]
        w_copies = [pltpu.make_async_copy(src, dst, w_sem.at[n_slab + i])
                    for i, (src, dst) in enumerate(((wout_h, wout), (wup_h, wup), (wdown_h, wdown)))]

        def tokens_of(u):
            return lax.div(u, per_seq), pl.multiple_of(lax.rem(u, per_seq) * tok, tok)

        def x_copy(u):
            q, first = tokens_of(u)
            return pltpu.make_async_copy(x_ref.at[q, pl.ds(first, tok), :], a_all.at[u], hsem.at[u])

        def x_again(u):
            q, first = tokens_of(u)
            slot = lax.rem(u, n_send)
            return pltpu.make_async_copy(x_ref.at[q, pl.ds(first, tok), :], xtmp.at[slot], x_sem.at[slot])

        def y_copy(u):
            q, first = tokens_of(u)
            rs = pl.ds(pl.multiple_of(first + side * half, half), half)
            slot = lax.rem(u, n_hand)
            return pltpu.make_async_copy(y_ref.at[q, rs, :], yslot.at[slot], ysem.at[slot])

        @pl.when(is_first)
        def _():
            @pl.loop(0, n_unit)
            def _(u):
                x_copy(u).start()

        for cp in qkv_copies + w_copies:
            cp.start()

        barrier = pltpu.get_barrier_semaphore()
        for i in range(1, nz * ns):
            dz, dst = i % nz, i // nz
            pl.semaphore_signal(barrier, inc=1, device_id_type=MESH,
                                device_id={"model": lax.rem(z + dz, nz), "stage": lax.rem(st + dst, ns)})
        qkv_all[...] = jnp.zeros_like(qkv_all)
        lossacc[...] = jnp.zeros_like(lossacc)
        ga8[...] = jnp.zeros_like(ga8)
        gb8[...] = jnp.zeros_like(gb8)
        gains[...] = gain_ref[...].astype(F32)
        pl.semaphore_wait(barrier, nz * ns - 1)

        def gain_send():
            return rdma(gains, gain_next, gain_sem.at[0], gain_sem.at[1], stage=st - 1)

        @pl.when(st > 0)
        def _():
            gain_send().start()

        class Gather:
            def __init__(self, buf, slot, rsem, si, so, sslot):
                self.buf, self.slot, self.rsem, self.si, self.so, self.sslot = buf, slot, rsem, si, so, sslot

            def block(self, k):
                return self.buf.at[self.slot, rows_of(k), :]

            def inward(self, k, q):
                return rdma(self.block(k), self.block(k), self.si.at[self.sslot, q], self.rsem.at[self.slot, k],
                            model=inner_peer)

            def outward(self, k):
                return rdma(self.block(k), self.block(k), self.so.at[self.sslot, k], self.rsem.at[self.slot, k],
                            model=outer_peer)

            def send(self, q):
                self.inward(near + q, q).start()
                self.outward(near + q).start()

            def relay(self):
                @pl.when(inner)
                def _():
                    for q in quarters:
                        self.outward(far + q).wait_recv()
                        self.outward(far + q).start()

            def collect(self):
                @pl.when(outer)
                def _():
                    for k in range(nz):
                        self.outward(k).wait_recv()

            def own(self):
                @pl.when(inner)
                def _():
                    for q in quarters:
                        self.outward(near + q).wait_recv()

            def drain(self):
                @pl.when(inner)
                def _():
                    for q in quarters:
                        self.outward(far + q).wait_send()

            def drain_own(self):
                @pl.when(inner)
                def _():
                    for q in quarters:
                        self.inward(near + q, q).wait_send()
                        self.outward(near + q).wait_send()

        def gather_a(u):
            return Gather(a_all, u, a_rs, g1_si, g1_so, lax.rem(u, n_gath))

        def gather_d(u):
            return Gather(d_all, u, d_rs, g1_si, g1_so, lax.rem(u, n_gath))

        def gather_b(u):
            return Gather(bbuf, lax.rem(u, n_gath), b_rs, g2_si, g2_so, lax.rem(u, n_gath))

        def gather_dm(u):
            return Gather(dmbuf, lax.rem(u, n_gath), dm_rs, g2_si, g2_so, lax.rem(u, n_gath))

        class Scatter:
            def __init__(self, op, u):
                self.op, self.ss, self.rs = op, lax.rem(u, n_send), lax.rem(u, n_recv)

            def in_copy(self, k):
                return rdma(send_p.at[self.op, self.ss, k], recv_o.at[self.op, self.rs, k],
                            rs_s.at[self.op, self.ss, k], rs_ro.at[self.op, self.rs, k], model=inner_peer)

            def cross_copy(self, k, q):
                return rdma(send_p.at[self.op, self.ss, k], recv_i.at[self.op, self.rs, q],
                            rs_s.at[self.op, self.ss, k], rs_ri.at[self.op, self.rs, q], model=inner_peer)

            def mine(self, k):
                return part[self.op, self.ss, rows_of(k), :]

            def start(self):
                @pl.when(outer)
                def _():
                    for k in (far, far + 1, near, near + 1):
                        send_p[self.op, self.ss, k] = self.mine(k).astype(BF16)
                        self.in_copy(k).start()

            def relay(self):
                @pl.when(inner)
                def _():
                    for q in quarters:
                        k = far + q
                        self.in_copy(k).wait_recv()
                        send_p[self.op, self.ss, k] = (
                            self.mine(k) + recv_o[self.op, self.rs, k].astype(F32)).astype(BF16)
                        self.cross_copy(k, q).start()

            def total(self, q):
                k = near + q
                self.in_copy(k).wait_recv()
                self.cross_copy(k, q).wait_recv()
                return (self.mine(k) + recv_o[self.op, self.rs, k].astype(F32)) + recv_i[self.op, self.rs, q].astype(F32)

            def drain(self):
                @pl.when(outer)
                def _():
                    for k in range(nz):
                        self.in_copy(k).wait_send()

                @pl.when(inner)
                def _():
                    for q in quarters:
                        self.cross_copy(far + q, q).wait_send()

        def save(kind, src, src_slot, dst, u):
            return pltpu.make_async_copy(src.at[src_slot], dst.at[u], save_sem.at[kind, lax.rem(u, n_gath)])

        def sslot(u):
            return lax.rem(u, n_send)

        def gslot(u):
            return lax.rem(u, n_gath)

        def q_rows(q):
            return pl.ds(q * row, row)

        def save_a(u):
            return save(0, a_all, u, a_out, u)

        def save_o(u):
            return save(1, ost, sslot(u), o_out, u)

        def save_b(u):
            return save(2, bbuf, gslot(u), b_out, u)

        def save_z(u):
            return save(3, zst, sslot(u), z_out, u)

        def save_d(u):
            return save(4, d_all, u, d_out, u)

        def save_du(u):
            return save(5, dust, sslot(u), du_out, u)

        def save_dm(u):
            return save(6, dmbuf, gslot(u), dm_out, u)

        def save_dqkv(u):
            return save(7, dqkvst, sslot(u), dqkv_out, u)

        gain_a = gains[0:1, :]
        gain_b = gains[1:2, :]

        def hand_h(u, j):
            s = lax.rem(j, n_hand)
            return rdma(hout.at[s], hslot.at[u], hand_sem.at[s, 6], hsem.at[u], stage=st + 1)

        def hand_quarter(buf, sems, u, j, q, next_stage, act):
            s = lax.rem(j, n_hand)
            k = near + q
            for i, peer in enumerate((inner_peer, outer_peer, z)):
                act(rdma(aout.at[s, q_rows(q), :], buf.at[u, rows_of(k), :], hand_sem.at[s, 3 * q + i], sems.at[u, k],
                         model=peer, stage=next_stage))

        def hand_sent(buf, sems, u, j, next_stage, with_h):
            for q in quarters:
                hand_quarter(buf, sems, u, j, q, next_stage, sent)
            if with_h:
                hand_h(u, j).wait_send()

        def begin(cp):
            cp.start()

        def sent(cp):
            cp.wait_send()

        def softmax_of(u, p, i):
            first = u - p
            cols = pl.ds(i * head_dim, head_dim)
            q = qkv_all[u, :, cols]
            k = qkv_all[pl.ds(first, per_seq), :, pl.ds(att_w + i * head_dim, head_dim)].reshape(seq_len, head_dim)
            v = qkv_all[pl.ds(first, per_seq), :, pl.ds(2 * att_w + i * head_dim, head_dim)].reshape(seq_len, head_dim)
            sc = dot_nt(q, k) * scale
            q_pos = p * tok + lax.broadcasted_iota(jnp.int32, sc.shape, 0)
            k_pos = lax.broadcasted_iota(jnp.int32, sc.shape, 1)
            sc = jnp.where(k_pos <= q_pos, sc, NEG_BIG)
            e = jnp.exp(sc - jnp.max(sc, axis=-1, keepdims=True))
            pr = e * (1.0 / jnp.sum(e, axis=-1, keepdims=True))
            return q, k, v, pr

        def fold(v):
            return jnp.sum(v.reshape(v.shape[0] // 8, 8, d_model), axis=0)

        def f_enter(j, u):
            @pl.when(is_first)
            def _():
                x_copy(u).wait()
                hslot[u] = a_all[u, my_half, :]
                for k in range(nz):
                    rs = pl.ds(k * row, row)
                    h32 = a_all[u, rs, :].astype(F32)
                    a_all[u, rs, :] = (h32 * rms_inverse(h32) * gain_a).astype(BF16)

        def f_relay_a(j, u):
            @pl.when(st > 0)
            def _():
                gather_a(u).relay()

        def f_collect_a(j, u):
            @pl.when(st > 0)
            def _():
                gather_a(u).collect()
                gather_a(u).own()

        def f_attention(j, u):
            @pl.when(j == 0)
            def _():
                for cp in qkv_copies:
                    cp.wait()
                w_copies[0].wait()

            s = sslot(u)
            p = lax.rem(u, per_seq)
            save_a(u).start()
            qkv_all[u] = dot_nn(a_all[u], wqkv[...]).astype(BF16)
            for i in range(n_head):
                _, _, v, pr = softmax_of(u, p, i)
                ost[s, :, pl.ds(i * head_dim, head_dim)] = dot_nn(pr.astype(BF16), v).astype(BF16)
            save_o(u).start()
            part[0, s] = dot_nn(ost[s], wout[...])
            Scatter(0, u).start()

        def scatter_relay(op):
            def run(j, u):
                Scatter(op, u).relay()
            return run

        def f_middle(j, u):
            sc = Scatter(0, u)

            @pl.when(inner)
            def _():
                @pl.when(st > 0)
                def _():
                    rdma(hout.at[0], hslot.at[u], hand_sem.at[0, 6], hsem.at[u], stage=st).wait_recv()

                for q in quarters:
                    m = hslot[u, q_rows(q), :].astype(F32) + sc.total(q)
                    m_all[u, q_rows(q), :] = m
                    bbuf[gslot(u), rows_of(near + q), :] = (m * rms_inverse(m) * gain_b).astype(BF16)
                    gather_b(u).send(q)

            sc.drain()
            save_o(u).wait()

            @pl.when(st > 0)
            def _():
                gather_a(u).drain()

        def f_relay_b(j, u):
            gather_b(u).relay()

        def f_collect_b(j, u):
            gather_b(u).collect()

        def f_mlp(j, u):
            @pl.when(j == 0)
            def _():
                w_copies[1].wait()
                w_copies[2].wait()

            s = sslot(u)
            save_a(u).wait()
            save_b(u).start()

            @pl.when(is_last & inner)
            def _():
                y_copy(u).start()

            u_all[u] = dot_nn(bbuf[gslot(u)], wup[...])

            def act(r, carry):
                rr = pl.ds(pl.multiple_of(r * sub_rows, sub_rows), sub_rows)
                v = u_all[u, rr, :]
                th = jnp.tanh(GELU_K * (v + GELU_C * (v * v * v)))
                zst[s, rr, :] = (0.5 * v * (1.0 + th)).astype(BF16)
                return carry

            lax.fori_loop(0, tok // sub_rows, act, 0)
            save_z(u).start()
            part[1, s] = dot_nn(zst[s], wdown[...])
            Scatter(1, u).start()

        def f_leave(j, u):
            sc = Scatter(1, u)
            s = lax.rem(j, n_hand)

            @pl.when((j == 0) & (st < last_s))
            def _():
                gain_send().wait_recv()

            @pl.when(inner)
            def _():
                @pl.when(st < last_s)
                def _():
                    @pl.when(j >= n_hand)
                    def _():
                        hand_sent(a_all, a_rs, u, j, st + 1, True)

                @pl.when(is_last)
                def _():
                    y_copy(u).wait()

                for q in quarters:
                    h_new = (m_all[u, q_rows(q), :] + sc.total(q)).astype(BF16)
                    h32 = h_new.astype(F32)

                    @pl.when(st < last_s)
                    def _():
                        aout[s, q_rows(q), :] = (h32 * rms_inverse(h32) * gain_next[0:1, :]).astype(BF16)
                        hand_quarter(a_all, a_rs, u, j, q, st + 1, begin)
                        hout[s, q_rows(q), :] = h_new

                    @pl.when(is_last)
                    def _():
                        diff = h32 - yslot[lax.rem(u, n_hand), q_rows(q), :].astype(F32)
                        d_all[u, rows_of(near + q), :] = (diff * inv_count).astype(BF16)
                        lossacc[...] += fold(diff * diff)

                @pl.when(st < last_s)
                def _():
                    hand_h(u, j).start()

            sc.drain()
            gather_b(u).drain()
            gather_b(u).drain_own()
            save_b(u).wait()
            save_z(u).wait()

        def run_phases(order, phases, back):
            lag = lags(order)

            def body(i, carry):
                for phase in order:
                    j = i - lag[phase]

                    @pl.when((j >= 0) & (j < n_unit))
                    def _():
                        phases[phase](j, (n_unit - 1 - j) if back else j)
                return carry

            lax.fori_loop(0, n_unit + lag[-1], body, 0)

        def hand_finish(buf, sems, next_stage, with_h):
            @pl.when(inner)
            def _():
                for j in range(n_unit - n_hand, n_unit):
                    hand_sent(buf, sems, j, j, next_stage, with_h)

        run_phases(FWD_ORDER, (
            f_enter, f_relay_a, f_collect_a, f_attention, scatter_relay(0), f_middle, f_relay_b, f_collect_b, f_mlp,
            scatter_relay(1), f_leave), False)

        def loss_send():
            return rdma(lossacc, lossacc, loss_sem.at[0], loss_sem.at[1], stage=st - 1)

        @pl.when(is_last)
        def _():
            loss_send().start()

        @pl.when(st < last_s)
        def _():
            hand_finish(a_all, a_rs, st + 1, True)

        def b_enter(j, u):
            @pl.when(is_last & inner)
            def _():
                for q in quarters:
                    gather_d(u).send(q)

        def b_relay_d(j, u):
            gather_d(u).relay()

        def b_collect_d(j, u):
            gather_d(u).collect()

            @pl.when(st < last_s)
            def _():
                gather_d(u).own()

        def b_mlp(j, u):
            s = sslot(u)
            save_d(u).start()
            part[0, s] = dot_nt(d_all[u], wdown[...])

            def act(r, carry):
                rr = pl.ds(pl.multiple_of(r * sub_rows, sub_rows), sub_rows)
                v = u_all[u, rr, :]
                v2 = v * v
                th = jnp.tanh(GELU_K * (v + GELU_C * (v2 * v)))
                slope = 0.5 * (1.0 + th) + 0.5 * v * (1.0 - th * th) * (GELU_K * (1.0 + 3.0 * GELU_C * v2))
                dust[s, rr, :] = (part[0, s, rr, :] * slope).astype(BF16)
                return carry

            lax.fori_loop(0, tok // sub_rows, act, 0)
            save_du(u).start()
            part[0, s] = dot_nt(dust[s], wup[...])
            Scatter(0, u).start()

        def b_middle(j, u):
            sc = Scatter(0, u)

            @pl.when(inner)
            def _():
                for q in quarters:
                    m = m_all[u, q_rows(q), :]
                    inv = rms_inverse(m)
                    normed = m * inv
                    dn = sc.total(q)
                    gb8[...] += fold(dn * normed)
                    dn = dn * gain_b
                    dm = d_all[u, rows_of(near + q), :].astype(F32) + inv * (
                        dn - normed * jnp.mean(dn * normed, axis=-1, keepdims=True))
                    m_all[u, q_rows(q), :] = dm
                    dmbuf[gslot(u), rows_of(near + q), :] = dm.astype(BF16)
                    gather_dm(u).send(q)

            sc.drain()
            gather_d(u).drain()

            @pl.when(is_last)
            def _():
                gather_d(u).drain_own()

            save_du(u).wait()

        def b_relay_dm(j, u):
            gather_dm(u).relay()

        def b_collect_dm(j, u):
            gather_dm(u).collect()

        def b_attention(j, u):
            s = sslot(u)
            p = lax.rem(u, per_seq)
            save_d(u).wait()
            save_dm(u).start()

            @pl.when(is_first)
            def _():
                x_again(u).start()

            @pl.when(p == per_seq - 1)
            def _():
                dkacc[...] = jnp.zeros_like(dkacc)
                dvacc[...] = jnp.zeros_like(dvacc)

            datt[...] = dot_nt(dmbuf[gslot(u)], wout[...]).astype(BF16)
            p_rows = pl.ds(pl.multiple_of(p * tok, tok), tok)
            for h in range(n_head):
                cols = pl.ds(h * head_dim, head_dim)
                q, k, v, pr = softmax_of(u, p, h)
                da = datt[:, cols]
                dp = dot_nt(da, v)
                ds = (pr * (dp - jnp.sum(pr * dp, axis=-1, keepdims=True)) * scale).astype(BF16)
                dvacc[:, cols] += dot_tn(pr.astype(BF16), da)
                dkacc[:, cols] += dot_tn(ds, q)
                dqkvst[s, :, cols] = dot_nn(ds, k).astype(BF16)
            dqkvst[s, :, pl.ds(att_w, att_w)] = dkacc[p_rows, :].astype(BF16)
            dqkvst[s, :, pl.ds(2 * att_w, att_w)] = dvacc[p_rows, :].astype(BF16)
            save_dqkv(u).start()
            part[1, s] = dot_nt(dqkvst[s], wqkv[...])

            @pl.when(st > 0)
            def _():
                Scatter(1, u).start()

        def b_relay_h(j, u):
            @pl.when(st > 0)
            def _():
                Scatter(1, u).relay()

        def b_leave(j, u):
            s = lax.rem(j, n_hand)

            @pl.when(st > 0)
            def _():
                sc = Scatter(1, u)

                @pl.when(inner)
                def _():
                    @pl.when(j >= n_hand)
                    def _():
                        hand_sent(d_all, d_rs, u, j, st - 1, False)

                    for q in quarters:
                        h32 = hslot[u, q_rows(q), :].astype(F32)
                        inv = rms_inverse(h32)
                        normed = h32 * inv
                        dn = sc.total(q)
                        ga8[...] += fold(dn * normed)
                        dg = dn * gain_a
                        aout[s, q_rows(q), :] = (m_all[u, q_rows(q), :] + inv * (
                            dg - normed * jnp.mean(dg * normed, axis=-1, keepdims=True))).astype(BF16)
                        hand_quarter(d_all, d_rs, u, j, q, st - 1, begin)

                sc.drain()

            @pl.when(is_first)
            def _():
                x_again(u).wait()
                for k in range(nz):
                    rs = pl.ds(k * row, row)
                    h32 = xtmp[sslot(u), rs, :].astype(F32)
                    ga8[...] += fold(part[1, sslot(u), rs, :] * (h32 * rms_inverse(h32)))

            gather_dm(u).drain()
            gather_dm(u).drain_own()
            save_dm(u).wait()
            save_dqkv(u).wait()

        run_phases(BWD_ORDER, (
            b_enter, b_relay_d, b_collect_d, b_mlp, scatter_relay(0), b_middle, b_relay_dm, b_collect_dm, b_attention,
            b_relay_h, b_leave), True)

        @pl.when(st > 0)
        def _():
            hand_finish(d_all, d_rs, st - 1, False)
            gain_send().wait_send()

        @pl.when(is_last)
        def _():
            loss_send().wait_send()

        @pl.when(st < last_s)
        def _():
            loss_send().wait_recv()

            @pl.when(st > 0)
            def _():
                loss_send().start()
                loss_send().wait_send()

        loss_row = jnp.sum(jnp.sum(lossacc[...], axis=0, keepdims=True), axis=1, keepdims=True)
        gx[z, 0:1, :] = jnp.sum(ga8[...], axis=0, keepdims=True)
        gx[z, 1:2, :] = jnp.sum(gb8[...], axis=0, keepdims=True)
        gx[z, 2:8, :] = jnp.broadcast_to(loss_row, (6, d_model))

        def gx_send(dz):
            return rdma(gx.at[z], gx.at[z], gx_s.at[dz], gx_r.at[z], model=lax.rem(z + dz, nz))

        def gx_recv(dz):
            k = lax.rem(z + dz, nz)
            return rdma(gx.at[k], gx.at[k], gx_s.at[dz], gx_r.at[k], model=k)

        for dz in range(1, nz):
            gx_send(dz).start()
        for dz in range(1, nz):
            gx_recv(dz).wait_recv()
        red_out[...] = gx[0] + gx[1] + gx[2] + gx[3]
        for dz in range(1, nz):
            gx_send(dz).wait_send()

    any_spec = pl.BlockSpec(memory_space=pl.ANY)
    vmem_spec = pl.BlockSpec(memory_space=pltpu.VMEM)

    def out(width):
        return jax.ShapeDtypeStruct((n_unit, tok, width), BF16)

    dma = pltpu.SemaphoreType.DMA
    vmem = pltpu.VMEM
    return pl.pallas_call(
        kernel,
        out_shape=(out(d_model), out(d_model), out(d_model), out(d_model), out(qkv_w), out(att_w), out(ff_w), out(ff_w),
                   jax.ShapeDtypeStruct((8, d_model), F32)),
        in_specs=[any_spec] * 6 + [vmem_spec],
        out_specs=(any_spec,) * 8 + (vmem_spec,),
        scratch_shapes=[
            vmem((d_model, qkv_w), BF16), vmem((att_w, d_model), BF16), vmem((d_model, ff_w), BF16), vmem((ff_w, d_model), BF16),
            vmem((n_unit, half, d_model), BF16), vmem((n_hand, half, d_model), BF16),
            vmem((n_unit, tok, d_model), BF16), vmem((n_unit, tok, d_model), BF16),
            vmem((n_gath, tok, d_model), BF16), vmem((n_gath, tok, d_model), BF16), vmem((n_send, tok, d_model), BF16),
            vmem((n_unit, tok, qkv_w), BF16), vmem((n_unit, tok, ff_w), F32), vmem((n_unit, half, d_model), F32),
            vmem((n_send, tok, att_w), BF16), vmem((n_send, tok, ff_w), BF16), vmem((n_send, tok, ff_w), BF16),
            vmem((n_send, tok, qkv_w), BF16), vmem((tok, att_w), BF16), vmem((2, n_send, tok, d_model), F32),
            vmem((2, n_recv, nz, row, d_model), BF16), vmem((2, n_recv, 2, row, d_model), BF16),
            vmem((2, n_send, nz, row, d_model), BF16),
            vmem((n_hand, half, d_model), BF16), vmem((n_hand, half, d_model), BF16),
            vmem((seq_len, att_w), F32), vmem((seq_len, att_w), F32),
            vmem((2, d_model), F32), vmem((2, d_model), F32),
            vmem((8, d_model), F32), vmem((8, d_model), F32), vmem((8, d_model), F32), vmem((nz, 8, d_model), F32),
            dma((n_slab + 3,)), dma((n_unit,)), dma((n_hand,)), dma((n_send,)), dma((2,)), dma((n_hand, 7)), dma((8, n_gath)),
            dma((n_unit, nz)), dma((n_unit, nz)), dma((n_gath, 2)), dma((n_gath, nz)),
            dma((n_gath, nz)), dma((n_gath, nz)), dma((n_gath, 2)), dma((n_gath, nz)),
            dma((2, n_recv, nz)), dma((2, n_recv, 2)), dma((2, n_send, nz)),
            dma((2,)), dma((nz,)), dma((nz,)),
        ],
        compiler_params=pltpu.CompilerParams(collective_id=0, has_side_effects=True, vmem_limit_bytes=67_043_328),
        name="layer_step",
    )(x_in, y_target, w_qkv, w_out, w_up, w_down, gain)


def weight_grad(act, grad):
    return lax.dot_general(act, grad, (((0, 1), (0, 1)), ((), ())), preferred_element_type=F32)


def solution(mesh):
    dims = dict(mesh.shape)

    def device_fn(x_in, y_target, w_qkv, w_out, w_up, w_down, norm_gain):
        n_batch, seq_len, d_model = x_in.shape
        heads, head_dim = w_qkv.shape[3], w_qkv.shape[4]
        a, b, d, dm, dqkv, o, zz, du, red = layer_step(
            dims, x_in, y_target,
            w_qkv[0].transpose(1, 2, 0, 3).reshape(3 * heads, d_model, head_dim),
            w_out[0].reshape(heads * head_dim, d_model), w_up[0], w_down[0], norm_gain[0])
        grad_qkv = weight_grad(a, dqkv).reshape(1, d_model, 3, heads, head_dim)
        grad_out = weight_grad(o, dm).reshape(1, heads, head_dim, d_model)
        grad_up = weight_grad(b, du)[None]
        grad_down = weight_grad(zz, d)[None]
        loss = 0.5 * red[2, 0:1] / (n_batch * seq_len * d_model)
        return loss, grad_qkv, grad_out, grad_up, grad_down, red[None, 0:2]

    act_spec = P("data", None, None)
    weight_specs = (
        P("stage", None, None, "model", None),
        P("stage", "model", None, None),
        P("stage", None, "model"),
        P("stage", "model", None),
        P("stage", None, None),
    )
    grad_specs = (
        P(("data", "stage"), None, None, "model", None),
        P(("data", "stage"), "model", None, None),
        P(("data", "stage"), None, "model"),
        P(("data", "stage"), "model", None),
        P(("data", "stage"), None, None),
    )
    return jax.shard_map(
        device_fn,
        mesh=mesh,
        in_specs=(act_spec, act_spec) + weight_specs,
        out_specs=(P("data"),) + grad_specs,
        check_vma=False,
    )
```

```python
import jax
import jax.numpy as jnp
from jax import lax
from jax.experimental import pallas as pl
from jax.experimental.pallas import tpu as pltpu
from jax.sharding import PartitionSpec as P

NORM_EPS = 1e-6
NEG_BIG = -1e30
MESH = pl.DeviceIdType.MESH
GELU_K = 0.7978845608028654
GELU_C = 0.044715
F32 = jnp.float32
BF16 = jnp.bfloat16


def dot_nn(a, b):
    return lax.dot_general(a, b, (((1,), (0,)), ((), ())), preferred_element_type=F32)


def dot_nt(a, b):
    return lax.dot_general(a, b, (((1,), (1,)), ((), ())), preferred_element_type=F32)


def dot_tn(a, b):
    return lax.dot_general(a, b, (((0,), (0,)), ((), ())), preferred_element_type=F32)


def rms_inverse(v32):
    return lax.rsqrt(jnp.mean(v32 * v32, axis=-1, keepdims=True) + NORM_EPS)


FWD_ORDER = (2, 6, 10, 0, 9, 5, 3, 7, 8, 1, 4)
BWD_ORDER = (2, 1, 9, 5, 0, 3, 7, 4, 10, 6, 8)


def lags(order):
    place = {phase: i for i, phase in enumerate(order)}
    lag = [0]
    for phase in range(1, len(order)):
        lag.append(lag[-1] + (1 if place[phase] < place[phase - 1] else 0))
    return lag


def layer_step(dims, x_in, y_target, w_qkv, w_out, w_up, w_down, gain):
    nz, ns = dims["model"], dims["stage"]
    n_seq, seq_len, d_model = x_in.shape
    n_slab, _, head_dim = w_qkv.shape
    qkv_w = n_slab * head_dim
    att_w = w_out.shape[0]
    ff_w = w_up.shape[1]
    n_head = att_w // head_dim
    tok = 64
    row = tok // nz
    per_seq = seq_len // tok
    n_unit = n_seq * per_seq
    scale = head_dim ** -0.5
    inv_count = 1.0 / (n_seq * seq_len * d_model)
    last_z, last_s = nz - 1, ns - 1
    sub_rows = 16
    half = tok // 2
    n_send, n_recv, n_gath, n_hand = 2, 3, 4, 2
    quarters = range(2)

    def kernel(x_ref, y_ref, wqkv_h, wout_h, wup_h, wdown_h, gain_ref,
               a_out, b_out, d_out, dm_out, dqkv_out, o_out, z_out, du_out, red_out,
               wqkv, wout, wup, wdown, hslot, yslot, a_all, d_all, bbuf, dmbuf, xtmp,
               qkv_all, u_all, m_all, ost, zst, dust, dqkvst, datt, part,
               recv_o, recv_i, send_p, hout, aout, dkacc, dvacc,
               gains, gain_next, lossacc, ga8, gb8, gx,
               w_sem, hsem, ysem, x_sem, gain_sem, hand_sem, save_sem,
               a_rs, d_rs, g1_si, g1_so, b_rs, dm_rs, g2_si, g2_so,
               rs_ro, rs_ri, rs_s, loss_sem, gx_s, gx_r):
        z = lax.axis_index("model")
        st = lax.axis_index("stage")
        is_first = st == 0
        is_last = st == last_s
        inner = (z > 0) & (z < last_z)
        outer = (z == 0) | (z == last_z)
        side = lax.div(z, 2)
        near = 2 * side
        far = 2 - near
        inner_peer = 1 + lax.rem(z, 2)
        outer_peer = last_z * side
        my_half = pl.ds(pl.multiple_of(side * half, half), half)

        def rdma(src, dst, ssem, rsem, **dev):
            return pltpu.make_async_remote_copy(src_ref=src, dst_ref=dst, send_sem=ssem, recv_sem=rsem,
                                                device_id=dev, device_id_type=MESH)

        def rows_of(k):
            return pl.ds(pl.multiple_of(k * row, row), row)

        qkv_copies = [pltpu.make_async_copy(wqkv_h.at[i], wqkv.at[:, pl.ds(i * head_dim, head_dim)], w_sem.at[i])
                      for i in range(n_slab)]
        w_copies = [pltpu.make_async_copy(src, dst, w_sem.at[n_slab + i])
                    for i, (src, dst) in enumerate(((wout_h, wout), (wup_h, wup), (wdown_h, wdown)))]

        def tokens_of(u):
            return lax.div(u, per_seq), pl.multiple_of(lax.rem(u, per_seq) * tok, tok)

        def x_copy(u):
            q, first = tokens_of(u)
            return pltpu.make_async_copy(x_ref.at[q, pl.ds(first, tok), :], a_all.at[u], hsem.at[u])

        def x_again(u):
            q, first = tokens_of(u)
            slot = lax.rem(u, n_send)
            return pltpu.make_async_copy(x_ref.at[q, pl.ds(first, tok), :], xtmp.at[slot], x_sem.at[slot])

        def y_copy(u):
            q, first = tokens_of(u)
            rs = pl.ds(pl.multiple_of(first + side * half, half), half)
            slot = lax.rem(u, n_hand)
            return pltpu.make_async_copy(y_ref.at[q, rs, :], yslot.at[slot], ysem.at[slot])

        @pl.when(is_first)
        def _():
            @pl.loop(0, n_unit)
            def _(u):
                x_copy(u).start()

        for cp in qkv_copies + w_copies:
            cp.start()

        barrier = pltpu.get_barrier_semaphore()
        for i in range(1, nz * ns):
            dz, dst = i % nz, i // nz
            pl.semaphore_signal(barrier, inc=1, device_id_type=MESH,
                                device_id={"model": lax.rem(z + dz, nz), "stage": lax.rem(st + dst, ns)})
        qkv_all[...] = jnp.zeros_like(qkv_all)
        lossacc[...] = jnp.zeros_like(lossacc)
        ga8[...] = jnp.zeros_like(ga8)
        gb8[...] = jnp.zeros_like(gb8)
        gains[...] = gain_ref[...].astype(F32)
        pl.semaphore_wait(barrier, nz * ns - 1)

        def gain_send():
            return rdma(gains, gain_next, gain_sem.at[0], gain_sem.at[1], stage=st - 1)

        @pl.when(st > 0)
        def _():
            gain_send().start()

        class Gather:
            def __init__(self, buf, slot, rsem, si, so, sslot):
                self.buf, self.slot, self.rsem, self.si, self.so, self.sslot = buf, slot, rsem, si, so, sslot

            def block(self, k):
                return self.buf.at[self.slot, rows_of(k), :]

            def inward(self, k, q):
                return rdma(self.block(k), self.block(k), self.si.at[self.sslot, q], self.rsem.at[self.slot, k],
                            model=inner_peer)

            def outward(self, k):
                return rdma(self.block(k), self.block(k), self.so.at[self.sslot, k], self.rsem.at[self.slot, k],
                            model=outer_peer)

            def send(self, q):
                self.inward(near + q, q).start()
                self.outward(near + q).start()

            def relay(self):
                @pl.when(inner)
                def _():
                    for q in quarters:
                        self.outward(far + q).wait_recv()
                        self.outward(far + q).start()

            def collect(self):
                @pl.when(outer)
                def _():
                    for k in range(nz):
                        self.outward(k).wait_recv()

            def own(self):
                @pl.when(inner)
                def _():
                    for q in quarters:
                        self.outward(near + q).wait_recv()

            def drain(self):
                @pl.when(inner)
                def _():
                    for q in quarters:
                        self.outward(far + q).wait_send()

            def drain_own(self):
                @pl.when(inner)
                def _():
                    for q in quarters:
                        self.inward(near + q, q).wait_send()
                        self.outward(near + q).wait_send()

        def gather_a(u):
            return Gather(a_all, u, a_rs, g1_si, g1_so, lax.rem(u, n_gath))

        def gather_d(u):
            return Gather(d_all, u, d_rs, g1_si, g1_so, lax.rem(u, n_gath))

        def gather_b(u):
            return Gather(bbuf, lax.rem(u, n_gath), b_rs, g2_si, g2_so, lax.rem(u, n_gath))

        def gather_dm(u):
            return Gather(dmbuf, lax.rem(u, n_gath), dm_rs, g2_si, g2_so, lax.rem(u, n_gath))

        class Scatter:
            def __init__(self, op, u):
                self.op, self.ss, self.rs = op, lax.rem(u, n_send), lax.rem(u, n_recv)

            def in_copy(self, k):
                return rdma(send_p.at[self.op, self.ss, k], recv_o.at[self.op, self.rs, k],
                            rs_s.at[self.op, self.ss, k], rs_ro.at[self.op, self.rs, k], model=inner_peer)

            def cross_copy(self, k, q):
                return rdma(send_p.at[self.op, self.ss, k], recv_i.at[self.op, self.rs, q],
                            rs_s.at[self.op, self.ss, k], rs_ri.at[self.op, self.rs, q], model=inner_peer)

            def mine(self, k):
                return part[self.op, self.ss, rows_of(k), :]

            def start(self):
                @pl.when(outer)
                def _():
                    for k in (far, far + 1, near, near + 1):
                        send_p[self.op, self.ss, k] = self.mine(k).astype(BF16)
                        self.in_copy(k).start()

            def relay(self):
                @pl.when(inner)
                def _():
                    for q in quarters:
                        k = far + q
                        self.in_copy(k).wait_recv()
                        send_p[self.op, self.ss, k] = (
                            self.mine(k) + recv_o[self.op, self.rs, k].astype(F32)).astype(BF16)
                        self.cross_copy(k, q).start()

            def total(self, q):
                k = near + q
                self.in_copy(k).wait_recv()
                self.cross_copy(k, q).wait_recv()
                return (self.mine(k) + recv_o[self.op, self.rs, k].astype(F32)) + recv_i[self.op, self.rs, q].astype(F32)

            def drain(self):
                @pl.when(outer)
                def _():
                    for k in range(nz):
                        self.in_copy(k).wait_send()

                @pl.when(inner)
                def _():
                    for q in quarters:
                        self.cross_copy(far + q, q).wait_send()

        def save(kind, src, src_slot, dst, u):
            return pltpu.make_async_copy(src.at[src_slot], dst.at[u], save_sem.at[kind, lax.rem(u, n_gath)])

        def sslot(u):
            return lax.rem(u, n_send)

        def gslot(u):
            return lax.rem(u, n_gath)

        def q_rows(q):
            return pl.ds(q * row, row)

        def save_a(u):
            return save(0, a_all, u, a_out, u)

        def save_o(u):
            return save(1, ost, sslot(u), o_out, u)

        def save_b(u):
            return save(2, bbuf, gslot(u), b_out, u)

        def save_z(u):
            return save(3, zst, sslot(u), z_out, u)

        def save_d(u):
            return save(4, d_all, u, d_out, u)

        def save_du(u):
            return save(5, dust, sslot(u), du_out, u)

        def save_dm(u):
            return save(6, dmbuf, gslot(u), dm_out, u)

        def save_dqkv(u):
            return save(7, dqkvst, sslot(u), dqkv_out, u)

        gain_a = gains[0:1, :]
        gain_b = gains[1:2, :]

        def hand_h(u, j):
            s = lax.rem(j, n_hand)
            return rdma(hout.at[s], hslot.at[u], hand_sem.at[s, 6], hsem.at[u], stage=st + 1)

        def hand_quarter(buf, sems, u, j, q, next_stage, act):
            s = lax.rem(j, n_hand)
            k = near + q
            for i, peer in enumerate((inner_peer, outer_peer, z)):
                act(rdma(aout.at[s, q_rows(q), :], buf.at[u, rows_of(k), :], hand_sem.at[s, 3 * q + i], sems.at[u, k],
                         model=peer, stage=next_stage))

        def hand_sent(buf, sems, u, j, next_stage, with_h):
            for q in quarters:
                hand_quarter(buf, sems, u, j, q, next_stage, sent)
            if with_h:
                hand_h(u, j).wait_send()

        def begin(cp):
            cp.start()

        def sent(cp):
            cp.wait_send()

        def softmax_of(u, p, i):
            first = u - p
            cols = pl.ds(i * head_dim, head_dim)
            q = qkv_all[u, :, cols]
            k = qkv_all[pl.ds(first, per_seq), :, pl.ds(att_w + i * head_dim, head_dim)].reshape(seq_len, head_dim)
            v = qkv_all[pl.ds(first, per_seq), :, pl.ds(2 * att_w + i * head_dim, head_dim)].reshape(seq_len, head_dim)
            sc = dot_nt(q, k) * scale
            q_pos = p * tok + lax.broadcasted_iota(jnp.int32, sc.shape, 0)
            k_pos = lax.broadcasted_iota(jnp.int32, sc.shape, 1)
            sc = jnp.where(k_pos <= q_pos, sc, NEG_BIG)
            e = jnp.exp(sc - jnp.max(sc, axis=-1, keepdims=True))
            pr = e * (1.0 / jnp.sum(e, axis=-1, keepdims=True))
            return q, k, v, pr

        def fold(v):
            return jnp.sum(v.reshape(v.shape[0] // 8, 8, d_model), axis=0)

        def f_enter(j, u):
            @pl.when(is_first)
            def _():
                x_copy(u).wait()
                hslot[u] = a_all[u, my_half, :]
                for k in range(nz):
                    rs = pl.ds(k * row, row)
                    h32 = a_all[u, rs, :].astype(F32)
                    a_all[u, rs, :] = (h32 * rms_inverse(h32) * gain_a).astype(BF16)

        def f_relay_a(j, u):
            @pl.when(st > 0)
            def _():
                gather_a(u).relay()

        def f_collect_a(j, u):
            @pl.when(st > 0)
            def _():
                gather_a(u).collect()
                gather_a(u).own()

        def f_attention(j, u):
            @pl.when(j == 0)
            def _():
                for cp in qkv_copies:
                    cp.wait()
                w_copies[0].wait()

            s = sslot(u)
            p = lax.rem(u, per_seq)
            save_a(u).start()
            qkv_all[u] = dot_nn(a_all[u], wqkv[...]).astype(BF16)
            for i in range(n_head):
                _, _, v, pr = softmax_of(u, p, i)
                ost[s, :, pl.ds(i * head_dim, head_dim)] = dot_nn(pr.astype(BF16), v).astype(BF16)
            save_o(u).start()
            part[0, s] = dot_nn(ost[s], wout[...])
            Scatter(0, u).start()

        def scatter_relay(op):
            def run(j, u):
                Scatter(op, u).relay()
            return run

        def f_middle(j, u):
            sc = Scatter(0, u)

            @pl.when(inner)
            def _():
                @pl.when(st > 0)
                def _():
                    rdma(hout.at[0], hslot.at[u], hand_sem.at[0, 6], hsem.at[u], stage=st).wait_recv()

                for q in quarters:
                    m = hslot[u, q_rows(q), :].astype(F32) + sc.total(q)
                    m_all[u, q_rows(q), :] = m
                    bbuf[gslot(u), rows_of(near + q), :] = (m * rms_inverse(m) * gain_b).astype(BF16)
                    gather_b(u).send(q)

            sc.drain()
            save_o(u).wait()

            @pl.when(st > 0)
            def _():
                gather_a(u).drain()

        def f_relay_b(j, u):
            gather_b(u).relay()

        def f_collect_b(j, u):
            gather_b(u).collect()

        def f_mlp(j, u):
            @pl.when(j == 0)
            def _():
                w_copies[1].wait()
                w_copies[2].wait()

            s = sslot(u)
            save_a(u).wait()
            save_b(u).start()

            @pl.when(is_last & inner)
            def _():
                y_copy(u).start()

            u_all[u] = dot_nn(bbuf[gslot(u)], wup[...])

            def act(r, carry):
                rr = pl.ds(pl.multiple_of(r * sub_rows, sub_rows), sub_rows)
                v = u_all[u, rr, :]
                th = jnp.tanh(GELU_K * (v + GELU_C * (v * v * v)))
                zst[s, rr, :] = (0.5 * v * (1.0 + th)).astype(BF16)
                return carry

            lax.fori_loop(0, tok // sub_rows, act, 0)
            save_z(u).start()
            part[1, s] = dot_nn(zst[s], wdown[...])
            Scatter(1, u).start()

        def f_leave(j, u):
            sc = Scatter(1, u)
            s = lax.rem(j, n_hand)

            @pl.when((j == 0) & (st < last_s))
            def _():
                gain_send().wait_recv()

            @pl.when(inner)
            def _():
                @pl.when(st < last_s)
                def _():
                    @pl.when(j >= n_hand)
                    def _():
                        hand_sent(a_all, a_rs, u, j, st + 1, True)

                @pl.when(is_last)
                def _():
                    y_copy(u).wait()

                for q in quarters:
                    h_new = (m_all[u, q_rows(q), :] + sc.total(q)).astype(BF16)
                    h32 = h_new.astype(F32)

                    @pl.when(st < last_s)
                    def _():
                        aout[s, q_rows(q), :] = (h32 * rms_inverse(h32) * gain_next[0:1, :]).astype(BF16)
                        hand_quarter(a_all, a_rs, u, j, q, st + 1, begin)
                        hout[s, q_rows(q), :] = h_new

                    @pl.when(is_last)
                    def _():
                        diff = h32 - yslot[lax.rem(u, n_hand), q_rows(q), :].astype(F32)
                        d_all[u, rows_of(near + q), :] = (diff * inv_count).astype(BF16)
                        lossacc[...] += fold(diff * diff)

                @pl.when(st < last_s)
                def _():
                    hand_h(u, j).start()

            sc.drain()
            gather_b(u).drain()
            gather_b(u).drain_own()
            save_b(u).wait()
            save_z(u).wait()

        def run_phases(order, phases, back):
            lag = lags(order)

            def body(i, carry):
                for phase in order:
                    j = i - lag[phase]

                    @pl.when((j >= 0) & (j < n_unit))
                    def _():
                        phases[phase](j, (n_unit - 1 - j) if back else j)
                return carry

            lax.fori_loop(0, n_unit + lag[-1], body, 0)

        def hand_finish(buf, sems, next_stage, with_h):
            @pl.when(inner)
            def _():
                for j in range(n_unit - n_hand, n_unit):
                    hand_sent(buf, sems, j, j, next_stage, with_h)

        run_phases(FWD_ORDER, (
            f_enter, f_relay_a, f_collect_a, f_attention, scatter_relay(0), f_middle, f_relay_b, f_collect_b, f_mlp,
            scatter_relay(1), f_leave), False)

        def loss_send():
            return rdma(lossacc, lossacc, loss_sem.at[0], loss_sem.at[1], stage=st - 1)

        @pl.when(is_last)
        def _():
            loss_send().start()

        @pl.when(st < last_s)
        def _():
            hand_finish(a_all, a_rs, st + 1, True)

        def b_enter(j, u):
            @pl.when(is_last & inner)
            def _():
                for q in quarters:
                    gather_d(u).send(q)

        def b_relay_d(j, u):
            gather_d(u).relay()

        def b_collect_d(j, u):
            gather_d(u).collect()

            @pl.when(st < last_s)
            def _():
                gather_d(u).own()

        def b_mlp(j, u):
            s = sslot(u)
            save_d(u).start()
            part[0, s] = dot_nt(d_all[u], wdown[...])

            def act(r, carry):
                rr = pl.ds(pl.multiple_of(r * sub_rows, sub_rows), sub_rows)
                v = u_all[u, rr, :]
                v2 = v * v
                th = jnp.tanh(GELU_K * (v + GELU_C * (v2 * v)))
                slope = 0.5 * (1.0 + th) + 0.5 * v * (1.0 - th * th) * (GELU_K * (1.0 + 3.0 * GELU_C * v2))
                dust[s, rr, :] = (part[0, s, rr, :] * slope).astype(BF16)
                return carry

            lax.fori_loop(0, tok // sub_rows, act, 0)
            save_du(u).start()
            part[0, s] = dot_nt(dust[s], wup[...])
            Scatter(0, u).start()

        def b_middle(j, u):
            sc = Scatter(0, u)

            @pl.when(inner)
            def _():
                for q in quarters:
                    m = m_all[u, q_rows(q), :]
                    inv = rms_inverse(m)
                    normed = m * inv
                    dn = sc.total(q)
                    gb8[...] += fold(dn * normed)
                    dn = dn * gain_b
                    dm = d_all[u, rows_of(near + q), :].astype(F32) + inv * (
                        dn - normed * jnp.mean(dn * normed, axis=-1, keepdims=True))
                    m_all[u, q_rows(q), :] = dm
                    dmbuf[gslot(u), rows_of(near + q), :] = dm.astype(BF16)
                    gather_dm(u).send(q)

            sc.drain()
            gather_d(u).drain()

            @pl.when(is_last)
            def _():
                gather_d(u).drain_own()

            save_du(u).wait()

        def b_relay_dm(j, u):
            gather_dm(u).relay()

        def b_collect_dm(j, u):
            gather_dm(u).collect()

        def b_attention(j, u):
            s = sslot(u)
            p = lax.rem(u, per_seq)
            save_d(u).wait()
            save_dm(u).start()

            @pl.when(is_first)
            def _():
                x_again(u).start()

            @pl.when(p == per_seq - 1)
            def _():
                dkacc[...] = jnp.zeros_like(dkacc)
                dvacc[...] = jnp.zeros_like(dvacc)

            datt[...] = dot_nt(dmbuf[gslot(u)], wout[...]).astype(BF16)
            p_rows = pl.ds(pl.multiple_of(p * tok, tok), tok)
            for h in range(n_head):
                cols = pl.ds(h * head_dim, head_dim)
                q, k, v, pr = softmax_of(u, p, h)
                da = datt[:, cols]
                dp = dot_nt(da, v)
                ds = (pr * (dp - jnp.sum(pr * dp, axis=-1, keepdims=True)) * scale).astype(BF16)
                dvacc[:, cols] += dot_tn(pr.astype(BF16), da)
                dkacc[:, cols] += dot_tn(ds, q)
                dqkvst[s, :, cols] = dot_nn(ds, k).astype(BF16)
            dqkvst[s, :, pl.ds(att_w, att_w)] = dkacc[p_rows, :].astype(BF16)
            dqkvst[s, :, pl.ds(2 * att_w, att_w)] = dvacc[p_rows, :].astype(BF16)
            save_dqkv(u).start()
            part[1, s] = dot_nt(dqkvst[s], wqkv[...])

            @pl.when(st > 0)
            def _():
                Scatter(1, u).start()

        def b_relay_h(j, u):
            @pl.when(st > 0)
            def _():
                Scatter(1, u).relay()

        def b_leave(j, u):
            s = lax.rem(j, n_hand)

            @pl.when(st > 0)
            def _():
                sc = Scatter(1, u)

                @pl.when(inner)
                def _():
                    @pl.when(j >= n_hand)
                    def _():
                        hand_sent(d_all, d_rs, u, j, st - 1, False)

                    for q in quarters:
                        h32 = hslot[u, q_rows(q), :].astype(F32)
                        inv = rms_inverse(h32)
                        normed = h32 * inv
                        dn = sc.total(q)
                        ga8[...] += fold(dn * normed)
                        dg = dn * gain_a
                        aout[s, q_rows(q), :] = (m_all[u, q_rows(q), :] + inv * (
                            dg - normed * jnp.mean(dg * normed, axis=-1, keepdims=True))).astype(BF16)
                        hand_quarter(d_all, d_rs, u, j, q, st - 1, begin)

                sc.drain()

            @pl.when(is_first)
            def _():
                x_again(u).wait()
                for k in range(nz):
                    rs = pl.ds(k * row, row)
                    h32 = xtmp[sslot(u), rs, :].astype(F32)
                    ga8[...] += fold(part[1, sslot(u), rs, :] * (h32 * rms_inverse(h32)))

            gather_dm(u).drain()
            gather_dm(u).drain_own()
            save_dm(u).wait()
            save_dqkv(u).wait()

        run_phases(BWD_ORDER, (
            b_enter, b_relay_d, b_collect_d, b_mlp, scatter_relay(0), b_middle, b_relay_dm, b_collect_dm, b_attention,
            b_relay_h, b_leave), True)

        @pl.when(st > 0)
        def _():
            hand_finish(d_all, d_rs, st - 1, False)
            gain_send().wait_send()

        @pl.when(is_last)
        def _():
            loss_send().wait_send()

        @pl.when(st < last_s)
        def _():
            loss_send().wait_recv()

            @pl.when(st > 0)
            def _():
                loss_send().start()
                loss_send().wait_send()

        loss_row = jnp.sum(jnp.sum(lossacc[...], axis=0, keepdims=True), axis=1, keepdims=True)
        gx[z, 0:1, :] = jnp.sum(ga8[...], axis=0, keepdims=True)
        gx[z, 1:2, :] = jnp.sum(gb8[...], axis=0, keepdims=True)
        gx[z, 2:8, :] = jnp.broadcast_to(loss_row, (6, d_model))

        def gx_send(dz):
            return rdma(gx.at[z], gx.at[z], gx_s.at[dz], gx_r.at[z], model=lax.rem(z + dz, nz))

        def gx_recv(dz):
            k = lax.rem(z + dz, nz)
            return rdma(gx.at[k], gx.at[k], gx_s.at[dz], gx_r.at[k], model=k)

        for dz in range(1, nz):
            gx_send(dz).start()
        for dz in range(1, nz):
            gx_recv(dz).wait_recv()
        red_out[...] = gx[0] + gx[1] + gx[2] + gx[3]
        for dz in range(1, nz):
            gx_send(dz).wait_send()

    any_spec = pl.BlockSpec(memory_space=pl.ANY)
    vmem_spec = pl.BlockSpec(memory_space=pltpu.VMEM)

    def out(width):
        return jax.ShapeDtypeStruct((n_unit, tok, width), BF16)

    dma = pltpu.SemaphoreType.DMA
    vmem = pltpu.VMEM
    return pl.pallas_call(
        kernel,
        out_shape=(out(d_model), out(d_model), out(d_model), out(d_model), out(qkv_w), out(att_w), out(ff_w), out(ff_w),
                   jax.ShapeDtypeStruct((8, d_model), F32)),
        in_specs=[any_spec] * 6 + [vmem_spec],
        out_specs=(any_spec,) * 8 + (vmem_spec,),
        scratch_shapes=[
            vmem((d_model, qkv_w), BF16), vmem((att_w, d_model), BF16), vmem((d_model, ff_w), BF16), vmem((ff_w, d_model), BF16),
            vmem((n_unit, half, d_model), BF16), vmem((n_hand, half, d_model), BF16),
            vmem((n_unit, tok, d_model), BF16), vmem((n_unit, tok, d_model), BF16),
            vmem((n_gath, tok, d_model), BF16), vmem((n_gath, tok, d_model), BF16), vmem((n_send, tok, d_model), BF16),
            vmem((n_unit, tok, qkv_w), BF16), vmem((n_unit, tok, ff_w), F32), vmem((n_unit, half, d_model), F32),
            vmem((n_send, tok, att_w), BF16), vmem((n_send, tok, ff_w), BF16), vmem((n_send, tok, ff_w), BF16),
            vmem((n_send, tok, qkv_w), BF16), vmem((tok, att_w), BF16), vmem((2, n_send, tok, d_model), F32),
            vmem((2, n_recv, nz, row, d_model), BF16), vmem((2, n_recv, 2, row, d_model), BF16),
            vmem((2, n_send, nz, row, d_model), BF16),
            vmem((n_hand, half, d_model), BF16), vmem((n_hand, half, d_model), BF16),
            vmem((seq_len, att_w), F32), vmem((seq_len, att_w), F32),
            vmem((2, d_model), F32), vmem((2, d_model), F32),
            vmem((8, d_model), F32), vmem((8, d_model), F32), vmem((8, d_model), F32), vmem((nz, 8, d_model), F32),
            dma((n_slab + 3,)), dma((n_unit,)), dma((n_hand,)), dma((n_send,)), dma((2,)), dma((n_hand, 7)), dma((8, n_gath)),
            dma((n_unit, nz)), dma((n_unit, nz)), dma((n_gath, 2)), dma((n_gath, nz)),
            dma((n_gath, nz)), dma((n_gath, nz)), dma((n_gath, 2)), dma((n_gath, nz)),
            dma((2, n_recv, nz)), dma((2, n_recv, 2)), dma((2, n_send, nz)),
            dma((2,)), dma((nz,)), dma((nz,)),
        ],
        compiler_params=pltpu.CompilerParams(collective_id=0, has_side_effects=True, vmem_limit_bytes=67_043_328),
        name="layer_step",
    )(x_in, y_target, w_qkv, w_out, w_up, w_down, gain)


def weight_grad(act, grad):
    return lax.dot_general(act, grad, (((0, 1), (0, 1)), ((), ())), preferred_element_type=F32)


def solution(mesh):
    dims = dict(mesh.shape)

    def device_fn(x_in, y_target, w_qkv, w_out, w_up, w_down, norm_gain):
        n_batch, seq_len, d_model = x_in.shape
        heads, head_dim = w_qkv.shape[3], w_qkv.shape[4]
        a, b, d, dm, dqkv, o, zz, du, red = layer_step(
            dims, x_in, y_target,
            w_qkv[0].transpose(1, 2, 0, 3).reshape(3 * heads, d_model, head_dim),
            w_out[0].reshape(heads * head_dim, d_model), w_up[0], w_down[0], norm_gain[0])
        grad_qkv = weight_grad(a, dqkv).reshape(1, d_model, 3, heads, head_dim)
        grad_out = weight_grad(o, dm).reshape(1, heads, head_dim, d_model)
        grad_up = weight_grad(b, du)[None]
        grad_down = weight_grad(zz, d)[None]
        loss = 0.5 * red[2, 0:1] / (n_batch * seq_len * d_model)
        return loss, grad_qkv, grad_out, grad_up, grad_down, red[None, 0:2]

    act_spec = P("data", None, None)
    weight_specs = (
        P("stage", None, None, "model", None),
        P("stage", "model", None, None),
        P("stage", None, "model"),
        P("stage", "model", None),
        P("stage", None, None),
    )
    grad_specs = (
        P(("data", "stage"), None, None, "model", None),
        P(("data", "stage"), "model", None, None),
        P(("data", "stage"), None, "model"),
        P(("data", "stage"), "model", None),
        P(("data", "stage"), None, None),
    )
    return jax.shard_map(
        device_fn,
        mesh=mesh,
        in_specs=(act_spec, act_spec) + weight_specs,
        out_specs=(P("data"),) + grad_specs,
        check_vma=False,
    )
```

```python
import jax
import jax.numpy as jnp
from jax import lax
from jax.experimental import pallas as pl
from jax.experimental.pallas import tpu as pltpu
from jax.sharding import PartitionSpec as P

NORM_EPS = 1e-6
NEG_BIG = -1e30
MESH = pl.DeviceIdType.MESH
GELU_K = 0.7978845608028654
GELU_C = 0.044715
F32 = jnp.float32
BF16 = jnp.bfloat16


def dot_nn(a, b):
    return lax.dot_general(a, b, (((1,), (0,)), ((), ())), preferred_element_type=F32)


def dot_nt(a, b):
    return lax.dot_general(a, b, (((1,), (1,)), ((), ())), preferred_element_type=F32)


def dot_tn(a, b):
    return lax.dot_general(a, b, (((0,), (0,)), ((), ())), preferred_element_type=F32)


def rms_inverse(v32):
    return lax.rsqrt(jnp.mean(v32 * v32, axis=-1, keepdims=True) + NORM_EPS)


FWD_ORDER = (2, 6, 10, 0, 9, 5, 3, 7, 8, 1, 4)
BWD_ORDER = (2, 1, 9, 5, 0, 3, 7, 4, 10, 6, 8)


def lags(order):
    place = {phase: i for i, phase in enumerate(order)}
    lag = [0]
    for phase in range(1, len(order)):
        lag.append(lag[-1] + (1 if place[phase] < place[phase - 1] else 0))
    return lag


def layer_step(dims, x_in, y_target, w_qkv, w_out, w_up, w_down, gain):
    nz, ns = dims["model"], dims["stage"]
    n_seq, seq_len, d_model = x_in.shape
    n_slab, _, head_dim = w_qkv.shape
    qkv_w = n_slab * head_dim
    att_w = w_out.shape[0]
    ff_w = w_up.shape[1]
    n_head = att_w // head_dim
    tok = 64
    row = tok // nz
    per_seq = seq_len // tok
    n_unit = n_seq * per_seq
    scale = head_dim ** -0.5
    inv_count = 1.0 / (n_seq * seq_len * d_model)
    last_z, last_s = nz - 1, ns - 1
    sub_rows = 16
    half = tok // 2
    n_send, n_recv, n_gath, n_hand = 2, 3, 4, 2
    quarters = range(2)

    def kernel(x_ref, y_ref, wqkv_h, wout_h, wup_h, wdown_h, gain_ref,
               a_out, b_out, d_out, dm_out, dqkv_out, o_out, z_out, du_out, red_out,
               wqkv, wout, wup, wdown, hslot, yslot, a_all, d_all, bbuf, dmbuf, xtmp,
               qkv_all, u_all, m_all, ost, zst, dust, dqkvst, datt, part,
               recv_o, recv_i, send_p, hout, aout, dkacc, dvacc,
               gains, gain_next, lossacc, ga8, gb8, gx,
               w_sem, hsem, ysem, x_sem, gain_sem, hand_sem, save_sem,
               a_rs, d_rs, g1_si, g1_so, b_rs, dm_rs, g2_si, g2_so,
               rs_ro, rs_ri, rs_s, loss_sem, gx_s, gx_r):
        z = lax.axis_index("model")
        st = lax.axis_index("stage")
        is_first = st == 0
        is_last = st == last_s
        inner = (z > 0) & (z < last_z)
        outer = (z == 0) | (z == last_z)
        side = lax.div(z, 2)
        near = 2 * side
        far = 2 - near
        inner_peer = 1 + lax.rem(z, 2)
        outer_peer = last_z * side
        my_half = pl.ds(pl.multiple_of(side * half, half), half)

        def rdma(src, dst, ssem, rsem, **dev):
            return pltpu.make_async_remote_copy(src_ref=src, dst_ref=dst, send_sem=ssem, recv_sem=rsem,
                                                device_id=dev, device_id_type=MESH)

        def rows_of(k):
            return pl.ds(pl.multiple_of(k * row, row), row)

        qkv_copies = [pltpu.make_async_copy(wqkv_h.at[i], wqkv.at[:, pl.ds(i * head_dim, head_dim)], w_sem.at[i])
                      for i in range(n_slab)]
        w_copies = [pltpu.make_async_copy(src, dst, w_sem.at[n_slab + i])
                    for i, (src, dst) in enumerate(((wout_h, wout), (wup_h, wup), (wdown_h, wdown)))]

        def tokens_of(u):
            return lax.div(u, per_seq), pl.multiple_of(lax.rem(u, per_seq) * tok, tok)

        def x_copy(u):
            q, first = tokens_of(u)
            return pltpu.make_async_copy(x_ref.at[q, pl.ds(first, tok), :], a_all.at[u], hsem.at[u])

        def x_again(u):
            q, first = tokens_of(u)
            slot = lax.rem(u, n_send)
            return pltpu.make_async_copy(x_ref.at[q, pl.ds(first, tok), :], xtmp.at[slot], x_sem.at[slot])

        def y_copy(u):
            q, first = tokens_of(u)
            rs = pl.ds(pl.multiple_of(first + side * half, half), half)
            slot = lax.rem(u, n_hand)
            return pltpu.make_async_copy(y_ref.at[q, rs, :], yslot.at[slot], ysem.at[slot])

        @pl.when(is_first)
        def _():
            @pl.loop(0, n_unit)
            def _(u):
                x_copy(u).start()

        for cp in qkv_copies + w_copies:
            cp.start()

        barrier = pltpu.get_barrier_semaphore()
        for i in range(1, nz * ns):
            dz, dst = i % nz, i // nz
            pl.semaphore_signal(barrier, inc=1, device_id_type=MESH,
                                device_id={"model": lax.rem(z + dz, nz), "stage": lax.rem(st + dst, ns)})
        qkv_all[...] = jnp.zeros_like(qkv_all)
        lossacc[...] = jnp.zeros_like(lossacc)
        ga8[...] = jnp.zeros_like(ga8)
        gb8[...] = jnp.zeros_like(gb8)
        gains[...] = gain_ref[...].astype(F32)
        pl.semaphore_wait(barrier, nz * ns - 1)

        def gain_send():
            return rdma(gains, gain_next, gain_sem.at[0], gain_sem.at[1], stage=st - 1)

        @pl.when(st > 0)
        def _():
            gain_send().start()

        class Gather:
            def __init__(self, buf, slot, rsem, si, so, sslot):
                self.buf, self.slot, self.rsem, self.si, self.so, self.sslot = buf, slot, rsem, si, so, sslot

            def block(self, k):
                return self.buf.at[self.slot, rows_of(k), :]

            def inward(self, k, q):
                return rdma(self.block(k), self.block(k), self.si.at[self.sslot, q], self.rsem.at[self.slot, k],
                            model=inner_peer)

            def outward(self, k):
                return rdma(self.block(k), self.block(k), self.so.at[self.sslot, k], self.rsem.at[self.slot, k],
                            model=outer_peer)

            def send(self, q):
                self.inward(near + q, q).start()
                self.outward(near + q).start()

            def relay(self):
                @pl.when(inner)
                def _():
                    for q in quarters:
                        self.outward(far + q).wait_recv()
                        self.outward(far + q).start()

            def collect(self):
                @pl.when(outer)
                def _():
                    for k in range(nz):
                        self.outward(k).wait_recv()

            def own(self):
                @pl.when(inner)
                def _():
                    for q in quarters:
                        self.outward(near + q).wait_recv()

            def drain(self):
                @pl.when(inner)
                def _():
                    for q in quarters:
                        self.outward(far + q).wait_send()

            def drain_own(self):
                @pl.when(inner)
                def _():
                    for q in quarters:
                        self.inward(near + q, q).wait_send()
                        self.outward(near + q).wait_send()

        def gather_a(u):
            return Gather(a_all, u, a_rs, g1_si, g1_so, lax.rem(u, n_gath))

        def gather_d(u):
            return Gather(d_all, u, d_rs, g1_si, g1_so, lax.rem(u, n_gath))

        def gather_b(u):
            return Gather(bbuf, lax.rem(u, n_gath), b_rs, g2_si, g2_so, lax.rem(u, n_gath))

        def gather_dm(u):
            return Gather(dmbuf, lax.rem(u, n_gath), dm_rs, g2_si, g2_so, lax.rem(u, n_gath))

        class Scatter:
            def __init__(self, op, u):
                self.op, self.ss, self.rs = op, lax.rem(u, n_send), lax.rem(u, n_recv)

            def in_copy(self, k):
                return rdma(send_p.at[self.op, self.ss, k], recv_o.at[self.op, self.rs, k],
                            rs_s.at[self.op, self.ss, k], rs_ro.at[self.op, self.rs, k], model=inner_peer)

            def cross_copy(self, k, q):
                return rdma(send_p.at[self.op, self.ss, k], recv_i.at[self.op, self.rs, q],
                            rs_s.at[self.op, self.ss, k], rs_ri.at[self.op, self.rs, q], model=inner_peer)

            def mine(self, k):
                return part[self.op, self.ss, rows_of(k), :]

            def start(self):
                @pl.when(outer)
                def _():
                    for k in (far, far + 1, near, near + 1):
                        send_p[self.op, self.ss, k] = self.mine(k).astype(BF16)
                        self.in_copy(k).start()

            def relay(self):
                @pl.when(inner)
                def _():
                    for q in quarters:
                        k = far + q
                        self.in_copy(k).wait_recv()
                        send_p[self.op, self.ss, k] = (
                            self.mine(k) + recv_o[self.op, self.rs, k].astype(F32)).astype(BF16)
                        self.cross_copy(k, q).start()

            def total(self, q):
                k = near + q
                self.in_copy(k).wait_recv()
                self.cross_copy(k, q).wait_recv()
                return (self.mine(k) + recv_o[self.op, self.rs, k].astype(F32)) + recv_i[self.op, self.rs, q].astype(F32)

            def drain(self):
                @pl.when(outer)
                def _():
                    for k in range(nz):
                        self.in_copy(k).wait_send()

                @pl.when(inner)
                def _():
                    for q in quarters:
                        self.cross_copy(far + q, q).wait_send()

        def save(kind, src, src_slot, dst, u):
            return pltpu.make_async_copy(src.at[src_slot], dst.at[u], save_sem.at[kind, lax.rem(u, n_gath)])

        def sslot(u):
            return lax.rem(u, n_send)

        def gslot(u):
            return lax.rem(u, n_gath)

        def q_rows(q):
            return pl.ds(q * row, row)

        def save_a(u):
            return save(0, a_all, u, a_out, u)

        def save_o(u):
            return save(1, ost, sslot(u), o_out, u)

        def save_b(u):
            return save(2, bbuf, gslot(u), b_out, u)

        def save_z(u):
            return save(3, zst, sslot(u), z_out, u)

        def save_d(u):
            return save(4, d_all, u, d_out, u)

        def save_du(u):
            return save(5, dust, sslot(u), du_out, u)

        def save_dm(u):
            return save(6, dmbuf, gslot(u), dm_out, u)

        def save_dqkv(u):
            return save(7, dqkvst, sslot(u), dqkv_out, u)

        gain_a = gains[0:1, :]
        gain_b = gains[1:2, :]

        def hand_h(u, j):
            s = lax.rem(j, n_hand)
            return rdma(hout.at[s], hslot.at[u], hand_sem.at[s, 6], hsem.at[u], stage=st + 1)

        def hand_quarter(buf, sems, u, j, q, next_stage, act):
            s = lax.rem(j, n_hand)
            k = near + q
            for i, peer in enumerate((inner_peer, outer_peer, z)):
                act(rdma(aout.at[s, q_rows(q), :], buf.at[u, rows_of(k), :], hand_sem.at[s, 3 * q + i], sems.at[u, k],
                         model=peer, stage=next_stage))

        def hand_sent(buf, sems, u, j, next_stage, with_h):
            for q in quarters:
                hand_quarter(buf, sems, u, j, q, next_stage, sent)
            if with_h:
                hand_h(u, j).wait_send()

        def begin(cp):
            cp.start()

        def sent(cp):
            cp.wait_send()

        def softmax_of(u, p, i):
            first = u - p
            cols = pl.ds(i * head_dim, head_dim)
            q = qkv_all[u, :, cols]
            k = qkv_all[pl.ds(first, per_seq), :, pl.ds(att_w + i * head_dim, head_dim)].reshape(seq_len, head_dim)
            v = qkv_all[pl.ds(first, per_seq), :, pl.ds(2 * att_w + i * head_dim, head_dim)].reshape(seq_len, head_dim)
            sc = dot_nt(q, k) * scale
            q_pos = p * tok + lax.broadcasted_iota(jnp.int32, sc.shape, 0)
            k_pos = lax.broadcasted_iota(jnp.int32, sc.shape, 1)
            sc = jnp.where(k_pos <= q_pos, sc, NEG_BIG)
            e = jnp.exp(sc - jnp.max(sc, axis=-1, keepdims=True))
            pr = e * (1.0 / jnp.sum(e, axis=-1, keepdims=True))
            return q, k, v, pr

        def fold(v):
            return jnp.sum(v.reshape(v.shape[0] // 8, 8, d_model), axis=0)

        def f_enter(j, u):
            @pl.when(is_first)
            def _():
                x_copy(u).wait()
                hslot[u] = a_all[u, my_half, :]
                for k in range(nz):
                    rs = pl.ds(k * row, row)
                    h32 = a_all[u, rs, :].astype(F32)
                    a_all[u, rs, :] = (h32 * rms_inverse(h32) * gain_a).astype(BF16)

        def f_relay_a(j, u):
            @pl.when(st > 0)
            def _():
                gather_a(u).relay()

        def f_collect_a(j, u):
            @pl.when(st > 0)
            def _():
                gather_a(u).collect()
                gather_a(u).own()

        def f_attention(j, u):
            @pl.when(j == 0)
            def _():
                for cp in qkv_copies:
                    cp.wait()
                w_copies[0].wait()

            s = sslot(u)
            p = lax.rem(u, per_seq)
            save_a(u).start()
            qkv_all[u] = dot_nn(a_all[u], wqkv[...]).astype(BF16)
            for i in range(n_head):
                _, _, v, pr = softmax_of(u, p, i)
                ost[s, :, pl.ds(i * head_dim, head_dim)] = dot_nn(pr.astype(BF16), v).astype(BF16)
            save_o(u).start()
            part[0, s] = dot_nn(ost[s], wout[...])
            Scatter(0, u).start()

        def scatter_relay(op):
            def run(j, u):
                Scatter(op, u).relay()
            return run

        def f_middle(j, u):
            sc = Scatter(0, u)

            @pl.when(inner)
            def _():
                @pl.when(st > 0)
                def _():
                    rdma(hout.at[0], hslot.at[u], hand_sem.at[0, 6], hsem.at[u], stage=st).wait_recv()

                for q in quarters:
                    m = hslot[u, q_rows(q), :].astype(F32) + sc.total(q)
                    m_all[u, q_rows(q), :] = m
                    bbuf[gslot(u), rows_of(near + q), :] = (m * rms_inverse(m) * gain_b).astype(BF16)
                    gather_b(u).send(q)

            sc.drain()
            save_o(u).wait()

            @pl.when(st > 0)
            def _():
                gather_a(u).drain()

        def f_relay_b(j, u):
            gather_b(u).relay()

        def f_collect_b(j, u):
            gather_b(u).collect()

        def f_mlp(j, u):
            @pl.when(j == 0)
            def _():
                w_copies[1].wait()
                w_copies[2].wait()

            s = sslot(u)
            save_a(u).wait()
            save_b(u).start()

            @pl.when(is_last & inner)
            def _():
                y_copy(u).start()

            u_all[u] = dot_nn(bbuf[gslot(u)], wup[...])

            def act(r, carry):
                rr = pl.ds(pl.multiple_of(r * sub_rows, sub_rows), sub_rows)
                v = u_all[u, rr, :]
                th = jnp.tanh(GELU_K * (v + GELU_C * (v * v * v)))
                zst[s, rr, :] = (0.5 * v * (1.0 + th)).astype(BF16)
                return carry

            lax.fori_loop(0, tok // sub_rows, act, 0)
            save_z(u).start()
            part[1, s] = dot_nn(zst[s], wdown[...])
            Scatter(1, u).start()

        def f_leave(j, u):
            sc = Scatter(1, u)
            s = lax.rem(j, n_hand)

            @pl.when((j == 0) & (st < last_s))
            def _():
                gain_send().wait_recv()

            @pl.when(inner)
            def _():
                @pl.when(st < last_s)
                def _():
                    @pl.when(j >= n_hand)
                    def _():
                        hand_sent(a_all, a_rs, u, j, st + 1, True)

                @pl.when(is_last)
                def _():
                    y_copy(u).wait()

                for q in quarters:
                    h_new = (m_all[u, q_rows(q), :] + sc.total(q)).astype(BF16)
                    h32 = h_new.astype(F32)

                    @pl.when(st < last_s)
                    def _():
                        aout[s, q_rows(q), :] = (h32 * rms_inverse(h32) * gain_next[0:1, :]).astype(BF16)
                        hand_quarter(a_all, a_rs, u, j, q, st + 1, begin)
                        hout[s, q_rows(q), :] = h_new

                    @pl.when(is_last)
                    def _():
                        diff = h32 - yslot[lax.rem(u, n_hand), q_rows(q), :].astype(F32)
                        d_all[u, rows_of(near + q), :] = (diff * inv_count).astype(BF16)
                        lossacc[...] += fold(diff * diff)

                @pl.when(st < last_s)
                def _():
                    hand_h(u, j).start()

            sc.drain()
            gather_b(u).drain()
            gather_b(u).drain_own()
            save_b(u).wait()
            save_z(u).wait()

        def run_phases(order, phases, back):
            lag = lags(order)

            def body(i, carry):
                for phase in order:
                    j = i - lag[phase]

                    @pl.when((j >= 0) & (j < n_unit))
                    def _():
                        phases[phase](j, (n_unit - 1 - j) if back else j)
                return carry

            lax.fori_loop(0, n_unit + lag[-1], body, 0)

        def hand_finish(buf, sems, next_stage, with_h):
            @pl.when(inner)
            def _():
                for j in range(n_unit - n_hand, n_unit):
                    hand_sent(buf, sems, j, j, next_stage, with_h)

        run_phases(FWD_ORDER, (
            f_enter, f_relay_a, f_collect_a, f_attention, scatter_relay(0), f_middle, f_relay_b, f_collect_b, f_mlp,
            scatter_relay(1), f_leave), False)

        def loss_send():
            return rdma(lossacc, lossacc, loss_sem.at[0], loss_sem.at[1], stage=st - 1)

        @pl.when(is_last)
        def _():
            loss_send().start()

        @pl.when(st < last_s)
        def _():
            hand_finish(a_all, a_rs, st + 1, True)

        def b_enter(j, u):
            @pl.when(is_last & inner)
            def _():
                for q in quarters:
                    gather_d(u).send(q)

        def b_relay_d(j, u):
            gather_d(u).relay()

        def b_collect_d(j, u):
            gather_d(u).collect()

            @pl.when(st < last_s)
            def _():
                gather_d(u).own()

        def b_mlp(j, u):
            s = sslot(u)
            save_d(u).start()
            part[0, s] = dot_nt(d_all[u], wdown[...])

            def act(r, carry):
                rr = pl.ds(pl.multiple_of(r * sub_rows, sub_rows), sub_rows)
                v = u_all[u, rr, :]
                v2 = v * v
                th = jnp.tanh(GELU_K * (v + GELU_C * (v2 * v)))
                slope = 0.5 * (1.0 + th) + 0.5 * v * (1.0 - th * th) * (GELU_K * (1.0 + 3.0 * GELU_C * v2))
                dust[s, rr, :] = (part[0, s, rr, :] * slope).astype(BF16)
                return carry

            lax.fori_loop(0, tok // sub_rows, act, 0)
            save_du(u).start()
            part[0, s] = dot_nt(dust[s], wup[...])
            Scatter(0, u).start()

        def b_middle(j, u):
            sc = Scatter(0, u)

            @pl.when(inner)
            def _():
                for q in quarters:
                    m = m_all[u, q_rows(q), :]
                    inv = rms_inverse(m)
                    normed = m * inv
                    dn = sc.total(q)
                    gb8[...] += fold(dn * normed)
                    dn = dn * gain_b
                    dm = d_all[u, rows_of(near + q), :].astype(F32) + inv * (
                        dn - normed * jnp.mean(dn * normed, axis=-1, keepdims=True))
                    m_all[u, q_rows(q), :] = dm
                    dmbuf[gslot(u), rows_of(near + q), :] = dm.astype(BF16)
                    gather_dm(u).send(q)

            sc.drain()
            gather_d(u).drain()

            @pl.when(is_last)
            def _():
                gather_d(u).drain_own()

            save_du(u).wait()

        def b_relay_dm(j, u):
            gather_dm(u).relay()

        def b_collect_dm(j, u):
            gather_dm(u).collect()

        def b_attention(j, u):
            s = sslot(u)
            p = lax.rem(u, per_seq)
            save_d(u).wait()
            save_dm(u).start()

            @pl.when(is_first)
            def _():
                x_again(u).start()

            @pl.when(p == per_seq - 1)
            def _():
                dkacc[...] = jnp.zeros_like(dkacc)
                dvacc[...] = jnp.zeros_like(dvacc)

            datt[...] = dot_nt(dmbuf[gslot(u)], wout[...]).astype(BF16)
            p_rows = pl.ds(pl.multiple_of(p * tok, tok), tok)
            for h in range(n_head):
                cols = pl.ds(h * head_dim, head_dim)
                q, k, v, pr = softmax_of(u, p, h)
                da = datt[:, cols]
                dp = dot_nt(da, v)
                ds = (pr * (dp - jnp.sum(pr * dp, axis=-1, keepdims=True)) * scale).astype(BF16)
                dvacc[:, cols] += dot_tn(pr.astype(BF16), da)
                dkacc[:, cols] += dot_tn(ds, q)
                dqkvst[s, :, cols] = dot_nn(ds, k).astype(BF16)
            dqkvst[s, :, pl.ds(att_w, att_w)] = dkacc[p_rows, :].astype(BF16)
            dqkvst[s, :, pl.ds(2 * att_w, att_w)] = dvacc[p_rows, :].astype(BF16)
            save_dqkv(u).start()
            part[1, s] = dot_nt(dqkvst[s], wqkv[...])

            @pl.when(st > 0)
            def _():
                Scatter(1, u).start()

        def b_relay_h(j, u):
            @pl.when(st > 0)
            def _():
                Scatter(1, u).relay()

        def b_leave(j, u):
            s = lax.rem(j, n_hand)

            @pl.when(st > 0)
            def _():
                sc = Scatter(1, u)

                @pl.when(inner)
                def _():
                    @pl.when(j >= n_hand)
                    def _():
                        hand_sent(d_all, d_rs, u, j, st - 1, False)

                    for q in quarters:
                        h32 = hslot[u, q_rows(q), :].astype(F32)
                        inv = rms_inverse(h32)
                        normed = h32 * inv
                        dn = sc.total(q)
                        ga8[...] += fold(dn * normed)
                        dg = dn * gain_a
                        aout[s, q_rows(q), :] = (m_all[u, q_rows(q), :] + inv * (
                            dg - normed * jnp.mean(dg * normed, axis=-1, keepdims=True))).astype(BF16)
                        hand_quarter(d_all, d_rs, u, j, q, st - 1, begin)

                sc.drain()

            @pl.when(is_first)
            def _():
                x_again(u).wait()
                for k in range(nz):
                    rs = pl.ds(k * row, row)
                    h32 = xtmp[sslot(u), rs, :].astype(F32)
                    ga8[...] += fold(part[1, sslot(u), rs, :] * (h32 * rms_inverse(h32)))

            gather_dm(u).drain()
            gather_dm(u).drain_own()
            save_dm(u).wait()
            save_dqkv(u).wait()

        run_phases(BWD_ORDER, (
            b_enter, b_relay_d, b_collect_d, b_mlp, scatter_relay(0), b_middle, b_relay_dm, b_collect_dm, b_attention,
            b_relay_h, b_leave), True)

        @pl.when(st > 0)
        def _():
            hand_finish(d_all, d_rs, st - 1, False)
            gain_send().wait_send()

        @pl.when(is_last)
        def _():
            loss_send().wait_send()

        @pl.when(st < last_s)
        def _():
            loss_send().wait_recv()

            @pl.when(st > 0)
            def _():
                loss_send().start()
                loss_send().wait_send()

        loss_row = jnp.sum(jnp.sum(lossacc[...], axis=0, keepdims=True), axis=1, keepdims=True)
        gx[z, 0:1, :] = jnp.sum(ga8[...], axis=0, keepdims=True)
        gx[z, 1:2, :] = jnp.sum(gb8[...], axis=0, keepdims=True)
        gx[z, 2:8, :] = jnp.broadcast_to(loss_row, (6, d_model))

        def gx_send(dz):
            return rdma(gx.at[z], gx.at[z], gx_s.at[dz], gx_r.at[z], model=lax.rem(z + dz, nz))

        def gx_recv(dz):
            k = lax.rem(z + dz, nz)
            return rdma(gx.at[k], gx.at[k], gx_s.at[dz], gx_r.at[k], model=k)

        for dz in range(1, nz):
            gx_send(dz).start()
        for dz in range(1, nz):
            gx_recv(dz).wait_recv()
        red_out[...] = gx[0] + gx[1] + gx[2] + gx[3]
        for dz in range(1, nz):
            gx_send(dz).wait_send()

    any_spec = pl.BlockSpec(memory_space=pl.ANY)
    vmem_spec = pl.BlockSpec(memory_space=pltpu.VMEM)

    def out(width):
        return jax.ShapeDtypeStruct((n_unit, tok, width), BF16)

    dma = pltpu.SemaphoreType.DMA
    vmem = pltpu.VMEM
    return pl.pallas_call(
        kernel,
        out_shape=(out(d_model), out(d_model), out(d_model), out(d_model), out(qkv_w), out(att_w), out(ff_w), out(ff_w),
                   jax.ShapeDtypeStruct((8, d_model), F32)),
        in_specs=[any_spec] * 6 + [vmem_spec],
        out_specs=(any_spec,) * 8 + (vmem_spec,),
        scratch_shapes=[
            vmem((d_model, qkv_w), BF16), vmem((att_w, d_model), BF16), vmem((d_model, ff_w), BF16), vmem((ff_w, d_model), BF16),
            vmem((n_unit, half, d_model), BF16), vmem((n_hand, half, d_model), BF16),
            vmem((n_unit, tok, d_model), BF16), vmem((n_unit, tok, d_model), BF16),
            vmem((n_gath, tok, d_model), BF16), vmem((n_gath, tok, d_model), BF16), vmem((n_send, tok, d_model), BF16),
            vmem((n_unit, tok, qkv_w), BF16), vmem((n_unit, tok, ff_w), F32), vmem((n_unit, half, d_model), F32),
            vmem((n_send, tok, att_w), BF16), vmem((n_send, tok, ff_w), BF16), vmem((n_send, tok, ff_w), BF16),
            vmem((n_send, tok, qkv_w), BF16), vmem((tok, att_w), BF16), vmem((2, n_send, tok, d_model), F32),
            vmem((2, n_recv, nz, row, d_model), BF16), vmem((2, n_recv, 2, row, d_model), BF16),
            vmem((2, n_send, nz, row, d_model), BF16),
            vmem((n_hand, half, d_model), BF16), vmem((n_hand, half, d_model), BF16),
            vmem((seq_len, att_w), F32), vmem((seq_len, att_w), F32),
            vmem((2, d_model), F32), vmem((2, d_model), F32),
            vmem((8, d_model), F32), vmem((8, d_model), F32), vmem((8, d_model), F32), vmem((nz, 8, d_model), F32),
            dma((n_slab + 3,)), dma((n_unit,)), dma((n_hand,)), dma((n_send,)), dma((2,)), dma((n_hand, 7)), dma((8, n_gath)),
            dma((n_unit, nz)), dma((n_unit, nz)), dma((n_gath, 2)), dma((n_gath, nz)),
            dma((n_gath, nz)), dma((n_gath, nz)), dma((n_gath, 2)), dma((n_gath, nz)),
            dma((2, n_recv, nz)), dma((2, n_recv, 2)), dma((2, n_send, nz)),
            dma((2,)), dma((nz,)), dma((nz,)),
        ],
        compiler_params=pltpu.CompilerParams(collective_id=0, has_side_effects=True, vmem_limit_bytes=67_043_328),
        name="layer_step",
    )(x_in, y_target, w_qkv, w_out, w_up, w_down, gain)


def weight_grads(o, dm, a, dqkv, b, du, zz, d, head_dim):
    n_tok = o.shape[0] * o.shape[1]
    rows = 256

    def flat(v):
        return v.reshape(n_tok, v.shape[2])

    acts = [flat(v) for v in (o, dm, a, dqkv, b, du, zz, d)]
    att_w, d_model = acts[0].shape[1], acts[1].shape[1]
    qkv_w, ff_w = acts[3].shape[1], acts[5].shape[1]
    n_slab = qkv_w // head_dim

    def kernel(*refs):
        src, outs, held, tiles = refs[:8], refs[8:12], refs[12:20], refs[20:24]
        in_sem, out_sem = refs[24:]
        loads = [pltpu.make_async_copy(src[i], held[i], in_sem.at[i]) for i in range(8)]
        for cp in loads:
            cp.start()

        def stores(pair, i, slot):
            n = tiles[pair].shape[1]
            at = pl.ds(pl.multiple_of(i * n, n), n)
            sem = out_sem.at[pair, slot]
            if pair == 1:
                return [pltpu.make_async_copy(tiles[1].at[slot, :, pl.ds(k * head_dim, head_dim)], outs[1].at[k, at, :], sem)
                        for k in range(n_slab)]
            return [pltpu.make_async_copy(tiles[pair].at[slot], outs[pair].at[at, :], sem)]

        def finish(cps):
            for cp in cps:
                cp.wait()

        counts = []
        for pair in range(4):
            loads[2 * pair].wait()
            loads[2 * pair + 1].wait()
            left, right, tile = held[2 * pair], held[2 * pair + 1], tiles[pair]
            n = tile.shape[1]
            count = left.shape[1] // n
            counts.append(count)

            def body(i, carry):
                slot = lax.rem(i, 2)

                @pl.when(i >= 2)
                def _():
                    finish(stores(pair, i - 2, slot))

                tile[slot] = dot_tn(left[:, pl.ds(pl.multiple_of(i * n, n), n)], right[...])
                for cp in stores(pair, i, slot):
                    cp.start()
                return carry

            lax.fori_loop(0, count, body, 0)
        for pair in range(4):
            for i in range(max(0, counts[pair] - 2), counts[pair]):
                finish(stores(pair, i, i % 2))

    any_spec = pl.BlockSpec(memory_space=pl.ANY)
    return pl.pallas_call(
        kernel,
        out_shape=(jax.ShapeDtypeStruct((att_w, d_model), F32), jax.ShapeDtypeStruct((n_slab, d_model, head_dim), F32),
                   jax.ShapeDtypeStruct((d_model, ff_w), F32), jax.ShapeDtypeStruct((ff_w, d_model), F32)),
        in_specs=[any_spec] * 8,
        out_specs=(any_spec,) * 4,
        scratch_shapes=[pltpu.VMEM(v.shape, BF16) for v in acts] + [
            pltpu.VMEM((1, att_w, d_model), F32), pltpu.VMEM((2, rows, qkv_w), F32),
            pltpu.VMEM((2, rows, ff_w), F32), pltpu.VMEM((2, rows, d_model), F32),
            pltpu.SemaphoreType.DMA((8,)), pltpu.SemaphoreType.DMA((4, 2))],
        compiler_params=pltpu.CompilerParams(vmem_limit_bytes=67_043_328),
        name="weight_grads",
    )(*acts)


def solution(mesh):
    dims = dict(mesh.shape)

    def device_fn(x_in, y_target, w_qkv, w_out, w_up, w_down, norm_gain):
        n_batch, seq_len, d_model = x_in.shape
        heads, head_dim = w_qkv.shape[3], w_qkv.shape[4]
        a, b, d, dm, dqkv, o, zz, du, red = layer_step(
            dims, x_in, y_target,
            w_qkv[0].transpose(1, 2, 0, 3).reshape(3 * heads, d_model, head_dim),
            w_out[0].reshape(heads * head_dim, d_model), w_up[0], w_down[0], norm_gain[0])
        g_out, g_qkv, g_up, g_down = weight_grads(o, dm, a, dqkv, b, du, zz, d, head_dim)
        grad_qkv = g_qkv.reshape(3, heads, d_model, head_dim).transpose(2, 0, 1, 3)[None]
        grad_out = g_out.reshape(1, heads, head_dim, d_model)
        grad_up = g_up[None]
        grad_down = g_down[None]
        loss = 0.5 * red[2, 0:1] / (n_batch * seq_len * d_model)
        return loss, grad_qkv, grad_out, grad_up, grad_down, red[None, 0:2]

    act_spec = P("data", None, None)
    weight_specs = (
        P("stage", None, None, "model", None),
        P("stage", "model", None, None),
        P("stage", None, "model"),
        P("stage", "model", None),
        P("stage", None, None),
    )
    grad_specs = (
        P(("data", "stage"), None, None, "model", None),
        P(("data", "stage"), "model", None, None),
        P(("data", "stage"), None, "model"),
        P(("data", "stage"), "model", None),
        P(("data", "stage"), None, None),
    )
    return jax.shard_map(
        device_fn,
        mesh=mesh,
        in_specs=(act_spec, act_spec) + weight_specs,
        out_specs=(P("data"),) + grad_specs,
        check_vma=False,
    )
```

```python
import jax
import jax.numpy as jnp
from jax import lax
from jax.experimental import pallas as pl
from jax.experimental.pallas import tpu as pltpu
from jax.sharding import PartitionSpec as P

NORM_EPS = 1e-6
NEG_BIG = -1e30
MESH = pl.DeviceIdType.MESH
GELU_K = 0.7978845608028654
GELU_C = 0.044715
F32 = jnp.float32
BF16 = jnp.bfloat16


def dot_nn(a, b):
    return lax.dot_general(a, b, (((1,), (0,)), ((), ())), preferred_element_type=F32)


def dot_nt(a, b):
    return lax.dot_general(a, b, (((1,), (1,)), ((), ())), preferred_element_type=F32)


def dot_tn(a, b):
    return lax.dot_general(a, b, (((0,), (0,)), ((), ())), preferred_element_type=F32)


def rms_inverse(v32):
    return lax.rsqrt(jnp.mean(v32 * v32, axis=-1, keepdims=True) + NORM_EPS)


ORDER = (
    (0, 3), (0, 7), (1, 2), (1, 9), (1, 3), (1, 1), (1, 5), (0, 8), (0, 4), (0, 0), (0, 1), (0, 6), (1, 10), (1,
    7), (0, 10), (1, 4), (1, 0), (1, 8), (1, 6), (0, 2), (0, 9), (0, 5),
)
BACK_START, BACK_STEP = 11, 13


def lags(back):
    place = {phase: i for i, (is_back, phase) in enumerate(ORDER) if is_back == int(back)}
    lag = [0]
    for phase in range(1, len(place)):
        lag.append(lag[-1] + (1 if place[phase] < place[phase - 1] else 0))
    return lag


def layer_step(dims, x_in, y_target, w_qkv, w_out, w_up, w_down, gain):
    nz, ns = dims["model"], dims["stage"]
    n_seq, seq_len, d_model = x_in.shape
    n_slab, _, head_dim = w_qkv.shape
    qkv_w = n_slab * head_dim
    att_w = w_out.shape[0]
    ff_w = w_up.shape[1]
    n_head = att_w // head_dim
    tok = 64
    n_part = 1
    row = tok // (2 * n_part)
    n_block = 2 * n_part
    per_seq = seq_len // tok
    n_unit = n_seq * per_seq
    scale = head_dim ** -0.5
    inv_count = 1.0 / (n_seq * seq_len * d_model)
    last_z, last_s = nz - 1, ns - 1
    sub_rows = 16
    half = tok // 2
    n_send, n_recv, n_gath, n_hand = 2, 3, 4, 2
    quarters = range(n_part)

    def kernel(x_ref, y_ref, wqkv_h, wout_h, wup_h, wdown_h, gain_ref,
               a_out, b_out, d_out, dm_out, dqkv_out, o_out, z_out, du_out, red_out,
               wqkv, wout, wup, wdown, hslot, yslot, a_all, d_all, bbuf, dmbuf, xtmp,
               qkv_all, u_all, m_all, ost, zst, dust, dqkvst, datt, part,
               recv_o, recv_i, send_p, hout, aout, dout, dkacc, dvacc,
               gains, gain_next, lossacc, ga8, gb8, gx,
               w_sem, hsem, ysem, x_sem, gain_sem, hand_sem, back_sem, save_sem,
               a_rs, d_rs, a_si, a_so, d_si, d_so, b_rs, dm_rs, b_si, b_so, dm_si, dm_so,
               rs_ro, rs_ri, rs_s, loss_sem, gx_s, gx_r):
        z = lax.axis_index("model")
        st = lax.axis_index("stage")
        is_first = st == 0
        is_last = st == last_s
        inner = (z > 0) & (z < last_z)
        outer = (z == 0) | (z == last_z)
        side = lax.div(z, 2)
        near = n_part * side
        far = n_part - near
        inner_peer = 1 + lax.rem(z, 2)
        outer_peer = last_z * side
        my_half = pl.ds(pl.multiple_of(side * half, half), half)

        def rdma(src, dst, ssem, rsem, **dev):
            return pltpu.make_async_remote_copy(src_ref=src, dst_ref=dst, send_sem=ssem, recv_sem=rsem,
                                                device_id=dev, device_id_type=MESH)

        def rows_of(k):
            return pl.ds(pl.multiple_of(k * row, row), row)

        qkv_copies = [pltpu.make_async_copy(wqkv_h.at[i], wqkv.at[:, pl.ds(i * head_dim, head_dim)], w_sem.at[i])
                      for i in range(n_slab)]
        w_copies = [pltpu.make_async_copy(src, dst, w_sem.at[n_slab + i])
                    for i, (src, dst) in enumerate(((wout_h, wout), (wup_h, wup), (wdown_h, wdown)))]

        def tokens_of(u):
            return lax.div(u, per_seq), pl.multiple_of(lax.rem(u, per_seq) * tok, tok)

        def x_copy(u):
            q, first = tokens_of(u)
            return pltpu.make_async_copy(x_ref.at[q, pl.ds(first, tok), :], a_all.at[u], hsem.at[u])

        def x_again(j, u):
            q, first = tokens_of(u)
            slot = lax.rem(j, n_send)
            return pltpu.make_async_copy(x_ref.at[q, pl.ds(first, tok), :], xtmp.at[slot], x_sem.at[slot])

        def y_copy(u):
            q, first = tokens_of(u)
            rs = pl.ds(pl.multiple_of(first + side * half, half), half)
            slot = lax.rem(u, n_hand)
            return pltpu.make_async_copy(y_ref.at[q, rs, :], yslot.at[slot], ysem.at[slot])

        @pl.when(is_first)
        def _():
            @pl.loop(0, n_unit)
            def _(u):
                x_copy(u).start()

        for cp in qkv_copies + w_copies:
            cp.start()

        barrier = pltpu.get_barrier_semaphore()
        for i in range(1, nz * ns):
            dz, dst = i % nz, i // nz
            pl.semaphore_signal(barrier, inc=1, device_id_type=MESH,
                                device_id={"model": lax.rem(z + dz, nz), "stage": lax.rem(st + dst, ns)})
        qkv_all[...] = jnp.zeros_like(qkv_all)
        lossacc[...] = jnp.zeros_like(lossacc)
        ga8[...] = jnp.zeros_like(ga8)
        gb8[...] = jnp.zeros_like(gb8)
        gains[...] = gain_ref[...].astype(F32)
        pl.semaphore_wait(barrier, nz * ns - 1)

        def gain_send():
            return rdma(gains, gain_next, gain_sem.at[0], gain_sem.at[1], stage=st - 1)

        @pl.when(st > 0)
        def _():
            gain_send().start()

        class Gather:
            def __init__(self, buf, slot, rsem, si, so, sslot):
                self.buf, self.slot, self.rsem, self.si, self.so, self.sslot = buf, slot, rsem, si, so, sslot

            def block(self, k):
                return self.buf.at[self.slot, rows_of(k), :]

            def inward(self, k, q):
                return rdma(self.block(k), self.block(k), self.si.at[self.sslot, q], self.rsem.at[self.slot, k],
                            model=inner_peer)

            def outward(self, k):
                return rdma(self.block(k), self.block(k), self.so.at[self.sslot, k], self.rsem.at[self.slot, k],
                            model=outer_peer)

            def send(self, q):
                self.inward(near + q, q).start()
                self.outward(near + q).start()

            def relay(self):
                @pl.when(inner)
                def _():
                    for q in quarters:
                        self.outward(far + q).wait_recv()
                        self.outward(far + q).start()

            def collect(self):
                @pl.when(outer)
                def _():
                    for k in range(n_block):
                        self.outward(k).wait_recv()

            def own(self):
                @pl.when(inner)
                def _():
                    for q in quarters:
                        self.outward(near + q).wait_recv()

            def drain(self):
                @pl.when(inner)
                def _():
                    for q in quarters:
                        self.outward(far + q).wait_send()

            def drain_own(self):
                @pl.when(inner)
                def _():
                    for q in quarters:
                        self.inward(near + q, q).wait_send()
                        self.outward(near + q).wait_send()

        def gather_a(u):
            return Gather(a_all, u, a_rs, a_si, a_so, lax.rem(u, n_gath))

        def gather_d(j, u):
            return Gather(d_all, u, d_rs, d_si, d_so, lax.rem(j, n_gath))

        def gather_b(u):
            return Gather(bbuf, lax.rem(u, n_gath), b_rs, b_si, b_so, lax.rem(u, n_gath))

        def gather_dm(j):
            return Gather(dmbuf, lax.rem(j, n_gath), dm_rs, dm_si, dm_so, lax.rem(j, n_gath))

        class Scatter:
            def __init__(self, op, u):
                self.op, self.ss, self.rs = op, lax.rem(u, n_send), lax.rem(u, n_recv)

            def in_copy(self, k):
                return rdma(send_p.at[self.op, self.ss, k], recv_o.at[self.op, self.rs, k],
                            rs_s.at[self.op, self.ss, k], rs_ro.at[self.op, self.rs, k], model=inner_peer)

            def cross_copy(self, k, q):
                return rdma(send_p.at[self.op, self.ss, k], recv_i.at[self.op, self.rs, q],
                            rs_s.at[self.op, self.ss, k], rs_ri.at[self.op, self.rs, q], model=inner_peer)

            def mine(self, k):
                return part[self.op, self.ss, rows_of(k), :]

            def start(self):
                @pl.when(outer)
                def _():
                    for k in [far + q for q in quarters] + [near + q for q in quarters]:
                        send_p[self.op, self.ss, k] = self.mine(k).astype(BF16)
                        self.in_copy(k).start()

            def relay(self):
                @pl.when(inner)
                def _():
                    for q in quarters:
                        k = far + q
                        self.in_copy(k).wait_recv()
                        send_p[self.op, self.ss, k] = (
                            self.mine(k) + recv_o[self.op, self.rs, k].astype(F32)).astype(BF16)
                        self.cross_copy(k, q).start()

            def total(self, q):
                k = near + q
                self.in_copy(k).wait_recv()
                self.cross_copy(k, q).wait_recv()
                return (self.mine(k) + recv_o[self.op, self.rs, k].astype(F32)) + recv_i[self.op, self.rs, q].astype(F32)

            def drain(self):
                @pl.when(outer)
                def _():
                    for k in range(n_block):
                        self.in_copy(k).wait_send()

                @pl.when(inner)
                def _():
                    for q in quarters:
                        self.cross_copy(far + q, q).wait_send()

        def save(kind, src, src_slot, dst, j, u):
            return pltpu.make_async_copy(src.at[src_slot], dst.at[u], save_sem.at[kind, lax.rem(j, n_gath)])

        def sslot(u):
            return lax.rem(u, n_send)

        def gslot(u):
            return lax.rem(u, n_gath)

        def q_rows(q):
            return pl.ds(q * row, row)

        def save_a(u):
            return save(0, a_all, u, a_out, u, u)

        def save_o(u):
            return save(1, ost, sslot(u), o_out, u, u)

        def save_b(u):
            return save(2, bbuf, gslot(u), b_out, u, u)

        def save_z(u):
            return save(3, zst, sslot(u), z_out, u, u)

        def save_d(j, u):
            return save(4, d_all, u, d_out, j, u)

        def save_du(j, u):
            return save(5, dust, sslot(j), du_out, j, u)

        def save_dm(j, u):
            return save(6, dmbuf, gslot(j), dm_out, j, u)

        def save_dqkv(j, u):
            return save(7, dqkvst, sslot(j), dqkv_out, j, u)

        gain_a = gains[0:1, :]
        gain_b = gains[1:2, :]

        def hand_h(u, j):
            s = lax.rem(j, n_hand)
            return rdma(hout.at[s], hslot.at[u], hand_sem.at[s, 3 * n_part], hsem.at[u], stage=st + 1)

        def hand_quarter(back, u, j, q, act):
            s = lax.rem(j, n_hand)
            k = near + q
            src, buf, sems, own = (dout, d_all, d_rs, back_sem) if back else (aout, a_all, a_rs, hand_sem)
            for i, peer in enumerate((inner_peer, outer_peer, z)):
                act(rdma(src.at[s, q_rows(q), :], buf.at[u, rows_of(k), :], own.at[s, 3 * q + i], sems.at[u, k],
                         model=peer, stage=(st - 1) if back else (st + 1)))

        def hand_sent(back, u, j):
            for q in quarters:
                hand_quarter(back, u, j, q, sent)
            if not back:
                hand_h(u, j).wait_send()

        def begin(cp):
            cp.start()

        def sent(cp):
            cp.wait_send()

        def softmax_of(u, p, i):
            first = u - p
            cols = pl.ds(i * head_dim, head_dim)
            q = qkv_all[u, :, cols]
            k = qkv_all[pl.ds(first, per_seq), :, pl.ds(att_w + i * head_dim, head_dim)].reshape(seq_len, head_dim)
            v = qkv_all[pl.ds(first, per_seq), :, pl.ds(2 * att_w + i * head_dim, head_dim)].reshape(seq_len, head_dim)
            sc = dot_nt(q, k) * scale
            q_pos = p * tok + lax.broadcasted_iota(jnp.int32, sc.shape, 0)
            k_pos = lax.broadcasted_iota(jnp.int32, sc.shape, 1)
            sc = jnp.where(k_pos <= q_pos, sc, NEG_BIG)
            e = jnp.exp(sc - jnp.max(sc, axis=-1, keepdims=True))
            pr = e * (1.0 / jnp.sum(e, axis=-1, keepdims=True))
            return q, k, v, pr

        def fold(v):
            return jnp.sum(v.reshape(v.shape[0] // 8, 8, d_model), axis=0)

        def f_enter(j, u):
            @pl.when(is_first)
            def _():
                x_copy(u).wait()
                hslot[u] = a_all[u, my_half, :]
                for k in range(n_block):
                    rs = pl.ds(k * row, row)
                    h32 = a_all[u, rs, :].astype(F32)
                    a_all[u, rs, :] = (h32 * rms_inverse(h32) * gain_a).astype(BF16)

        def f_relay_a(j, u):
            @pl.when(st > 0)
            def _():
                gather_a(u).relay()

        def f_collect_a(j, u):
            @pl.when(st > 0)
            def _():
                gather_a(u).collect()
                gather_a(u).own()

        def f_attention(j, u):
            @pl.when(j == 0)
            def _():
                for cp in qkv_copies:
                    cp.wait()
                w_copies[0].wait()

            s = sslot(u)
            p = lax.rem(u, per_seq)
            save_a(u).start()
            qkv_all[u] = dot_nn(a_all[u], wqkv[...]).astype(BF16)
            for i in range(n_head):
                _, _, v, pr = softmax_of(u, p, i)
                ost[s, :, pl.ds(i * head_dim, head_dim)] = dot_nn(pr.astype(BF16), v).astype(BF16)
            save_o(u).start()
            part[0, s] = dot_nn(ost[s], wout[...])
            Scatter(0, u).start()

        def scatter_relay(op):
            def run(j, u):
                Scatter(op, j).relay()
            return run

        def f_middle(j, u):
            sc = Scatter(0, u)

            @pl.when(inner)
            def _():
                @pl.when(st > 0)
                def _():
                    rdma(hout.at[0], hslot.at[u], hand_sem.at[0, 3 * n_part], hsem.at[u], stage=st).wait_recv()

                for q in quarters:
                    m = hslot[u, q_rows(q), :].astype(F32) + sc.total(q)
                    m_all[u, q_rows(q), :] = m
                    bbuf[gslot(u), rows_of(near + q), :] = (m * rms_inverse(m) * gain_b).astype(BF16)
                    gather_b(u).send(q)

            sc.drain()
            save_o(u).wait()

            @pl.when(st > 0)
            def _():
                gather_a(u).drain()

        def f_relay_b(j, u):
            gather_b(u).relay()

        def f_collect_b(j, u):
            gather_b(u).collect()

        def f_mlp(j, u):
            @pl.when(j == 0)
            def _():
                w_copies[1].wait()
                w_copies[2].wait()

            s = sslot(u)
            save_a(u).wait()
            save_b(u).start()

            @pl.when(is_last & inner)
            def _():
                y_copy(u).start()

            u_all[u] = dot_nn(bbuf[gslot(u)], wup[...])

            def act(r, carry):
                rr = pl.ds(pl.multiple_of(r * sub_rows, sub_rows), sub_rows)
                v = u_all[u, rr, :]
                th = jnp.tanh(GELU_K * (v + GELU_C * (v * v * v)))
                zst[s, rr, :] = (0.5 * v * (1.0 + th)).astype(BF16)
                return carry

            lax.fori_loop(0, tok // sub_rows, act, 0)
            save_z(u).start()
            part[1, s] = dot_nn(zst[s], wdown[...])
            Scatter(1, u).start()

        def f_leave(j, u):
            sc = Scatter(1, u)
            s = lax.rem(j, n_hand)

            @pl.when((j == 0) & (st < last_s))
            def _():
                gain_send().wait_recv()

            @pl.when(inner)
            def _():
                @pl.when(st < last_s)
                def _():
                    @pl.when(j >= n_hand)
                    def _():
                        hand_sent(False, u, j)

                @pl.when(is_last)
                def _():
                    y_copy(u).wait()

                for q in quarters:
                    h_new = (m_all[u, q_rows(q), :] + sc.total(q)).astype(BF16)
                    h32 = h_new.astype(F32)

                    @pl.when(st < last_s)
                    def _():
                        aout[s, q_rows(q), :] = (h32 * rms_inverse(h32) * gain_next[0:1, :]).astype(BF16)
                        hand_quarter(False, u, j, q, begin)
                        hout[s, q_rows(q), :] = h_new

                    @pl.when(is_last)
                    def _():
                        diff = h32 - yslot[lax.rem(u, n_hand), q_rows(q), :].astype(F32)
                        d_all[u, rows_of(near + q), :] = (diff * inv_count).astype(BF16)
                        lossacc[...] += fold(diff * diff)

                @pl.when(st < last_s)
                def _():
                    hand_h(u, j).start()

            sc.drain()
            gather_b(u).drain()
            gather_b(u).drain_own()
            save_b(u).wait()
            save_z(u).wait()

        forward = (f_enter, f_relay_a, f_collect_a, f_attention, scatter_relay(0), f_middle, f_relay_b, f_collect_b, f_mlp,
                   scatter_relay(1), f_leave)

        def b_enter(j, u):
            @pl.when(is_last & inner)
            def _():
                for q in quarters:
                    gather_d(j, u).send(q)

        def b_relay_d(j, u):
            gather_d(j, u).relay()

        def b_collect_d(j, u):
            gather_d(j, u).collect()

            @pl.when(st < last_s)
            def _():
                gather_d(j, u).own()

        def b_mlp(j, u):
            s = sslot(j)
            save_d(j, u).start()
            part[2, s] = dot_nt(d_all[u], wdown[...])

            def act(r, carry):
                rr = pl.ds(pl.multiple_of(r * sub_rows, sub_rows), sub_rows)
                v = u_all[u, rr, :]
                v2 = v * v
                th = jnp.tanh(GELU_K * (v + GELU_C * (v2 * v)))
                slope = 0.5 * (1.0 + th) + 0.5 * v * (1.0 - th * th) * (GELU_K * (1.0 + 3.0 * GELU_C * v2))
                dust[s, rr, :] = (part[2, s, rr, :] * slope).astype(BF16)
                return carry

            lax.fori_loop(0, tok // sub_rows, act, 0)
            save_du(j, u).start()
            part[2, s] = dot_nt(dust[s], wup[...])
            Scatter(2, j).start()

        def b_middle(j, u):
            sc = Scatter(2, j)

            @pl.when(inner)
            def _():
                for q in quarters:
                    m = m_all[u, q_rows(q), :]
                    inv = rms_inverse(m)
                    normed = m * inv
                    dn = sc.total(q)
                    gb8[...] += fold(dn * normed)
                    dn = dn * gain_b
                    dm = d_all[u, rows_of(near + q), :].astype(F32) + inv * (
                        dn - normed * jnp.mean(dn * normed, axis=-1, keepdims=True))
                    m_all[u, q_rows(q), :] = dm
                    dmbuf[gslot(j), rows_of(near + q), :] = dm.astype(BF16)
                    gather_dm(j).send(q)

            sc.drain()
            gather_d(j, u).drain()

            @pl.when(is_last)
            def _():
                gather_d(j, u).drain_own()

            save_du(j, u).wait()

        def b_relay_dm(j, u):
            gather_dm(j).relay()

        def b_collect_dm(j, u):
            gather_dm(j).collect()

        def b_attention(j, u):
            s = sslot(j)
            p = lax.rem(u, per_seq)
            save_d(j, u).wait()
            save_dm(j, u).start()

            @pl.when(is_first)
            def _():
                x_again(j, u).start()

            @pl.when(p == per_seq - 1)
            def _():
                dkacc[...] = jnp.zeros_like(dkacc)
                dvacc[...] = jnp.zeros_like(dvacc)

            datt[...] = dot_nt(dmbuf[gslot(j)], wout[...]).astype(BF16)
            p_rows = pl.ds(pl.multiple_of(p * tok, tok), tok)
            for h in range(n_head):
                cols = pl.ds(h * head_dim, head_dim)
                q, k, v, pr = softmax_of(u, p, h)
                da = datt[:, cols]
                dp = dot_nt(da, v)
                ds = (pr * (dp - jnp.sum(pr * dp, axis=-1, keepdims=True)) * scale).astype(BF16)
                dvacc[:, cols] += dot_tn(pr.astype(BF16), da)
                dkacc[:, cols] += dot_tn(ds, q)
                dqkvst[s, :, cols] = dot_nn(ds, k).astype(BF16)
            dqkvst[s, :, pl.ds(att_w, att_w)] = dkacc[p_rows, :].astype(BF16)
            dqkvst[s, :, pl.ds(2 * att_w, att_w)] = dvacc[p_rows, :].astype(BF16)
            save_dqkv(j, u).start()
            part[3, s] = dot_nt(dqkvst[s], wqkv[...])

            @pl.when(st > 0)
            def _():
                Scatter(3, j).start()

        def b_relay_h(j, u):
            @pl.when(st > 0)
            def _():
                Scatter(3, j).relay()

        def b_leave(j, u):
            s = lax.rem(j, n_hand)

            @pl.when(st > 0)
            def _():
                sc = Scatter(3, j)

                @pl.when(inner)
                def _():
                    @pl.when(j >= n_hand)
                    def _():
                        hand_sent(True, u, j)

                    for q in quarters:
                        h32 = hslot[u, q_rows(q), :].astype(F32)
                        inv = rms_inverse(h32)
                        normed = h32 * inv
                        dn = sc.total(q)
                        ga8[...] += fold(dn * normed)
                        dg = dn * gain_a
                        dout[s, q_rows(q), :] = (m_all[u, q_rows(q), :] + inv * (
                            dg - normed * jnp.mean(dg * normed, axis=-1, keepdims=True))).astype(BF16)
                        hand_quarter(True, u, j, q, begin)

                sc.drain()

            @pl.when(is_first)
            def _():
                x_again(j, u).wait()
                for k in range(n_block):
                    rs = pl.ds(k * row, row)
                    h32 = xtmp[sslot(j), rs, :].astype(F32)
                    ga8[...] += fold(part[3, sslot(j), rs, :] * (h32 * rms_inverse(h32)))

            gather_dm(j).drain()
            gather_dm(j).drain_own()
            save_dm(j, u).wait()
            save_dqkv(j, u).wait()

        backward = (b_enter, b_relay_d, b_collect_d, b_mlp, scatter_relay(2), b_middle, b_relay_dm, b_collect_dm,
                    b_attention, b_relay_h, b_leave)
        f_lag, b_lag = lags(False), lags(True)
        back_from = BACK_START + BACK_STEP * (last_s - st)

        def turn(i, carry):
            for back, phase in ORDER:
                j = (i - back_from - b_lag[phase]) if back else (i - f_lag[phase])

                @pl.when((j >= 0) & (j < n_unit))
                def _():
                    if back:
                        seq = lax.div(j, per_seq)
                        backward[phase](j, 2 * seq * per_seq + (per_seq - 1) - j)
                    else:
                        forward[phase](j, j)
            return carry

        lax.fori_loop(0, n_unit + back_from + b_lag[-1], turn, 0)

        def loss_send():
            return rdma(lossacc, lossacc, loss_sem.at[0], loss_sem.at[1], stage=st - 1)

        def hand_finish(back):
            @pl.when(inner)
            def _():
                for j in range(n_unit - n_hand, n_unit):
                    hand_sent(back, j, j)

        @pl.when(is_last)
        def _():
            loss_send().start()

        @pl.when(st < last_s)
        def _():
            hand_finish(False)

        @pl.when(st > 0)
        def _():
            hand_finish(True)
            gain_send().wait_send()

        @pl.when(is_last)
        def _():
            loss_send().wait_send()

        @pl.when(st < last_s)
        def _():
            loss_send().wait_recv()

            @pl.when(st > 0)
            def _():
                loss_send().start()
                loss_send().wait_send()

        loss_row = jnp.sum(jnp.sum(lossacc[...], axis=0, keepdims=True), axis=1, keepdims=True)
        gx[z, 0:1, :] = jnp.sum(ga8[...], axis=0, keepdims=True)
        gx[z, 1:2, :] = jnp.sum(gb8[...], axis=0, keepdims=True)
        gx[z, 2:8, :] = jnp.broadcast_to(loss_row, (6, d_model))

        def gx_send(dz):
            return rdma(gx.at[z], gx.at[z], gx_s.at[dz], gx_r.at[z], model=lax.rem(z + dz, nz))

        def gx_recv(dz):
            k = lax.rem(z + dz, nz)
            return rdma(gx.at[k], gx.at[k], gx_s.at[dz], gx_r.at[k], model=k)

        for dz in range(1, nz):
            gx_send(dz).start()
        for dz in range(1, nz):
            gx_recv(dz).wait_recv()
        red_out[...] = gx[0] + gx[1] + gx[2] + gx[3]
        for dz in range(1, nz):
            gx_send(dz).wait_send()

    any_spec = pl.BlockSpec(memory_space=pl.ANY)
    vmem_spec = pl.BlockSpec(memory_space=pltpu.VMEM)

    def out(width):
        return jax.ShapeDtypeStruct((n_unit, tok, width), BF16)

    dma = pltpu.SemaphoreType.DMA
    vmem = pltpu.VMEM
    return pl.pallas_call(
        kernel,
        out_shape=(out(d_model), out(d_model), out(d_model), out(d_model), out(qkv_w), out(att_w), out(ff_w), out(ff_w),
                   jax.ShapeDtypeStruct((8, d_model), F32)),
        in_specs=[any_spec] * 6 + [vmem_spec],
        out_specs=(any_spec,) * 8 + (vmem_spec,),
        scratch_shapes=[
            vmem((d_model, qkv_w), BF16), vmem((att_w, d_model), BF16), vmem((d_model, ff_w), BF16), vmem((ff_w, d_model), BF16),
            vmem((n_unit, half, d_model), BF16), vmem((n_hand, half, d_model), BF16),
            vmem((n_unit, tok, d_model), BF16), vmem((n_unit, tok, d_model), BF16),
            vmem((n_gath, tok, d_model), BF16), vmem((n_gath, tok, d_model), BF16), vmem((n_send, tok, d_model), BF16),
            vmem((n_unit, tok, qkv_w), BF16), vmem((n_unit, tok, ff_w), F32), vmem((n_unit, half, d_model), F32),
            vmem((n_send, tok, att_w), BF16), vmem((n_send, tok, ff_w), BF16), vmem((n_send, tok, ff_w), BF16),
            vmem((n_send, tok, qkv_w), BF16), vmem((tok, att_w), BF16), vmem((4, n_send, tok, d_model), F32),
            vmem((4, n_recv, n_block, row, d_model), BF16), vmem((4, n_recv, n_part, row, d_model), BF16),
            vmem((4, n_send, n_block, row, d_model), BF16),
            vmem((n_hand, half, d_model), BF16), vmem((n_hand, half, d_model), BF16), vmem((n_hand, half, d_model), BF16),
            vmem((seq_len, att_w), F32), vmem((seq_len, att_w), F32),
            vmem((2, d_model), F32), vmem((2, d_model), F32),
            vmem((8, d_model), F32), vmem((8, d_model), F32), vmem((8, d_model), F32), vmem((nz, 8, d_model), F32),
            dma((n_slab + 3,)), dma((n_unit,)), dma((n_hand,)), dma((n_send,)), dma((2,)), dma((n_hand, 3 * n_part + 1)), dma((n_hand, 3 * n_part)), dma((8, n_gath)),
            dma((n_unit, n_block)), dma((n_unit, n_block)), dma((n_gath, n_part)), dma((n_gath, n_block)),
            dma((n_gath, n_part)), dma((n_gath, n_block)), dma((n_gath, n_block)), dma((n_gath, n_block)),
            dma((n_gath, n_part)), dma((n_gath, n_block)), dma((n_gath, n_part)), dma((n_gath, n_block)),
            dma((4, n_recv, n_block)), dma((4, n_recv, n_part)), dma((4, n_send, n_block)),
            dma((2,)), dma((nz,)), dma((nz,)),
        ],
        compiler_params=pltpu.CompilerParams(collective_id=0, has_side_effects=True, vmem_limit_bytes=67_043_328),
        name="layer_step",
    )(x_in, y_target, w_qkv, w_out, w_up, w_down, gain)


def weight_grads(o, dm, a, dqkv, b, du, zz, d, red, head_dim, loss_scale):
    n_tok = o.shape[0] * o.shape[1]
    rows = 256

    def flat(v):
        return v.reshape(n_tok, v.shape[2])

    acts = [flat(v) for v in (o, dm, a, dqkv, b, du, zz, d)]
    att_w, d_model = acts[0].shape[1], acts[1].shape[1]
    qkv_w, ff_w = acts[3].shape[1], acts[5].shape[1]
    n_slab = qkv_w // head_dim

    def kernel(*refs):
        src, red_ref, outs = refs[:8], refs[8], refs[9:13]
        gain_out, loss_out = refs[13:15]
        held, tiles = refs[15:23], refs[23:27]
        in_sem, out_sem = refs[27:]
        loads = [pltpu.make_async_copy(src[i], held[i], in_sem.at[i]) for i in range(8)]
        for cp in loads:
            cp.start()

        def stores(pair, i, slot):
            n = tiles[pair].shape[1]
            at = pl.ds(pl.multiple_of(i * n, n), n)
            sem = out_sem.at[pair, slot]
            if pair == 1:
                return [pltpu.make_async_copy(tiles[1].at[slot, :, pl.ds(k * head_dim, head_dim)], outs[1].at[k, at, :], sem)
                        for k in range(n_slab)]
            return [pltpu.make_async_copy(tiles[pair].at[slot], outs[pair].at[at, :], sem)]

        def finish(cps):
            for cp in cps:
                cp.wait()

        gain_out[...] = red_ref[0:2, :]
        loss_out[...] = red_ref[2:3, 0:1] * loss_scale
        counts = []
        for pair in range(4):
            loads[2 * pair].wait()
            loads[2 * pair + 1].wait()
            left, right, tile = held[2 * pair], held[2 * pair + 1], tiles[pair]
            n = tile.shape[1]
            count = left.shape[1] // n
            counts.append(count)

            def body(i, carry):
                slot = lax.rem(i, 2)

                @pl.when(i >= 2)
                def _():
                    finish(stores(pair, i - 2, slot))

                tile[slot] = dot_tn(left[:, pl.ds(pl.multiple_of(i * n, n), n)], right[...])
                for cp in stores(pair, i, slot):
                    cp.start()
                return carry

            lax.fori_loop(0, count, body, 0)
        for pair in range(4):
            for i in range(max(0, counts[pair] - 2), counts[pair]):
                finish(stores(pair, i, i % 2))

    any_spec = pl.BlockSpec(memory_space=pl.ANY)
    vmem_spec = pl.BlockSpec(memory_space=pltpu.VMEM)
    return pl.pallas_call(
        kernel,
        out_shape=(jax.ShapeDtypeStruct((att_w, d_model), F32), jax.ShapeDtypeStruct((n_slab, d_model, head_dim), F32),
                   jax.ShapeDtypeStruct((d_model, ff_w), F32), jax.ShapeDtypeStruct((ff_w, d_model), F32),
                   jax.ShapeDtypeStruct((2, d_model), F32), jax.ShapeDtypeStruct((1, 1), F32)),
        in_specs=[any_spec] * 8 + [vmem_spec],
        out_specs=(any_spec,) * 4 + (vmem_spec,) * 2,
        scratch_shapes=[pltpu.VMEM(v.shape, BF16) for v in acts] + [
            pltpu.VMEM((1, att_w, d_model), F32), pltpu.VMEM((2, rows, qkv_w), F32),
            pltpu.VMEM((2, rows, ff_w), F32), pltpu.VMEM((2, rows, d_model), F32),
            pltpu.SemaphoreType.DMA((8,)), pltpu.SemaphoreType.DMA((4, 2))],
        compiler_params=pltpu.CompilerParams(vmem_limit_bytes=67_043_328),
        name="weight_grads",
    )(*acts, red)


def solution(mesh):
    dims = dict(mesh.shape)

    def device_fn(x_in, y_target, w_qkv, w_out, w_up, w_down, norm_gain):
        n_batch, seq_len, d_model = x_in.shape
        heads, head_dim = w_qkv.shape[3], w_qkv.shape[4]
        a, b, d, dm, dqkv, o, zz, du, red = layer_step(
            dims, x_in, y_target,
            w_qkv[0].transpose(1, 2, 0, 3).reshape(3 * heads, d_model, head_dim),
            w_out[0].reshape(heads * head_dim, d_model), w_up[0], w_down[0], norm_gain[0])
        g_out, g_qkv, g_up, g_down, g_gain, loss = weight_grads(
            o, dm, a, dqkv, b, du, zz, d, red, head_dim, 0.5 / (n_batch * seq_len * d_model))
        grad_qkv = g_qkv.reshape(3, heads, d_model, head_dim).transpose(2, 0, 1, 3)[None]
        grad_out = g_out.reshape(1, heads, head_dim, d_model)
        grad_up = g_up[None]
        grad_down = g_down[None]
        return loss.reshape(1), grad_qkv, grad_out, grad_up, grad_down, g_gain[None]

    act_spec = P("data", None, None)
    weight_specs = (
        P("stage", None, None, "model", None),
        P("stage", "model", None, None),
        P("stage", None, "model"),
        P("stage", "model", None),
        P("stage", None, None),
    )
    grad_specs = (
        P(("data", "stage"), None, None, "model", None),
        P(("data", "stage"), "model", None, None),
        P(("data", "stage"), None, "model"),
        P(("data", "stage"), "model", None),
        P(("data", "stage"), None, None),
    )
    return jax.shard_map(
        device_fn,
        mesh=mesh,
        in_specs=(act_spec, act_spec) + weight_specs,
        out_specs=(P("data"),) + grad_specs,
        check_vma=False,
    )
```

```python
import jax
import jax.numpy as jnp
from jax import lax
from jax.experimental import pallas as pl
from jax.experimental.pallas import tpu as pltpu
from jax.sharding import PartitionSpec as P

NORM_EPS = 1e-6
NEG_BIG = -1e30
MESH = pl.DeviceIdType.MESH
GELU_K = 0.7978845608028654
GELU_C = 0.044715
F32 = jnp.float32
BF16 = jnp.bfloat16


def dot_nn(a, b):
    return lax.dot_general(a, b, (((1,), (0,)), ((), ())), preferred_element_type=F32)


def dot_nt(a, b):
    return lax.dot_general(a, b, (((1,), (1,)), ((), ())), preferred_element_type=F32)


def dot_tn(a, b):
    return lax.dot_general(a, b, (((0,), (0,)), ((), ())), preferred_element_type=F32)


def rms_inverse(v32):
    return lax.rsqrt(jnp.mean(v32 * v32, axis=-1, keepdims=True) + NORM_EPS)


ORDER = (
    (1, 6), (0, 3), (1, 2), (0, 7), (0, 9), (0, 5), (1, 3), (0, 8), (1, 9), (0, 1), (1, 1), (1, 7), (0, 0), (0,
    2), (1, 5), (1, 8), (0, 4), (0, 6), (1, 0), (0, 10), (1, 4), (1, 10),
)
BACK_START, BACK_STEP = 13, 10


def lags(back):
    place = {phase: i for i, (is_back, phase) in enumerate(ORDER) if is_back == int(back)}
    lag = [0]
    for phase in range(1, len(place)):
        lag.append(lag[-1] + (1 if place[phase] < place[phase - 1] else 0))
    return lag


def layer_step(dims, x_in, y_target, w_qkv, w_out, w_up, w_down, gain):
    nz, ns = dims["model"], dims["stage"]
    n_seq, seq_len, d_model = x_in.shape
    n_slab, _, head_dim = w_qkv.shape
    qkv_w = n_slab * head_dim
    att_w = w_out.shape[0]
    ff_w = w_up.shape[1]
    n_head = att_w // head_dim
    tok = 64
    n_part = 2
    row = tok // (2 * n_part)
    n_block = 2 * n_part
    per_seq = seq_len // tok
    n_unit = n_seq * per_seq
    scale = head_dim ** -0.5
    inv_count = 1.0 / (n_seq * seq_len * d_model)
    last_z, last_s = nz - 1, ns - 1
    sub_rows = 16
    half = tok // 2
    n_send, n_recv, n_gath, n_hand = 2, 3, 4, 2
    quarters = range(n_part)

    def kernel(x_ref, y_ref, wqkv_h, wout_h, wup_h, wdown_h, gain_ref,
               a_out, b_out, d_out, dm_out, dqkv_out, o_out, z_out, du_out, red_out,
               wqkv, wout, wup, wdown, hslot, yslot, a_all, d_all, bbuf, dmbuf, xtmp,
               qkv_all, u_all, m_all, ost, zst, dust, dqkvst, datt, part,
               recv_o, recv_i, send_p, hout, aout, dout, dkacc, dvacc,
               gains, gain_next, lossacc, ga8, gb8, gx,
               w_sem, hsem, ysem, x_sem, gain_sem, hand_sem, back_sem, save_sem,
               a_rs, d_rs, a_si, a_so, d_si, d_so, b_rs, dm_rs, b_si, b_so, dm_si, dm_so,
               rs_ro, rs_ri, rs_s, loss_sem, gx_s, gx_r):
        z = lax.axis_index("model")
        st = lax.axis_index("stage")
        is_first = st == 0
        is_last = st == last_s
        inner = (z > 0) & (z < last_z)
        outer = (z == 0) | (z == last_z)
        side = lax.div(z, 2)
        near = n_part * side
        far = n_part - near
        inner_peer = 1 + lax.rem(z, 2)
        outer_peer = last_z * side
        my_half = pl.ds(pl.multiple_of(side * half, half), half)

        def rdma(src, dst, ssem, rsem, **dev):
            return pltpu.make_async_remote_copy(src_ref=src, dst_ref=dst, send_sem=ssem, recv_sem=rsem,
                                                device_id=dev, device_id_type=MESH)

        def rows_of(k):
            return pl.ds(pl.multiple_of(k * row, row), row)

        qkv_copies = [pltpu.make_async_copy(wqkv_h.at[i], wqkv.at[:, pl.ds(i * head_dim, head_dim)], w_sem.at[i])
                      for i in range(n_slab)]
        w_copies = [pltpu.make_async_copy(src, dst, w_sem.at[n_slab + i])
                    for i, (src, dst) in enumerate(((wout_h, wout), (wup_h, wup), (wdown_h, wdown)))]

        def tokens_of(u):
            return lax.div(u, per_seq), pl.multiple_of(lax.rem(u, per_seq) * tok, tok)

        def x_copy(u):
            q, first = tokens_of(u)
            return pltpu.make_async_copy(x_ref.at[q, pl.ds(first, tok), :], a_all.at[u], hsem.at[u])

        def x_again(j, u):
            q, first = tokens_of(u)
            slot = lax.rem(j, n_send)
            return pltpu.make_async_copy(x_ref.at[q, pl.ds(first, tok), :], xtmp.at[slot], x_sem.at[slot])

        def y_copy(u):
            q, first = tokens_of(u)
            rs = pl.ds(pl.multiple_of(first + side * half, half), half)
            slot = lax.rem(u, n_hand)
            return pltpu.make_async_copy(y_ref.at[q, rs, :], yslot.at[slot], ysem.at[slot])

        @pl.when(is_first)
        def _():
            @pl.loop(0, n_unit)
            def _(u):
                x_copy(u).start()

        for cp in qkv_copies + w_copies:
            cp.start()

        barrier = pltpu.get_barrier_semaphore()
        for i in range(1, nz * ns):
            dz, dst = i % nz, i // nz
            pl.semaphore_signal(barrier, inc=1, device_id_type=MESH,
                                device_id={"model": lax.rem(z + dz, nz), "stage": lax.rem(st + dst, ns)})
        qkv_all[...] = jnp.zeros_like(qkv_all)
        lossacc[...] = jnp.zeros_like(lossacc)
        ga8[...] = jnp.zeros_like(ga8)
        gb8[...] = jnp.zeros_like(gb8)
        gains[...] = gain_ref[...].astype(F32)
        pl.semaphore_wait(barrier, nz * ns - 1)

        def gain_send():
            return rdma(gains, gain_next, gain_sem.at[0], gain_sem.at[1], stage=st - 1)

        @pl.when(st > 0)
        def _():
            gain_send().start()

        class Gather:
            def __init__(self, buf, slot, rsem, si, so, sslot):
                self.buf, self.slot, self.rsem, self.si, self.so, self.sslot = buf, slot, rsem, si, so, sslot

            def block(self, k):
                return self.buf.at[self.slot, rows_of(k), :]

            def inward(self, k, q):
                return rdma(self.block(k), self.block(k), self.si.at[self.sslot, q], self.rsem.at[self.slot, k],
                            model=inner_peer)

            def outward(self, k):
                return rdma(self.block(k), self.block(k), self.so.at[self.sslot, k], self.rsem.at[self.slot, k],
                            model=outer_peer)

            def send(self, q):
                self.inward(near + q, q).start()
                self.outward(near + q).start()

            def relay(self):
                @pl.when(inner)
                def _():
                    for q in quarters:
                        self.outward(far + q).wait_recv()
                        self.outward(far + q).start()

            def collect(self):
                @pl.when(outer)
                def _():
                    for k in range(n_block):
                        self.outward(k).wait_recv()

            def own(self):
                @pl.when(inner)
                def _():
                    for q in quarters:
                        self.outward(near + q).wait_recv()

            def drain(self):
                @pl.when(inner)
                def _():
                    for q in quarters:
                        self.outward(far + q).wait_send()

            def drain_own(self):
                @pl.when(inner)
                def _():
                    for q in quarters:
                        self.inward(near + q, q).wait_send()
                        self.outward(near + q).wait_send()

        def gather_a(u):
            return Gather(a_all, u, a_rs, a_si, a_so, lax.rem(u, n_gath))

        def gather_d(j, u):
            return Gather(d_all, u, d_rs, d_si, d_so, lax.rem(j, n_gath))

        def gather_b(u):
            return Gather(bbuf, lax.rem(u, n_gath), b_rs, b_si, b_so, lax.rem(u, n_gath))

        def gather_dm(j):
            return Gather(dmbuf, lax.rem(j, n_gath), dm_rs, dm_si, dm_so, lax.rem(j, n_gath))

        class Scatter:
            def __init__(self, op, u):
                self.op, self.ss, self.rs = op, lax.rem(u, n_send), lax.rem(u, n_recv)

            def in_copy(self, k):
                return rdma(send_p.at[self.op, self.ss, k], recv_o.at[self.op, self.rs, k],
                            rs_s.at[self.op, self.ss, k], rs_ro.at[self.op, self.rs, k], model=inner_peer)

            def cross_copy(self, k, q):
                return rdma(send_p.at[self.op, self.ss, k], recv_i.at[self.op, self.rs, q],
                            rs_s.at[self.op, self.ss, k], rs_ri.at[self.op, self.rs, q], model=inner_peer)

            def mine(self, k):
                return part[self.op, self.ss, rows_of(k), :]

            def start(self):
                @pl.when(outer)
                def _():
                    for k in [far + q for q in quarters] + [near + q for q in quarters]:
                        send_p[self.op, self.ss, k] = self.mine(k).astype(BF16)
                        self.in_copy(k).start()

            def relay(self):
                @pl.when(inner)
                def _():
                    for q in quarters:
                        k = far + q
                        self.in_copy(k).wait_recv()
                        send_p[self.op, self.ss, k] = (
                            self.mine(k) + recv_o[self.op, self.rs, k].astype(F32)).astype(BF16)
                        self.cross_copy(k, q).start()

            def total(self, q):
                k = near + q
                self.in_copy(k).wait_recv()
                self.cross_copy(k, q).wait_recv()
                return (self.mine(k) + recv_o[self.op, self.rs, k].astype(F32)) + recv_i[self.op, self.rs, q].astype(F32)

            def drain(self):
                @pl.when(outer)
                def _():
                    for k in range(n_block):
                        self.in_copy(k).wait_send()

                @pl.when(inner)
                def _():
                    for q in quarters:
                        self.cross_copy(far + q, q).wait_send()

        def save(kind, src, src_slot, dst, j, u):
            return pltpu.make_async_copy(src.at[src_slot], dst.at[u], save_sem.at[kind, lax.rem(j, n_gath)])

        def sslot(u):
            return lax.rem(u, n_send)

        def gslot(u):
            return lax.rem(u, n_gath)

        def q_rows(q):
            return pl.ds(q * row, row)

        def save_a(u):
            return save(0, a_all, u, a_out, u, u)

        def save_o(u):
            return save(1, ost, sslot(u), o_out, u, u)

        def save_b(u):
            return save(2, bbuf, gslot(u), b_out, u, u)

        def save_z(u):
            return save(3, zst, sslot(u), z_out, u, u)

        def save_d(j, u):
            return save(4, d_all, u, d_out, j, u)

        def save_du(j, u):
            return save(5, dust, sslot(j), du_out, j, u)

        def save_dm(j, u):
            return save(6, dmbuf, gslot(j), dm_out, j, u)

        def save_dqkv(j, u):
            return save(7, dqkvst, sslot(j), dqkv_out, j, u)

        gain_a = gains[0:1, :]
        gain_b = gains[1:2, :]

        def hand_h(u, j):
            s = lax.rem(j, n_hand)
            return rdma(hout.at[s], hslot.at[u], hand_sem.at[s, 3 * n_part], hsem.at[u], stage=st + 1)

        def hand_quarter(back, u, j, q, act):
            s = lax.rem(j, n_hand)
            k = near + q
            src, buf, sems, own = (dout, d_all, d_rs, back_sem) if back else (aout, a_all, a_rs, hand_sem)
            for i, peer in enumerate((inner_peer, outer_peer, z)):
                act(rdma(src.at[s, q_rows(q), :], buf.at[u, rows_of(k), :], own.at[s, 3 * q + i], sems.at[u, k],
                         model=peer, stage=(st - 1) if back else (st + 1)))

        def hand_sent(back, u, j):
            for q in quarters:
                hand_quarter(back, u, j, q, sent)
            if not back:
                hand_h(u, j).wait_send()

        def begin(cp):
            cp.start()

        def sent(cp):
            cp.wait_send()

        def softmax_of(u, p, i):
            first = u - p
            cols = pl.ds(i * head_dim, head_dim)
            q = qkv_all[u, :, cols]
            k = qkv_all[pl.ds(first, per_seq), :, pl.ds(att_w + i * head_dim, head_dim)].reshape(seq_len, head_dim)
            v = qkv_all[pl.ds(first, per_seq), :, pl.ds(2 * att_w + i * head_dim, head_dim)].reshape(seq_len, head_dim)
            sc = dot_nt(q, k) * scale
            q_pos = p * tok + lax.broadcasted_iota(jnp.int32, sc.shape, 0)
            k_pos = lax.broadcasted_iota(jnp.int32, sc.shape, 1)
            sc = jnp.where(k_pos <= q_pos, sc, NEG_BIG)
            e = jnp.exp(sc - jnp.max(sc, axis=-1, keepdims=True))
            pr = e * (1.0 / jnp.sum(e, axis=-1, keepdims=True))
            return q, k, v, pr

        def fold(v):
            return jnp.sum(v.reshape(v.shape[0] // 8, 8, d_model), axis=0)

        def f_enter(j, u):
            @pl.when(is_first)
            def _():
                x_copy(u).wait()
                hslot[u] = a_all[u, my_half, :]
                for k in range(n_block):
                    rs = pl.ds(k * row, row)
                    h32 = a_all[u, rs, :].astype(F32)
                    a_all[u, rs, :] = (h32 * rms_inverse(h32) * gain_a).astype(BF16)

        def f_relay_a(j, u):
            @pl.when(st > 0)
            def _():
                gather_a(u).relay()

        def f_collect_a(j, u):
            @pl.when(st > 0)
            def _():
                gather_a(u).collect()
                gather_a(u).own()

        def f_attention(j, u):
            @pl.when(j == 0)
            def _():
                for cp in qkv_copies:
                    cp.wait()
                w_copies[0].wait()

            s = sslot(u)
            p = lax.rem(u, per_seq)
            save_a(u).start()
            qkv_all[u] = dot_nn(a_all[u], wqkv[...]).astype(BF16)
            for i in range(n_head):
                _, _, v, pr = softmax_of(u, p, i)
                ost[s, :, pl.ds(i * head_dim, head_dim)] = dot_nn(pr.astype(BF16), v).astype(BF16)
            save_o(u).start()
            part[0, s] = dot_nn(ost[s], wout[...])
            Scatter(0, u).start()

        def scatter_relay(op):
            def run(j, u):
                Scatter(op, j).relay()
            return run

        def f_middle(j, u):
            sc = Scatter(0, u)

            @pl.when(inner)
            def _():
                @pl.when(st > 0)
                def _():
                    rdma(hout.at[0], hslot.at[u], hand_sem.at[0, 3 * n_part], hsem.at[u], stage=st).wait_recv()

                for q in quarters:
                    m = hslot[u, q_rows(q), :].astype(F32) + sc.total(q)
                    m_all[u, q_rows(q), :] = m
                    bbuf[gslot(u), rows_of(near + q), :] = (m * rms_inverse(m) * gain_b).astype(BF16)
                    gather_b(u).send(q)

            sc.drain()
            save_o(u).wait()

            @pl.when(st > 0)
            def _():
                gather_a(u).drain()

        def f_relay_b(j, u):
            gather_b(u).relay()

        def f_collect_b(j, u):
            gather_b(u).collect()

        def f_mlp(j, u):
            @pl.when(j == 0)
            def _():
                w_copies[1].wait()
                w_copies[2].wait()

            s = sslot(u)
            save_a(u).wait()
            save_b(u).start()

            @pl.when(is_last & inner)
            def _():
                y_copy(u).start()

            u_all[u] = dot_nn(bbuf[gslot(u)], wup[...])

            def act(r, carry):
                rr = pl.ds(pl.multiple_of(r * sub_rows, sub_rows), sub_rows)
                v = u_all[u, rr, :]
                th = jnp.tanh(GELU_K * (v + GELU_C * (v * v * v)))
                zst[s, rr, :] = (0.5 * v * (1.0 + th)).astype(BF16)
                return carry

            lax.fori_loop(0, tok // sub_rows, act, 0)
            save_z(u).start()
            part[1, s] = dot_nn(zst[s], wdown[...])
            Scatter(1, u).start()

        def f_leave(j, u):
            sc = Scatter(1, u)
            s = lax.rem(j, n_hand)

            @pl.when((j == 0) & (st < last_s))
            def _():
                gain_send().wait_recv()

            @pl.when(inner)
            def _():
                @pl.when(st < last_s)
                def _():
                    @pl.when(j >= n_hand)
                    def _():
                        hand_sent(False, u, j)

                @pl.when(is_last)
                def _():
                    y_copy(u).wait()

                for q in quarters:
                    h_new = (m_all[u, q_rows(q), :] + sc.total(q)).astype(BF16)
                    h32 = h_new.astype(F32)

                    @pl.when(st < last_s)
                    def _():
                        aout[s, q_rows(q), :] = (h32 * rms_inverse(h32) * gain_next[0:1, :]).astype(BF16)
                        hand_quarter(False, u, j, q, begin)
                        hout[s, q_rows(q), :] = h_new

                    @pl.when(is_last)
                    def _():
                        diff = h32 - yslot[lax.rem(u, n_hand), q_rows(q), :].astype(F32)
                        d_all[u, rows_of(near + q), :] = (diff * inv_count).astype(BF16)
                        lossacc[...] += fold(diff * diff)

                @pl.when(st < last_s)
                def _():
                    hand_h(u, j).start()

            sc.drain()
            gather_b(u).drain()
            gather_b(u).drain_own()
            save_b(u).wait()
            save_z(u).wait()

        forward = (f_enter, f_relay_a, f_collect_a, f_attention, scatter_relay(0), f_middle, f_relay_b, f_collect_b, f_mlp,
                   scatter_relay(1), f_leave)

        def b_enter(j, u):
            @pl.when(is_last & inner)
            def _():
                for q in quarters:
                    gather_d(j, u).send(q)

        def b_relay_d(j, u):
            gather_d(j, u).relay()

        def b_collect_d(j, u):
            gather_d(j, u).collect()

            @pl.when(st < last_s)
            def _():
                gather_d(j, u).own()

        def b_mlp(j, u):
            s = sslot(j)
            save_d(j, u).start()
            part[2, s] = dot_nt(d_all[u], wdown[...])

            def act(r, carry):
                rr = pl.ds(pl.multiple_of(r * sub_rows, sub_rows), sub_rows)
                v = u_all[u, rr, :]
                v2 = v * v
                th = jnp.tanh(GELU_K * (v + GELU_C * (v2 * v)))
                slope = 0.5 * (1.0 + th) + 0.5 * v * (1.0 - th * th) * (GELU_K * (1.0 + 3.0 * GELU_C * v2))
                dust[s, rr, :] = (part[2, s, rr, :] * slope).astype(BF16)
                return carry

            lax.fori_loop(0, tok // sub_rows, act, 0)
            save_du(j, u).start()
            part[2, s] = dot_nt(dust[s], wup[...])
            Scatter(2, j).start()

        def b_middle(j, u):
            sc = Scatter(2, j)

            @pl.when(inner)
            def _():
                for q in quarters:
                    m = m_all[u, q_rows(q), :]
                    inv = rms_inverse(m)
                    normed = m * inv
                    dn = sc.total(q)
                    gb8[...] += fold(dn * normed)
                    dn = dn * gain_b
                    dm = d_all[u, rows_of(near + q), :].astype(F32) + inv * (
                        dn - normed * jnp.mean(dn * normed, axis=-1, keepdims=True))
                    m_all[u, q_rows(q), :] = dm
                    dmbuf[gslot(j), rows_of(near + q), :] = dm.astype(BF16)
                    gather_dm(j).send(q)

            sc.drain()
            gather_d(j, u).drain()

            @pl.when(is_last)
            def _():
                gather_d(j, u).drain_own()

            save_du(j, u).wait()

        def b_relay_dm(j, u):
            gather_dm(j).relay()

        def b_collect_dm(j, u):
            gather_dm(j).collect()

        def b_attention(j, u):
            s = sslot(j)
            p = lax.rem(u, per_seq)
            save_d(j, u).wait()
            save_dm(j, u).start()

            @pl.when(is_first)
            def _():
                x_again(j, u).start()

            @pl.when(p == per_seq - 1)
            def _():
                dkacc[...] = jnp.zeros_like(dkacc)
                dvacc[...] = jnp.zeros_like(dvacc)

            datt[...] = dot_nt(dmbuf[gslot(j)], wout[...]).astype(BF16)
            p_rows = pl.ds(pl.multiple_of(p * tok, tok), tok)
            for h in range(n_head):
                cols = pl.ds(h * head_dim, head_dim)
                q, k, v, pr = softmax_of(u, p, h)
                da = datt[:, cols]
                dp = dot_nt(da, v)
                ds = (pr * (dp - jnp.sum(pr * dp, axis=-1, keepdims=True)) * scale).astype(BF16)
                dvacc[:, cols] += dot_tn(pr.astype(BF16), da)
                dkacc[:, cols] += dot_tn(ds, q)
                dqkvst[s, :, cols] = dot_nn(ds, k).astype(BF16)
            dqkvst[s, :, pl.ds(att_w, att_w)] = dkacc[p_rows, :].astype(BF16)
            dqkvst[s, :, pl.ds(2 * att_w, att_w)] = dvacc[p_rows, :].astype(BF16)
            save_dqkv(j, u).start()
            part[3, s] = dot_nt(dqkvst[s], wqkv[...])

            @pl.when(st > 0)
            def _():
                Scatter(3, j).start()

        def b_relay_h(j, u):
            @pl.when(st > 0)
            def _():
                Scatter(3, j).relay()

        def b_leave(j, u):
            s = lax.rem(j, n_hand)

            @pl.when(st > 0)
            def _():
                sc = Scatter(3, j)

                @pl.when(inner)
                def _():
                    @pl.when(j >= n_hand)
                    def _():
                        hand_sent(True, u, j)

                    for q in quarters:
                        h32 = hslot[u, q_rows(q), :].astype(F32)
                        inv = rms_inverse(h32)
                        normed = h32 * inv
                        dn = sc.total(q)
                        ga8[...] += fold(dn * normed)
                        dg = dn * gain_a
                        dout[s, q_rows(q), :] = (m_all[u, q_rows(q), :] + inv * (
                            dg - normed * jnp.mean(dg * normed, axis=-1, keepdims=True))).astype(BF16)
                        hand_quarter(True, u, j, q, begin)

                sc.drain()

            @pl.when(is_first)
            def _():
                x_again(j, u).wait()
                for k in range(n_block):
                    rs = pl.ds(k * row, row)
                    h32 = xtmp[sslot(j), rs, :].astype(F32)
                    ga8[...] += fold(part[3, sslot(j), rs, :] * (h32 * rms_inverse(h32)))

            gather_dm(j).drain()
            gather_dm(j).drain_own()
            save_dm(j, u).wait()
            save_dqkv(j, u).wait()

        backward = (b_enter, b_relay_d, b_collect_d, b_mlp, scatter_relay(2), b_middle, b_relay_dm, b_collect_dm,
                    b_attention, b_relay_h, b_leave)
        f_lag, b_lag = lags(False), lags(True)
        back_from = BACK_START + BACK_STEP * (last_s - st)

        def turn(i, carry):
            for back, phase in ORDER:
                j = (i - back_from - b_lag[phase]) if back else (i - f_lag[phase])

                @pl.when((j >= 0) & (j < n_unit))
                def _():
                    if back:
                        seq = lax.div(j, per_seq)
                        backward[phase](j, 2 * seq * per_seq + (per_seq - 1) - j)
                    else:
                        forward[phase](j, j)
            return carry

        lax.fori_loop(0, n_unit + back_from + b_lag[-1], turn, 0)

        def loss_send():
            return rdma(lossacc, lossacc, loss_sem.at[0], loss_sem.at[1], stage=st - 1)

        def hand_finish(back):
            @pl.when(inner)
            def _():
                for j in range(n_unit - n_hand, n_unit):
                    hand_sent(back, j, j)

        @pl.when(is_last)
        def _():
            loss_send().start()

        @pl.when(st < last_s)
        def _():
            hand_finish(False)

        @pl.when(st > 0)
        def _():
            hand_finish(True)
            gain_send().wait_send()

        @pl.when(is_last)
        def _():
            loss_send().wait_send()

        @pl.when(st < last_s)
        def _():
            loss_send().wait_recv()

            @pl.when(st > 0)
            def _():
                loss_send().start()
                loss_send().wait_send()

        loss_row = jnp.sum(jnp.sum(lossacc[...], axis=0, keepdims=True), axis=1, keepdims=True)
        gx[z, 0:1, :] = jnp.sum(ga8[...], axis=0, keepdims=True)
        gx[z, 1:2, :] = jnp.sum(gb8[...], axis=0, keepdims=True)
        gx[z, 2:8, :] = jnp.broadcast_to(loss_row, (6, d_model))

        def gx_send(dz):
            return rdma(gx.at[z], gx.at[z], gx_s.at[dz], gx_r.at[z], model=lax.rem(z + dz, nz))

        def gx_recv(dz):
            k = lax.rem(z + dz, nz)
            return rdma(gx.at[k], gx.at[k], gx_s.at[dz], gx_r.at[k], model=k)

        for dz in range(1, nz):
            gx_send(dz).start()
        for dz in range(1, nz):
            gx_recv(dz).wait_recv()
        red_out[...] = gx[0] + gx[1] + gx[2] + gx[3]
        for dz in range(1, nz):
            gx_send(dz).wait_send()

    any_spec = pl.BlockSpec(memory_space=pl.ANY)
    vmem_spec = pl.BlockSpec(memory_space=pltpu.VMEM)

    def out(width):
        return jax.ShapeDtypeStruct((n_unit, tok, width), BF16)

    dma = pltpu.SemaphoreType.DMA
    vmem = pltpu.VMEM
    return pl.pallas_call(
        kernel,
        out_shape=(out(d_model), out(d_model), out(d_model), out(d_model), out(qkv_w), out(att_w), out(ff_w), out(ff_w),
                   jax.ShapeDtypeStruct((8, d_model), F32)),
        in_specs=[any_spec] * 6 + [vmem_spec],
        out_specs=(any_spec,) * 8 + (vmem_spec,),
        scratch_shapes=[
            vmem((d_model, qkv_w), BF16), vmem((att_w, d_model), BF16), vmem((d_model, ff_w), BF16), vmem((ff_w, d_model), BF16),
            vmem((n_unit, half, d_model), BF16), vmem((n_hand, half, d_model), BF16),
            vmem((n_unit, tok, d_model), BF16), vmem((n_unit, tok, d_model), BF16),
            vmem((n_gath, tok, d_model), BF16), vmem((n_gath, tok, d_model), BF16), vmem((n_send, tok, d_model), BF16),
            vmem((n_unit, tok, qkv_w), BF16), vmem((n_unit, tok, ff_w), F32), vmem((n_unit, half, d_model), F32),
            vmem((n_send, tok, att_w), BF16), vmem((n_send, tok, ff_w), BF16), vmem((n_send, tok, ff_w), BF16),
            vmem((n_send, tok, qkv_w), BF16), vmem((tok, att_w), BF16), vmem((4, n_send, tok, d_model), F32),
            vmem((4, n_recv, n_block, row, d_model), BF16), vmem((4, n_recv, n_part, row, d_model), BF16),
            vmem((4, n_send, n_block, row, d_model), BF16),
            vmem((n_hand, half, d_model), BF16), vmem((n_hand, half, d_model), BF16), vmem((n_hand, half, d_model), BF16),
            vmem((seq_len, att_w), F32), vmem((seq_len, att_w), F32),
            vmem((2, d_model), F32), vmem((2, d_model), F32),
            vmem((8, d_model), F32), vmem((8, d_model), F32), vmem((8, d_model), F32), vmem((nz, 8, d_model), F32),
            dma((n_slab + 3,)), dma((n_unit,)), dma((n_hand,)), dma((n_send,)), dma((2,)), dma((n_hand, 3 * n_part + 1)), dma((n_hand, 3 * n_part)), dma((8, n_gath)),
            dma((n_unit, n_block)), dma((n_unit, n_block)), dma((n_gath, n_part)), dma((n_gath, n_block)),
            dma((n_gath, n_part)), dma((n_gath, n_block)), dma((n_gath, n_block)), dma((n_gath, n_block)),
            dma((n_gath, n_part)), dma((n_gath, n_block)), dma((n_gath, n_part)), dma((n_gath, n_block)),
            dma((4, n_recv, n_block)), dma((4, n_recv, n_part)), dma((4, n_send, n_block)),
            dma((2,)), dma((nz,)), dma((nz,)),
        ],
        compiler_params=pltpu.CompilerParams(collective_id=0, has_side_effects=True, vmem_limit_bytes=67_043_328),
        name="layer_step",
    )(x_in, y_target, w_qkv, w_out, w_up, w_down, gain)


def weight_grads(o, dm, a, dqkv, b, du, zz, d, red, head_dim, loss_scale):
    n_tok = o.shape[0] * o.shape[1]
    rows = 256

    def flat(v):
        return v.reshape(n_tok, v.shape[2])

    acts = [flat(v) for v in (o, dm, a, dqkv, b, du, zz, d)]
    att_w, d_model = acts[0].shape[1], acts[1].shape[1]
    qkv_w, ff_w = acts[3].shape[1], acts[5].shape[1]
    n_slab = qkv_w // head_dim

    def kernel(*refs):
        src, red_ref, outs = refs[:8], refs[8], refs[9:13]
        gain_out, loss_out = refs[13:15]
        held, tiles = refs[15:23], refs[23:27]
        in_sem, out_sem = refs[27:]
        loads = [pltpu.make_async_copy(src[i], held[i], in_sem.at[i]) for i in range(8)]
        for cp in loads:
            cp.start()

        def stores(pair, i, slot):
            n = tiles[pair].shape[1]
            at = pl.ds(pl.multiple_of(i * n, n), n)
            sem = out_sem.at[pair, slot]
            if pair == 1:
                return [pltpu.make_async_copy(tiles[1].at[slot, :, pl.ds(k * head_dim, head_dim)], outs[1].at[k, at, :], sem)
                        for k in range(n_slab)]
            return [pltpu.make_async_copy(tiles[pair].at[slot], outs[pair].at[at, :], sem)]

        def finish(cps):
            for cp in cps:
                cp.wait()

        gain_out[...] = red_ref[0:2, :]
        loss_out[...] = red_ref[2:3, 0:1] * loss_scale
        counts = []
        for pair in range(4):
            loads[2 * pair].wait()
            loads[2 * pair + 1].wait()
            left, right, tile = held[2 * pair], held[2 * pair + 1], tiles[pair]
            n = tile.shape[1]
            count = left.shape[1] // n
            counts.append(count)

            def body(i, carry):
                slot = lax.rem(i, 2)

                @pl.when(i >= 2)
                def _():
                    finish(stores(pair, i - 2, slot))

                tile[slot] = dot_tn(left[:, pl.ds(pl.multiple_of(i * n, n), n)], right[...])
                for cp in stores(pair, i, slot):
                    cp.start()
                return carry

            lax.fori_loop(0, count, body, 0)
        for pair in range(4):
            for i in range(max(0, counts[pair] - 2), counts[pair]):
                finish(stores(pair, i, i % 2))

    any_spec = pl.BlockSpec(memory_space=pl.ANY)
    vmem_spec = pl.BlockSpec(memory_space=pltpu.VMEM)
    return pl.pallas_call(
        kernel,
        out_shape=(jax.ShapeDtypeStruct((att_w, d_model), F32), jax.ShapeDtypeStruct((n_slab, d_model, head_dim), F32),
                   jax.ShapeDtypeStruct((d_model, ff_w), F32), jax.ShapeDtypeStruct((ff_w, d_model), F32),
                   jax.ShapeDtypeStruct((2, d_model), F32), jax.ShapeDtypeStruct((1, 1), F32)),
        in_specs=[any_spec] * 8 + [vmem_spec],
        out_specs=(any_spec,) * 4 + (vmem_spec,) * 2,
        scratch_shapes=[pltpu.VMEM(v.shape, BF16) for v in acts] + [
            pltpu.VMEM((1, att_w, d_model), F32), pltpu.VMEM((2, rows, qkv_w), F32),
            pltpu.VMEM((2, rows, ff_w), F32), pltpu.VMEM((2, rows, d_model), F32),
            pltpu.SemaphoreType.DMA((8,)), pltpu.SemaphoreType.DMA((4, 2))],
        compiler_params=pltpu.CompilerParams(vmem_limit_bytes=67_043_328),
        name="weight_grads",
    )(*acts, red)


def solution(mesh):
    dims = dict(mesh.shape)

    def device_fn(x_in, y_target, w_qkv, w_out, w_up, w_down, norm_gain):
        n_batch, seq_len, d_model = x_in.shape
        heads, head_dim = w_qkv.shape[3], w_qkv.shape[4]
        a, b, d, dm, dqkv, o, zz, du, red = layer_step(
            dims, x_in, y_target,
            w_qkv[0].transpose(1, 2, 0, 3).reshape(3 * heads, d_model, head_dim),
            w_out[0].reshape(heads * head_dim, d_model), w_up[0], w_down[0], norm_gain[0])
        g_out, g_qkv, g_up, g_down, g_gain, loss = weight_grads(
            o, dm, a, dqkv, b, du, zz, d, red, head_dim, 0.5 / (n_batch * seq_len * d_model))
        grad_qkv = g_qkv.reshape(3, heads, d_model, head_dim).transpose(2, 0, 1, 3)[None]
        grad_out = g_out.reshape(1, heads, head_dim, d_model)
        grad_up = g_up[None]
        grad_down = g_down[None]
        return loss.reshape(1), grad_qkv, grad_out, grad_up, grad_down, g_gain[None]

    act_spec = P("data", None, None)
    weight_specs = (
        P("stage", None, None, "model", None),
        P("stage", "model", None, None),
        P("stage", None, "model"),
        P("stage", "model", None),
        P("stage", None, None),
    )
    grad_specs = (
        P(("data", "stage"), None, None, "model", None),
        P(("data", "stage"), "model", None, None),
        P(("data", "stage"), None, "model"),
        P(("data", "stage"), "model", None),
        P(("data", "stage"), None, None),
    )
    return jax.shard_map(
        device_fn,
        mesh=mesh,
        in_specs=(act_spec, act_spec) + weight_specs,
        out_specs=(P("data"),) + grad_specs,
        check_vma=False,
    )
```

```python
import jax
import jax.numpy as jnp
from jax import lax
from jax.experimental import pallas as pl
from jax.experimental.pallas import tpu as pltpu
from jax.sharding import PartitionSpec as P

NORM_EPS = 1e-6
NEG_BIG = -1e30
MESH = pl.DeviceIdType.MESH
GELU_K = 0.7978845608028654
GELU_C = 0.044715
F32 = jnp.float32
BF16 = jnp.bfloat16


def dot_nn(a, b):
    return lax.dot_general(a, b, (((1,), (0,)), ((), ())), preferred_element_type=F32)


def dot_nt(a, b):
    return lax.dot_general(a, b, (((1,), (1,)), ((), ())), preferred_element_type=F32)


def dot_tn(a, b):
    return lax.dot_general(a, b, (((0,), (0,)), ((), ())), preferred_element_type=F32)


def rms_inverse(v32):
    return lax.rsqrt(jnp.mean(v32 * v32, axis=-1, keepdims=True) + NORM_EPS)


ORDER = (
    (1, 6), (0, 3), (1, 2), (0, 7), (0, 9), (0, 5), (1, 3), (0, 8), (1, 9), (0, 1), (1, 1), (1, 7), (0, 0), (0,
    2), (1, 5), (1, 8), (0, 4), (0, 6), (1, 0), (0, 10), (1, 4), (1, 10),
)
BACK_START, BACK_STEP = 13, 10


def lags(back):
    place = {phase: i for i, (is_back, phase) in enumerate(ORDER) if is_back == int(back)}
    lag = [0]
    for phase in range(1, len(place)):
        lag.append(lag[-1] + (1 if place[phase] < place[phase - 1] else 0))
    return lag


def layer_step(dims, x_in, y_target, w_qkv, w_out, w_up, w_down, gain):
    nz, ns = dims["model"], dims["stage"]
    n_seq, seq_len, d_model = x_in.shape
    n_slab, _, head_dim = w_qkv.shape
    qkv_w = n_slab * head_dim
    att_w = w_out.shape[0]
    ff_w = w_up.shape[1]
    n_head = att_w // head_dim
    tok = 64
    n_part = 2
    row = tok // (2 * n_part)
    n_block = 2 * n_part
    per_seq = seq_len // tok
    n_unit = n_seq * per_seq
    scale = head_dim ** -0.5
    inv_count = 1.0 / (n_seq * seq_len * d_model)
    last_z, last_s = nz - 1, ns - 1
    sub_rows = 16
    half = tok // 2
    n_send, n_recv, n_gath, n_hand = 2, 3, 4, 2
    quarters = range(n_part)

    def kernel(x_ref, y_ref, wqkv_h, wout_h, wup_h, wdown_h, gain_ref,
               a_out, b_out, d_out, dm_out, dqkv_out, o_out, z_out, du_out, red_out,
               wqkv, wout, wup, wdown, hslot, yslot, a_all, d_all, bbuf, dmbuf, xtmp,
               qkv_all, u_all, m_all, ost, zst, dust, dqkvst, datt, part,
               recv_o, recv_i, send_p, hout, aout, dout, dkacc, dvacc,
               gains, gain_next, lossacc, ga8, gb8, gx,
               w_sem, hsem, ysem, x_sem, gain_sem, hand_sem, back_sem, save_sem,
               a_rs, d_rs, a_si, a_so, d_si, d_so, b_rs, dm_rs, b_si, b_so, dm_si, dm_so,
               rs_ro, rs_ri, rs_s, loss_sem, gx_s, gx_r):
        z = lax.axis_index("model")
        st = lax.axis_index("stage")
        is_first = st == 0
        is_last = st == last_s
        inner = (z > 0) & (z < last_z)
        outer = (z == 0) | (z == last_z)
        side = lax.div(z, 2)
        near = n_part * side
        far = n_part - near
        inner_peer = 1 + lax.rem(z, 2)
        outer_peer = last_z * side
        my_half = pl.ds(pl.multiple_of(side * half, half), half)

        def rdma(src, dst, ssem, rsem, **dev):
            return pltpu.make_async_remote_copy(src_ref=src, dst_ref=dst, send_sem=ssem, recv_sem=rsem,
                                                device_id=dev, device_id_type=MESH)

        def rows_of(k):
            return pl.ds(pl.multiple_of(k * row, row), row)

        qkv_copies = [pltpu.make_async_copy(wqkv_h.at[i], wqkv.at[:, pl.ds(i * head_dim, head_dim)], w_sem.at[i])
                      for i in range(n_slab)]
        w_copies = [pltpu.make_async_copy(src, dst, w_sem.at[n_slab + i])
                    for i, (src, dst) in enumerate(((wout_h, wout), (wup_h, wup), (wdown_h, wdown)))]

        def tokens_of(u):
            return lax.div(u, per_seq), pl.multiple_of(lax.rem(u, per_seq) * tok, tok)

        def x_copy(u):
            q, first = tokens_of(u)
            return pltpu.make_async_copy(x_ref.at[q, pl.ds(first, tok), :], a_all.at[u], hsem.at[u])

        def x_again(j, u):
            q, first = tokens_of(u)
            slot = lax.rem(j, n_send)
            return pltpu.make_async_copy(x_ref.at[q, pl.ds(first, tok), :], xtmp.at[slot], x_sem.at[slot])

        def y_copy(u):
            q, first = tokens_of(u)
            rs = pl.ds(pl.multiple_of(first + side * half, half), half)
            slot = lax.rem(u, n_hand)
            return pltpu.make_async_copy(y_ref.at[q, rs, :], yslot.at[slot], ysem.at[slot])

        @pl.when(is_first)
        def _():
            @pl.loop(0, n_unit)
            def _(u):
                x_copy(u).start()

        for cp in qkv_copies + w_copies:
            cp.start()

        barrier = pltpu.get_barrier_semaphore()
        for i in range(1, nz * ns):
            dz, dst = i % nz, i // nz
            pl.semaphore_signal(barrier, inc=1, device_id_type=MESH,
                                device_id={"model": lax.rem(z + dz, nz), "stage": lax.rem(st + dst, ns)})
        qkv_all[...] = jnp.zeros_like(qkv_all)
        lossacc[...] = jnp.zeros_like(lossacc)
        ga8[...] = jnp.zeros_like(ga8)
        gb8[...] = jnp.zeros_like(gb8)
        gains[...] = gain_ref[...].astype(F32)
        pl.semaphore_wait(barrier, nz * ns - 1)

        def gain_send():
            return rdma(gains, gain_next, gain_sem.at[0], gain_sem.at[1], stage=st - 1)

        @pl.when(st > 0)
        def _():
            gain_send().start()

        class Gather:
            def __init__(self, buf, slot, rsem, si, so, sslot):
                self.buf, self.slot, self.rsem, self.si, self.so, self.sslot = buf, slot, rsem, si, so, sslot

            def block(self, k):
                return self.buf.at[self.slot, rows_of(k), :]

            def inward(self, k, q):
                return rdma(self.block(k), self.block(k), self.si.at[self.sslot, q], self.rsem.at[self.slot, k],
                            model=inner_peer)

            def outward(self, k):
                return rdma(self.block(k), self.block(k), self.so.at[self.sslot, k], self.rsem.at[self.slot, k],
                            model=outer_peer)

            def send(self, q):
                self.inward(near + q, q).start()
                self.outward(near + q).start()

            def relay(self):
                @pl.when(inner)
                def _():
                    for q in quarters:
                        self.outward(far + q).wait_recv()
                        self.outward(far + q).start()

            def collect(self):
                @pl.when(outer)
                def _():
                    for k in range(n_block):
                        self.outward(k).wait_recv()

            def own(self):
                @pl.when(inner)
                def _():
                    for q in quarters:
                        self.outward(near + q).wait_recv()

            def drain(self):
                @pl.when(inner)
                def _():
                    for q in quarters:
                        self.outward(far + q).wait_send()

            def drain_own(self):
                @pl.when(inner)
                def _():
                    for q in quarters:
                        self.inward(near + q, q).wait_send()
                        self.outward(near + q).wait_send()

        def gather_a(u):
            return Gather(a_all, u, a_rs, a_si, a_so, lax.rem(u, n_gath))

        def gather_d(j, u):
            return Gather(d_all, u, d_rs, d_si, d_so, lax.rem(j, n_gath))

        def gather_b(u):
            return Gather(bbuf, lax.rem(u, n_gath), b_rs, b_si, b_so, lax.rem(u, n_gath))

        def gather_dm(j):
            return Gather(dmbuf, lax.rem(j, n_gath), dm_rs, dm_si, dm_so, lax.rem(j, n_gath))

        class Scatter:
            def __init__(self, op, u):
                self.op, self.ss, self.rs = op, lax.rem(u, n_send), lax.rem(u, n_recv)

            def in_copy(self, k):
                return rdma(send_p.at[self.op, self.ss, k], recv_o.at[self.op, self.rs, k],
                            rs_s.at[self.op, self.ss, k], rs_ro.at[self.op, self.rs, k], model=inner_peer)

            def cross_copy(self, k, q):
                return rdma(send_p.at[self.op, self.ss, k], recv_i.at[self.op, self.rs, q],
                            rs_s.at[self.op, self.ss, k], rs_ri.at[self.op, self.rs, q], model=inner_peer)

            def mine(self, k):
                return part[self.op, self.ss, rows_of(k), :]

            def start(self, j):
                @pl.when(outer)
                def _():
                    @pl.when(j >= n_send)
                    def _():
                        self.drain_outer()

                    for k in [far + q for q in quarters] + [near + q for q in quarters]:
                        send_p[self.op, self.ss, k] = self.mine(k).astype(BF16)
                        self.in_copy(k).start()

            def relay(self, j):
                @pl.when(inner)
                def _():
                    @pl.when(j >= n_send)
                    def _():
                        self.drain_inner()

                    for q in quarters:
                        k = far + q
                        self.in_copy(k).wait_recv()
                        send_p[self.op, self.ss, k] = (
                            self.mine(k) + recv_o[self.op, self.rs, k].astype(F32)).astype(BF16)
                        self.cross_copy(k, q).start()

            def total(self, q):
                k = near + q
                self.in_copy(k).wait_recv()
                self.cross_copy(k, q).wait_recv()
                return (self.mine(k) + recv_o[self.op, self.rs, k].astype(F32)) + recv_i[self.op, self.rs, q].astype(F32)

            def drain_outer(self):
                for k in range(n_block):
                    self.in_copy(k).wait_send()

            def drain_inner(self):
                for q in quarters:
                    self.cross_copy(far + q, q).wait_send()

            def drain(self):
                @pl.when(outer)
                def _():
                    self.drain_outer()

                @pl.when(inner)
                def _():
                    self.drain_inner()

        def save(kind, src, src_slot, dst, j, u):
            return pltpu.make_async_copy(src.at[src_slot], dst.at[u],
                                         save_sem.at[kind, lax.rem(j, n_send if kind % 2 else n_gath)])

        def sslot(u):
            return lax.rem(u, n_send)

        def gslot(u):
            return lax.rem(u, n_gath)

        def q_rows(q):
            return pl.ds(q * row, row)

        def save_a(u):
            return save(0, a_all, u, a_out, u, u)

        def save_o(u):
            return save(1, ost, sslot(u), o_out, u, u)

        def save_b(u):
            return save(2, bbuf, gslot(u), b_out, u, u)

        def save_z(u):
            return save(3, zst, sslot(u), z_out, u, u)

        def save_d(j, u):
            return save(4, d_all, u, d_out, j, u)

        def save_du(j, u):
            return save(5, dust, sslot(j), du_out, j, u)

        def save_dm(j, u):
            return save(6, dmbuf, gslot(j), dm_out, j, u)

        def save_dqkv(j, u):
            return save(7, dqkvst, sslot(j), dqkv_out, j, u)

        gain_a = gains[0:1, :]
        gain_b = gains[1:2, :]

        def hand_h(u, j):
            s = lax.rem(j, n_hand)
            return rdma(hout.at[s], hslot.at[u], hand_sem.at[s, 3 * n_part], hsem.at[u], stage=st + 1)

        def hand_quarter(back, u, j, q, act):
            s = lax.rem(j, n_hand)
            k = near + q
            src, buf, sems, own = (dout, d_all, d_rs, back_sem) if back else (aout, a_all, a_rs, hand_sem)
            for i, peer in enumerate((inner_peer, outer_peer, z)):
                act(rdma(src.at[s, q_rows(q), :], buf.at[u, rows_of(k), :], own.at[s, 3 * q + i], sems.at[u, k],
                         model=peer, stage=(st - 1) if back else (st + 1)))

        def hand_sent(back, u, j):
            for q in quarters:
                hand_quarter(back, u, j, q, sent)
            if not back:
                hand_h(u, j).wait_send()

        def begin(cp):
            cp.start()

        def sent(cp):
            cp.wait_send()

        def softmax_of(u, p, i):
            first = u - p
            cols = pl.ds(i * head_dim, head_dim)
            q = qkv_all[u, :, cols]
            k = qkv_all[pl.ds(first, per_seq), :, pl.ds(att_w + i * head_dim, head_dim)].reshape(seq_len, head_dim)
            v = qkv_all[pl.ds(first, per_seq), :, pl.ds(2 * att_w + i * head_dim, head_dim)].reshape(seq_len, head_dim)
            sc = dot_nt(q, k) * scale
            q_pos = p * tok + lax.broadcasted_iota(jnp.int32, sc.shape, 0)
            k_pos = lax.broadcasted_iota(jnp.int32, sc.shape, 1)
            sc = jnp.where(k_pos <= q_pos, sc, NEG_BIG)
            e = jnp.exp(sc - jnp.max(sc, axis=-1, keepdims=True))
            pr = e * (1.0 / jnp.sum(e, axis=-1, keepdims=True))
            return q, k, v, pr

        def fold(v):
            return jnp.sum(v.reshape(v.shape[0] // 8, 8, d_model), axis=0)

        def f_enter(j, u):
            @pl.when(is_first)
            def _():
                x_copy(u).wait()
                hslot[u] = a_all[u, my_half, :]
                for k in range(n_block):
                    rs = pl.ds(k * row, row)
                    h32 = a_all[u, rs, :].astype(F32)
                    a_all[u, rs, :] = (h32 * rms_inverse(h32) * gain_a).astype(BF16)

        def f_relay_a(j, u):
            @pl.when(st > 0)
            def _():
                @pl.when(j >= n_gath)
                def _():
                    gather_a(u).drain()

                gather_a(u).relay()

        def f_collect_a(j, u):
            @pl.when(st > 0)
            def _():
                gather_a(u).collect()
                gather_a(u).own()

        def f_attention(j, u):
            @pl.when(j == 0)
            def _():
                for cp in qkv_copies:
                    cp.wait()
                w_copies[0].wait()

            @pl.when(j >= n_gath)
            def _():
                save_a(u).wait()
                save_b(u).wait()
                gather_b(u).drain()
                gather_b(u).drain_own()

            @pl.when(j >= n_send)
            def _():
                save_o(u).wait()

            s = sslot(u)
            p = lax.rem(u, per_seq)
            save_a(u).start()
            qkv_all[u] = dot_nn(a_all[u], wqkv[...]).astype(BF16)
            for i in range(n_head):
                _, _, v, pr = softmax_of(u, p, i)
                ost[s, :, pl.ds(i * head_dim, head_dim)] = dot_nn(pr.astype(BF16), v).astype(BF16)
            save_o(u).start()
            part[0, s] = dot_nn(ost[s], wout[...])
            Scatter(0, u).start(j)

        def scatter_relay(op):
            def run(j, u):
                Scatter(op, j).relay(j)
            return run

        def f_middle(j, u):
            sc = Scatter(0, u)

            @pl.when(inner)
            def _():
                @pl.when(st > 0)
                def _():
                    rdma(hout.at[0], hslot.at[u], hand_sem.at[0, 3 * n_part], hsem.at[u], stage=st).wait_recv()

                for q in quarters:
                    m = hslot[u, q_rows(q), :].astype(F32) + sc.total(q)
                    m_all[u, q_rows(q), :] = m
                    bbuf[gslot(u), rows_of(near + q), :] = (m * rms_inverse(m) * gain_b).astype(BF16)
                    gather_b(u).send(q)

        def f_relay_b(j, u):
            gather_b(u).relay()

        def f_collect_b(j, u):
            gather_b(u).collect()

        def f_mlp(j, u):
            @pl.when(j == 0)
            def _():
                w_copies[1].wait()
                w_copies[2].wait()

            s = sslot(u)
            @pl.when(j >= n_send)
            def _():
                save_z(u).wait()

            save_b(u).start()

            @pl.when(is_last & inner)
            def _():
                y_copy(u).start()

            u_all[u] = dot_nn(bbuf[gslot(u)], wup[...])

            def act(r, carry):
                rr = pl.ds(pl.multiple_of(r * sub_rows, sub_rows), sub_rows)
                v = u_all[u, rr, :]
                th = jnp.tanh(GELU_K * (v + GELU_C * (v * v * v)))
                zst[s, rr, :] = (0.5 * v * (1.0 + th)).astype(BF16)
                return carry

            lax.fori_loop(0, tok // sub_rows, act, 0)
            save_z(u).start()
            part[1, s] = dot_nn(zst[s], wdown[...])
            Scatter(1, u).start(j)

        def f_leave(j, u):
            sc = Scatter(1, u)
            s = lax.rem(j, n_hand)

            @pl.when((j == 0) & (st < last_s))
            def _():
                gain_send().wait_recv()

            @pl.when(inner)
            def _():
                @pl.when(st < last_s)
                def _():
                    @pl.when(j >= n_hand)
                    def _():
                        hand_sent(False, u, j)

                @pl.when(is_last)
                def _():
                    y_copy(u).wait()

                for q in quarters:
                    h_new = (m_all[u, q_rows(q), :] + sc.total(q)).astype(BF16)
                    h32 = h_new.astype(F32)

                    @pl.when(st < last_s)
                    def _():
                        aout[s, q_rows(q), :] = (h32 * rms_inverse(h32) * gain_next[0:1, :]).astype(BF16)
                        hand_quarter(False, u, j, q, begin)
                        hout[s, q_rows(q), :] = h_new

                    @pl.when(is_last)
                    def _():
                        diff = h32 - yslot[lax.rem(u, n_hand), q_rows(q), :].astype(F32)
                        d_all[u, rows_of(near + q), :] = (diff * inv_count).astype(BF16)
                        lossacc[...] += fold(diff * diff)

                @pl.when(st < last_s)
                def _():
                    hand_h(u, j).start()

        forward = (f_enter, f_relay_a, f_collect_a, f_attention, scatter_relay(0), f_middle, f_relay_b, f_collect_b, f_mlp,
                   scatter_relay(1), f_leave)

        def b_enter(j, u):
            @pl.when(is_last & inner)
            def _():
                @pl.when(j >= n_gath)
                def _():
                    gather_d(j, u).drain_own()

                for q in quarters:
                    gather_d(j, u).send(q)

        def b_relay_d(j, u):
            @pl.when(j >= n_gath)
            def _():
                gather_d(j, u).drain()

            gather_d(j, u).relay()

        def b_collect_d(j, u):
            gather_d(j, u).collect()

            @pl.when(st < last_s)
            def _():
                gather_d(j, u).own()

        def b_mlp(j, u):
            @pl.when(j >= n_gath)
            def _():
                save_d(j, u).wait()
                save_dm(j, u).wait()
                gather_dm(j).drain()
                gather_dm(j).drain_own()

            @pl.when(j >= n_send)
            def _():
                save_du(j, u).wait()

            s = sslot(j)
            save_d(j, u).start()
            part[2, s] = dot_nt(d_all[u], wdown[...])

            def act(r, carry):
                rr = pl.ds(pl.multiple_of(r * sub_rows, sub_rows), sub_rows)
                v = u_all[u, rr, :]
                v2 = v * v
                th = jnp.tanh(GELU_K * (v + GELU_C * (v2 * v)))
                slope = 0.5 * (1.0 + th) + 0.5 * v * (1.0 - th * th) * (GELU_K * (1.0 + 3.0 * GELU_C * v2))
                dust[s, rr, :] = (part[2, s, rr, :] * slope).astype(BF16)
                return carry

            lax.fori_loop(0, tok // sub_rows, act, 0)
            save_du(j, u).start()
            part[2, s] = dot_nt(dust[s], wup[...])
            Scatter(2, j).start(j)

        def b_middle(j, u):
            sc = Scatter(2, j)

            @pl.when(inner)
            def _():
                for q in quarters:
                    m = m_all[u, q_rows(q), :]
                    inv = rms_inverse(m)
                    normed = m * inv
                    dn = sc.total(q)
                    gb8[...] += fold(dn * normed)
                    dn = dn * gain_b
                    dm = d_all[u, rows_of(near + q), :].astype(F32) + inv * (
                        dn - normed * jnp.mean(dn * normed, axis=-1, keepdims=True))
                    m_all[u, q_rows(q), :] = dm
                    dmbuf[gslot(j), rows_of(near + q), :] = dm.astype(BF16)
                    gather_dm(j).send(q)

        def b_relay_dm(j, u):
            gather_dm(j).relay()

        def b_collect_dm(j, u):
            gather_dm(j).collect()

        def b_attention(j, u):
            s = sslot(j)
            p = lax.rem(u, per_seq)
            @pl.when(j >= n_send)
            def _():
                save_dqkv(j, u).wait()

            save_dm(j, u).start()

            @pl.when(is_first)
            def _():
                x_again(j, u).start()

            @pl.when(p == per_seq - 1)
            def _():
                dkacc[...] = jnp.zeros_like(dkacc)
                dvacc[...] = jnp.zeros_like(dvacc)

            datt[...] = dot_nt(dmbuf[gslot(j)], wout[...]).astype(BF16)
            p_rows = pl.ds(pl.multiple_of(p * tok, tok), tok)
            for h in range(n_head):
                cols = pl.ds(h * head_dim, head_dim)
                q, k, v, pr = softmax_of(u, p, h)
                da = datt[:, cols]
                dp = dot_nt(da, v)
                ds = (pr * (dp - jnp.sum(pr * dp, axis=-1, keepdims=True)) * scale).astype(BF16)
                dvacc[:, cols] += dot_tn(pr.astype(BF16), da)
                dkacc[:, cols] += dot_tn(ds, q)
                dqkvst[s, :, cols] = dot_nn(ds, k).astype(BF16)
            dqkvst[s, :, pl.ds(att_w, att_w)] = dkacc[p_rows, :].astype(BF16)
            dqkvst[s, :, pl.ds(2 * att_w, att_w)] = dvacc[p_rows, :].astype(BF16)
            save_dqkv(j, u).start()
            part[3, s] = dot_nt(dqkvst[s], wqkv[...])

            @pl.when(st > 0)
            def _():
                Scatter(3, j).start(j)

        def b_relay_h(j, u):
            @pl.when(st > 0)
            def _():
                Scatter(3, j).relay(j)

        def b_leave(j, u):
            s = lax.rem(j, n_hand)

            @pl.when(st > 0)
            def _():
                sc = Scatter(3, j)

                @pl.when(inner)
                def _():
                    @pl.when(j >= n_hand)
                    def _():
                        hand_sent(True, u, j)

                    for q in quarters:
                        h32 = hslot[u, q_rows(q), :].astype(F32)
                        inv = rms_inverse(h32)
                        normed = h32 * inv
                        dn = sc.total(q)
                        ga8[...] += fold(dn * normed)
                        dg = dn * gain_a
                        dout[s, q_rows(q), :] = (m_all[u, q_rows(q), :] + inv * (
                            dg - normed * jnp.mean(dg * normed, axis=-1, keepdims=True))).astype(BF16)
                        hand_quarter(True, u, j, q, begin)

            @pl.when(is_first)
            def _():
                x_again(j, u).wait()
                for k in range(n_block):
                    rs = pl.ds(k * row, row)
                    h32 = xtmp[sslot(j), rs, :].astype(F32)
                    ga8[...] += fold(part[3, sslot(j), rs, :] * (h32 * rms_inverse(h32)))

        backward = (b_enter, b_relay_d, b_collect_d, b_mlp, scatter_relay(2), b_middle, b_relay_dm, b_collect_dm,
                    b_attention, b_relay_h, b_leave)
        f_lag, b_lag = lags(False), lags(True)
        back_from = BACK_START + BACK_STEP * (last_s - st)

        def hand_finish(back):
            @pl.when(inner)
            def _():
                for j in range(n_unit - n_hand, n_unit):
                    hand_sent(back, j, j)

        def finish_forward():
            for j in range(n_unit - n_gath, n_unit):
                save_a(j).wait()
                save_b(j).wait()
                gather_b(j).drain()
                gather_b(j).drain_own()

                @pl.when(st > 0)
                def _():
                    gather_a(j).drain()

            for j in range(n_unit - n_send, n_unit):
                save_o(j).wait()
                save_z(j).wait()
                Scatter(0, j).drain()
                Scatter(1, j).drain()

            @pl.when(st < last_s)
            def _():
                hand_finish(False)

        def finish_backward():
            for j in range(n_unit - n_gath, n_unit):
                save_d(j, j).wait()
                save_dm(j, j).wait()
                gather_dm(j).drain()
                gather_dm(j).drain_own()
                gather_d(j, j).drain()

                @pl.when(is_last)
                def _():
                    gather_d(j, j).drain_own()

            for j in range(n_unit - n_send, n_unit):
                save_du(j, j).wait()
                save_dqkv(j, j).wait()
                Scatter(2, j).drain()

                @pl.when(st > 0)
                def _():
                    Scatter(3, j).drain()

            @pl.when(st > 0)
            def _():
                hand_finish(True)
                gain_send().wait_send()

        def turn(i, carry):
            @pl.when(i == n_unit + f_lag[-1])
            def _():
                finish_forward()

            for back, phase in ORDER:
                j = (i - back_from - b_lag[phase]) if back else (i - f_lag[phase])

                @pl.when((j >= 0) & (j < n_unit))
                def _():
                    if back:
                        seq = lax.div(j, per_seq)
                        backward[phase](j, 2 * seq * per_seq + (per_seq - 1) - j)
                    else:
                        forward[phase](j, j)
            return carry

        lax.fori_loop(0, n_unit + back_from + b_lag[-1], turn, 0)

        def loss_send():
            return rdma(lossacc, lossacc, loss_sem.at[0], loss_sem.at[1], stage=st - 1)

        @pl.when(is_last)
        def _():
            loss_send().start()

        @pl.when(st < last_s)
        def _():
            loss_send().wait_recv()

            @pl.when(st > 0)
            def _():
                loss_send().start()

        loss_row = jnp.sum(jnp.sum(lossacc[...], axis=0, keepdims=True), axis=1, keepdims=True)
        gx[z, 0:1, :] = jnp.sum(ga8[...], axis=0, keepdims=True)
        gx[z, 1:2, :] = jnp.sum(gb8[...], axis=0, keepdims=True)
        gx[z, 2:8, :] = jnp.broadcast_to(loss_row, (6, d_model))

        def gx_send(dz):
            return rdma(gx.at[z], gx.at[z], gx_s.at[dz], gx_r.at[z], model=lax.rem(z + dz, nz))

        def gx_recv(dz):
            k = lax.rem(z + dz, nz)
            return rdma(gx.at[k], gx.at[k], gx_s.at[dz], gx_r.at[k], model=k)

        for dz in range(1, nz):
            gx_send(dz).start()
        finish_backward()

        @pl.when(st > 0)
        def _():
            loss_send().wait_send()

        for dz in range(1, nz):
            gx_recv(dz).wait_recv()
        red_out[...] = gx[0] + gx[1] + gx[2] + gx[3]
        for dz in range(1, nz):
            gx_send(dz).wait_send()

    any_spec = pl.BlockSpec(memory_space=pl.ANY)
    vmem_spec = pl.BlockSpec(memory_space=pltpu.VMEM)

    def out(width):
        return jax.ShapeDtypeStruct((n_unit, tok, width), BF16)

    dma = pltpu.SemaphoreType.DMA
    vmem = pltpu.VMEM
    return pl.pallas_call(
        kernel,
        out_shape=(out(d_model), out(d_model), out(d_model), out(d_model), out(qkv_w), out(att_w), out(ff_w), out(ff_w),
                   jax.ShapeDtypeStruct((8, d_model), F32)),
        in_specs=[any_spec] * 6 + [vmem_spec],
        out_specs=(any_spec,) * 8 + (vmem_spec,),
        scratch_shapes=[
            vmem((d_model, qkv_w), BF16), vmem((att_w, d_model), BF16), vmem((d_model, ff_w), BF16), vmem((ff_w, d_model), BF16),
            vmem((n_unit, half, d_model), BF16), vmem((n_hand, half, d_model), BF16),
            vmem((n_unit, tok, d_model), BF16), vmem((n_unit, tok, d_model), BF16),
            vmem((n_gath, tok, d_model), BF16), vmem((n_gath, tok, d_model), BF16), vmem((n_send, tok, d_model), BF16),
            vmem((n_unit, tok, qkv_w), BF16), vmem((n_unit, tok, ff_w), F32), vmem((n_unit, half, d_model), F32),
            vmem((n_send, tok, att_w), BF16), vmem((n_send, tok, ff_w), BF16), vmem((n_send, tok, ff_w), BF16),
            vmem((n_send, tok, qkv_w), BF16), vmem((tok, att_w), BF16), vmem((4, n_send, tok, d_model), F32),
            vmem((4, n_recv, n_block, row, d_model), BF16), vmem((4, n_recv, n_part, row, d_model), BF16),
            vmem((4, n_send, n_block, row, d_model), BF16),
            vmem((n_hand, half, d_model), BF16), vmem((n_hand, half, d_model), BF16), vmem((n_hand, half, d_model), BF16),
            vmem((seq_len, att_w), F32), vmem((seq_len, att_w), F32),
            vmem((2, d_model), F32), vmem((2, d_model), F32),
            vmem((8, d_model), F32), vmem((8, d_model), F32), vmem((8, d_model), F32), vmem((nz, 8, d_model), F32),
            dma((n_slab + 3,)), dma((n_unit,)), dma((n_hand,)), dma((n_send,)), dma((2,)), dma((n_hand, 3 * n_part + 1)), dma((n_hand, 3 * n_part)), dma((8, n_gath)),
            dma((n_unit, n_block)), dma((n_unit, n_block)), dma((n_gath, n_part)), dma((n_gath, n_block)),
            dma((n_gath, n_part)), dma((n_gath, n_block)), dma((n_gath, n_block)), dma((n_gath, n_block)),
            dma((n_gath, n_part)), dma((n_gath, n_block)), dma((n_gath, n_part)), dma((n_gath, n_block)),
            dma((4, n_recv, n_block)), dma((4, n_recv, n_part)), dma((4, n_send, n_block)),
            dma((2,)), dma((nz,)), dma((nz,)),
        ],
        compiler_params=pltpu.CompilerParams(collective_id=0, has_side_effects=True, vmem_limit_bytes=67_043_328),
        name="layer_step",
    )(x_in, y_target, w_qkv, w_out, w_up, w_down, gain)


def weight_grads(o, dm, a, dqkv, b, du, zz, d, red, head_dim, loss_scale):
    n_tok = o.shape[0] * o.shape[1]
    rows = 256

    def flat(v):
        return v.reshape(n_tok, v.shape[2])

    acts = [flat(v) for v in (o, dm, a, dqkv, b, du, zz, d)]
    att_w, d_model = acts[0].shape[1], acts[1].shape[1]
    qkv_w, ff_w = acts[3].shape[1], acts[5].shape[1]
    n_slab = qkv_w // head_dim

    def kernel(*refs):
        src, red_ref, outs = refs[:8], refs[8], refs[9:13]
        gain_out, loss_out = refs[13:15]
        held, tiles = refs[15:23], refs[23:27]
        in_sem, out_sem = refs[27:]
        loads = [pltpu.make_async_copy(src[i], held[i], in_sem.at[i]) for i in range(8)]
        for cp in loads:
            cp.start()

        def stores(pair, i, slot):
            n = tiles[pair].shape[1]
            at = pl.ds(pl.multiple_of(i * n, n), n)
            sem = out_sem.at[pair, slot]
            if pair == 1:
                return [pltpu.make_async_copy(tiles[1].at[slot, :, pl.ds(k * head_dim, head_dim)], outs[1].at[k, at, :], sem)
                        for k in range(n_slab)]
            return [pltpu.make_async_copy(tiles[pair].at[slot], outs[pair].at[at, :], sem)]

        def finish(cps):
            for cp in cps:
                cp.wait()

        gain_out[...] = red_ref[0:2, :]
        loss_out[...] = red_ref[2:3, 0:1] * loss_scale
        counts = []
        for pair in range(4):
            loads[2 * pair].wait()
            loads[2 * pair + 1].wait()
            left, right, tile = held[2 * pair], held[2 * pair + 1], tiles[pair]
            n = tile.shape[1]
            count = left.shape[1] // n
            counts.append(count)

            def body(i, carry):
                slot = lax.rem(i, 2)

                @pl.when(i >= 2)
                def _():
                    finish(stores(pair, i - 2, slot))

                tile[slot] = dot_tn(left[:, pl.ds(pl.multiple_of(i * n, n), n)], right[...])
                for cp in stores(pair, i, slot):
                    cp.start()
                return carry

            lax.fori_loop(0, count, body, 0)
        for pair in range(4):
            for i in range(max(0, counts[pair] - 2), counts[pair]):
                finish(stores(pair, i, i % 2))

    any_spec = pl.BlockSpec(memory_space=pl.ANY)
    vmem_spec = pl.BlockSpec(memory_space=pltpu.VMEM)
    return pl.pallas_call(
        kernel,
        out_shape=(jax.ShapeDtypeStruct((att_w, d_model), F32), jax.ShapeDtypeStruct((n_slab, d_model, head_dim), F32),
                   jax.ShapeDtypeStruct((d_model, ff_w), F32), jax.ShapeDtypeStruct((ff_w, d_model), F32),
                   jax.ShapeDtypeStruct((2, d_model), F32), jax.ShapeDtypeStruct((1, 1), F32)),
        in_specs=[any_spec] * 8 + [vmem_spec],
        out_specs=(any_spec,) * 4 + (vmem_spec,) * 2,
        scratch_shapes=[pltpu.VMEM(v.shape, BF16) for v in acts] + [
            pltpu.VMEM((1, att_w, d_model), F32), pltpu.VMEM((2, rows, qkv_w), F32),
            pltpu.VMEM((2, rows, ff_w), F32), pltpu.VMEM((2, rows, d_model), F32),
            pltpu.SemaphoreType.DMA((8,)), pltpu.SemaphoreType.DMA((4, 2))],
        compiler_params=pltpu.CompilerParams(vmem_limit_bytes=67_043_328),
        name="weight_grads",
    )(*acts, red)


def solution(mesh):
    dims = dict(mesh.shape)

    def device_fn(x_in, y_target, w_qkv, w_out, w_up, w_down, norm_gain):
        n_batch, seq_len, d_model = x_in.shape
        heads, head_dim = w_qkv.shape[3], w_qkv.shape[4]
        a, b, d, dm, dqkv, o, zz, du, red = layer_step(
            dims, x_in, y_target,
            w_qkv[0].transpose(1, 2, 0, 3).reshape(3 * heads, d_model, head_dim),
            w_out[0].reshape(heads * head_dim, d_model), w_up[0], w_down[0], norm_gain[0])
        g_out, g_qkv, g_up, g_down, g_gain, loss = weight_grads(
            o, dm, a, dqkv, b, du, zz, d, red, head_dim, 0.5 / (n_batch * seq_len * d_model))
        grad_qkv = g_qkv.reshape(3, heads, d_model, head_dim).transpose(2, 0, 1, 3)[None]
        grad_out = g_out.reshape(1, heads, head_dim, d_model)
        grad_up = g_up[None]
        grad_down = g_down[None]
        return loss.reshape(1), grad_qkv, grad_out, grad_up, grad_down, g_gain[None]

    act_spec = P("data", None, None)
    weight_specs = (
        P("stage", None, None, "model", None),
        P("stage", "model", None, None),
        P("stage", None, "model"),
        P("stage", "model", None),
        P("stage", None, None),
    )
    grad_specs = (
        P(("data", "stage"), None, None, "model", None),
        P(("data", "stage"), "model", None, None),
        P(("data", "stage"), None, "model"),
        P(("data", "stage"), "model", None),
        P(("data", "stage"), None, None),
    )
    return jax.shard_map(
        device_fn,
        mesh=mesh,
        in_specs=(act_spec, act_spec) + weight_specs,
        out_specs=(P("data"),) + grad_specs,
        check_vma=False,
    )
```

```python
import jax
import jax.numpy as jnp
from jax import lax
from jax.experimental import pallas as pl
from jax.experimental.pallas import tpu as pltpu
from jax.sharding import PartitionSpec as P

NORM_EPS = 1e-6
NEG_BIG = -1e30
MESH = pl.DeviceIdType.MESH
GELU_K = 0.7978845608028654
GELU_C = 0.044715
F32 = jnp.float32
BF16 = jnp.bfloat16


def dot_nn(a, b):
    return lax.dot_general(a, b, (((1,), (0,)), ((), ())), preferred_element_type=F32)


def dot_nt(a, b):
    return lax.dot_general(a, b, (((1,), (1,)), ((), ())), preferred_element_type=F32)


def dot_tn(a, b):
    return lax.dot_general(a, b, (((0,), (0,)), ((), ())), preferred_element_type=F32)


def rms_inverse(v32):
    return lax.rsqrt(jnp.mean(v32 * v32, axis=-1, keepdims=True) + NORM_EPS)


ORDER = (
    (1, 6), (1, 3), (0, 4), (0, 0), (1, 9), (0, 1), (1, 1), (0, 12), (1, 7), (0, 6), (1, 5), (0, 10), (1, 0), (0,
    9), (1, 8), (0, 5), (0, 2), (1, 4), (0, 11), (1, 10), (1, 2), (0, 3), (0, 7), (0, 8),
)
BACK_START, BACK_STEP = 11, 12


def lags(back):
    place = {phase: i for i, (is_back, phase) in enumerate(ORDER) if is_back == int(back)}
    lag = [0]
    for phase in range(1, len(place)):
        lag.append(lag[-1] + (1 if place[phase] < place[phase - 1] else 0))
    return lag


def layer_step(dims, x_in, y_target, w_qkv, w_out, w_up, w_down, gain):
    nz, ns = dims["model"], dims["stage"]
    n_seq, seq_len, d_model = x_in.shape
    n_slab, _, head_dim = w_qkv.shape
    qkv_w = n_slab * head_dim
    att_w = w_out.shape[0]
    ff_w = w_up.shape[1]
    n_head = att_w // head_dim
    tok = 64
    n_part = 2
    row = tok // (2 * n_part)
    n_block = 2 * n_part
    per_seq = seq_len // tok
    n_unit = n_seq * per_seq
    key_step = per_seq // 4
    scale = head_dim ** -0.5
    inv_count = 1.0 / (n_seq * seq_len * d_model)
    last_z, last_s = nz - 1, ns - 1
    sub_rows = 16
    half = tok // 2
    n_send, n_recv, n_gath, n_hand = 2, 3, 4, 2
    quarters = range(n_part)

    def kernel(x_ref, y_ref, wqkv_h, wout_h, wup_h, wdown_h, gain_ref,
               a_out, b_out, d_out, dm_out, dqkv_out, o_out, z_out, du_out, red_out,
               wqkv, wout, wup, wdown, hslot, yslot, a_all, d_all, nbuf, bbuf, dmbuf, xtmp,
               qkv_all, u_all, m_all, ost, zst, dust, dqkvst, datt, part,
               recv_o, recv_i, send_p, hout, aout, dout, dkacc, dvacc,
               gains, gain_next, lossacc, ga8, gb8, gx,
               w_sem, hsem, ysem, x_sem, gain_sem, hand_sem, back_sem, save_sem,
               a_rs, d_rs, a_si, a_so, d_si, d_so, n_rs, n_si, n_so, n_fw, b_rs, dm_rs, b_si, b_so, dm_si, dm_so,
               rs_ro, rs_ri, rs_s, loss_sem, gx_s, gx_r):
        z = lax.axis_index("model")
        st = lax.axis_index("stage")
        is_first = st == 0
        is_last = st == last_s
        crosses = st == ns // 2 - 1
        crossed = st == ns // 2
        inner = (z > 0) & (z < last_z)
        outer = (z == 0) | (z == last_z)
        side = lax.div(z, 2)
        near = n_part * side
        far = n_part - near
        inner_peer = 1 + lax.rem(z, 2)
        outer_peer = last_z * side
        my_half = pl.ds(pl.multiple_of(side * half, half), half)

        def rdma(src, dst, ssem, rsem, **dev):
            return pltpu.make_async_remote_copy(src_ref=src, dst_ref=dst, send_sem=ssem, recv_sem=rsem,
                                                device_id=dev, device_id_type=MESH)

        def rows_of(k):
            return pl.ds(pl.multiple_of(k * row, row), row)

        qkv_copies = [pltpu.make_async_copy(wqkv_h.at[i], wqkv.at[:, pl.ds(i * head_dim, head_dim)], w_sem.at[i])
                      for i in range(n_slab)]
        w_copies = [pltpu.make_async_copy(src, dst, w_sem.at[n_slab + i])
                    for i, (src, dst) in enumerate(((wout_h, wout), (wup_h, wup), (wdown_h, wdown)))]

        def tokens_of(u):
            return lax.div(u, per_seq), pl.multiple_of(lax.rem(u, per_seq) * tok, tok)

        def x_copy(u):
            q, first = tokens_of(u)
            return pltpu.make_async_copy(x_ref.at[q, pl.ds(first, tok), :], a_all.at[u], hsem.at[u])

        def x_again(j, u):
            q, first = tokens_of(u)
            slot = lax.rem(j, n_send)
            return pltpu.make_async_copy(x_ref.at[q, pl.ds(first, tok), :], xtmp.at[slot], x_sem.at[slot])

        def y_copy(u):
            q, first = tokens_of(u)
            rs = pl.ds(pl.multiple_of(first + side * half, half), half)
            slot = lax.rem(u, n_hand)
            return pltpu.make_async_copy(y_ref.at[q, rs, :], yslot.at[slot], ysem.at[slot])

        @pl.when(is_first)
        def _():
            for u in range(n_send):
                x_copy(u).start()

        for cp in qkv_copies + w_copies:
            cp.start()

        @pl.when(is_first)
        def _():
            @pl.loop(n_send, n_unit)
            def _(u):
                x_copy(u).start()

        barrier = pltpu.get_barrier_semaphore()
        for i in range(1, nz * ns):
            dz, dst = i % nz, i // nz
            pl.semaphore_signal(barrier, inc=1, device_id_type=MESH,
                                device_id={"model": lax.rem(z + dz, nz), "stage": lax.rem(st + dst, ns)})
        qkv_all[...] = jnp.zeros_like(qkv_all)
        lossacc[...] = jnp.zeros_like(lossacc)
        ga8[...] = jnp.zeros_like(ga8)
        gb8[...] = jnp.zeros_like(gb8)
        gains[...] = gain_ref[...].astype(F32)
        pl.semaphore_wait(barrier, nz * ns - 1)

        def gain_send():
            return rdma(gains, gain_next, gain_sem.at[0], gain_sem.at[1], stage=st - 1)

        @pl.when(st > 0)
        def _():
            gain_send().start()

        class Gather:
            def __init__(self, buf, slot, rsem, si, so, sslot):
                self.buf, self.slot, self.rsem, self.si, self.so, self.sslot = buf, slot, rsem, si, so, sslot

            def block(self, k):
                return self.buf.at[self.slot, rows_of(k), :]

            def inward(self, k, q):
                return rdma(self.block(k), self.block(k), self.si.at[self.sslot, q], self.rsem.at[self.slot, k],
                            model=inner_peer)

            def outward(self, k):
                return rdma(self.block(k), self.block(k), self.so.at[self.sslot, k], self.rsem.at[self.slot, k],
                            model=outer_peer)

            def send(self, q):
                self.inward(near + q, q).start()
                self.outward(near + q).start()

            def relay(self):
                @pl.when(inner)
                def _():
                    for q in quarters:
                        self.outward(far + q).wait_recv()
                        self.outward(far + q).start()

            def collect(self):
                @pl.when(outer)
                def _():
                    for k in range(n_block):
                        self.outward(k).wait_recv()

            def own(self):
                @pl.when(inner)
                def _():
                    for q in quarters:
                        self.outward(near + q).wait_recv()

            def drain(self):
                @pl.when(inner)
                def _():
                    for q in quarters:
                        self.outward(far + q).wait_send()

            def drain_own(self):
                @pl.when(inner)
                def _():
                    for q in quarters:
                        self.inward(near + q, q).wait_send()
                        self.outward(near + q).wait_send()

        def gather_a(u):
            return Gather(a_all, u, a_rs, a_si, a_so, lax.rem(u, n_gath))

        def gather_d(j, u):
            return Gather(d_all, u, d_rs, d_si, d_so, lax.rem(j, n_gath))

        def gather_n(u):
            return Gather(nbuf, lax.rem(u, n_gath), n_rs, n_si, n_so, lax.rem(u, n_gath))

        def forward_n(u, k):
            g = lax.rem(u, n_gath)
            return rdma(nbuf.at[g, rows_of(k), :], a_all.at[u, rows_of(k), :], n_fw.at[g, k], a_rs.at[u, k], stage=st + 1)

        def gather_b(u):
            return Gather(bbuf, lax.rem(u, n_gath), b_rs, b_si, b_so, lax.rem(u, n_gath))

        def gather_dm(j):
            return Gather(dmbuf, lax.rem(j, n_gath), dm_rs, dm_si, dm_so, lax.rem(j, n_gath))

        class Scatter:
            def __init__(self, op, u):
                self.op, self.ss, self.rs = op, lax.rem(u, n_send), lax.rem(u, n_recv)

            def in_copy(self, k):
                return rdma(send_p.at[self.op, self.ss, k], recv_o.at[self.op, self.rs, k],
                            rs_s.at[self.op, self.ss, k], rs_ro.at[self.op, self.rs, k], model=inner_peer)

            def cross_copy(self, k, q):
                return rdma(send_p.at[self.op, self.ss, k], recv_i.at[self.op, self.rs, q],
                            rs_s.at[self.op, self.ss, k], rs_ri.at[self.op, self.rs, q], model=inner_peer)

            def mine(self, k):
                return part[self.op, self.ss, rows_of(k), :]

            def start(self, j):
                @pl.when(outer)
                def _():
                    @pl.when(j >= n_send)
                    def _():
                        self.drain_outer()

                    for k in [far + q for q in quarters] + [near + q for q in quarters]:
                        send_p[self.op, self.ss, k] = self.mine(k).astype(BF16)
                        self.in_copy(k).start()

            def relay(self, j):
                @pl.when(inner)
                def _():
                    @pl.when(j >= n_send)
                    def _():
                        self.drain_inner()

                    for q in quarters:
                        k = far + q
                        self.in_copy(k).wait_recv()
                        send_p[self.op, self.ss, k] = (
                            self.mine(k) + recv_o[self.op, self.rs, k].astype(F32)).astype(BF16)
                        self.cross_copy(k, q).start()

            def total(self, q):
                k = near + q
                self.in_copy(k).wait_recv()
                self.cross_copy(k, q).wait_recv()
                return (self.mine(k) + recv_o[self.op, self.rs, k].astype(F32)) + recv_i[self.op, self.rs, q].astype(F32)

            def drain_outer(self):
                for k in range(n_block):
                    self.in_copy(k).wait_send()

            def drain_inner(self):
                for q in quarters:
                    self.cross_copy(far + q, q).wait_send()

            def drain(self):
                @pl.when(outer)
                def _():
                    self.drain_outer()

                @pl.when(inner)
                def _():
                    self.drain_inner()

        def save(kind, src, src_slot, dst, j, u):
            return pltpu.make_async_copy(src.at[src_slot], dst.at[u],
                                         save_sem.at[kind, lax.rem(j, n_send if kind % 2 else n_gath)])

        def sslot(u):
            return lax.rem(u, n_send)

        def gslot(u):
            return lax.rem(u, n_gath)

        def q_rows(q):
            return pl.ds(q * row, row)

        def save_a(u):
            return save(0, a_all, u, a_out, u, u)

        def save_o(u):
            return save(1, ost, sslot(u), o_out, u, u)

        def save_b(u):
            return save(2, bbuf, gslot(u), b_out, u, u)

        def save_z(u):
            return save(3, zst, sslot(u), z_out, u, u)

        def save_d(j, u):
            return save(4, d_all, u, d_out, j, u)

        def save_du(j, u):
            return save(5, dust, sslot(j), du_out, j, u)

        def save_dm(j, u):
            return save(6, dmbuf, gslot(j), dm_out, j, u)

        def save_dqkv(j, u):
            return save(7, dqkvst, sslot(j), dqkv_out, j, u)

        gain_a = gains[0:1, :]
        gain_b = gains[1:2, :]

        def hand_h(u, j):
            s = lax.rem(j, n_hand)
            return rdma(hout.at[s], hslot.at[u], hand_sem.at[s, 3 * n_part], hsem.at[u], stage=st + 1)

        def hand_quarter(back, u, j, q, act):
            s = lax.rem(j, n_hand)
            k = near + q
            src, buf, sems, own = (dout, d_all, d_rs, back_sem) if back else (aout, a_all, a_rs, hand_sem)
            for i, peer in enumerate((inner_peer, outer_peer, z)):
                act(rdma(src.at[s, q_rows(q), :], buf.at[u, rows_of(k), :], own.at[s, 3 * q + i], sems.at[u, k],
                         model=peer, stage=(st - 1) if back else (st + 1)))

        def hand_sent(u, j):
            @pl.when(st != ns // 2 - 1)
            def _():
                for q in quarters:
                    hand_quarter(False, u, j, q, sent)

            hand_h(u, j).wait_send()

        def begin(cp):
            cp.start()

        def sent(cp):
            cp.wait_send()

        def softmax_of(u, p, i, n_tile):
            first = u - p
            n_key = n_tile * tok
            cols = pl.ds(i * head_dim, head_dim)
            q = qkv_all[u, :, cols]
            k = qkv_all[pl.ds(first, n_tile), :, pl.ds(att_w + i * head_dim, head_dim)].reshape(n_key, head_dim)
            v = qkv_all[pl.ds(first, n_tile), :, pl.ds(2 * att_w + i * head_dim, head_dim)].reshape(n_key, head_dim)
            sc = dot_nt(q, k) * scale
            q_pos = p * tok + lax.broadcasted_iota(jnp.int32, sc.shape, 0)
            k_pos = lax.broadcasted_iota(jnp.int32, sc.shape, 1)
            sc = jnp.where(k_pos <= q_pos, sc, NEG_BIG)
            e = jnp.exp(sc - jnp.max(sc, axis=-1, keepdims=True))
            pr = e * (1.0 / jnp.sum(e, axis=-1, keepdims=True))
            return q, k, v, pr

        def by_reach(p, body):
            for n_tile in range(key_step, per_seq + 1, key_step):
                @pl.when((p >= n_tile - key_step) & (p < n_tile))
                def _():
                    body(n_tile)

        def fold(v):
            return jnp.sum(v.reshape(v.shape[0] // 8, 8, d_model), axis=0)

        def f_enter(j, u):
            @pl.when(is_first)
            def _():
                x_copy(u).wait()
                hslot[u] = a_all[u, my_half, :]
                for k in range(n_block):
                    rs = pl.ds(k * row, row)
                    h32 = a_all[u, rs, :].astype(F32)
                    a_all[u, rs, :] = (h32 * rms_inverse(h32) * gain_a).astype(BF16)

        def f_relay_a(j, u):
            @pl.when((st > 0) & (st != ns // 2))
            def _():
                @pl.when(j >= n_gath)
                def _():
                    gather_a(u).drain()

                gather_a(u).relay()

        def f_collect_a(j, u):
            @pl.when((st > 0) & (st != ns // 2))
            def _():
                gather_a(u).collect()
                gather_a(u).own()

            @pl.when(crossed)
            def _():
                for k in range(n_block):
                    forward_n(u, k).wait_recv()

        def f_attention(j, u):
            @pl.when(j == 0)
            def _():
                for cp in qkv_copies:
                    cp.wait()
                w_copies[0].wait()

            @pl.when(j >= n_gath)
            def _():
                save_a(u).wait()
                save_b(u).wait()
                gather_b(u).drain()
                gather_b(u).drain_own()

            @pl.when(j >= n_send)
            def _():
                save_o(u).wait()

            s = sslot(u)
            p = lax.rem(u, per_seq)
            save_a(u).start()
            qkv_all[u] = dot_nn(a_all[u], wqkv[...]).astype(BF16)
            def attend(n_tile):
                for i in range(n_head):
                    _, _, v, pr = softmax_of(u, p, i, n_tile)
                    ost[s, :, pl.ds(i * head_dim, head_dim)] = dot_nn(pr.astype(BF16), v).astype(BF16)

            by_reach(p, attend)
            save_o(u).start()
            part[0, s] = dot_nn(ost[s], wout[...])
            Scatter(0, u).start(j)

        def scatter_relay(op):
            def run(j, u):
                Scatter(op, j).relay(j)
            return run

        def f_middle(j, u):
            sc = Scatter(0, u)

            @pl.when(inner)
            def _():
                @pl.when(st > 0)
                def _():
                    rdma(hout.at[0], hslot.at[u], hand_sem.at[0, 3 * n_part], hsem.at[u], stage=st).wait_recv()

                for q in quarters:
                    m = hslot[u, q_rows(q), :].astype(F32) + sc.total(q)
                    m_all[u, q_rows(q), :] = m
                    bbuf[gslot(u), rows_of(near + q), :] = (m * rms_inverse(m) * gain_b).astype(BF16)
                    gather_b(u).send(q)

        def f_relay_b(j, u):
            gather_b(u).relay()

        def f_collect_b(j, u):
            gather_b(u).collect()

        def f_mlp(j, u):
            @pl.when(j == 0)
            def _():
                w_copies[1].wait()
                w_copies[2].wait()

            s = sslot(u)
            @pl.when(j >= n_send)
            def _():
                save_z(u).wait()

            @pl.when(crosses & (j >= n_gath))
            def _():
                drain_n(u)

            save_b(u).start()

            @pl.when(is_last & inner)
            def _():
                y_copy(u).start()

            u_all[u] = dot_nn(bbuf[gslot(u)], wup[...])

            def act(r, carry):
                rr = pl.ds(pl.multiple_of(r * sub_rows, sub_rows), sub_rows)
                v = u_all[u, rr, :]
                th = jnp.tanh(GELU_K * (v + GELU_C * (v * v * v)))
                zst[s, rr, :] = (0.5 * v * (1.0 + th)).astype(BF16)
                return carry

            lax.fori_loop(0, tok // sub_rows, act, 0)
            save_z(u).start()
            part[1, s] = dot_nn(zst[s], wdown[...])
            Scatter(1, u).start(j)

        def f_leave(j, u):
            sc = Scatter(1, u)
            s = lax.rem(j, n_hand)

            @pl.when((j == 0) & (st < last_s))
            def _():
                gain_send().wait_recv()

            @pl.when(inner)
            def _():
                @pl.when(st < last_s)
                def _():
                    @pl.when(j >= n_hand)
                    def _():
                        hand_sent(u, j)

                @pl.when(is_last)
                def _():
                    y_copy(u).wait()

                for q in quarters:
                    h_new = (m_all[u, q_rows(q), :] + sc.total(q)).astype(BF16)
                    h32 = h_new.astype(F32)

                    @pl.when(st < last_s)
                    def _():
                        a_new = (h32 * rms_inverse(h32) * gain_next[0:1, :]).astype(BF16)

                        @pl.when(crosses)
                        def _():
                            nbuf[gslot(u), rows_of(near + q), :] = a_new
                            gather_n(u).send(q)
                            forward_n(u, near + q).start()

                        @pl.when(st != ns // 2 - 1)
                        def _():
                            aout[s, q_rows(q), :] = a_new
                            hand_quarter(False, u, j, q, begin)

                        hout[s, q_rows(q), :] = h_new

                    @pl.when(is_last)
                    def _():
                        diff = h32 - yslot[lax.rem(u, n_hand), q_rows(q), :].astype(F32)
                        d_all[u, rows_of(near + q), :] = (diff * inv_count).astype(BF16)
                        lossacc[...] += fold(diff * diff)

                @pl.when(st < last_s)
                def _():
                    hand_h(u, j).start()

        def f_relay_n(j, u):
            @pl.when(crosses & inner)
            def _():
                gather_n(u).relay()
                for q in quarters:
                    forward_n(u, far + q).start()

        def f_forward_n(j, u):
            @pl.when(crosses & outer)
            def _():
                gather_n(u).collect()
                for k in range(n_block):
                    forward_n(u, k).start()

        def drain_n(u):
            for k in range(n_block):
                forward_n(u, k).wait_send()
            gather_n(u).drain()
            gather_n(u).drain_own()

        forward = (f_enter, f_relay_a, f_collect_a, f_attention, scatter_relay(0), f_middle, f_relay_b, f_collect_b, f_mlp,
                   scatter_relay(1), f_leave, f_relay_n, f_forward_n)

        def b_enter(j, u):
            @pl.when(is_last & inner)
            def _():
                @pl.when(j >= n_gath)
                def _():
                    gather_d(j, u).drain_own()

                for q in quarters:
                    gather_d(j, u).send(q)

        def b_relay_d(j, u):
            @pl.when(j >= n_gath)
            def _():
                gather_d(j, u).drain()

            gather_d(j, u).relay()

        def b_collect_d(j, u):
            gather_d(j, u).collect()

            @pl.when(st < last_s)
            def _():
                gather_d(j, u).own()

        def b_mlp(j, u):
            @pl.when(j >= n_gath)
            def _():
                save_d(j, u).wait()
                save_dm(j, u).wait()
                gather_dm(j).drain()
                gather_dm(j).drain_own()

            @pl.when(j >= n_send)
            def _():
                save_du(j, u).wait()

            s = sslot(j)
            save_d(j, u).start()
            part[2, s] = dot_nt(d_all[u], wdown[...])

            def act(r, carry):
                rr = pl.ds(pl.multiple_of(r * sub_rows, sub_rows), sub_rows)
                v = u_all[u, rr, :]
                v2 = v * v
                th = jnp.tanh(GELU_K * (v + GELU_C * (v2 * v)))
                slope = 0.5 * (1.0 + th) + 0.5 * v * (1.0 - th * th) * (GELU_K * (1.0 + 3.0 * GELU_C * v2))
                dust[s, rr, :] = (part[2, s, rr, :] * slope).astype(BF16)
                return carry

            lax.fori_loop(0, tok // sub_rows, act, 0)
            save_du(j, u).start()
            part[2, s] = dot_nt(dust[s], wup[...])
            Scatter(2, j).start(j)

        def b_middle(j, u):
            sc = Scatter(2, j)

            @pl.when(inner)
            def _():
                for q in quarters:
                    m = m_all[u, q_rows(q), :]
                    inv = rms_inverse(m)
                    normed = m * inv
                    dn = sc.total(q)
                    gb8[...] += fold(dn * normed)
                    dn = dn * gain_b
                    dm = d_all[u, rows_of(near + q), :].astype(F32) + inv * (
                        dn - normed * jnp.mean(dn * normed, axis=-1, keepdims=True))
                    m_all[u, q_rows(q), :] = dm
                    dmbuf[gslot(j), rows_of(near + q), :] = dm.astype(BF16)
                    gather_dm(j).send(q)

        def b_relay_dm(j, u):
            gather_dm(j).relay()

        def b_collect_dm(j, u):
            gather_dm(j).collect()

        def b_attention(j, u):
            s = sslot(j)
            p = lax.rem(u, per_seq)
            @pl.when(j >= n_send)
            def _():
                save_dqkv(j, u).wait()

            save_dm(j, u).start()

            @pl.when(is_first)
            def _():
                x_again(j, u).start()

            @pl.when(p == per_seq - 1)
            def _():
                dkacc[...] = jnp.zeros_like(dkacc)
                dvacc[...] = jnp.zeros_like(dvacc)

            datt[...] = dot_nt(dmbuf[gslot(j)], wout[...]).astype(BF16)
            p_rows = pl.ds(pl.multiple_of(p * tok, tok), tok)

            def attend_back(n_tile):
                keys = pl.ds(0, n_tile * tok)
                for h in range(n_head):
                    cols = pl.ds(h * head_dim, head_dim)
                    q, k, v, pr = softmax_of(u, p, h, n_tile)
                    da = datt[:, cols]
                    dp = dot_nt(da, v)
                    ds = (pr * (dp - jnp.sum(pr * dp, axis=-1, keepdims=True)) * scale).astype(BF16)
                    dvacc[keys, cols] += dot_tn(pr.astype(BF16), da)
                    dkacc[keys, cols] += dot_tn(ds, q)
                    dqkvst[s, :, cols] = dot_nn(ds, k).astype(BF16)

            by_reach(p, attend_back)
            dqkvst[s, :, pl.ds(att_w, att_w)] = dkacc[p_rows, :].astype(BF16)
            dqkvst[s, :, pl.ds(2 * att_w, att_w)] = dvacc[p_rows, :].astype(BF16)
            save_dqkv(j, u).start()
            part[3, s] = dot_nt(dqkvst[s], wqkv[...])

            @pl.when(st > 0)
            def _():
                Scatter(3, j).start(j)

        def b_relay_h(j, u):
            @pl.when(st > 0)
            def _():
                Scatter(3, j).relay(j)

        def b_leave(j, u):
            s = lax.rem(j, n_hand)

            @pl.when(st > 0)
            def _():
                sc = Scatter(3, j)

                @pl.when(inner)
                def _():
                    @pl.when(j >= n_hand)
                    def _():
                        for q in quarters:
                            hand_quarter(True, u, j, q, sent)

                    for q in quarters:
                        h32 = hslot[u, q_rows(q), :].astype(F32)
                        inv = rms_inverse(h32)
                        normed = h32 * inv
                        dn = sc.total(q)
                        ga8[...] += fold(dn * normed)
                        dg = dn * gain_a
                        dout[s, q_rows(q), :] = (m_all[u, q_rows(q), :] + inv * (
                            dg - normed * jnp.mean(dg * normed, axis=-1, keepdims=True))).astype(BF16)
                        hand_quarter(True, u, j, q, begin)

            @pl.when(is_first)
            def _():
                x_again(j, u).wait()
                for k in range(n_block):
                    rs = pl.ds(k * row, row)
                    h32 = xtmp[sslot(j), rs, :].astype(F32)
                    ga8[...] += fold(part[3, sslot(j), rs, :] * (h32 * rms_inverse(h32)))

        backward = (b_enter, b_relay_d, b_collect_d, b_mlp, scatter_relay(2), b_middle, b_relay_dm, b_collect_dm,
                    b_attention, b_relay_h, b_leave)
        f_lag, b_lag = lags(False), lags(True)
        back_from = BACK_START + BACK_STEP * (last_s - st)

        def hand_finish(back):
            @pl.when(inner)
            def _():
                for j in range(n_unit - n_hand, n_unit):
                    if back:
                        for q in quarters:
                            hand_quarter(True, j, j, q, sent)
                    else:
                        hand_sent(j, j)

        def finish_forward():
            for j in range(n_unit - n_gath, n_unit):
                save_a(j).wait()
                save_b(j).wait()
                gather_b(j).drain()
                gather_b(j).drain_own()

                @pl.when((st > 0) & (st != ns // 2))
                def _():
                    gather_a(j).drain()

                @pl.when(crosses)
                def _():
                    drain_n(j)

            for j in range(n_unit - n_send, n_unit):
                save_o(j).wait()
                save_z(j).wait()
                Scatter(0, j).drain()
                Scatter(1, j).drain()

            @pl.when(st < last_s)
            def _():
                hand_finish(False)

        def finish_backward():
            for j in range(n_unit - n_gath, n_unit):
                save_d(j, j).wait()
                save_dm(j, j).wait()
                gather_dm(j).drain()
                gather_dm(j).drain_own()
                gather_d(j, j).drain()

                @pl.when(is_last)
                def _():
                    gather_d(j, j).drain_own()

            for j in range(n_unit - n_send, n_unit):
                save_du(j, j).wait()
                save_dqkv(j, j).wait()
                Scatter(2, j).drain()

                @pl.when(st > 0)
                def _():
                    Scatter(3, j).drain()

            @pl.when(st > 0)
            def _():
                hand_finish(True)
                gain_send().wait_send()

        def turn(i, carry):
            @pl.when(i == n_unit + f_lag[-1])
            def _():
                finish_forward()

            for back, phase in ORDER:
                j = (i - back_from - b_lag[phase]) if back else (i - f_lag[phase])

                @pl.when((j >= 0) & (j < n_unit))
                def _():
                    if back:
                        seq = lax.div(j, per_seq)
                        backward[phase](j, 2 * seq * per_seq + (per_seq - 1) - j)
                    else:
                        forward[phase](j, j)
            return carry

        lax.fori_loop(0, n_unit + back_from + b_lag[-1], turn, 0)

        def loss_send():
            return rdma(lossacc, lossacc, loss_sem.at[0], loss_sem.at[1], stage=st - 1)

        @pl.when(is_last)
        def _():
            loss_send().start()

        @pl.when(st < last_s)
        def _():
            loss_send().wait_recv()

            @pl.when(st > 0)
            def _():
                loss_send().start()

        loss_row = jnp.sum(jnp.sum(lossacc[...], axis=0, keepdims=True), axis=1, keepdims=True)
        gx[z, 0:1, :] = jnp.sum(ga8[...], axis=0, keepdims=True)
        gx[z, 1:2, :] = jnp.sum(gb8[...], axis=0, keepdims=True)
        gx[z, 2:8, :] = jnp.broadcast_to(loss_row, (6, d_model))

        def gx_send(dz):
            return rdma(gx.at[z], gx.at[z], gx_s.at[dz], gx_r.at[z], model=lax.rem(z + dz, nz))

        def gx_recv(dz):
            k = lax.rem(z + dz, nz)
            return rdma(gx.at[k], gx.at[k], gx_s.at[dz], gx_r.at[k], model=k)

        for dz in range(1, nz):
            gx_send(dz).start()
        finish_backward()

        @pl.when(st > 0)
        def _():
            loss_send().wait_send()

        for dz in range(1, nz):
            gx_recv(dz).wait_recv()
        red_out[...] = gx[0] + gx[1] + gx[2] + gx[3]
        for dz in range(1, nz):
            gx_send(dz).wait_send()

    any_spec = pl.BlockSpec(memory_space=pl.ANY)
    vmem_spec = pl.BlockSpec(memory_space=pltpu.VMEM)

    def out(width):
        return jax.ShapeDtypeStruct((n_unit, tok, width), BF16)

    dma = pltpu.SemaphoreType.DMA
    vmem = pltpu.VMEM
    return pl.pallas_call(
        kernel,
        out_shape=(out(d_model), out(d_model), out(d_model), out(d_model), out(qkv_w), out(att_w), out(ff_w), out(ff_w),
                   jax.ShapeDtypeStruct((8, d_model), F32)),
        in_specs=[any_spec] * 6 + [vmem_spec],
        out_specs=(any_spec,) * 8 + (vmem_spec,),
        scratch_shapes=[
            vmem((d_model, qkv_w), BF16), vmem((att_w, d_model), BF16), vmem((d_model, ff_w), BF16), vmem((ff_w, d_model), BF16),
            vmem((n_unit, half, d_model), BF16), vmem((n_hand, half, d_model), BF16),
            vmem((n_unit, tok, d_model), BF16), vmem((n_unit, tok, d_model), BF16),
            vmem((n_gath, tok, d_model), BF16), vmem((n_gath, tok, d_model), BF16), vmem((n_gath, tok, d_model), BF16),
            vmem((n_send, tok, d_model), BF16),
            vmem((n_unit, tok, qkv_w), BF16), vmem((n_unit, tok, ff_w), F32), vmem((n_unit, half, d_model), F32),
            vmem((n_send, tok, att_w), BF16), vmem((n_send, tok, ff_w), BF16), vmem((n_send, tok, ff_w), BF16),
            vmem((n_send, tok, qkv_w), BF16), vmem((tok, att_w), BF16), vmem((4, n_send, tok, d_model), F32),
            vmem((4, n_recv, n_block, row, d_model), BF16), vmem((4, n_recv, n_part, row, d_model), BF16),
            vmem((4, n_send, n_block, row, d_model), BF16),
            vmem((n_hand, half, d_model), BF16), vmem((n_hand, half, d_model), BF16), vmem((n_hand, half, d_model), BF16),
            vmem((seq_len, att_w), F32), vmem((seq_len, att_w), F32),
            vmem((2, d_model), F32), vmem((2, d_model), F32),
            vmem((8, d_model), F32), vmem((8, d_model), F32), vmem((8, d_model), F32), vmem((nz, 8, d_model), F32),
            dma((n_slab + 3,)), dma((n_unit,)), dma((n_hand,)), dma((n_send,)), dma((2,)), dma((n_hand, 3 * n_part + 1)), dma((n_hand, 3 * n_part)), dma((8, n_gath)),
            dma((n_unit, n_block)), dma((n_unit, n_block)), dma((n_gath, n_part)), dma((n_gath, n_block)),
            dma((n_gath, n_part)), dma((n_gath, n_block)),
            dma((n_gath, n_block)), dma((n_gath, n_part)), dma((n_gath, n_block)), dma((n_gath, n_block)),
            dma((n_gath, n_block)), dma((n_gath, n_block)),
            dma((n_gath, n_part)), dma((n_gath, n_block)), dma((n_gath, n_part)), dma((n_gath, n_block)),
            dma((4, n_recv, n_block)), dma((4, n_recv, n_part)), dma((4, n_send, n_block)),
            dma((2,)), dma((nz,)), dma((nz,)),
        ],
        compiler_params=pltpu.CompilerParams(collective_id=0, has_side_effects=True, vmem_limit_bytes=67_043_328),
        name="layer_step",
    )(x_in, y_target, w_qkv, w_out, w_up, w_down, gain)


def weight_grads(o, dm, a, dqkv, b, du, zz, d, red, head_dim, loss_scale):
    n_tok = o.shape[0] * o.shape[1]
    rows = 256

    def flat(v):
        return v.reshape(n_tok, v.shape[2])

    acts = [flat(v) for v in (o, dm, a, dqkv, b, du, zz, d)]
    att_w, d_model = acts[0].shape[1], acts[1].shape[1]
    qkv_w, ff_w = acts[3].shape[1], acts[5].shape[1]
    n_slab = qkv_w // head_dim

    def kernel(*refs):
        src, red_ref, outs = refs[:8], refs[8], refs[9:13]
        gain_out, loss_out = refs[13:15]
        held, tiles = refs[15:23], refs[23:27]
        in_sem, out_sem = refs[27:]
        loads = [pltpu.make_async_copy(src[i], held[i], in_sem.at[i]) for i in range(8)]
        for cp in loads:
            cp.start()

        def stores(pair, i, slot):
            n = tiles[pair].shape[1]
            at = pl.ds(pl.multiple_of(i * n, n), n)
            sem = out_sem.at[pair, slot]
            if pair == 1:
                return [pltpu.make_async_copy(tiles[1].at[slot, :, pl.ds(k * head_dim, head_dim)], outs[1].at[k, at, :], sem)
                        for k in range(n_slab)]
            return [pltpu.make_async_copy(tiles[pair].at[slot], outs[pair].at[at, :], sem)]

        def finish(cps):
            for cp in cps:
                cp.wait()

        gain_out[...] = red_ref[0:2, :]
        loss_out[...] = red_ref[2:3, 0:1] * loss_scale
        counts = []
        for pair in range(4):
            loads[2 * pair].wait()
            loads[2 * pair + 1].wait()
            left, right, tile = held[2 * pair], held[2 * pair + 1], tiles[pair]
            n = tile.shape[1]
            count = left.shape[1] // n
            counts.append(count)

            def body(i, carry):
                slot = lax.rem(i, 2)

                @pl.when(i >= 2)
                def _():
                    finish(stores(pair, i - 2, slot))

                tile[slot] = dot_tn(left[:, pl.ds(pl.multiple_of(i * n, n), n)], right[...])
                for cp in stores(pair, i, slot):
                    cp.start()
                return carry

            lax.fori_loop(0, count, body, 0)
        for pair in range(4):
            for i in range(max(0, counts[pair] - 2), counts[pair]):
                finish(stores(pair, i, i % 2))

    any_spec = pl.BlockSpec(memory_space=pl.ANY)
    vmem_spec = pl.BlockSpec(memory_space=pltpu.VMEM)
    return pl.pallas_call(
        kernel,
        out_shape=(jax.ShapeDtypeStruct((att_w, d_model), F32), jax.ShapeDtypeStruct((n_slab, d_model, head_dim), F32),
                   jax.ShapeDtypeStruct((d_model, ff_w), F32), jax.ShapeDtypeStruct((ff_w, d_model), F32),
                   jax.ShapeDtypeStruct((2, d_model), F32), jax.ShapeDtypeStruct((1, 1), F32)),
        in_specs=[any_spec] * 8 + [vmem_spec],
        out_specs=(any_spec,) * 4 + (vmem_spec,) * 2,
        scratch_shapes=[pltpu.VMEM(v.shape, BF16) for v in acts] + [
            pltpu.VMEM((1, att_w, d_model), F32), pltpu.VMEM((2, rows, qkv_w), F32),
            pltpu.VMEM((2, rows, ff_w), F32), pltpu.VMEM((2, rows, d_model), F32),
            pltpu.SemaphoreType.DMA((8,)), pltpu.SemaphoreType.DMA((4, 2))],
        compiler_params=pltpu.CompilerParams(vmem_limit_bytes=67_043_328),
        name="weight_grads",
    )(*acts, red)


def solution(mesh):
    dims = dict(mesh.shape)

    def device_fn(x_in, y_target, w_qkv, w_out, w_up, w_down, norm_gain):
        n_batch, seq_len, d_model = x_in.shape
        heads, head_dim = w_qkv.shape[3], w_qkv.shape[4]
        a, b, d, dm, dqkv, o, zz, du, red = layer_step(
            dims, x_in, y_target,
            w_qkv[0].transpose(1, 2, 0, 3).reshape(3 * heads, d_model, head_dim),
            w_out[0].reshape(heads * head_dim, d_model), w_up[0], w_down[0], norm_gain[0])
        g_out, g_qkv, g_up, g_down, g_gain, loss = weight_grads(
            o, dm, a, dqkv, b, du, zz, d, red, head_dim, 0.5 / (n_batch * seq_len * d_model))
        grad_qkv = g_qkv.reshape(3, heads, d_model, head_dim).transpose(2, 0, 1, 3)[None]
        grad_out = g_out.reshape(1, heads, head_dim, d_model)
        grad_up = g_up[None]
        grad_down = g_down[None]
        return loss.reshape(1), grad_qkv, grad_out, grad_up, grad_down, g_gain[None]

    act_spec = P("data", None, None)
    weight_specs = (
        P("stage", None, None, "model", None),
        P("stage", "model", None, None),
        P("stage", None, "model"),
        P("stage", "model", None),
        P("stage", None, None),
    )
    grad_specs = (
        P(("data", "stage"), None, None, "model", None),
        P(("data", "stage"), "model", None, None),
        P(("data", "stage"), None, "model"),
        P(("data", "stage"), "model", None),
        P(("data", "stage"), None, None),
    )
    return jax.shard_map(
        device_fn,
        mesh=mesh,
        in_specs=(act_spec, act_spec) + weight_specs,
        out_specs=(P("data"),) + grad_specs,
        check_vma=False,
    )
```

```python
import jax
import jax.numpy as jnp
from jax import lax
from jax.experimental import pallas as pl
from jax.experimental.pallas import tpu as pltpu
from jax.sharding import PartitionSpec as P

NORM_EPS = 1e-6
NEG_BIG = -1e30
MESH = pl.DeviceIdType.MESH
GELU_K = 0.7978845608028654
GELU_C = 0.044715
F32 = jnp.float32
BF16 = jnp.bfloat16


def dot_nn(a, b):
    return lax.dot_general(a, b, (((1,), (0,)), ((), ())), preferred_element_type=F32)


def dot_nt(a, b):
    return lax.dot_general(a, b, (((1,), (1,)), ((), ())), preferred_element_type=F32)


def dot_tn(a, b):
    return lax.dot_general(a, b, (((0,), (0,)), ((), ())), preferred_element_type=F32)


def rms_inverse(v32):
    return lax.rsqrt(jnp.mean(v32 * v32, axis=-1, keepdims=True) + NORM_EPS)


ORDER = (
    (1, 6), (0, 3), (1, 2), (0, 7), (0, 9), (0, 5), (1, 3), (0, 8), (1, 9), (0, 1), (1, 1), (1, 7), (0, 0), (0,
    2), (1, 5), (1, 8), (0, 4), (0, 6), (1, 0), (0, 10), (1, 4), (1, 10),
)
BACK_START, BACK_STEP = 13, 10


def lags(back):
    place = {phase: i for i, (is_back, phase) in enumerate(ORDER) if is_back == int(back)}
    lag = [0]
    for phase in range(1, len(place)):
        lag.append(lag[-1] + (1 if place[phase] < place[phase - 1] else 0))
    return lag


def layer_step(dims, x_in, y_target, w_qkv, w_out, w_up, w_down, gain):
    nz, ns = dims["model"], dims["stage"]
    n_seq, seq_len, d_model = x_in.shape
    n_slab, _, head_dim = w_qkv.shape
    qkv_w = n_slab * head_dim
    att_w = w_out.shape[0]
    ff_w = w_up.shape[1]
    n_head = att_w // head_dim
    tok = 64
    n_part = 2
    row = tok // (2 * n_part)
    n_block = 2 * n_part
    per_seq = seq_len // tok
    n_unit = n_seq * per_seq
    key_step = per_seq // 4
    scale = head_dim ** -0.5
    inv_count = 1.0 / (n_seq * seq_len * d_model)
    last_z, last_s = nz - 1, ns - 1
    sub_rows = 16
    half = tok // 2
    n_send, n_recv, n_gath, n_hand = 2, 3, 4, 2
    quarters = range(n_part)

    def kernel(x_ref, y_ref, wqkv_h, wout_h, wup_h, wdown_h, gain_ref,
               a_out, b_out, d_out, dm_out, dqkv_out, o_out, z_out, du_out, red_out,
               wqkv, wout, wup, wdown, hslot, yslot, a_all, d_all, bbuf, dmbuf, xtmp,
               qkv_all, u_all, m_all, ost, zst, dust, dqkvst, datt, part,
               recv_o, recv_i, send_p, hout, aout, dout, dkacc, dvacc,
               gains, gain_next, lossacc, ga8, gb8, gx,
               w_sem, hsem, ysem, x_sem, gain_sem, hand_sem, back_sem, save_sem,
               a_rs, d_rs, a_si, a_so, d_si, d_so, b_rs, dm_rs, b_si, b_so, dm_si, dm_so,
               rs_ro, rs_ri, rs_s, loss_sem, gx_s, gx_r):
        z = lax.axis_index("model")
        st = lax.axis_index("stage")
        is_first = st == 0
        is_last = st == last_s
        inner = (z > 0) & (z < last_z)
        outer = (z == 0) | (z == last_z)
        side = lax.div(z, 2)
        near = n_part * side
        far = n_part - near
        inner_peer = 1 + lax.rem(z, 2)
        outer_peer = last_z * side
        my_half = pl.ds(pl.multiple_of(side * half, half), half)

        def rdma(src, dst, ssem, rsem, **dev):
            return pltpu.make_async_remote_copy(src_ref=src, dst_ref=dst, send_sem=ssem, recv_sem=rsem,
                                                device_id=dev, device_id_type=MESH)

        def rows_of(k):
            return pl.ds(pl.multiple_of(k * row, row), row)

        qkv_copies = [pltpu.make_async_copy(wqkv_h.at[i], wqkv.at[:, pl.ds(i * head_dim, head_dim)], w_sem.at[i])
                      for i in range(n_slab)]
        w_copies = [pltpu.make_async_copy(src, dst, w_sem.at[n_slab + i])
                    for i, (src, dst) in enumerate(((wout_h, wout), (wup_h, wup), (wdown_h, wdown)))]

        def tokens_of(u):
            return lax.div(u, per_seq), pl.multiple_of(lax.rem(u, per_seq) * tok, tok)

        def x_copy(u):
            q, first = tokens_of(u)
            return pltpu.make_async_copy(x_ref.at[q, pl.ds(first, tok), :], a_all.at[u], hsem.at[u])

        def x_again(j, u):
            q, first = tokens_of(u)
            slot = lax.rem(j, n_send)
            return pltpu.make_async_copy(x_ref.at[q, pl.ds(first, tok), :], xtmp.at[slot], x_sem.at[slot])

        def y_copy(u):
            q, first = tokens_of(u)
            rs = pl.ds(pl.multiple_of(first + side * half, half), half)
            slot = lax.rem(u, n_hand)
            return pltpu.make_async_copy(y_ref.at[q, rs, :], yslot.at[slot], ysem.at[slot])

        @pl.when(is_first)
        def _():
            for u in range(n_send):
                x_copy(u).start()

        for cp in qkv_copies + w_copies:
            cp.start()

        @pl.when(is_first)
        def _():
            @pl.loop(n_send, n_unit)
            def _(u):
                x_copy(u).start()

        barrier = pltpu.get_barrier_semaphore()
        for i in range(1, nz * ns):
            dz, dst = i % nz, i // nz
            pl.semaphore_signal(barrier, inc=1, device_id_type=MESH,
                                device_id={"model": lax.rem(z + dz, nz), "stage": lax.rem(st + dst, ns)})
        qkv_all[...] = jnp.zeros_like(qkv_all)
        lossacc[...] = jnp.zeros_like(lossacc)
        ga8[...] = jnp.zeros_like(ga8)
        gb8[...] = jnp.zeros_like(gb8)
        gains[...] = gain_ref[...].astype(F32)
        pl.semaphore_wait(barrier, nz * ns - 1)

        def gain_send():
            return rdma(gains, gain_next, gain_sem.at[0], gain_sem.at[1], stage=st - 1)

        @pl.when(st > 0)
        def _():
            gain_send().start()

        class Gather:
            def __init__(self, buf, slot, rsem, si, so, sslot):
                self.buf, self.slot, self.rsem, self.si, self.so, self.sslot = buf, slot, rsem, si, so, sslot

            def block(self, k):
                return self.buf.at[self.slot, rows_of(k), :]

            def inward(self, k, q):
                return rdma(self.block(k), self.block(k), self.si.at[self.sslot, q], self.rsem.at[self.slot, k],
                            model=inner_peer)

            def outward(self, k):
                return rdma(self.block(k), self.block(k), self.so.at[self.sslot, k], self.rsem.at[self.slot, k],
                            model=outer_peer)

            def send(self, q):
                self.inward(near + q, q).start()
                self.outward(near + q).start()

            def relay(self):
                @pl.when(inner)
                def _():
                    for q in quarters:
                        self.outward(far + q).wait_recv()
                        self.outward(far + q).start()

            def collect(self):
                @pl.when(outer)
                def _():
                    for k in range(n_block):
                        self.outward(k).wait_recv()

            def own(self):
                @pl.when(inner)
                def _():
                    for q in quarters:
                        self.outward(near + q).wait_recv()

            def drain(self):
                @pl.when(inner)
                def _():
                    for q in quarters:
                        self.outward(far + q).wait_send()

            def drain_own(self):
                @pl.when(inner)
                def _():
                    for q in quarters:
                        self.inward(near + q, q).wait_send()
                        self.outward(near + q).wait_send()

        def gather_a(u):
            return Gather(a_all, u, a_rs, a_si, a_so, lax.rem(u, n_gath))

        def gather_d(j, u):
            return Gather(d_all, u, d_rs, d_si, d_so, lax.rem(j, n_gath))

        def gather_b(u):
            return Gather(bbuf, lax.rem(u, n_gath), b_rs, b_si, b_so, lax.rem(u, n_gath))

        def gather_dm(j):
            return Gather(dmbuf, lax.rem(j, n_gath), dm_rs, dm_si, dm_so, lax.rem(j, n_gath))

        class Scatter:
            def __init__(self, op, u):
                self.op, self.ss, self.rs = op, lax.rem(u, n_send), lax.rem(u, n_recv)

            def in_copy(self, k):
                return rdma(send_p.at[self.op, self.ss, k], recv_o.at[self.op, self.rs, k],
                            rs_s.at[self.op, self.ss, k], rs_ro.at[self.op, self.rs, k], model=inner_peer)

            def cross_copy(self, k, q):
                return rdma(send_p.at[self.op, self.ss, k], recv_i.at[self.op, self.rs, q],
                            rs_s.at[self.op, self.ss, k], rs_ri.at[self.op, self.rs, q], model=inner_peer)

            def mine(self, k):
                return part[self.op, self.ss, rows_of(k), :]

            def start(self, j):
                @pl.when(outer)
                def _():
                    @pl.when(j >= n_send)
                    def _():
                        self.drain_outer()

                    for k in [far + q for q in quarters] + [near + q for q in quarters]:
                        send_p[self.op, self.ss, k] = self.mine(k).astype(BF16)
                        self.in_copy(k).start()

            def relay(self, j):
                @pl.when(inner)
                def _():
                    @pl.when(j >= n_send)
                    def _():
                        self.drain_inner()

                    for q in quarters:
                        k = far + q
                        self.in_copy(k).wait_recv()
                        send_p[self.op, self.ss, k] = (
                            self.mine(k) + recv_o[self.op, self.rs, k].astype(F32)).astype(BF16)
                        self.cross_copy(k, q).start()

            def total(self, q):
                k = near + q
                self.in_copy(k).wait_recv()
                self.cross_copy(k, q).wait_recv()
                return (self.mine(k) + recv_o[self.op, self.rs, k].astype(F32)) + recv_i[self.op, self.rs, q].astype(F32)

            def drain_outer(self):
                for k in range(n_block):
                    self.in_copy(k).wait_send()

            def drain_inner(self):
                for q in quarters:
                    self.cross_copy(far + q, q).wait_send()

            def drain(self):
                @pl.when(outer)
                def _():
                    self.drain_outer()

                @pl.when(inner)
                def _():
                    self.drain_inner()

        def save(kind, src, src_slot, dst, j, u):
            return pltpu.make_async_copy(src.at[src_slot], dst.at[u],
                                         save_sem.at[kind, lax.rem(j, n_send if kind % 2 else n_gath)])

        def sslot(u):
            return lax.rem(u, n_send)

        def gslot(u):
            return lax.rem(u, n_gath)

        def q_rows(q):
            return pl.ds(q * row, row)

        def save_a(u):
            return save(0, a_all, u, a_out, u, u)

        def save_o(u):
            return save(1, ost, sslot(u), o_out, u, u)

        def save_b(u):
            return save(2, bbuf, gslot(u), b_out, u, u)

        def save_z(u):
            return save(3, zst, sslot(u), z_out, u, u)

        def save_d(j, u):
            return save(4, d_all, u, d_out, j, u)

        def save_du(j, u):
            return save(5, dust, sslot(j), du_out, j, u)

        def save_dm(j, u):
            return save(6, dmbuf, gslot(j), dm_out, j, u)

        def save_dqkv(j, u):
            return save(7, dqkvst, sslot(j), dqkv_out, j, u)

        gain_a = gains[0:1, :]
        gain_b = gains[1:2, :]

        def hand_h(u, j):
            s = lax.rem(j, n_hand)
            return rdma(hout.at[s], hslot.at[u], hand_sem.at[s, 3 * n_part], hsem.at[u], stage=st + 1)

        def hand_quarter(back, u, j, q, act):
            s = lax.rem(j, n_hand)
            k = near + q
            src, buf, sems, own = (dout, d_all, d_rs, back_sem) if back else (aout, a_all, a_rs, hand_sem)
            for i, peer in enumerate((inner_peer, outer_peer, z)):
                act(rdma(src.at[s, q_rows(q), :], buf.at[u, rows_of(k), :], own.at[s, 3 * q + i], sems.at[u, k],
                         model=peer, stage=(st - 1) if back else (st + 1)))

        def hand_sent(back, u, j):
            for q in quarters:
                hand_quarter(back, u, j, q, sent)
            if not back:
                hand_h(u, j).wait_send()

        def begin(cp):
            cp.start()

        def sent(cp):
            cp.wait_send()

        def softmax_of(u, p, i, n_tile):
            first = u - p
            n_key = n_tile * tok
            cols = pl.ds(i * head_dim, head_dim)
            q = qkv_all[u, :, cols]
            k = qkv_all[pl.ds(first, n_tile), :, pl.ds(att_w + i * head_dim, head_dim)].reshape(n_key, head_dim)
            v = qkv_all[pl.ds(first, n_tile), :, pl.ds(2 * att_w + i * head_dim, head_dim)].reshape(n_key, head_dim)
            sc = dot_nt(q, k) * scale
            q_pos = p * tok + lax.broadcasted_iota(jnp.int32, sc.shape, 0)
            k_pos = lax.broadcasted_iota(jnp.int32, sc.shape, 1)
            sc = jnp.where(k_pos <= q_pos, sc, NEG_BIG)
            e = jnp.exp(sc - jnp.max(sc, axis=-1, keepdims=True))
            pr = e * (1.0 / jnp.sum(e, axis=-1, keepdims=True))
            return q, k, v, pr

        def by_reach(p, body):
            for n_tile in range(key_step, per_seq + 1, key_step):
                @pl.when((p >= n_tile - key_step) & (p < n_tile))
                def _():
                    body(n_tile)

        def fold(v):
            return jnp.sum(v.reshape(v.shape[0] // 8, 8, d_model), axis=0)

        def f_enter(j, u):
            @pl.when(is_first)
            def _():
                x_copy(u).wait()
                hslot[u] = a_all[u, my_half, :]
                for k in range(n_block):
                    rs = pl.ds(k * row, row)
                    h32 = a_all[u, rs, :].astype(F32)
                    a_all[u, rs, :] = (h32 * rms_inverse(h32) * gain_a).astype(BF16)

        def f_relay_a(j, u):
            @pl.when(st > 0)
            def _():
                @pl.when(j >= n_gath)
                def _():
                    gather_a(u).drain()

                gather_a(u).relay()

        def f_collect_a(j, u):
            @pl.when(st > 0)
            def _():
                gather_a(u).collect()
                gather_a(u).own()

        def f_attention(j, u):
            @pl.when(j == 0)
            def _():
                for cp in qkv_copies:
                    cp.wait()
                w_copies[0].wait()

            @pl.when(j >= n_gath)
            def _():
                save_a(u).wait()
                save_b(u).wait()
                gather_b(u).drain()
                gather_b(u).drain_own()

            @pl.when(j >= n_send)
            def _():
                save_o(u).wait()

            s = sslot(u)
            p = lax.rem(u, per_seq)
            save_a(u).start()
            qkv_all[u] = dot_nn(a_all[u], wqkv[...]).astype(BF16)
            def attend(n_tile):
                for i in range(n_head):
                    _, _, v, pr = softmax_of(u, p, i, n_tile)
                    ost[s, :, pl.ds(i * head_dim, head_dim)] = dot_nn(pr.astype(BF16), v).astype(BF16)

            by_reach(p, attend)
            save_o(u).start()
            part[0, s] = dot_nn(ost[s], wout[...])
            Scatter(0, u).start(j)

        def scatter_relay(op):
            def run(j, u):
                Scatter(op, j).relay(j)
            return run

        def f_middle(j, u):
            sc = Scatter(0, u)

            @pl.when(inner)
            def _():
                @pl.when(st > 0)
                def _():
                    rdma(hout.at[0], hslot.at[u], hand_sem.at[0, 3 * n_part], hsem.at[u], stage=st).wait_recv()

                for q in quarters:
                    m = hslot[u, q_rows(q), :].astype(F32) + sc.total(q)
                    m_all[u, q_rows(q), :] = m
                    bbuf[gslot(u), rows_of(near + q), :] = (m * rms_inverse(m) * gain_b).astype(BF16)
                    gather_b(u).send(q)

        def f_relay_b(j, u):
            gather_b(u).relay()

        def f_collect_b(j, u):
            gather_b(u).collect()

        def f_mlp(j, u):
            @pl.when(j == 0)
            def _():
                w_copies[1].wait()
                w_copies[2].wait()

            s = sslot(u)
            @pl.when(j >= n_send)
            def _():
                save_z(u).wait()

            save_b(u).start()

            @pl.when(is_last & inner)
            def _():
                y_copy(u).start()

            u_all[u] = dot_nn(bbuf[gslot(u)], wup[...])

            def act(r, carry):
                rr = pl.ds(pl.multiple_of(r * sub_rows, sub_rows), sub_rows)
                v = u_all[u, rr, :]
                th = jnp.tanh(GELU_K * (v + GELU_C * (v * v * v)))
                zst[s, rr, :] = (0.5 * v * (1.0 + th)).astype(BF16)
                return carry

            lax.fori_loop(0, tok // sub_rows, act, 0)
            save_z(u).start()
            part[1, s] = dot_nn(zst[s], wdown[...])
            Scatter(1, u).start(j)

        def f_leave(j, u):
            sc = Scatter(1, u)
            s = lax.rem(j, n_hand)

            @pl.when((j == 0) & (st < last_s))
            def _():
                gain_send().wait_recv()

            @pl.when(inner)
            def _():
                @pl.when(st < last_s)
                def _():
                    @pl.when(j >= n_hand)
                    def _():
                        hand_sent(False, u, j)

                @pl.when(is_last)
                def _():
                    y_copy(u).wait()

                for q in quarters:
                    h_new = (m_all[u, q_rows(q), :] + sc.total(q)).astype(BF16)
                    h32 = h_new.astype(F32)

                    @pl.when(st < last_s)
                    def _():
                        aout[s, q_rows(q), :] = (h32 * rms_inverse(h32) * gain_next[0:1, :]).astype(BF16)
                        hand_quarter(False, u, j, q, begin)
                        hout[s, q_rows(q), :] = h_new

                    @pl.when(is_last)
                    def _():
                        diff = h32 - yslot[lax.rem(u, n_hand), q_rows(q), :].astype(F32)
                        d_all[u, rows_of(near + q), :] = (diff * inv_count).astype(BF16)
                        lossacc[...] += fold(diff * diff)

                @pl.when(st < last_s)
                def _():
                    hand_h(u, j).start()

        forward = (f_enter, f_relay_a, f_collect_a, f_attention, scatter_relay(0), f_middle, f_relay_b, f_collect_b, f_mlp,
                   scatter_relay(1), f_leave)

        def b_enter(j, u):
            @pl.when(is_last & inner)
            def _():
                @pl.when(j >= n_gath)
                def _():
                    gather_d(j, u).drain_own()

                for q in quarters:
                    gather_d(j, u).send(q)

        def b_relay_d(j, u):
            @pl.when(j >= n_gath)
            def _():
                gather_d(j, u).drain()

            gather_d(j, u).relay()

        def b_collect_d(j, u):
            gather_d(j, u).collect()

            @pl.when(st < last_s)
            def _():
                gather_d(j, u).own()

        def b_mlp(j, u):
            @pl.when(j >= n_gath)
            def _():
                save_d(j, u).wait()
                save_dm(j, u).wait()
                gather_dm(j).drain()
                gather_dm(j).drain_own()

            @pl.when(j >= n_send)
            def _():
                save_du(j, u).wait()

            s = sslot(j)
            save_d(j, u).start()
            part[2, s] = dot_nt(d_all[u], wdown[...])

            def act(r, carry):
                rr = pl.ds(pl.multiple_of(r * sub_rows, sub_rows), sub_rows)
                v = u_all[u, rr, :]
                v2 = v * v
                th = jnp.tanh(GELU_K * (v + GELU_C * (v2 * v)))
                slope = 0.5 * (1.0 + th) + 0.5 * v * (1.0 - th * th) * (GELU_K * (1.0 + 3.0 * GELU_C * v2))
                dust[s, rr, :] = (part[2, s, rr, :] * slope).astype(BF16)
                return carry

            lax.fori_loop(0, tok // sub_rows, act, 0)
            save_du(j, u).start()
            part[2, s] = dot_nt(dust[s], wup[...])
            Scatter(2, j).start(j)

        def b_middle(j, u):
            sc = Scatter(2, j)

            @pl.when(inner)
            def _():
                for q in quarters:
                    m = m_all[u, q_rows(q), :]
                    inv = rms_inverse(m)
                    normed = m * inv
                    dn = sc.total(q)
                    gb8[...] += fold(dn * normed)
                    dn = dn * gain_b
                    dm = d_all[u, rows_of(near + q), :].astype(F32) + inv * (
                        dn - normed * jnp.mean(dn * normed, axis=-1, keepdims=True))
                    m_all[u, q_rows(q), :] = dm
                    dmbuf[gslot(j), rows_of(near + q), :] = dm.astype(BF16)
                    gather_dm(j).send(q)

        def b_relay_dm(j, u):
            gather_dm(j).relay()

        def b_collect_dm(j, u):
            gather_dm(j).collect()

        def b_attention(j, u):
            s = sslot(j)
            p = lax.rem(u, per_seq)
            @pl.when(j >= n_send)
            def _():
                save_dqkv(j, u).wait()

            save_dm(j, u).start()

            @pl.when(is_first)
            def _():
                x_again(j, u).start()

            @pl.when(p == per_seq - 1)
            def _():
                dkacc[...] = jnp.zeros_like(dkacc)
                dvacc[...] = jnp.zeros_like(dvacc)

            datt[...] = dot_nt(dmbuf[gslot(j)], wout[...]).astype(BF16)
            p_rows = pl.ds(pl.multiple_of(p * tok, tok), tok)

            def attend_back(n_tile):
                keys = pl.ds(0, n_tile * tok)
                for h in range(n_head):
                    cols = pl.ds(h * head_dim, head_dim)
                    q, k, v, pr = softmax_of(u, p, h, n_tile)
                    da = datt[:, cols]
                    dp = dot_nt(da, v)
                    ds = (pr * (dp - jnp.sum(pr * dp, axis=-1, keepdims=True)) * scale).astype(BF16)
                    dvacc[keys, cols] += dot_tn(pr.astype(BF16), da)
                    dkacc[keys, cols] += dot_tn(ds, q)
                    dqkvst[s, :, cols] = dot_nn(ds, k).astype(BF16)

            by_reach(p, attend_back)
            dqkvst[s, :, pl.ds(att_w, att_w)] = dkacc[p_rows, :].astype(BF16)
            dqkvst[s, :, pl.ds(2 * att_w, att_w)] = dvacc[p_rows, :].astype(BF16)
            save_dqkv(j, u).start()
            part[3, s] = dot_nt(dqkvst[s], wqkv[...])

            @pl.when(st > 0)
            def _():
                Scatter(3, j).start(j)

        def b_relay_h(j, u):
            @pl.when(st > 0)
            def _():
                Scatter(3, j).relay(j)

        def b_leave(j, u):
            s = lax.rem(j, n_hand)

            @pl.when(st > 0)
            def _():
                sc = Scatter(3, j)

                @pl.when(inner)
                def _():
                    @pl.when(j >= n_hand)
                    def _():
                        hand_sent(True, u, j)

                    for q in quarters:
                        h32 = hslot[u, q_rows(q), :].astype(F32)
                        inv = rms_inverse(h32)
                        normed = h32 * inv
                        dn = sc.total(q)
                        ga8[...] += fold(dn * normed)
                        dg = dn * gain_a
                        dout[s, q_rows(q), :] = (m_all[u, q_rows(q), :] + inv * (
                            dg - normed * jnp.mean(dg * normed, axis=-1, keepdims=True))).astype(BF16)
                        hand_quarter(True, u, j, q, begin)

            @pl.when(is_first)
            def _():
                x_again(j, u).wait()
                for k in range(n_block):
                    rs = pl.ds(k * row, row)
                    h32 = xtmp[sslot(j), rs, :].astype(F32)
                    ga8[...] += fold(part[3, sslot(j), rs, :] * (h32 * rms_inverse(h32)))

        backward = (b_enter, b_relay_d, b_collect_d, b_mlp, scatter_relay(2), b_middle, b_relay_dm, b_collect_dm,
                    b_attention, b_relay_h, b_leave)
        f_lag, b_lag = lags(False), lags(True)
        back_from = BACK_START + BACK_STEP * (last_s - st)

        def hand_finish(back):
            @pl.when(inner)
            def _():
                for j in range(n_unit - n_hand, n_unit):
                    hand_sent(back, j, j)

        def finish_forward():
            for j in range(n_unit - n_gath, n_unit):
                save_a(j).wait()
                save_b(j).wait()
                gather_b(j).drain()
                gather_b(j).drain_own()

                @pl.when(st > 0)
                def _():
                    gather_a(j).drain()

            for j in range(n_unit - n_send, n_unit):
                save_o(j).wait()
                save_z(j).wait()
                Scatter(0, j).drain()
                Scatter(1, j).drain()

            @pl.when(st < last_s)
            def _():
                hand_finish(False)

        def finish_backward():
            for j in range(n_unit - n_gath, n_unit):
                save_d(j, j).wait()
                save_dm(j, j).wait()
                gather_dm(j).drain()
                gather_dm(j).drain_own()
                gather_d(j, j).drain()

                @pl.when(is_last)
                def _():
                    gather_d(j, j).drain_own()

            for j in range(n_unit - n_send, n_unit):
                save_du(j, j).wait()
                save_dqkv(j, j).wait()
                Scatter(2, j).drain()

                @pl.when(st > 0)
                def _():
                    Scatter(3, j).drain()

            @pl.when(st > 0)
            def _():
                hand_finish(True)
                gain_send().wait_send()

        def turn(i, carry):
            @pl.when(i == n_unit + f_lag[-1])
            def _():
                finish_forward()

            for back, phase in ORDER:
                j = (i - back_from - b_lag[phase]) if back else (i - f_lag[phase])

                @pl.when((j >= 0) & (j < n_unit))
                def _():
                    if back:
                        seq = lax.div(j, per_seq)
                        backward[phase](j, 2 * seq * per_seq + (per_seq - 1) - j)
                    else:
                        forward[phase](j, j)
            return carry

        lax.fori_loop(0, n_unit + back_from + b_lag[-1], turn, 0)

        def loss_send():
            return rdma(lossacc, lossacc, loss_sem.at[0], loss_sem.at[1], stage=st - 1)

        @pl.when(is_last)
        def _():
            loss_send().start()

        @pl.when(st < last_s)
        def _():
            loss_send().wait_recv()

            @pl.when(st > 0)
            def _():
                loss_send().start()

        loss_row = jnp.sum(jnp.sum(lossacc[...], axis=0, keepdims=True), axis=1, keepdims=True)
        gx[z, 0:1, :] = jnp.sum(ga8[...], axis=0, keepdims=True)
        gx[z, 1:2, :] = jnp.sum(gb8[...], axis=0, keepdims=True)
        gx[z, 2:8, :] = jnp.broadcast_to(loss_row, (6, d_model))

        def gx_send(dz):
            return rdma(gx.at[z], gx.at[z], gx_s.at[dz], gx_r.at[z], model=lax.rem(z + dz, nz))

        def gx_recv(dz):
            k = lax.rem(z + dz, nz)
            return rdma(gx.at[k], gx.at[k], gx_s.at[dz], gx_r.at[k], model=k)

        for dz in range(1, nz):
            gx_send(dz).start()
        finish_backward()

        @pl.when(st > 0)
        def _():
            loss_send().wait_send()

        for dz in range(1, nz):
            gx_recv(dz).wait_recv()
        red_out[...] = gx[0] + gx[1] + gx[2] + gx[3]
        for dz in range(1, nz):
            gx_send(dz).wait_send()

    any_spec = pl.BlockSpec(memory_space=pl.ANY)
    vmem_spec = pl.BlockSpec(memory_space=pltpu.VMEM)

    def out(width):
        return jax.ShapeDtypeStruct((n_unit, tok, width), BF16)

    dma = pltpu.SemaphoreType.DMA
    vmem = pltpu.VMEM
    return pl.pallas_call(
        kernel,
        out_shape=(out(d_model), out(d_model), out(d_model), out(d_model), out(qkv_w), out(att_w), out(ff_w), out(ff_w),
                   jax.ShapeDtypeStruct((8, d_model), F32)),
        in_specs=[any_spec] * 6 + [vmem_spec],
        out_specs=(any_spec,) * 8 + (vmem_spec,),
        scratch_shapes=[
            vmem((d_model, qkv_w), BF16), vmem((att_w, d_model), BF16), vmem((d_model, ff_w), BF16), vmem((ff_w, d_model), BF16),
            vmem((n_unit, half, d_model), BF16), vmem((n_hand, half, d_model), BF16),
            vmem((n_unit, tok, d_model), BF16), vmem((n_unit, tok, d_model), BF16),
            vmem((n_gath, tok, d_model), BF16), vmem((n_gath, tok, d_model), BF16), vmem((n_send, tok, d_model), BF16),
            vmem((n_unit, tok, qkv_w), BF16), vmem((n_unit, tok, ff_w), F32), vmem((n_unit, half, d_model), F32),
            vmem((n_send, tok, att_w), BF16), vmem((n_send, tok, ff_w), BF16), vmem((n_send, tok, ff_w), BF16),
            vmem((n_send, tok, qkv_w), BF16), vmem((tok, att_w), BF16), vmem((4, n_send, tok, d_model), F32),
            vmem((4, n_recv, n_block, row, d_model), BF16), vmem((4, n_recv, n_part, row, d_model), BF16),
            vmem((4, n_send, n_block, row, d_model), BF16),
            vmem((n_hand, half, d_model), BF16), vmem((n_hand, half, d_model), BF16), vmem((n_hand, half, d_model), BF16),
            vmem((seq_len, att_w), F32), vmem((seq_len, att_w), F32),
            vmem((2, d_model), F32), vmem((2, d_model), F32),
            vmem((8, d_model), F32), vmem((8, d_model), F32), vmem((8, d_model), F32), vmem((nz, 8, d_model), F32),
            dma((n_slab + 3,)), dma((n_unit,)), dma((n_hand,)), dma((n_send,)), dma((2,)), dma((n_hand, 3 * n_part + 1)), dma((n_hand, 3 * n_part)), dma((8, n_gath)),
            dma((n_unit, n_block)), dma((n_unit, n_block)), dma((n_gath, n_part)), dma((n_gath, n_block)),
            dma((n_gath, n_part)), dma((n_gath, n_block)), dma((n_gath, n_block)), dma((n_gath, n_block)),
            dma((n_gath, n_part)), dma((n_gath, n_block)), dma((n_gath, n_part)), dma((n_gath, n_block)),
            dma((4, n_recv, n_block)), dma((4, n_recv, n_part)), dma((4, n_send, n_block)),
            dma((2,)), dma((nz,)), dma((nz,)),
        ],
        compiler_params=pltpu.CompilerParams(collective_id=0, has_side_effects=True, vmem_limit_bytes=67_043_328),
        name="layer_step",
    )(x_in, y_target, w_qkv, w_out, w_up, w_down, gain)


def weight_grads(o, dm, a, dqkv, b, du, zz, d, red, head_dim, loss_scale):
    n_tok = o.shape[0] * o.shape[1]
    rows = 256

    def flat(v):
        return v.reshape(n_tok, v.shape[2])

    acts = [flat(v) for v in (o, dm, a, dqkv, b, du, zz, d)]
    att_w, d_model = acts[0].shape[1], acts[1].shape[1]
    qkv_w, ff_w = acts[3].shape[1], acts[5].shape[1]
    n_slab = qkv_w // head_dim

    def kernel(*refs):
        src, red_ref, outs = refs[:8], refs[8], refs[9:13]
        gain_out, loss_out = refs[13:15]
        held, tiles = refs[15:23], refs[23:27]
        in_sem, out_sem = refs[27:]
        loads = [pltpu.make_async_copy(src[i], held[i], in_sem.at[i]) for i in range(8)]
        for cp in loads:
            cp.start()

        def stores(pair, i, slot):
            n = tiles[pair].shape[1]
            at = pl.ds(pl.multiple_of(i * n, n), n)
            sem = out_sem.at[pair, slot]
            if pair == 1:
                return [pltpu.make_async_copy(tiles[1].at[slot, :, pl.ds(k * head_dim, head_dim)], outs[1].at[k, at, :], sem)
                        for k in range(n_slab)]
            return [pltpu.make_async_copy(tiles[pair].at[slot], outs[pair].at[at, :], sem)]

        def finish(cps):
            for cp in cps:
                cp.wait()

        gain_out[...] = red_ref[0:2, :]
        loss_out[...] = red_ref[2:3, 0:1] * loss_scale
        counts = []
        for pair in range(4):
            loads[2 * pair].wait()
            loads[2 * pair + 1].wait()
            left, right, tile = held[2 * pair], held[2 * pair + 1], tiles[pair]
            n = tile.shape[1]
            count = left.shape[1] // n
            counts.append(count)

            def body(i, carry):
                slot = lax.rem(i, 2)

                @pl.when(i >= 2)
                def _():
                    finish(stores(pair, i - 2, slot))

                tile[slot] = dot_tn(left[:, pl.ds(pl.multiple_of(i * n, n), n)], right[...])
                for cp in stores(pair, i, slot):
                    cp.start()
                return carry

            lax.fori_loop(0, count, body, 0)
        for pair in range(4):
            for i in range(max(0, counts[pair] - 2), counts[pair]):
                finish(stores(pair, i, i % 2))

    any_spec = pl.BlockSpec(memory_space=pl.ANY)
    vmem_spec = pl.BlockSpec(memory_space=pltpu.VMEM)
    return pl.pallas_call(
        kernel,
        out_shape=(jax.ShapeDtypeStruct((att_w, d_model), F32), jax.ShapeDtypeStruct((n_slab, d_model, head_dim), F32),
                   jax.ShapeDtypeStruct((d_model, ff_w), F32), jax.ShapeDtypeStruct((ff_w, d_model), F32),
                   jax.ShapeDtypeStruct((2, d_model), F32), jax.ShapeDtypeStruct((1, 1), F32)),
        in_specs=[any_spec] * 8 + [vmem_spec],
        out_specs=(any_spec,) * 4 + (vmem_spec,) * 2,
        scratch_shapes=[pltpu.VMEM(v.shape, BF16) for v in acts] + [
            pltpu.VMEM((1, att_w, d_model), F32), pltpu.VMEM((2, rows, qkv_w), F32),
            pltpu.VMEM((2, rows, ff_w), F32), pltpu.VMEM((2, rows, d_model), F32),
            pltpu.SemaphoreType.DMA((8,)), pltpu.SemaphoreType.DMA((4, 2))],
        compiler_params=pltpu.CompilerParams(vmem_limit_bytes=67_043_328),
        name="weight_grads",
    )(*acts, red)


def solution(mesh):
    dims = dict(mesh.shape)

    def device_fn(x_in, y_target, w_qkv, w_out, w_up, w_down, norm_gain):
        n_batch, seq_len, d_model = x_in.shape
        heads, head_dim = w_qkv.shape[3], w_qkv.shape[4]
        a, b, d, dm, dqkv, o, zz, du, red = layer_step(
            dims, x_in, y_target,
            w_qkv[0].transpose(1, 2, 0, 3).reshape(3 * heads, d_model, head_dim),
            w_out[0].reshape(heads * head_dim, d_model), w_up[0], w_down[0], norm_gain[0])
        g_out, g_qkv, g_up, g_down, g_gain, loss = weight_grads(
            o, dm, a, dqkv, b, du, zz, d, red, head_dim, 0.5 / (n_batch * seq_len * d_model))
        grad_qkv = g_qkv.reshape(3, heads, d_model, head_dim).transpose(2, 0, 1, 3)[None]
        grad_out = g_out.reshape(1, heads, head_dim, d_model)
        grad_up = g_up[None]
        grad_down = g_down[None]
        return loss.reshape(1), grad_qkv, grad_out, grad_up, grad_down, g_gain[None]

    act_spec = P("data", None, None)
    weight_specs = (
        P("stage", None, None, "model", None),
        P("stage", "model", None, None),
        P("stage", None, "model"),
        P("stage", "model", None),
        P("stage", None, None),
    )
    grad_specs = (
        P(("data", "stage"), None, None, "model", None),
        P(("data", "stage"), "model", None, None),
        P(("data", "stage"), None, "model"),
        P(("data", "stage"), "model", None),
        P(("data", "stage"), None, None),
    )
    return jax.shard_map(
        device_fn,
        mesh=mesh,
        in_specs=(act_spec, act_spec) + weight_specs,
        out_specs=(P("data"),) + grad_specs,
        check_vma=False,
    )
```

```python
import jax
import jax.numpy as jnp
from jax import lax
from jax.experimental import pallas as pl
from jax.experimental.pallas import tpu as pltpu
from jax.sharding import PartitionSpec as P

NORM_EPS = 1e-6
NEG_BIG = -1e30
MESH = pl.DeviceIdType.MESH
GELU_K = 0.7978845608028654
GELU_C = 0.044715
F32 = jnp.float32
BF16 = jnp.bfloat16


def dot_nn(a, b):
    return lax.dot_general(a, b, (((1,), (0,)), ((), ())), preferred_element_type=F32)


def dot_nt(a, b):
    return lax.dot_general(a, b, (((1,), (1,)), ((), ())), preferred_element_type=F32)


def dot_tn(a, b):
    return lax.dot_general(a, b, (((0,), (0,)), ((), ())), preferred_element_type=F32)


def rms_inverse(v32):
    return lax.rsqrt(jnp.mean(v32 * v32, axis=-1, keepdims=True) + NORM_EPS)


ORDER = (
    (1, 6), (0, 3), (1, 2), (0, 7), (0, 9), (0, 5), (1, 3), (0, 8), (1, 9), (0, 1), (1, 1), (1, 7), (0, 0), (0,
    2), (1, 5), (1, 8), (0, 4), (0, 6), (1, 0), (0, 10), (1, 4), (1, 10),
)
BACK_START, BACK_STEP = 13, 10


def lags(back):
    place = {phase: i for i, (is_back, phase) in enumerate(ORDER) if is_back == int(back)}
    lag = [0]
    for phase in range(1, len(place)):
        lag.append(lag[-1] + (1 if place[phase] < place[phase - 1] else 0))
    return lag


def layer_step(dims, x_in, y_target, w_qkv, w_out, w_up, w_down, gain):
    nz, ns = dims["model"], dims["stage"]
    n_seq, seq_len, d_model = x_in.shape
    n_slab, _, head_dim = w_qkv.shape
    qkv_w = n_slab * head_dim
    att_w = w_out.shape[0]
    ff_w = w_up.shape[1]
    n_head = att_w // head_dim
    tok = 64
    n_part = 2
    row = tok // (2 * n_part)
    n_block = 2 * n_part
    per_seq = seq_len // tok
    n_unit = n_seq * per_seq
    scale = head_dim ** -0.5
    inv_count = 1.0 / (n_seq * seq_len * d_model)
    last_z, last_s = nz - 1, ns - 1
    sub_rows = 16
    half = tok // 2
    n_send, n_recv, n_gath, n_hand = 2, 3, 4, 2
    quarters = range(n_part)

    def kernel(x_ref, y_ref, wqkv_h, wout_h, wup_h, wdown_h, gain_ref,
               a_out, b_out, d_out, dm_out, dqkv_out, o_out, z_out, du_out, red_out,
               wqkv, wout, wup, wdown, hslot, yslot, a_all, d_all, bbuf, dmbuf, xtmp,
               qkv_all, u_all, m_all, ost, zst, dust, dqkvst, datt, part,
               recv_o, recv_i, send_p, hout, aout, dout, dkacc, dvacc,
               gains, gain_next, lossacc, ga8, gb8, gx,
               w_sem, hsem, ysem, x_sem, gain_sem, hand_sem, back_sem, save_sem,
               a_rs, d_rs, a_si, a_so, d_si, d_so, b_rs, dm_rs, b_si, b_so, dm_si, dm_so,
               rs_ro, rs_ri, rs_s, loss_sem, gx_s, gx_r):
        z = lax.axis_index("model")
        st = lax.axis_index("stage")
        is_first = st == 0
        is_last = st == last_s
        inner = (z > 0) & (z < last_z)
        outer = (z == 0) | (z == last_z)
        side = lax.div(z, 2)
        near = n_part * side
        far = n_part - near
        inner_peer = 1 + lax.rem(z, 2)
        outer_peer = last_z * side
        my_half = pl.ds(pl.multiple_of(side * half, half), half)

        def rdma(src, dst, ssem, rsem, **dev):
            return pltpu.make_async_remote_copy(src_ref=src, dst_ref=dst, send_sem=ssem, recv_sem=rsem,
                                                device_id=dev, device_id_type=MESH)

        def rows_of(k):
            return pl.ds(pl.multiple_of(k * row, row), row)

        qkv_copies = [pltpu.make_async_copy(wqkv_h.at[i], wqkv.at[:, pl.ds(i * head_dim, head_dim)], w_sem.at[i])
                      for i in range(n_slab)]
        w_copies = [pltpu.make_async_copy(src, dst, w_sem.at[n_slab + i])
                    for i, (src, dst) in enumerate(((wout_h, wout), (wup_h, wup), (wdown_h, wdown)))]

        def tokens_of(u):
            return lax.div(u, per_seq), pl.multiple_of(lax.rem(u, per_seq) * tok, tok)

        def x_copy(u):
            q, first = tokens_of(u)
            return pltpu.make_async_copy(x_ref.at[q, pl.ds(first, tok), :], a_all.at[u], hsem.at[u])

        def x_again(j, u):
            q, first = tokens_of(u)
            slot = lax.rem(j, n_send)
            return pltpu.make_async_copy(x_ref.at[q, pl.ds(first, tok), :], xtmp.at[slot], x_sem.at[slot])

        def y_copy(u):
            q, first = tokens_of(u)
            rs = pl.ds(pl.multiple_of(first + side * half, half), half)
            slot = lax.rem(u, n_hand)
            return pltpu.make_async_copy(y_ref.at[q, rs, :], yslot.at[slot], ysem.at[slot])

        @pl.when(is_first)
        def _():
            @pl.loop(0, n_unit)
            def _(u):
                x_copy(u).start()

        for cp in qkv_copies + w_copies:
            cp.start()

        barrier = pltpu.get_barrier_semaphore()
        for i in range(1, nz * ns):
            dz, dst = i % nz, i // nz
            pl.semaphore_signal(barrier, inc=1, device_id_type=MESH,
                                device_id={"model": lax.rem(z + dz, nz), "stage": lax.rem(st + dst, ns)})
        qkv_all[...] = jnp.zeros_like(qkv_all)
        lossacc[...] = jnp.zeros_like(lossacc)
        ga8[...] = jnp.zeros_like(ga8)
        gb8[...] = jnp.zeros_like(gb8)
        gains[...] = gain_ref[...].astype(F32)
        pl.semaphore_wait(barrier, nz * ns - 1)

        def gain_send():
            return rdma(gains, gain_next, gain_sem.at[0], gain_sem.at[1], stage=st - 1)

        @pl.when(st > 0)
        def _():
            gain_send().start()

        class Gather:
            def __init__(self, buf, slot, rsem, own_sem, far_sem, sslot):
                self.buf, self.slot, self.rsem = buf, slot, rsem
                self.own_sem, self.far_sem = own_sem.at[sslot], far_sem.at[sslot]

            def block(self, k):
                return self.buf.at[self.slot, rows_of(k), :]

            def inward(self, k):
                return rdma(self.block(k), self.block(k), self.own_sem, self.rsem.at[self.slot, k], model=inner_peer)

            def outward(self, k, sem):
                return rdma(self.block(k), self.block(k), sem, self.rsem.at[self.slot, n_block], model=outer_peer)

            def unit(self):
                ref = self.buf.at[self.slot]
                return rdma(ref, ref, self.own_sem, self.rsem.at[self.slot, n_block], model=outer_peer)

            def half_unit(self):
                ref = self.buf.at[self.slot, my_half, :]
                return rdma(ref, ref, self.far_sem, self.rsem.at[self.slot, n_block], model=outer_peer)

            def send(self, q):
                self.inward(near + q).start()
                self.outward(near + q, self.own_sem).start()

            def relay(self):
                @pl.when(inner)
                def _():
                    for q in quarters:
                        self.inward(far + q).wait_recv()
                        self.outward(far + q, self.far_sem).start()

            def collect(self):
                @pl.when(outer)
                def _():
                    self.unit().wait_recv()

            def own(self):
                @pl.when(inner)
                def _():
                    self.half_unit().wait_recv()

            def drain(self):
                @pl.when(inner)
                def _():
                    self.half_unit().wait_send()

            def drain_own(self):
                @pl.when(inner)
                def _():
                    self.unit().wait_send()

        def gather_a(u):
            return Gather(a_all, u, a_rs, a_si, a_so, lax.rem(u, n_gath))

        def gather_d(j, u):
            return Gather(d_all, u, d_rs, d_si, d_so, lax.rem(j, n_gath))

        def gather_b(u):
            return Gather(bbuf, lax.rem(u, n_gath), b_rs, b_si, b_so, lax.rem(u, n_gath))

        def gather_dm(j):
            return Gather(dmbuf, lax.rem(j, n_gath), dm_rs, dm_si, dm_so, lax.rem(j, n_gath))

        class Scatter:
            def __init__(self, op, u):
                self.op, self.ss, self.rs = op, lax.rem(u, n_send), lax.rem(u, n_recv)

            def in_copy(self, k, q):
                return rdma(send_p.at[self.op, self.ss, k], recv_o.at[self.op, self.rs, k],
                            rs_s.at[self.op, self.ss], rs_ro.at[self.op, self.rs, q], model=inner_peer)

            def cross_copy(self, k, q):
                return rdma(send_p.at[self.op, self.ss, k], recv_i.at[self.op, self.rs, q],
                            rs_s.at[self.op, self.ss], rs_ri.at[self.op, self.rs, q], model=inner_peer)

            def near_copies(self):
                return rdma(send_p.at[self.op, self.ss, pl.ds(near, n_part)], recv_o.at[self.op, self.rs, pl.ds(near, n_part)],
                            rs_s.at[self.op, self.ss], rs_ro.at[self.op, self.rs, n_part], model=inner_peer)

            def mine(self, k):
                return part[self.op, self.ss, rows_of(k), :]

            def start(self, j):
                @pl.when(outer)
                def _():
                    @pl.when(j >= n_send)
                    def _():
                        self.drain_outer()

                    for k, q in [(far + q, q) for q in quarters] + [(near + q, n_part) for q in quarters]:
                        send_p[self.op, self.ss, k] = self.mine(k).astype(BF16)
                        self.in_copy(k, q).start()

            def relay(self, j):
                @pl.when(inner)
                def _():
                    @pl.when(j >= n_send)
                    def _():
                        self.drain_inner()

                    for q in quarters:
                        k = far + q
                        self.in_copy(k, q).wait_recv()
                        send_p[self.op, self.ss, k] = (
                            self.mine(k) + recv_o[self.op, self.rs, k].astype(F32)).astype(BF16)
                        self.cross_copy(k, q).start()

            def total(self, q):
                k = near + q
                if q == 0:
                    self.near_copies().wait_recv()
                self.cross_copy(k, q).wait_recv()
                return (self.mine(k) + recv_o[self.op, self.rs, k].astype(F32)) + recv_i[self.op, self.rs, q].astype(F32)

            def drain_outer(self):
                ref = send_p.at[self.op, self.ss]
                rdma(ref, ref, rs_s.at[self.op, self.ss], rs_ro.at[self.op, self.rs, 0], model=inner_peer).wait_send()

            def drain_inner(self):
                self.near_copies().wait_send()

            def drain(self):
                @pl.when(outer)
                def _():
                    self.drain_outer()

                @pl.when(inner)
                def _():
                    self.drain_inner()

        def save(kind, src, src_slot, dst, j, u):
            return pltpu.make_async_copy(src.at[src_slot], dst.at[u],
                                         save_sem.at[kind, lax.rem(j, n_send if kind % 2 else n_gath)])

        def sslot(u):
            return lax.rem(u, n_send)

        def gslot(u):
            return lax.rem(u, n_gath)

        def q_rows(q):
            return pl.ds(q * row, row)

        def save_a(u):
            return save(0, a_all, u, a_out, u, u)

        def save_o(u):
            return save(1, ost, sslot(u), o_out, u, u)

        def save_b(u):
            return save(2, bbuf, gslot(u), b_out, u, u)

        def save_z(u):
            return save(3, zst, sslot(u), z_out, u, u)

        def save_d(j, u):
            return save(4, d_all, u, d_out, j, u)

        def save_du(j, u):
            return save(5, dust, sslot(j), du_out, j, u)

        def save_dm(j, u):
            return save(6, dmbuf, gslot(j), dm_out, j, u)

        def save_dqkv(j, u):
            return save(7, dqkvst, sslot(j), dqkv_out, j, u)

        gain_a = gains[0:1, :]
        gain_b = gains[1:2, :]

        def hand_h(u, j):
            s = lax.rem(j, n_hand)
            return rdma(hout.at[s], hslot.at[u], hand_sem.at[s, 1], hsem.at[u], stage=st + 1)

        def hand_quarter(back, u, j, q):
            s = lax.rem(j, n_hand)
            k = near + q
            src, buf, sems, own = (dout, d_all, d_rs, back_sem) if back else (aout, a_all, a_rs, hand_sem)
            for peer, side_sem, to in ((inner_peer, 0, k), (outer_peer, 0, n_block), (z, 1, n_block)):
                rdma(src.at[s, q_rows(q), :], buf.at[u, rows_of(k), :], own.at[s, side_sem], sems.at[u, to],
                     model=peer, stage=(st - 1) if back else (st + 1)).start()

        def hand_sent(back, u, j):
            s = lax.rem(j, n_hand)
            own = back_sem if back else hand_sem
            whole, part_of = d_all.at[u], hslot.at[u]
            rdma(whole, whole, own.at[s, 0], d_rs.at[u, 0], model=z).wait_send()
            last = part_of if back else whole
            rdma(last, last, own.at[s, 1], d_rs.at[u, 0], model=z).wait_send()

        def softmax_of(u, p, i):
            first = u - p
            cols = pl.ds(i * head_dim, head_dim)
            q = qkv_all[u, :, cols]
            k = qkv_all[pl.ds(first, per_seq), :, pl.ds(att_w + i * head_dim, head_dim)].reshape(seq_len, head_dim)
            v = qkv_all[pl.ds(first, per_seq), :, pl.ds(2 * att_w + i * head_dim, head_dim)].reshape(seq_len, head_dim)
            sc = dot_nt(q, k) * scale
            q_pos = p * tok + lax.broadcasted_iota(jnp.int32, sc.shape, 0)
            k_pos = lax.broadcasted_iota(jnp.int32, sc.shape, 1)
            sc = jnp.where(k_pos <= q_pos, sc, NEG_BIG)
            e = jnp.exp(sc - jnp.max(sc, axis=-1, keepdims=True))
            pr = e * (1.0 / jnp.sum(e, axis=-1, keepdims=True))
            return q, k, v, pr

        def fold(v):
            return jnp.sum(v.reshape(v.shape[0] // 8, 8, d_model), axis=0)

        def f_enter(j, u):
            @pl.when(is_first)
            def _():
                x_copy(u).wait()
                hslot[u] = a_all[u, my_half, :]
                for k in range(n_block):
                    rs = pl.ds(k * row, row)
                    h32 = a_all[u, rs, :].astype(F32)
                    a_all[u, rs, :] = (h32 * rms_inverse(h32) * gain_a).astype(BF16)

        def f_relay_a(j, u):
            @pl.when(st > 0)
            def _():
                @pl.when(j >= n_gath)
                def _():
                    gather_a(u).drain()

                gather_a(u).relay()

        def f_collect_a(j, u):
            @pl.when(st > 0)
            def _():
                gather_a(u).collect()
                gather_a(u).own()

        def f_attention(j, u):
            @pl.when(j == 0)
            def _():
                for cp in qkv_copies:
                    cp.wait()
                w_copies[0].wait()

            @pl.when(j >= n_gath)
            def _():
                save_a(u).wait()
                save_b(u).wait()
                gather_b(u).drain()
                gather_b(u).drain_own()

            @pl.when(j >= n_send)
            def _():
                save_o(u).wait()

            s = sslot(u)
            p = lax.rem(u, per_seq)
            save_a(u).start()
            qkv_all[u] = dot_nn(a_all[u], wqkv[...]).astype(BF16)
            for i in range(n_head):
                _, _, v, pr = softmax_of(u, p, i)
                ost[s, :, pl.ds(i * head_dim, head_dim)] = dot_nn(pr.astype(BF16), v).astype(BF16)
            save_o(u).start()
            part[0, s] = dot_nn(ost[s], wout[...])
            Scatter(0, u).start(j)

        def scatter_relay(op):
            def run(j, u):
                Scatter(op, j).relay(j)
            return run

        def f_middle(j, u):
            sc = Scatter(0, u)

            @pl.when(inner)
            def _():
                @pl.when(st > 0)
                def _():
                    rdma(hout.at[0], hslot.at[u], hand_sem.at[0, 1], hsem.at[u], stage=st).wait_recv()

                for q in quarters:
                    m = hslot[u, q_rows(q), :].astype(F32) + sc.total(q)
                    m_all[u, q_rows(q), :] = m
                    bbuf[gslot(u), rows_of(near + q), :] = (m * rms_inverse(m) * gain_b).astype(BF16)
                    gather_b(u).send(q)

        def f_relay_b(j, u):
            gather_b(u).relay()

        def f_collect_b(j, u):
            gather_b(u).collect()

        def f_mlp(j, u):
            @pl.when(j == 0)
            def _():
                w_copies[1].wait()
                w_copies[2].wait()

            s = sslot(u)
            @pl.when(j >= n_send)
            def _():
                save_z(u).wait()

            save_b(u).start()

            @pl.when(is_last & inner)
            def _():
                y_copy(u).start()

            u_all[u] = dot_nn(bbuf[gslot(u)], wup[...])

            def act(r, carry):
                rr = pl.ds(pl.multiple_of(r * sub_rows, sub_rows), sub_rows)
                v = u_all[u, rr, :]
                th = jnp.tanh(GELU_K * (v + GELU_C * (v * v * v)))
                zst[s, rr, :] = (0.5 * v * (1.0 + th)).astype(BF16)
                return carry

            lax.fori_loop(0, tok // sub_rows, act, 0)
            save_z(u).start()
            part[1, s] = dot_nn(zst[s], wdown[...])
            Scatter(1, u).start(j)

        def f_leave(j, u):
            sc = Scatter(1, u)
            s = lax.rem(j, n_hand)

            @pl.when((j == 0) & (st < last_s))
            def _():
                gain_send().wait_recv()

            @pl.when(inner)
            def _():
                @pl.when(st < last_s)
                def _():
                    @pl.when(j >= n_hand)
                    def _():
                        hand_sent(False, u, j)

                @pl.when(is_last)
                def _():
                    y_copy(u).wait()

                for q in quarters:
                    h_new = (m_all[u, q_rows(q), :] + sc.total(q)).astype(BF16)
                    h32 = h_new.astype(F32)

                    @pl.when(st < last_s)
                    def _():
                        aout[s, q_rows(q), :] = (h32 * rms_inverse(h32) * gain_next[0:1, :]).astype(BF16)
                        hand_quarter(False, u, j, q)
                        hout[s, q_rows(q), :] = h_new

                    @pl.when(is_last)
                    def _():
                        diff = h32 - yslot[lax.rem(u, n_hand), q_rows(q), :].astype(F32)
                        d_all[u, rows_of(near + q), :] = (diff * inv_count).astype(BF16)
                        lossacc[...] += fold(diff * diff)

                @pl.when(st < last_s)
                def _():
                    hand_h(u, j).start()

        forward = (f_enter, f_relay_a, f_collect_a, f_attention, scatter_relay(0), f_middle, f_relay_b, f_collect_b, f_mlp,
                   scatter_relay(1), f_leave)

        def b_enter(j, u):
            @pl.when(is_last & inner)
            def _():
                @pl.when(j >= n_gath)
                def _():
                    gather_d(j, u).drain_own()

                for q in quarters:
                    gather_d(j, u).send(q)

        def b_relay_d(j, u):
            @pl.when(j >= n_gath)
            def _():
                gather_d(j, u).drain()

            gather_d(j, u).relay()

        def b_collect_d(j, u):
            gather_d(j, u).collect()

            @pl.when(st < last_s)
            def _():
                gather_d(j, u).own()

        def b_mlp(j, u):
            @pl.when(j >= n_gath)
            def _():
                save_d(j, u).wait()
                save_dm(j, u).wait()
                gather_dm(j).drain()
                gather_dm(j).drain_own()

            @pl.when(j >= n_send)
            def _():
                save_du(j, u).wait()

            s = sslot(j)
            save_d(j, u).start()
            part[2, s] = dot_nt(d_all[u], wdown[...])

            def act(r, carry):
                rr = pl.ds(pl.multiple_of(r * sub_rows, sub_rows), sub_rows)
                v = u_all[u, rr, :]
                v2 = v * v
                th = jnp.tanh(GELU_K * (v + GELU_C * (v2 * v)))
                slope = 0.5 * (1.0 + th) + 0.5 * v * (1.0 - th * th) * (GELU_K * (1.0 + 3.0 * GELU_C * v2))
                dust[s, rr, :] = (part[2, s, rr, :] * slope).astype(BF16)
                return carry

            lax.fori_loop(0, tok // sub_rows, act, 0)
            save_du(j, u).start()
            part[2, s] = dot_nt(dust[s], wup[...])
            Scatter(2, j).start(j)

        def b_middle(j, u):
            sc = Scatter(2, j)

            @pl.when(inner)
            def _():
                for q in quarters:
                    m = m_all[u, q_rows(q), :]
                    inv = rms_inverse(m)
                    normed = m * inv
                    dn = sc.total(q)
                    gb8[...] += fold(dn * normed)
                    dn = dn * gain_b
                    dm = d_all[u, rows_of(near + q), :].astype(F32) + inv * (
                        dn - normed * jnp.mean(dn * normed, axis=-1, keepdims=True))
                    m_all[u, q_rows(q), :] = dm
                    dmbuf[gslot(j), rows_of(near + q), :] = dm.astype(BF16)
                    gather_dm(j).send(q)

        def b_relay_dm(j, u):
            gather_dm(j).relay()

        def b_collect_dm(j, u):
            gather_dm(j).collect()

        def b_attention(j, u):
            s = sslot(j)
            p = lax.rem(u, per_seq)
            @pl.when(j >= n_send)
            def _():
                save_dqkv(j, u).wait()

            save_dm(j, u).start()

            @pl.when(is_first)
            def _():
                x_again(j, u).start()

            @pl.when(p == per_seq - 1)
            def _():
                dkacc[...] = jnp.zeros_like(dkacc)
                dvacc[...] = jnp.zeros_like(dvacc)

            datt[...] = dot_nt(dmbuf[gslot(j)], wout[...]).astype(BF16)
            p_rows = pl.ds(pl.multiple_of(p * tok, tok), tok)
            for h in range(n_head):
                cols = pl.ds(h * head_dim, head_dim)
                q, k, v, pr = softmax_of(u, p, h)
                da = datt[:, cols]
                dp = dot_nt(da, v)
                ds = (pr * (dp - jnp.sum(pr * dp, axis=-1, keepdims=True)) * scale).astype(BF16)
                dvacc[:, cols] += dot_tn(pr.astype(BF16), da)
                dkacc[:, cols] += dot_tn(ds, q)
                dqkvst[s, :, cols] = dot_nn(ds, k).astype(BF16)
            dqkvst[s, :, pl.ds(att_w, att_w)] = dkacc[p_rows, :].astype(BF16)
            dqkvst[s, :, pl.ds(2 * att_w, att_w)] = dvacc[p_rows, :].astype(BF16)
            save_dqkv(j, u).start()
            part[3, s] = dot_nt(dqkvst[s], wqkv[...])

            @pl.when(st > 0)
            def _():
                Scatter(3, j).start(j)

        def b_relay_h(j, u):
            @pl.when(st > 0)
            def _():
                Scatter(3, j).relay(j)

        def b_leave(j, u):
            s = lax.rem(j, n_hand)

            @pl.when(st > 0)
            def _():
                sc = Scatter(3, j)

                @pl.when(inner)
                def _():
                    @pl.when(j >= n_hand)
                    def _():
                        hand_sent(True, u, j)

                    for q in quarters:
                        h32 = hslot[u, q_rows(q), :].astype(F32)
                        inv = rms_inverse(h32)
                        normed = h32 * inv
                        dn = sc.total(q)
                        ga8[...] += fold(dn * normed)
                        dg = dn * gain_a
                        dout[s, q_rows(q), :] = (m_all[u, q_rows(q), :] + inv * (
                            dg - normed * jnp.mean(dg * normed, axis=-1, keepdims=True))).astype(BF16)
                        hand_quarter(True, u, j, q)

            @pl.when(is_first)
            def _():
                x_again(j, u).wait()
                for k in range(n_block):
                    rs = pl.ds(k * row, row)
                    h32 = xtmp[sslot(j), rs, :].astype(F32)
                    ga8[...] += fold(part[3, sslot(j), rs, :] * (h32 * rms_inverse(h32)))

        backward = (b_enter, b_relay_d, b_collect_d, b_mlp, scatter_relay(2), b_middle, b_relay_dm, b_collect_dm,
                    b_attention, b_relay_h, b_leave)
        f_lag, b_lag = lags(False), lags(True)
        back_from = BACK_START + BACK_STEP * (last_s - st)

        def hand_finish(back):
            @pl.when(inner)
            def _():
                for j in range(n_unit - n_hand, n_unit):
                    hand_sent(back, j, j)

        def finish_forward():
            for j in range(n_unit - n_gath, n_unit):
                save_a(j).wait()
                save_b(j).wait()
                gather_b(j).drain()
                gather_b(j).drain_own()

                @pl.when(st > 0)
                def _():
                    gather_a(j).drain()

            for j in range(n_unit - n_send, n_unit):
                save_o(j).wait()
                save_z(j).wait()
                Scatter(0, j).drain()
                Scatter(1, j).drain()

            @pl.when(st < last_s)
            def _():
                hand_finish(False)

        def finish_backward():
            for j in range(n_unit - n_gath, n_unit):
                save_d(j, j).wait()
                save_dm(j, j).wait()
                gather_dm(j).drain()
                gather_dm(j).drain_own()
                gather_d(j, j).drain()

                @pl.when(is_last)
                def _():
                    gather_d(j, j).drain_own()

            for j in range(n_unit - n_send, n_unit):
                save_du(j, j).wait()
                save_dqkv(j, j).wait()
                Scatter(2, j).drain()

                @pl.when(st > 0)
                def _():
                    Scatter(3, j).drain()

            @pl.when(st > 0)
            def _():
                hand_finish(True)
                gain_send().wait_send()

        def turn(i, carry):
            @pl.when(i == n_unit + f_lag[-1])
            def _():
                finish_forward()

            for back, phase in ORDER:
                j = (i - back_from - b_lag[phase]) if back else (i - f_lag[phase])

                @pl.when((j >= 0) & (j < n_unit))
                def _():
                    if back:
                        seq = lax.div(j, per_seq)
                        backward[phase](j, 2 * seq * per_seq + (per_seq - 1) - j)
                    else:
                        forward[phase](j, j)
            return carry

        lax.fori_loop(0, n_unit + back_from + b_lag[-1], turn, 0)

        def loss_send():
            return rdma(lossacc, lossacc, loss_sem.at[0], loss_sem.at[1], stage=st - 1)

        @pl.when(is_last)
        def _():
            loss_send().start()

        @pl.when(st < last_s)
        def _():
            loss_send().wait_recv()

            @pl.when(st > 0)
            def _():
                loss_send().start()

        loss_row = jnp.sum(jnp.sum(lossacc[...], axis=0, keepdims=True), axis=1, keepdims=True)
        gx[z, 0:1, :] = jnp.sum(ga8[...], axis=0, keepdims=True)
        gx[z, 1:2, :] = jnp.sum(gb8[...], axis=0, keepdims=True)
        gx[z, 2:8, :] = jnp.broadcast_to(loss_row, (6, d_model))

        def gx_send(dz):
            return rdma(gx.at[z], gx.at[z], gx_s.at[dz], gx_r.at[z], model=lax.rem(z + dz, nz))

        def gx_recv(dz):
            k = lax.rem(z + dz, nz)
            return rdma(gx.at[k], gx.at[k], gx_s.at[dz], gx_r.at[k], model=k)

        for dz in range(1, nz):
            gx_send(dz).start()
        finish_backward()

        @pl.when(st > 0)
        def _():
            loss_send().wait_send()

        for dz in range(1, nz):
            gx_recv(dz).wait_recv()
        red_out[...] = gx[0] + gx[1] + gx[2] + gx[3]
        for dz in range(1, nz):
            gx_send(dz).wait_send()

    any_spec = pl.BlockSpec(memory_space=pl.ANY)
    vmem_spec = pl.BlockSpec(memory_space=pltpu.VMEM)

    def out(width):
        return jax.ShapeDtypeStruct((n_unit, tok, width), BF16)

    dma = pltpu.SemaphoreType.DMA
    vmem = pltpu.VMEM
    return pl.pallas_call(
        kernel,
        out_shape=(out(d_model), out(d_model), out(d_model), out(d_model), out(qkv_w), out(att_w), out(ff_w), out(ff_w),
                   jax.ShapeDtypeStruct((8, d_model), F32)),
        in_specs=[any_spec] * 6 + [vmem_spec],
        out_specs=(any_spec,) * 8 + (vmem_spec,),
        scratch_shapes=[
            vmem((d_model, qkv_w), BF16), vmem((att_w, d_model), BF16), vmem((d_model, ff_w), BF16), vmem((ff_w, d_model), BF16),
            vmem((n_unit, half, d_model), BF16), vmem((n_hand, half, d_model), BF16),
            vmem((n_unit, tok, d_model), BF16), vmem((n_unit, tok, d_model), BF16),
            vmem((n_gath, tok, d_model), BF16), vmem((n_gath, tok, d_model), BF16), vmem((n_send, tok, d_model), BF16),
            vmem((n_unit, tok, qkv_w), BF16), vmem((n_unit, tok, ff_w), F32), vmem((n_unit, half, d_model), F32),
            vmem((n_send, tok, att_w), BF16), vmem((n_send, tok, ff_w), BF16), vmem((n_send, tok, ff_w), BF16),
            vmem((n_send, tok, qkv_w), BF16), vmem((tok, att_w), BF16), vmem((4, n_send, tok, d_model), F32),
            vmem((4, n_recv, n_block, row, d_model), BF16), vmem((4, n_recv, n_part, row, d_model), BF16),
            vmem((4, n_send, n_block, row, d_model), BF16),
            vmem((n_hand, half, d_model), BF16), vmem((n_hand, half, d_model), BF16), vmem((n_hand, half, d_model), BF16),
            vmem((seq_len, att_w), F32), vmem((seq_len, att_w), F32),
            vmem((2, d_model), F32), vmem((2, d_model), F32),
            vmem((8, d_model), F32), vmem((8, d_model), F32), vmem((8, d_model), F32), vmem((nz, 8, d_model), F32),
            dma((n_slab + 3,)), dma((n_unit,)), dma((n_hand,)), dma((n_send,)), dma((2,)), dma((n_hand, 2)), dma((n_hand, 2)),
            dma((8, n_gath)),
            dma((n_unit, n_block + 1)), dma((n_unit, n_block + 1)), dma((n_gath,)), dma((n_gath,)), dma((n_gath,)), dma((n_gath,)),
            dma((n_gath, n_block + 1)), dma((n_gath, n_block + 1)),
            dma((n_gath,)), dma((n_gath,)), dma((n_gath,)), dma((n_gath,)),
            dma((4, n_recv, n_part + 1)), dma((4, n_recv, n_part)), dma((4, n_send)),
            dma((2,)), dma((nz,)), dma((nz,)),
        ],
        compiler_params=pltpu.CompilerParams(collective_id=0, has_side_effects=True, vmem_limit_bytes=67_043_328),
        name="layer_step",
    )(x_in, y_target, w_qkv, w_out, w_up, w_down, gain)


def weight_grads(o, dm, a, dqkv, b, du, zz, d, red, head_dim, loss_scale):
    n_tok = o.shape[0] * o.shape[1]
    rows = 256

    def flat(v):
        return v.reshape(n_tok, v.shape[2])

    acts = [flat(v) for v in (o, dm, a, dqkv, b, du, zz, d)]
    att_w, d_model = acts[0].shape[1], acts[1].shape[1]
    qkv_w, ff_w = acts[3].shape[1], acts[5].shape[1]
    n_slab = qkv_w // head_dim

    def kernel(*refs):
        src, red_ref, outs = refs[:8], refs[8], refs[9:13]
        gain_out, loss_out = refs[13:15]
        held, tiles = refs[15:23], refs[23:27]
        in_sem, out_sem = refs[27:]
        loads = [pltpu.make_async_copy(src[i], held[i], in_sem.at[i]) for i in range(8)]
        for cp in loads:
            cp.start()

        def stores(pair, i, slot):
            n = tiles[pair].shape[1]
            at = pl.ds(pl.multiple_of(i * n, n), n)
            sem = out_sem.at[pair, slot]
            if pair == 1:
                return [pltpu.make_async_copy(tiles[1].at[slot, :, pl.ds(k * head_dim, head_dim)], outs[1].at[k, at, :], sem)
                        for k in range(n_slab)]
            return [pltpu.make_async_copy(tiles[pair].at[slot], outs[pair].at[at, :], sem)]

        def finish(cps):
            for cp in cps:
                cp.wait()

        gain_out[...] = red_ref[0:2, :]
        loss_out[...] = red_ref[2:3, 0:1] * loss_scale
        counts = []
        for pair in range(4):
            loads[2 * pair].wait()
            loads[2 * pair + 1].wait()
            left, right, tile = held[2 * pair], held[2 * pair + 1], tiles[pair]
            n = tile.shape[1]
            count = left.shape[1] // n
            counts.append(count)

            def body(i, carry):
                slot = lax.rem(i, 2)

                @pl.when(i >= 2)
                def _():
                    finish(stores(pair, i - 2, slot))

                tile[slot] = dot_tn(left[:, pl.ds(pl.multiple_of(i * n, n), n)], right[...])
                for cp in stores(pair, i, slot):
                    cp.start()
                return carry

            lax.fori_loop(0, count, body, 0)
        for pair in range(4):
            for i in range(max(0, counts[pair] - 2), counts[pair]):
                finish(stores(pair, i, i % 2))

    any_spec = pl.BlockSpec(memory_space=pl.ANY)
    vmem_spec = pl.BlockSpec(memory_space=pltpu.VMEM)
    return pl.pallas_call(
        kernel,
        out_shape=(jax.ShapeDtypeStruct((att_w, d_model), F32), jax.ShapeDtypeStruct((n_slab, d_model, head_dim), F32),
                   jax.ShapeDtypeStruct((d_model, ff_w), F32), jax.ShapeDtypeStruct((ff_w, d_model), F32),
                   jax.ShapeDtypeStruct((2, d_model), F32), jax.ShapeDtypeStruct((1, 1), F32)),
        in_specs=[any_spec] * 8 + [vmem_spec],
        out_specs=(any_spec,) * 4 + (vmem_spec,) * 2,
        scratch_shapes=[pltpu.VMEM(v.shape, BF16) for v in acts] + [
            pltpu.VMEM((1, att_w, d_model), F32), pltpu.VMEM((2, rows, qkv_w), F32),
            pltpu.VMEM((2, rows, ff_w), F32), pltpu.VMEM((2, rows, d_model), F32),
            pltpu.SemaphoreType.DMA((8,)), pltpu.SemaphoreType.DMA((4, 2))],
        compiler_params=pltpu.CompilerParams(vmem_limit_bytes=67_043_328),
        name="weight_grads",
    )(*acts, red)


def solution(mesh):
    dims = dict(mesh.shape)

    def device_fn(x_in, y_target, w_qkv, w_out, w_up, w_down, norm_gain):
        n_batch, seq_len, d_model = x_in.shape
        heads, head_dim = w_qkv.shape[3], w_qkv.shape[4]
        a, b, d, dm, dqkv, o, zz, du, red = layer_step(
            dims, x_in, y_target,
            w_qkv[0].transpose(1, 2, 0, 3).reshape(3 * heads, d_model, head_dim),
            w_out[0].reshape(heads * head_dim, d_model), w_up[0], w_down[0], norm_gain[0])
        g_out, g_qkv, g_up, g_down, g_gain, loss = weight_grads(
            o, dm, a, dqkv, b, du, zz, d, red, head_dim, 0.5 / (n_batch * seq_len * d_model))
        grad_qkv = g_qkv.reshape(3, heads, d_model, head_dim).transpose(2, 0, 1, 3)[None]
        grad_out = g_out.reshape(1, heads, head_dim, d_model)
        grad_up = g_up[None]
        grad_down = g_down[None]
        return loss.reshape(1), grad_qkv, grad_out, grad_up, grad_down, g_gain[None]

    act_spec = P("data", None, None)
    weight_specs = (
        P("stage", None, None, "model", None),
        P("stage", "model", None, None),
        P("stage", None, "model"),
        P("stage", "model", None),
        P("stage", None, None),
    )
    grad_specs = (
        P(("data", "stage"), None, None, "model", None),
        P(("data", "stage"), "model", None, None),
        P(("data", "stage"), None, "model"),
        P(("data", "stage"), "model", None),
        P(("data", "stage"), None, None),
    )
    return jax.shard_map(
        device_fn,
        mesh=mesh,
        in_specs=(act_spec, act_spec) + weight_specs,
        out_specs=(P("data"),) + grad_specs,
        check_vma=False,
    )
```

```python
import jax
import jax.numpy as jnp
from jax import lax
from jax.experimental import pallas as pl
from jax.experimental.pallas import tpu as pltpu
from jax.sharding import PartitionSpec as P

NORM_EPS = 1e-6
NEG_BIG = -1e30
MESH = pl.DeviceIdType.MESH
GELU_K = 0.7978845608028654
GELU_C = 0.044715
F32 = jnp.float32
BF16 = jnp.bfloat16


def dot_nn(a, b):
    return lax.dot_general(a, b, (((1,), (0,)), ((), ())), preferred_element_type=F32)


def dot_nt(a, b):
    return lax.dot_general(a, b, (((1,), (1,)), ((), ())), preferred_element_type=F32)


def dot_tn(a, b):
    return lax.dot_general(a, b, (((0,), (0,)), ((), ())), preferred_element_type=F32)


def rms_inverse(v32):
    return lax.rsqrt(jnp.mean(v32 * v32, axis=-1, keepdims=True) + NORM_EPS)


ORDER = (
    (1, 6), (0, 3), (1, 2), (0, 7), (0, 9), (0, 5), (1, 3), (0, 8), (1, 9), (0, 1), (1, 1), (1, 7), (0, 0), (0,
    2), (1, 5), (1, 8), (0, 4), (0, 6), (1, 0), (0, 10), (1, 4), (1, 10),
)
BACK_START, BACK_STEP = 13, 10


def lags(back):
    place = {phase: i for i, (is_back, phase) in enumerate(ORDER) if is_back == int(back)}
    lag = [0]
    for phase in range(1, len(place)):
        lag.append(lag[-1] + (1 if place[phase] < place[phase - 1] else 0))
    return lag


def layer_step(dims, x_in, y_target, w_qkv, w_out, w_up, w_down, gain):
    nz, ns = dims["model"], dims["stage"]
    n_seq, seq_len, d_model = x_in.shape
    n_slab, _, head_dim = w_qkv.shape
    qkv_w = n_slab * head_dim
    att_w = w_out.shape[0]
    ff_w = w_up.shape[1]
    n_head = att_w // head_dim
    tok = 64
    n_part = 2
    row = tok // (2 * n_part)
    n_block = 2 * n_part
    per_seq = seq_len // tok
    n_unit = n_seq * per_seq
    scale = head_dim ** -0.5
    inv_count = 1.0 / (n_seq * seq_len * d_model)
    last_z, last_s = nz - 1, ns - 1
    sub_rows = 16
    half = tok // 2
    n_send, n_recv, n_gath, n_hand = 2, 3, 4, 2
    quarters = range(n_part)

    def kernel(x_ref, y_ref, wqkv_h, wout_h, wup_h, wdown_h, gain_ref,
               a_out, b_out, d_out, dm_out, dqkv_out, o_out, z_out, du_out, red_out,
               wqkv, wout, wup, wdown, hslot, yslot, a_all, d_all, bbuf, dmbuf, xtmp,
               qkv_all, u_all, m_all, ost, zst, dust, dqkvst, datt, part,
               recv_o, recv_i, send_p, hout, aout, dout, dkacc, dvacc,
               gains, gain_next, lossacc, ga8, gb8, gx,
               w_sem, hsem, ysem, x_sem, gain_sem, hand_sem, back_sem, save_sem,
               a_rs, d_rs, a_si, a_so, d_si, d_so, b_rs, dm_rs, b_si, b_so, dm_si, dm_so,
               rs_ro, rs_ri, rs_s, loss_sem, gx_s, gx_r):
        z = lax.axis_index("model")
        st = lax.axis_index("stage")
        is_first = st == 0
        is_last = st == last_s
        inner = (z > 0) & (z < last_z)
        outer = (z == 0) | (z == last_z)
        side = lax.div(z, 2)
        near = n_part * side
        far = n_part - near
        inner_peer = 1 + lax.rem(z, 2)
        outer_peer = last_z * side
        outer_count = 1 - lax.rem(lax.div(z + 1, 2), 2)
        first_count = lax.div(ns - st, ns)
        my_half = pl.ds(pl.multiple_of(side * half, half), half)

        def rdma(src, dst, ssem, rsem, **dev):
            return pltpu.make_async_remote_copy(src_ref=src, dst_ref=dst, send_sem=ssem, recv_sem=rsem,
                                                device_id=dev, device_id_type=MESH)

        def repeat(count, body):
            def turn(i, carry):
                body(i)
                return carry

            lax.fori_loop(0, count, turn, 0)

        def rows_of(k):
            return pl.ds(pl.multiple_of(k * row, row), row)

        qkv_copies = [pltpu.make_async_copy(wqkv_h.at[i], wqkv.at[:, pl.ds(i * head_dim, head_dim)], w_sem.at[i])
                      for i in range(n_slab)]
        w_copies = [pltpu.make_async_copy(src, dst, w_sem.at[n_slab + i])
                    for i, (src, dst) in enumerate(((wout_h, wout), (wup_h, wup), (wdown_h, wdown)))]

        def tokens_of(u):
            return lax.div(u, per_seq), pl.multiple_of(lax.rem(u, per_seq) * tok, tok)

        def x_copy(u):
            q, first = tokens_of(u)
            return pltpu.make_async_copy(x_ref.at[q, pl.ds(first, tok), :], a_all.at[u], hsem.at[u])

        def x_again(j, u):
            q, first = tokens_of(u)
            slot = lax.rem(j, n_send)
            return pltpu.make_async_copy(x_ref.at[q, pl.ds(first, tok), :], xtmp.at[slot], x_sem.at[slot])

        def y_copy(u):
            q, first = tokens_of(u)
            rs = pl.ds(pl.multiple_of(first + side * half, half), half)
            slot = lax.rem(u, n_hand)
            return pltpu.make_async_copy(y_ref.at[q, rs, :], yslot.at[slot], ysem.at[slot])

        @pl.when(is_first)
        def _():
            for u in range(n_send):
                x_copy(u).start()

        for cp in qkv_copies + w_copies:
            cp.start()

        @pl.when(is_first)
        def _():
            @pl.loop(n_send, n_unit)
            def _(u):
                x_copy(u).start()

        barrier = pltpu.get_barrier_semaphore()
        for i in range(1, nz * ns):
            dz, dst = i % nz, i // nz
            pl.semaphore_signal(barrier, inc=1, device_id_type=MESH,
                                device_id={"model": lax.rem(z + dz, nz), "stage": lax.rem(st + dst, ns)})
        qkv_all[...] = jnp.zeros_like(qkv_all)
        lossacc[...] = jnp.zeros_like(lossacc)
        ga8[...] = jnp.zeros_like(ga8)
        gb8[...] = jnp.zeros_like(gb8)
        gains[...] = gain_ref[...].astype(F32)
        pl.semaphore_wait(barrier, nz * ns - 1)

        def gain_send():
            return rdma(gains, gain_next, gain_sem.at[0], gain_sem.at[1], stage=st - 1)

        @pl.when(st > 0)
        def _():
            gain_send().start()

        class Gather:
            def __init__(self, buf, slot, rsem, own_sem, far_sem, sslot):
                self.buf, self.slot, self.rsem = buf, slot, rsem
                self.own_sem, self.far_sem = own_sem.at[sslot], far_sem.at[sslot]

            def block(self, k):
                return self.buf.at[self.slot, rows_of(k), :]

            def inward(self, k):
                return rdma(self.block(k), self.block(k), self.own_sem, self.rsem.at[self.slot, k], model=inner_peer)

            def outward(self, k, sem):
                return rdma(self.block(k), self.block(k), sem, self.rsem.at[self.slot, n_block], model=outer_peer)

            def unit(self):
                ref = self.buf.at[self.slot]
                return rdma(ref, ref, self.own_sem, self.rsem.at[self.slot, n_block], model=outer_peer)

            def half_unit(self):
                ref = self.buf.at[self.slot, my_half, :]
                return rdma(ref, ref, self.far_sem, self.rsem.at[self.slot, n_block], model=outer_peer)

            def send(self, q):
                self.inward(near + q).start()
                self.outward(near + q, self.own_sem).start()

            def relay(self):
                @pl.when(inner)
                def _():
                    for q in quarters:
                        self.inward(far + q).wait_recv()
                        self.outward(far + q, self.far_sem).start()

            def collect(self):
                @pl.when(outer)
                def _():
                    self.unit().wait_recv()

            def own(self):
                @pl.when(inner)
                def _():
                    self.half_unit().wait_recv()

            def drain(self):
                @pl.when(inner)
                def _():
                    self.half_unit().wait_send()

            def drain_own(self):
                @pl.when(inner)
                def _():
                    self.unit().wait_send()

        def gather_a(u):
            return Gather(a_all, u, a_rs, a_si, a_so, lax.rem(u, n_gath))

        def gather_d(j, u):
            return Gather(d_all, u, d_rs, d_si, d_so, lax.rem(j, n_gath))

        def gather_b(u):
            return Gather(bbuf, lax.rem(u, n_gath), b_rs, b_si, b_so, lax.rem(u, n_gath))

        def gather_dm(j):
            return Gather(dmbuf, lax.rem(j, n_gath), dm_rs, dm_si, dm_so, lax.rem(j, n_gath))

        class Scatter:
            def __init__(self, op, u):
                self.op, self.ss, self.rs = op, lax.rem(u, n_send), lax.rem(u, n_recv)

            def in_copy(self, k, q):
                return rdma(send_p.at[self.op, self.ss, k], recv_o.at[self.op, self.rs, k],
                            rs_s.at[self.op, self.ss], rs_ro.at[self.op, self.rs, q], model=inner_peer)

            def cross_copy(self, k, q):
                return rdma(send_p.at[self.op, self.ss, k], recv_i.at[self.op, self.rs, q],
                            rs_s.at[self.op, self.ss], rs_ri.at[self.op, self.rs, q], model=inner_peer)

            def near_copies(self):
                return rdma(send_p.at[self.op, self.ss, pl.ds(near, n_part)], recv_o.at[self.op, self.rs, pl.ds(near, n_part)],
                            rs_s.at[self.op, self.ss], rs_ro.at[self.op, self.rs, n_part], model=inner_peer)

            def mine(self, k):
                return part[self.op, self.ss, rows_of(k), :]

            def start(self, j):
                @pl.when(outer & (j >= n_send))
                def _():
                    self.drain_outer()

                def send(k, q):
                    send_p[self.op, self.ss, k] = self.mine(k).astype(BF16)
                    self.in_copy(k, q).start()

                repeat(outer_count * n_part, lambda q: send(far + q, q))
                repeat(outer_count * n_part, lambda q: send(near + q, n_part))

            def relay(self, j):
                @pl.when(inner)
                def _():
                    @pl.when(j >= n_send)
                    def _():
                        self.drain_inner()

                    for q in quarters:
                        k = far + q
                        self.in_copy(k, q).wait_recv()
                        send_p[self.op, self.ss, k] = (
                            self.mine(k) + recv_o[self.op, self.rs, k].astype(F32)).astype(BF16)
                        self.cross_copy(k, q).start()

            def total(self, q):
                k = near + q
                if q == 0:
                    self.near_copies().wait_recv()
                self.cross_copy(k, q).wait_recv()
                return (self.mine(k) + recv_o[self.op, self.rs, k].astype(F32)) + recv_i[self.op, self.rs, q].astype(F32)

            def drain_outer(self):
                ref = send_p.at[self.op, self.ss]
                rdma(ref, ref, rs_s.at[self.op, self.ss], rs_ro.at[self.op, self.rs, 0], model=inner_peer).wait_send()

            def drain_inner(self):
                self.near_copies().wait_send()

            def drain(self):
                @pl.when(outer)
                def _():
                    self.drain_outer()

                @pl.when(inner)
                def _():
                    self.drain_inner()

        def save(kind, src, src_slot, dst, j, u):
            return pltpu.make_async_copy(src.at[src_slot], dst.at[u],
                                         save_sem.at[kind, lax.rem(j, n_send if kind % 2 else n_gath)])

        def sslot(u):
            return lax.rem(u, n_send)

        def gslot(u):
            return lax.rem(u, n_gath)

        def q_rows(q):
            return pl.ds(q * row, row)

        def save_a(u):
            return save(0, a_all, u, a_out, u, u)

        def save_o(u):
            return save(1, ost, sslot(u), o_out, u, u)

        def save_b(u):
            return save(2, bbuf, gslot(u), b_out, u, u)

        def save_z(u):
            return save(3, zst, sslot(u), z_out, u, u)

        def save_d(j, u):
            return save(4, d_all, u, d_out, j, u)

        def save_du(j, u):
            return save(5, dust, sslot(j), du_out, j, u)

        def save_dm(j, u):
            return save(6, dmbuf, gslot(j), dm_out, j, u)

        def save_dqkv(j, u):
            return save(7, dqkvst, sslot(j), dqkv_out, j, u)

        gain_a = gains[0:1, :]
        gain_b = gains[1:2, :]

        def hand_h(u, j):
            s = lax.rem(j, n_hand)
            return rdma(hout.at[s], hslot.at[u], hand_sem.at[s, 1], hsem.at[u], stage=st + 1)

        def hand_quarter(back, u, j, q):
            s = lax.rem(j, n_hand)
            k = near + q
            src, buf, sems, own = (dout, d_all, d_rs, back_sem) if back else (aout, a_all, a_rs, hand_sem)
            for peer, side_sem, to in ((inner_peer, 0, k), (outer_peer, 0, n_block), (z, 1, n_block)):
                rdma(src.at[s, q_rows(q), :], buf.at[u, rows_of(k), :], own.at[s, side_sem], sems.at[u, to],
                     model=peer, stage=(st - 1) if back else (st + 1)).start()

        def hand_sent(back, u, j):
            s = lax.rem(j, n_hand)
            own = back_sem if back else hand_sem
            whole, part_of = d_all.at[u], hslot.at[u]
            rdma(whole, whole, own.at[s, 0], d_rs.at[u, 0], model=z).wait_send()
            last = part_of if back else whole
            rdma(last, last, own.at[s, 1], d_rs.at[u, 0], model=z).wait_send()

        def softmax_of(u, p, i):
            first = u - p
            cols = pl.ds(i * head_dim, head_dim)
            q = qkv_all[u, :, cols]
            k = qkv_all[pl.ds(first, per_seq), :, pl.ds(att_w + i * head_dim, head_dim)].reshape(seq_len, head_dim)
            v = qkv_all[pl.ds(first, per_seq), :, pl.ds(2 * att_w + i * head_dim, head_dim)].reshape(seq_len, head_dim)
            sc = dot_nt(q, k) * scale
            q_pos = p * tok + lax.broadcasted_iota(jnp.int32, sc.shape, 0)
            k_pos = lax.broadcasted_iota(jnp.int32, sc.shape, 1)
            sc = jnp.where(k_pos <= q_pos, sc, NEG_BIG)
            e = jnp.exp(sc - jnp.max(sc, axis=-1, keepdims=True))
            pr = e * (1.0 / jnp.sum(e, axis=-1, keepdims=True))
            return q, k, v, pr

        def fold(v):
            return jnp.sum(v.reshape(v.shape[0] // 8, 8, d_model), axis=0)

        def f_enter(j, u):
            @pl.when(is_first)
            def _():
                x_copy(u).wait()

            def keep(i):
                hslot[u] = a_all[u, my_half, :]

            def norm(k):
                h32 = a_all[u, rows_of(k), :].astype(F32)
                a_all[u, rows_of(k), :] = (h32 * rms_inverse(h32) * gain_a).astype(BF16)

            repeat(first_count, keep)
            repeat(first_count * n_block, norm)

        def f_relay_a(j, u):
            @pl.when(st > 0)
            def _():
                @pl.when(j >= n_gath)
                def _():
                    gather_a(u).drain()

                gather_a(u).relay()

        def f_collect_a(j, u):
            @pl.when(st > 0)
            def _():
                gather_a(u).collect()
                gather_a(u).own()

        def f_attention(j, u):
            @pl.when(j == 0)
            def _():
                for cp in qkv_copies:
                    cp.wait()
                w_copies[0].wait()

            @pl.when(j >= n_gath)
            def _():
                save_a(u).wait()
                save_b(u).wait()
                gather_b(u).drain()
                gather_b(u).drain_own()

            @pl.when(j >= n_send)
            def _():
                save_o(u).wait()

            s = sslot(u)
            p = lax.rem(u, per_seq)
            save_a(u).start()
            qkv_all[u] = dot_nn(a_all[u], wqkv[...]).astype(BF16)
            for i in range(n_head):
                _, _, v, pr = softmax_of(u, p, i)
                ost[s, :, pl.ds(i * head_dim, head_dim)] = dot_nn(pr.astype(BF16), v).astype(BF16)
            save_o(u).start()
            part[0, s] = dot_nn(ost[s], wout[...])
            Scatter(0, u).start(j)

        def scatter_relay(op):
            def run(j, u):
                Scatter(op, j).relay(j)
            return run

        def f_middle(j, u):
            sc = Scatter(0, u)

            @pl.when(inner)
            def _():
                @pl.when(st > 0)
                def _():
                    rdma(hout.at[0], hslot.at[u], hand_sem.at[0, 1], hsem.at[u], stage=st).wait_recv()

                for q in quarters:
                    m = hslot[u, q_rows(q), :].astype(F32) + sc.total(q)
                    m_all[u, q_rows(q), :] = m
                    bbuf[gslot(u), rows_of(near + q), :] = (m * rms_inverse(m) * gain_b).astype(BF16)
                    gather_b(u).send(q)

        def f_relay_b(j, u):
            gather_b(u).relay()

        def f_collect_b(j, u):
            gather_b(u).collect()

        def f_mlp(j, u):
            @pl.when(j == 0)
            def _():
                w_copies[1].wait()
                w_copies[2].wait()

            s = sslot(u)
            @pl.when(j >= n_send)
            def _():
                save_z(u).wait()

            save_b(u).start()

            @pl.when(is_last & inner)
            def _():
                y_copy(u).start()

            u_all[u] = dot_nn(bbuf[gslot(u)], wup[...])

            def act(r, carry):
                rr = pl.ds(pl.multiple_of(r * sub_rows, sub_rows), sub_rows)
                v = u_all[u, rr, :]
                th = jnp.tanh(GELU_K * (v + GELU_C * (v * v * v)))
                zst[s, rr, :] = (0.5 * v * (1.0 + th)).astype(BF16)
                return carry

            lax.fori_loop(0, tok // sub_rows, act, 0)
            save_z(u).start()
            part[1, s] = dot_nn(zst[s], wdown[...])
            Scatter(1, u).start(j)

        def f_leave(j, u):
            sc = Scatter(1, u)
            s = lax.rem(j, n_hand)

            @pl.when((j == 0) & (st < last_s))
            def _():
                gain_send().wait_recv()

            @pl.when(inner)
            def _():
                @pl.when(st < last_s)
                def _():
                    @pl.when(j >= n_hand)
                    def _():
                        hand_sent(False, u, j)

                @pl.when(is_last)
                def _():
                    y_copy(u).wait()

                for q in quarters:
                    h_new = (m_all[u, q_rows(q), :] + sc.total(q)).astype(BF16)
                    h32 = h_new.astype(F32)

                    @pl.when(st < last_s)
                    def _():
                        aout[s, q_rows(q), :] = (h32 * rms_inverse(h32) * gain_next[0:1, :]).astype(BF16)
                        hand_quarter(False, u, j, q)
                        hout[s, q_rows(q), :] = h_new

                    @pl.when(is_last)
                    def _():
                        diff = h32 - yslot[lax.rem(u, n_hand), q_rows(q), :].astype(F32)
                        d_all[u, rows_of(near + q), :] = (diff * inv_count).astype(BF16)
                        lossacc[...] += fold(diff * diff)

                @pl.when(st < last_s)
                def _():
                    hand_h(u, j).start()

        forward = (f_enter, f_relay_a, f_collect_a, f_attention, scatter_relay(0), f_middle, f_relay_b, f_collect_b, f_mlp,
                   scatter_relay(1), f_leave)

        def b_enter(j, u):
            @pl.when(is_last & inner)
            def _():
                @pl.when(j >= n_gath)
                def _():
                    gather_d(j, u).drain_own()

                for q in quarters:
                    gather_d(j, u).send(q)

        def b_relay_d(j, u):
            @pl.when(j >= n_gath)
            def _():
                gather_d(j, u).drain()

            gather_d(j, u).relay()

        def b_collect_d(j, u):
            gather_d(j, u).collect()

            @pl.when(st < last_s)
            def _():
                gather_d(j, u).own()

        def b_mlp(j, u):
            @pl.when(j >= n_gath)
            def _():
                save_d(j, u).wait()
                save_dm(j, u).wait()
                gather_dm(j).drain()
                gather_dm(j).drain_own()

            @pl.when(j >= n_send)
            def _():
                save_du(j, u).wait()

            s = sslot(j)
            save_d(j, u).start()
            part[2, s] = dot_nt(d_all[u], wdown[...])

            def act(r, carry):
                rr = pl.ds(pl.multiple_of(r * sub_rows, sub_rows), sub_rows)
                v = u_all[u, rr, :]
                v2 = v * v
                th = jnp.tanh(GELU_K * (v + GELU_C * (v2 * v)))
                slope = 0.5 * (1.0 + th) + 0.5 * v * (1.0 - th * th) * (GELU_K * (1.0 + 3.0 * GELU_C * v2))
                dust[s, rr, :] = (part[2, s, rr, :] * slope).astype(BF16)
                return carry

            lax.fori_loop(0, tok // sub_rows, act, 0)
            save_du(j, u).start()
            part[2, s] = dot_nt(dust[s], wup[...])
            Scatter(2, j).start(j)

        def b_middle(j, u):
            sc = Scatter(2, j)

            @pl.when(inner)
            def _():
                for q in quarters:
                    m = m_all[u, q_rows(q), :]
                    inv = rms_inverse(m)
                    normed = m * inv
                    dn = sc.total(q)
                    gb8[...] += fold(dn * normed)
                    dn = dn * gain_b
                    dm = d_all[u, rows_of(near + q), :].astype(F32) + inv * (
                        dn - normed * jnp.mean(dn * normed, axis=-1, keepdims=True))
                    m_all[u, q_rows(q), :] = dm
                    dmbuf[gslot(j), rows_of(near + q), :] = dm.astype(BF16)
                    gather_dm(j).send(q)

        def b_relay_dm(j, u):
            gather_dm(j).relay()

        def b_collect_dm(j, u):
            gather_dm(j).collect()

        def b_attention(j, u):
            s = sslot(j)
            p = lax.rem(u, per_seq)
            @pl.when(j >= n_send)
            def _():
                save_dqkv(j, u).wait()

            save_dm(j, u).start()

            @pl.when(is_first)
            def _():
                x_again(j, u).start()

            @pl.when(p == per_seq - 1)
            def _():
                dkacc[...] = jnp.zeros_like(dkacc)
                dvacc[...] = jnp.zeros_like(dvacc)

            datt[...] = dot_nt(dmbuf[gslot(j)], wout[...]).astype(BF16)
            p_rows = pl.ds(pl.multiple_of(p * tok, tok), tok)
            for h in range(n_head):
                cols = pl.ds(h * head_dim, head_dim)
                q, k, v, pr = softmax_of(u, p, h)
                da = datt[:, cols]
                dp = dot_nt(da, v)
                ds = (pr * (dp - jnp.sum(pr * dp, axis=-1, keepdims=True)) * scale).astype(BF16)
                dvacc[:, cols] += dot_tn(pr.astype(BF16), da)
                dkacc[:, cols] += dot_tn(ds, q)
                dqkvst[s, :, cols] = dot_nn(ds, k).astype(BF16)
            dqkvst[s, :, pl.ds(att_w, att_w)] = dkacc[p_rows, :].astype(BF16)
            dqkvst[s, :, pl.ds(2 * att_w, att_w)] = dvacc[p_rows, :].astype(BF16)
            save_dqkv(j, u).start()
            part[3, s] = dot_nt(dqkvst[s], wqkv[...])

            @pl.when(st > 0)
            def _():
                Scatter(3, j).start(j)

        def b_relay_h(j, u):
            @pl.when(st > 0)
            def _():
                Scatter(3, j).relay(j)

        def b_leave(j, u):
            s = lax.rem(j, n_hand)

            @pl.when(st > 0)
            def _():
                sc = Scatter(3, j)

                @pl.when(inner)
                def _():
                    @pl.when(j >= n_hand)
                    def _():
                        hand_sent(True, u, j)

                    for q in quarters:
                        h32 = hslot[u, q_rows(q), :].astype(F32)
                        inv = rms_inverse(h32)
                        normed = h32 * inv
                        dn = sc.total(q)
                        ga8[...] += fold(dn * normed)
                        dg = dn * gain_a
                        dout[s, q_rows(q), :] = (m_all[u, q_rows(q), :] + inv * (
                            dg - normed * jnp.mean(dg * normed, axis=-1, keepdims=True))).astype(BF16)
                        hand_quarter(True, u, j, q)

            @pl.when(is_first)
            def _():
                x_again(j, u).wait()

            def gain_rows(k):
                h32 = xtmp[sslot(j), rows_of(k), :].astype(F32)
                ga8[...] += fold(part[3, sslot(j), rows_of(k), :] * (h32 * rms_inverse(h32)))

            repeat(first_count * n_block, gain_rows)

        backward = (b_enter, b_relay_d, b_collect_d, b_mlp, scatter_relay(2), b_middle, b_relay_dm, b_collect_dm,
                    b_attention, b_relay_h, b_leave)
        f_lag, b_lag = lags(False), lags(True)
        back_from = BACK_START + BACK_STEP * (last_s - st)

        def hand_finish(back):
            @pl.when(inner)
            def _():
                for j in range(n_unit - n_hand, n_unit):
                    hand_sent(back, j, j)

        def finish_forward():
            for j in range(n_unit - n_gath, n_unit):
                save_a(j).wait()
                save_b(j).wait()
                gather_b(j).drain()
                gather_b(j).drain_own()

                @pl.when(st > 0)
                def _():
                    gather_a(j).drain()

            for j in range(n_unit - n_send, n_unit):
                save_o(j).wait()
                save_z(j).wait()
                Scatter(0, j).drain()
                Scatter(1, j).drain()

            @pl.when(st < last_s)
            def _():
                hand_finish(False)

        def finish_backward():
            for j in range(n_unit - n_gath, n_unit):
                save_d(j, j).wait()
                save_dm(j, j).wait()
                gather_dm(j).drain()
                gather_dm(j).drain_own()
                gather_d(j, j).drain()

                @pl.when(is_last)
                def _():
                    gather_d(j, j).drain_own()

            for j in range(n_unit - n_send, n_unit):
                save_du(j, j).wait()
                save_dqkv(j, j).wait()
                Scatter(2, j).drain()

                @pl.when(st > 0)
                def _():
                    Scatter(3, j).drain()

            @pl.when(st > 0)
            def _():
                hand_finish(True)
                gain_send().wait_send()

        def turn(i, carry):
            @pl.when(i == n_unit + f_lag[-1])
            def _():
                finish_forward()

            for back, phase in ORDER:
                j = (i - back_from - b_lag[phase]) if back else (i - f_lag[phase])

                @pl.when((j >= 0) & (j < n_unit))
                def _():
                    if back:
                        seq = lax.div(j, per_seq)
                        backward[phase](j, 2 * seq * per_seq + (per_seq - 1) - j)
                    else:
                        forward[phase](j, j)
            return carry

        lax.fori_loop(0, n_unit + back_from + b_lag[-1], turn, 0)

        def loss_send():
            return rdma(lossacc, lossacc, loss_sem.at[0], loss_sem.at[1], stage=st - 1)

        @pl.when(is_last)
        def _():
            loss_send().start()

        @pl.when(st < last_s)
        def _():
            loss_send().wait_recv()

            @pl.when(st > 0)
            def _():
                loss_send().start()

        loss_row = jnp.sum(jnp.sum(lossacc[...], axis=0, keepdims=True), axis=1, keepdims=True)
        gx[z, 0:1, :] = jnp.sum(ga8[...], axis=0, keepdims=True)
        gx[z, 1:2, :] = jnp.sum(gb8[...], axis=0, keepdims=True)
        gx[z, 2:8, :] = jnp.broadcast_to(loss_row, (6, d_model))

        def gx_send(dz):
            return rdma(gx.at[z], gx.at[z], gx_s.at[dz], gx_r.at[z], model=lax.rem(z + dz, nz))

        def gx_recv(dz):
            k = lax.rem(z + dz, nz)
            return rdma(gx.at[k], gx.at[k], gx_s.at[dz], gx_r.at[k], model=k)

        for dz in range(1, nz):
            gx_send(dz).start()
        finish_backward()

        @pl.when(st > 0)
        def _():
            loss_send().wait_send()

        for dz in range(1, nz):
            gx_recv(dz).wait_recv()
        red_out[...] = gx[0] + gx[1] + gx[2] + gx[3]
        for dz in range(1, nz):
            gx_send(dz).wait_send()

    any_spec = pl.BlockSpec(memory_space=pl.ANY)
    vmem_spec = pl.BlockSpec(memory_space=pltpu.VMEM)

    def out(width):
        return jax.ShapeDtypeStruct((n_unit, tok, width), BF16)

    dma = pltpu.SemaphoreType.DMA
    vmem = pltpu.VMEM
    return pl.pallas_call(
        kernel,
        out_shape=(out(d_model), out(d_model), out(d_model), out(d_model), out(qkv_w), out(att_w), out(ff_w), out(ff_w),
                   jax.ShapeDtypeStruct((8, d_model), F32)),
        in_specs=[any_spec] * 6 + [vmem_spec],
        out_specs=(any_spec,) * 8 + (vmem_spec,),
        scratch_shapes=[
            vmem((d_model, qkv_w), BF16), vmem((att_w, d_model), BF16), vmem((d_model, ff_w), BF16), vmem((ff_w, d_model), BF16),
            vmem((n_unit, half, d_model), BF16), vmem((n_hand, half, d_model), BF16),
            vmem((n_unit, tok, d_model), BF16), vmem((n_unit, tok, d_model), BF16),
            vmem((n_gath, tok, d_model), BF16), vmem((n_gath, tok, d_model), BF16), vmem((n_send, tok, d_model), BF16),
            vmem((n_unit, tok, qkv_w), BF16), vmem((n_unit, tok, ff_w), F32), vmem((n_unit, half, d_model), F32),
            vmem((n_send, tok, att_w), BF16), vmem((n_send, tok, ff_w), BF16), vmem((n_send, tok, ff_w), BF16),
            vmem((n_send, tok, qkv_w), BF16), vmem((tok, att_w), BF16), vmem((4, n_send, tok, d_model), F32),
            vmem((4, n_recv, n_block, row, d_model), BF16), vmem((4, n_recv, n_part, row, d_model), BF16),
            vmem((4, n_send, n_block, row, d_model), BF16),
            vmem((n_hand, half, d_model), BF16), vmem((n_hand, half, d_model), BF16), vmem((n_hand, half, d_model), BF16),
            vmem((seq_len, att_w), F32), vmem((seq_len, att_w), F32),
            vmem((2, d_model), F32), vmem((2, d_model), F32),
            vmem((8, d_model), F32), vmem((8, d_model), F32), vmem((8, d_model), F32), vmem((nz, 8, d_model), F32),
            dma((n_slab + 3,)), dma((n_unit,)), dma((n_hand,)), dma((n_send,)), dma((2,)), dma((n_hand, 2)), dma((n_hand, 2)),
            dma((8, n_gath)),
            dma((n_unit, n_block + 1)), dma((n_unit, n_block + 1)), dma((n_gath,)), dma((n_gath,)), dma((n_gath,)), dma((n_gath,)),
            dma((n_gath, n_block + 1)), dma((n_gath, n_block + 1)),
            dma((n_gath,)), dma((n_gath,)), dma((n_gath,)), dma((n_gath,)),
            dma((4, n_recv, n_part + 1)), dma((4, n_recv, n_part)), dma((4, n_send)),
            dma((2,)), dma((nz,)), dma((nz,)),
        ],
        compiler_params=pltpu.CompilerParams(collective_id=0, has_side_effects=True, vmem_limit_bytes=67_043_328),
        name="layer_step",
    )(x_in, y_target, w_qkv, w_out, w_up, w_down, gain)


def weight_grads(o, dm, a, dqkv, b, du, zz, d, red, head_dim, loss_scale):
    n_tok = o.shape[0] * o.shape[1]
    rows, n_piece = 256, 3

    def flat(v):
        return v.reshape(n_tok, v.shape[2])

    acts = [flat(v) for v in (o, dm, a, dqkv, b, du, zz, d)]
    att_w, d_model = acts[0].shape[1], acts[1].shape[1]
    qkv_w, ff_w = acts[3].shape[1], acts[5].shape[1]
    n_slab = qkv_w // head_dim

    def kernel(*refs):
        src, red_ref, outs = refs[:8], refs[8], refs[9:13]
        gain_out, loss_out = refs[13:15]
        held, tiles = refs[15:23], refs[23:27]
        in_sem, out_sem = refs[27:]
        piece = n_tok // n_piece
        first = [[pltpu.make_async_copy(src[i].at[pl.ds(c * piece, piece), :], held[i].at[pl.ds(c * piece, piece), :],
                                        in_sem.at[8 + 2 * c + i]) for i in range(2)] for c in range(n_piece)]
        loads = [pltpu.make_async_copy(src[i], held[i], in_sem.at[i]) for i in range(2, 8)]
        for cp in sum(first, []) + loads:
            cp.start()

        def stores(pair, i, slot):
            n = tiles[pair].shape[1]
            at = pl.ds(pl.multiple_of(i * n, n), n)
            sem = out_sem.at[pair, slot]
            if pair == 1:
                return [pltpu.make_async_copy(tiles[1].at[slot, :, pl.ds(k * head_dim, head_dim)], outs[1].at[k, at, :], sem)
                        for k in range(n_slab)]
            return [pltpu.make_async_copy(tiles[pair].at[slot], outs[pair].at[at, :], sem)]

        def finish(cps):
            for cp in cps:
                cp.wait()

        gain_out[...] = red_ref[0:2, :]
        loss_out[...] = red_ref[2:3, 0:1] * loss_scale
        counts = []
        for c in range(n_piece):
            at = pl.ds(c * piece, piece)
            for cp in first[c]:
                cp.wait()
            sums = dot_tn(held[0][at, :], held[1][at, :])
            tiles[0][0] = sums if c == 0 else tiles[0][0] + sums
        for cp in stores(0, 0, 0):
            cp.start()
        counts.append(1)
        for pair in range(1, 4):
            loads[2 * pair - 2].wait()
            loads[2 * pair - 1].wait()
            left, right, tile = held[2 * pair], held[2 * pair + 1], tiles[pair]
            n = tile.shape[1]
            count = left.shape[1] // n
            counts.append(count)

            def body(i, carry):
                slot = lax.rem(i, 2)

                @pl.when(i >= 2)
                def _():
                    finish(stores(pair, i - 2, slot))

                tile[slot] = dot_tn(left[:, pl.ds(pl.multiple_of(i * n, n), n)], right[...])
                for cp in stores(pair, i, slot):
                    cp.start()
                return carry

            lax.fori_loop(0, count, body, 0)
        for pair in range(4):
            for i in range(max(0, counts[pair] - 2), counts[pair]):
                finish(stores(pair, i, i % 2))

    any_spec = pl.BlockSpec(memory_space=pl.ANY)
    vmem_spec = pl.BlockSpec(memory_space=pltpu.VMEM)
    return pl.pallas_call(
        kernel,
        out_shape=(jax.ShapeDtypeStruct((att_w, d_model), F32), jax.ShapeDtypeStruct((n_slab, d_model, head_dim), F32),
                   jax.ShapeDtypeStruct((d_model, ff_w), F32), jax.ShapeDtypeStruct((ff_w, d_model), F32),
                   jax.ShapeDtypeStruct((2, d_model), F32), jax.ShapeDtypeStruct((1, 1), F32)),
        in_specs=[any_spec] * 8 + [vmem_spec],
        out_specs=(any_spec,) * 4 + (vmem_spec,) * 2,
        scratch_shapes=[pltpu.VMEM(v.shape, BF16) for v in acts] + [
            pltpu.VMEM((1, att_w, d_model), F32), pltpu.VMEM((2, rows, qkv_w), F32),
            pltpu.VMEM((2, rows, ff_w), F32), pltpu.VMEM((2, rows, d_model), F32),
            pltpu.SemaphoreType.DMA((8 + 2 * n_piece,)), pltpu.SemaphoreType.DMA((4, 2))],
        compiler_params=pltpu.CompilerParams(vmem_limit_bytes=67_043_328),
        name="weight_grads",
    )(*acts, red)


def solution(mesh):
    dims = dict(mesh.shape)

    def device_fn(x_in, y_target, w_qkv, w_out, w_up, w_down, norm_gain):
        n_batch, seq_len, d_model = x_in.shape
        heads, head_dim = w_qkv.shape[3], w_qkv.shape[4]
        a, b, d, dm, dqkv, o, zz, du, red = layer_step(
            dims, x_in, y_target,
            w_qkv[0].transpose(1, 2, 0, 3).reshape(3 * heads, d_model, head_dim),
            w_out[0].reshape(heads * head_dim, d_model), w_up[0], w_down[0], norm_gain[0])
        g_out, g_qkv, g_up, g_down, g_gain, loss = weight_grads(
            o, dm, a, dqkv, b, du, zz, d, red, head_dim, 0.5 / (n_batch * seq_len * d_model))
        grad_qkv = g_qkv.reshape(3, heads, d_model, head_dim).transpose(2, 0, 1, 3)[None]
        grad_out = g_out.reshape(1, heads, head_dim, d_model)
        grad_up = g_up[None]
        grad_down = g_down[None]
        return loss.reshape(1), grad_qkv, grad_out, grad_up, grad_down, g_gain[None]

    act_spec = P("data", None, None)
    weight_specs = (
        P("stage", None, None, "model", None),
        P("stage", "model", None, None),
        P("stage", None, "model"),
        P("stage", "model", None),
        P("stage", None, None),
    )
    grad_specs = (
        P(("data", "stage"), None, None, "model", None),
        P(("data", "stage"), "model", None, None),
        P(("data", "stage"), None, "model"),
        P(("data", "stage"), "model", None),
        P(("data", "stage"), None, None),
    )
    return jax.shard_map(
        device_fn,
        mesh=mesh,
        in_specs=(act_spec, act_spec) + weight_specs,
        out_specs=(P("data"),) + grad_specs,
        check_vma=False,
    )
```

```python
import jax
import jax.numpy as jnp
from jax import lax
from jax.experimental import pallas as pl
from jax.experimental.pallas import tpu as pltpu
from jax.sharding import PartitionSpec as P

NORM_EPS = 1e-6
NEG_BIG = -1e30
MESH = pl.DeviceIdType.MESH
GELU_K = 0.7978845608028654
GELU_C = 0.044715
F32 = jnp.float32
BF16 = jnp.bfloat16


def dot_nn(a, b):
    return lax.dot_general(a, b, (((1,), (0,)), ((), ())), preferred_element_type=F32)


def dot_nt(a, b):
    return lax.dot_general(a, b, (((1,), (1,)), ((), ())), preferred_element_type=F32)


def dot_tn(a, b):
    return lax.dot_general(a, b, (((0,), (0,)), ((), ())), preferred_element_type=F32)


def rms_inverse(v32):
    return lax.rsqrt(jnp.mean(v32 * v32, axis=-1, keepdims=True) + NORM_EPS)


ORDER = (
    (1, 6), (0, 3), (1, 2), (0, 7), (0, 9), (0, 5), (1, 3), (0, 8), (1, 9), (0, 1), (1, 1), (1, 7), (0, 0), (0,
    2), (1, 5), (1, 8), (0, 4), (0, 6), (1, 0), (0, 10), (1, 4), (1, 10),
)
BACK_START, BACK_STEP = 13, 10


def lags(back):
    place = {phase: i for i, (is_back, phase) in enumerate(ORDER) if is_back == int(back)}
    lag = [0]
    for phase in range(1, len(place)):
        lag.append(lag[-1] + (1 if place[phase] < place[phase - 1] else 0))
    return lag


def layer_step(dims, x_in, y_target, w_qkv, w_out, w_up, w_down, gain):
    nz, ns = dims["model"], dims["stage"]
    n_seq, seq_len, d_model = x_in.shape
    n_slab, _, head_dim = w_qkv.shape
    qkv_w = n_slab * head_dim
    att_w = w_out.shape[0]
    ff_w = w_up.shape[1]
    n_head = att_w // head_dim
    tok = 64
    n_part = 2
    row = tok // (2 * n_part)
    n_block = 2 * n_part
    per_seq = seq_len // tok
    n_unit = n_seq * per_seq
    scale = head_dim ** -0.5
    inv_count = 1.0 / (n_seq * seq_len * d_model)
    last_z, last_s = nz - 1, ns - 1
    sub_rows = 16
    half = tok // 2
    n_send, n_recv, n_gath, n_hand = 2, 3, 4, 2
    quarters = range(n_part)

    def kernel(x_ref, y_ref, wqkv_h, wout_h, wup_h, wdown_h, gain_ref,
               a_out, b_out, d_out, dm_out, dqkv_out, o_out, z_out, du_out, red_out,
               wqkv, wout, wup, wdown, hslot, yslot, a_all, d_all, bbuf, dmbuf, xtmp,
               qkv_all, u_all, m_all, ost, zst, dust, dqkvst, datt, part,
               recv_o, recv_i, send_p, hout, aout, dout, dkacc, dvacc,
               gains, gain_next, lossacc, ga8, gb8, gx,
               w_sem, hsem, ysem, x_sem, gain_sem, hand_sem, back_sem, save_sem,
               a_rs, d_rs, a_si, a_so, d_si, d_so, b_rs, dm_rs, b_si, b_so, dm_si, dm_so,
               rs_ro, rs_ri, rs_s, loss_sem, gx_s, gx_r):
        z = lax.axis_index("model")
        st = lax.axis_index("stage")
        is_first = st == 0
        is_last = st == last_s
        inner = (z > 0) & (z < last_z)
        outer = (z == 0) | (z == last_z)
        side = lax.div(z, 2)
        near = n_part * side
        far = n_part - near
        inner_peer = 1 + lax.rem(z, 2)
        outer_peer = last_z * side
        my_half = pl.ds(pl.multiple_of(side * half, half), half)

        def rdma(src, dst, ssem, rsem, **dev):
            return pltpu.make_async_remote_copy(src_ref=src, dst_ref=dst, send_sem=ssem, recv_sem=rsem,
                                                device_id=dev, device_id_type=MESH)

        def rows_of(k):
            return pl.ds(pl.multiple_of(k * row, row), row)

        qkv_copies = [pltpu.make_async_copy(wqkv_h.at[i], wqkv.at[:, pl.ds(i * head_dim, head_dim)], w_sem.at[i])
                      for i in range(n_slab)]
        w_copies = [pltpu.make_async_copy(src, dst, w_sem.at[n_slab + i])
                    for i, (src, dst) in enumerate(((wout_h, wout), (wup_h, wup), (wdown_h, wdown)))]

        def tokens_of(u):
            return lax.div(u, per_seq), pl.multiple_of(lax.rem(u, per_seq) * tok, tok)

        def x_copy(u):
            q, first = tokens_of(u)
            return pltpu.make_async_copy(x_ref.at[q, pl.ds(first, tok), :], a_all.at[u], hsem.at[u])

        def x_again(j, u):
            q, first = tokens_of(u)
            slot = lax.rem(j, n_send)
            return pltpu.make_async_copy(x_ref.at[q, pl.ds(first, tok), :], xtmp.at[slot], x_sem.at[slot])

        def y_copy(u):
            q, first = tokens_of(u)
            rs = pl.ds(pl.multiple_of(first + side * half, half), half)
            slot = lax.rem(u, n_hand)
            return pltpu.make_async_copy(y_ref.at[q, rs, :], yslot.at[slot], ysem.at[slot])

        @pl.when(is_first)
        def _():
            @pl.loop(0, n_unit)
            def _(u):
                x_copy(u).start()

        for cp in qkv_copies + w_copies:
            cp.start()

        barrier = pltpu.get_barrier_semaphore()
        for i in range(1, nz * ns):
            dz, dst = i % nz, i // nz
            pl.semaphore_signal(barrier, inc=1, device_id_type=MESH,
                                device_id={"model": lax.rem(z + dz, nz), "stage": lax.rem(st + dst, ns)})
        qkv_all[...] = jnp.zeros_like(qkv_all)
        lossacc[...] = jnp.zeros_like(lossacc)
        ga8[...] = jnp.zeros_like(ga8)
        gb8[...] = jnp.zeros_like(gb8)
        gains[...] = gain_ref[...].astype(F32)
        pl.semaphore_wait(barrier, nz * ns - 1)

        def gain_send():
            return rdma(gains, gain_next, gain_sem.at[0], gain_sem.at[1], stage=st - 1)

        @pl.when(st > 0)
        def _():
            gain_send().start()

        class Gather:
            def __init__(self, buf, slot, rsem, own_sem, far_sem, sslot):
                self.buf, self.slot, self.rsem = buf, slot, rsem
                self.own_sem, self.far_sem = own_sem.at[sslot], far_sem.at[sslot]

            def block(self, k):
                return self.buf.at[self.slot, rows_of(k), :]

            def inward(self, k):
                return rdma(self.block(k), self.block(k), self.own_sem, self.rsem.at[self.slot, k], model=inner_peer)

            def outward(self, k, sem):
                return rdma(self.block(k), self.block(k), sem, self.rsem.at[self.slot, n_block], model=outer_peer)

            def unit(self):
                ref = self.buf.at[self.slot]
                return rdma(ref, ref, self.own_sem, self.rsem.at[self.slot, n_block], model=outer_peer)

            def half_unit(self):
                ref = self.buf.at[self.slot, my_half, :]
                return rdma(ref, ref, self.far_sem, self.rsem.at[self.slot, n_block], model=outer_peer)

            def send(self, q):
                self.inward(near + q).start()
                self.outward(near + q, self.own_sem).start()

            def relay(self):
                @pl.when(inner)
                def _():
                    for q in quarters:
                        self.inward(far + q).wait_recv()
                        self.outward(far + q, self.far_sem).start()

            def collect(self):
                @pl.when(outer)
                def _():
                    self.unit().wait_recv()

            def own(self):
                @pl.when(inner)
                def _():
                    self.half_unit().wait_recv()

            def drain(self):
                @pl.when(inner)
                def _():
                    self.half_unit().wait_send()

            def drain_own(self):
                @pl.when(inner)
                def _():
                    self.unit().wait_send()

        def gather_a(u):
            return Gather(a_all, u, a_rs, a_si, a_so, lax.rem(u, n_gath))

        def gather_d(j, u):
            return Gather(d_all, u, d_rs, d_si, d_so, lax.rem(j, n_gath))

        def gather_b(u):
            return Gather(bbuf, lax.rem(u, n_gath), b_rs, b_si, b_so, lax.rem(u, n_gath))

        def gather_dm(j):
            return Gather(dmbuf, lax.rem(j, n_gath), dm_rs, dm_si, dm_so, lax.rem(j, n_gath))

        class Scatter:
            def __init__(self, op, u):
                self.op, self.ss, self.rs = op, lax.rem(u, n_send), lax.rem(u, n_recv)

            def in_copy(self, k, q):
                return rdma(send_p.at[self.op, self.ss, k], recv_o.at[self.op, self.rs, k],
                            rs_s.at[self.op, self.ss], rs_ro.at[self.op, self.rs, q], model=inner_peer)

            def cross_copy(self, k, q):
                return rdma(send_p.at[self.op, self.ss, k], recv_i.at[self.op, self.rs, q],
                            rs_s.at[self.op, self.ss], rs_ri.at[self.op, self.rs, q], model=inner_peer)

            def near_copies(self):
                return rdma(send_p.at[self.op, self.ss, pl.ds(near, n_part)], recv_o.at[self.op, self.rs, pl.ds(near, n_part)],
                            rs_s.at[self.op, self.ss], rs_ro.at[self.op, self.rs, n_part], model=inner_peer)

            def mine(self, k):
                return part[self.op, self.ss, rows_of(k), :]

            def start(self, j):
                @pl.when(outer)
                def _():
                    @pl.when(j >= n_send)
                    def _():
                        self.drain_outer()

                    for k, q in [(far + q, q) for q in quarters] + [(near + q, n_part) for q in quarters]:
                        send_p[self.op, self.ss, k] = self.mine(k).astype(BF16)
                        self.in_copy(k, q).start()

            def relay(self, j):
                @pl.when(inner)
                def _():
                    @pl.when(j >= n_send)
                    def _():
                        self.drain_inner()

                    for q in quarters:
                        k = far + q
                        self.in_copy(k, q).wait_recv()
                        send_p[self.op, self.ss, k] = (
                            self.mine(k) + recv_o[self.op, self.rs, k].astype(F32)).astype(BF16)
                        self.cross_copy(k, q).start()

            def total(self, q):
                k = near + q
                if q == 0:
                    self.near_copies().wait_recv()
                self.cross_copy(k, q).wait_recv()
                return (self.mine(k) + recv_o[self.op, self.rs, k].astype(F32)) + recv_i[self.op, self.rs, q].astype(F32)

            def drain_outer(self):
                ref = send_p.at[self.op, self.ss]
                rdma(ref, ref, rs_s.at[self.op, self.ss], rs_ro.at[self.op, self.rs, 0], model=inner_peer).wait_send()

            def drain_inner(self):
                self.near_copies().wait_send()

            def drain(self):
                @pl.when(outer)
                def _():
                    self.drain_outer()

                @pl.when(inner)
                def _():
                    self.drain_inner()

        def save(kind, src, src_slot, dst, j, u):
            return pltpu.make_async_copy(src.at[src_slot], dst.at[u],
                                         save_sem.at[kind, lax.rem(j, n_send if kind % 2 else n_gath)])

        def sslot(u):
            return lax.rem(u, n_send)

        def gslot(u):
            return lax.rem(u, n_gath)

        def q_rows(q):
            return pl.ds(q * row, row)

        def save_a(u):
            return save(0, a_all, u, a_out, u, u)

        def save_o(u):
            return save(1, ost, sslot(u), o_out, u, u)

        def save_b(u):
            return save(2, bbuf, gslot(u), b_out, u, u)

        def save_z(u):
            return save(3, zst, sslot(u), z_out, u, u)

        def save_d(j, u):
            return save(4, d_all, u, d_out, j, u)

        def save_du(j, u):
            return save(5, dust, sslot(j), du_out, j, u)

        def save_dm(j, u):
            return save(6, dmbuf, gslot(j), dm_out, j, u)

        def save_dqkv(j, u):
            return save(7, dqkvst, sslot(j), dqkv_out, j, u)

        gain_a = gains[0:1, :]
        gain_b = gains[1:2, :]

        def hand_h(u, j):
            s = lax.rem(j, n_hand)
            return rdma(hout.at[s], hslot.at[u], hand_sem.at[s, 1], hsem.at[u], stage=st + 1)

        def hand_quarter(back, u, j, q):
            s = lax.rem(j, n_hand)
            k = near + q
            src, buf, sems, own = (dout, d_all, d_rs, back_sem) if back else (aout, a_all, a_rs, hand_sem)
            for peer, side_sem, to in ((inner_peer, 0, k), (outer_peer, 0, n_block), (z, 1, n_block)):
                rdma(src.at[s, q_rows(q), :], buf.at[u, rows_of(k), :], own.at[s, side_sem], sems.at[u, to],
                     model=peer, stage=(st - 1) if back else (st + 1)).start()

        def hand_sent(back, u, j):
            s = lax.rem(j, n_hand)
            own = back_sem if back else hand_sem
            whole, part_of = d_all.at[u], hslot.at[u]
            rdma(whole, whole, own.at[s, 0], d_rs.at[u, 0], model=z).wait_send()
            last = part_of if back else whole
            rdma(last, last, own.at[s, 1], d_rs.at[u, 0], model=z).wait_send()

        def softmax_of(u, p, i):
            first = u - p
            cols = pl.ds(i * head_dim, head_dim)
            q = qkv_all[u, :, cols]
            k = qkv_all[pl.ds(first, per_seq), :, pl.ds(att_w + i * head_dim, head_dim)].reshape(seq_len, head_dim)
            v = qkv_all[pl.ds(first, per_seq), :, pl.ds(2 * att_w + i * head_dim, head_dim)].reshape(seq_len, head_dim)
            sc = dot_nt(q, k) * scale
            q_pos = p * tok + lax.broadcasted_iota(jnp.int32, sc.shape, 0)
            k_pos = lax.broadcasted_iota(jnp.int32, sc.shape, 1)
            sc = jnp.where(k_pos <= q_pos, sc, NEG_BIG)
            e = jnp.exp(sc - jnp.max(sc, axis=-1, keepdims=True))
            pr = e * (1.0 / jnp.sum(e, axis=-1, keepdims=True))
            return q, k, v, pr

        def fold(v):
            return jnp.sum(v.reshape(v.shape[0] // 8, 8, d_model), axis=0)

        def f_enter(j, u):
            @pl.when(is_first)
            def _():
                x_copy(u).wait()
                hslot[u] = a_all[u, my_half, :]
                for k in range(n_block):
                    rs = pl.ds(k * row, row)
                    h32 = a_all[u, rs, :].astype(F32)
                    a_all[u, rs, :] = (h32 * rms_inverse(h32) * gain_a).astype(BF16)

        def f_relay_a(j, u):
            @pl.when(st > 0)
            def _():
                @pl.when(j >= n_gath)
                def _():
                    gather_a(u).drain()

                gather_a(u).relay()

        def f_collect_a(j, u):
            @pl.when(st > 0)
            def _():
                gather_a(u).collect()
                gather_a(u).own()

        def f_attention(j, u):
            @pl.when(j == 0)
            def _():
                for cp in qkv_copies:
                    cp.wait()
                w_copies[0].wait()

            @pl.when(j >= n_gath)
            def _():
                save_a(u).wait()
                save_b(u).wait()
                gather_b(u).drain()
                gather_b(u).drain_own()

            @pl.when(j >= n_send)
            def _():
                save_o(u).wait()

            s = sslot(u)
            p = lax.rem(u, per_seq)
            save_a(u).start()
            qkv_all[u] = dot_nn(a_all[u], wqkv[...]).astype(BF16)
            for i in range(n_head):
                _, _, v, pr = softmax_of(u, p, i)
                ost[s, :, pl.ds(i * head_dim, head_dim)] = dot_nn(pr.astype(BF16), v).astype(BF16)
            save_o(u).start()
            part[0, s] = dot_nn(ost[s], wout[...])
            Scatter(0, u).start(j)

        def scatter_relay(op):
            def run(j, u):
                Scatter(op, j).relay(j)
            return run

        def f_middle(j, u):
            sc = Scatter(0, u)

            @pl.when(inner)
            def _():
                @pl.when(st > 0)
                def _():
                    rdma(hout.at[0], hslot.at[u], hand_sem.at[0, 1], hsem.at[u], stage=st).wait_recv()

                for q in quarters:
                    m = hslot[u, q_rows(q), :].astype(F32) + sc.total(q)
                    m_all[u, q_rows(q), :] = m
                    bbuf[gslot(u), rows_of(near + q), :] = (m * rms_inverse(m) * gain_b).astype(BF16)
                    gather_b(u).send(q)

        def f_relay_b(j, u):
            gather_b(u).relay()

        def f_collect_b(j, u):
            gather_b(u).collect()

        def f_mlp(j, u):
            @pl.when(j == 0)
            def _():
                w_copies[1].wait()
                w_copies[2].wait()

            s = sslot(u)
            @pl.when(j >= n_send)
            def _():
                save_z(u).wait()

            save_b(u).start()

            @pl.when(is_last & inner)
            def _():
                y_copy(u).start()

            u_all[u] = dot_nn(bbuf[gslot(u)], wup[...])

            for r in range(tok // sub_rows):
                rr = pl.ds(r * sub_rows, sub_rows)
                v = u_all[u, rr, :]
                th = jnp.tanh(GELU_K * (v + GELU_C * (v * v * v)))
                zst[s, rr, :] = (0.5 * v * (1.0 + th)).astype(BF16)

            save_z(u).start()
            part[1, s] = dot_nn(zst[s], wdown[...])
            Scatter(1, u).start(j)

        def f_leave(j, u):
            sc = Scatter(1, u)
            s = lax.rem(j, n_hand)

            @pl.when((j == 0) & (st < last_s))
            def _():
                gain_send().wait_recv()

            @pl.when(inner)
            def _():
                @pl.when(st < last_s)
                def _():
                    @pl.when(j >= n_hand)
                    def _():
                        hand_sent(False, u, j)

                @pl.when(is_last)
                def _():
                    y_copy(u).wait()

                for q in quarters:
                    h_new = (m_all[u, q_rows(q), :] + sc.total(q)).astype(BF16)
                    h32 = h_new.astype(F32)

                    @pl.when(st < last_s)
                    def _():
                        aout[s, q_rows(q), :] = (h32 * rms_inverse(h32) * gain_next[0:1, :]).astype(BF16)
                        hand_quarter(False, u, j, q)
                        hout[s, q_rows(q), :] = h_new

                    @pl.when(is_last)
                    def _():
                        diff = h32 - yslot[lax.rem(u, n_hand), q_rows(q), :].astype(F32)
                        d_all[u, rows_of(near + q), :] = (diff * inv_count).astype(BF16)
                        lossacc[...] += fold(diff * diff)

                @pl.when(st < last_s)
                def _():
                    hand_h(u, j).start()

        forward = (f_enter, f_relay_a, f_collect_a, f_attention, scatter_relay(0), f_middle, f_relay_b, f_collect_b, f_mlp,
                   scatter_relay(1), f_leave)

        def b_enter(j, u):
            @pl.when(is_last & inner)
            def _():
                @pl.when(j >= n_gath)
                def _():
                    gather_d(j, u).drain_own()

                for q in quarters:
                    gather_d(j, u).send(q)

        def b_relay_d(j, u):
            @pl.when(j >= n_gath)
            def _():
                gather_d(j, u).drain()

            gather_d(j, u).relay()

        def b_collect_d(j, u):
            gather_d(j, u).collect()

            @pl.when(st < last_s)
            def _():
                gather_d(j, u).own()

        def b_mlp(j, u):
            @pl.when(j >= n_gath)
            def _():
                save_d(j, u).wait()
                save_dm(j, u).wait()
                gather_dm(j).drain()
                gather_dm(j).drain_own()

            @pl.when(j >= n_send)
            def _():
                save_du(j, u).wait()

            s = sslot(j)
            save_d(j, u).start()
            part[2, s] = dot_nt(d_all[u], wdown[...])

            for r in range(tok // sub_rows):
                rr = pl.ds(r * sub_rows, sub_rows)
                v = u_all[u, rr, :]
                v2 = v * v
                th = jnp.tanh(GELU_K * (v + GELU_C * (v2 * v)))
                slope = 0.5 * (1.0 + th) + 0.5 * v * (1.0 - th * th) * (GELU_K * (1.0 + 3.0 * GELU_C * v2))
                dust[s, rr, :] = (part[2, s, rr, :] * slope).astype(BF16)

            save_du(j, u).start()
            part[2, s] = dot_nt(dust[s], wup[...])
            Scatter(2, j).start(j)

        def b_middle(j, u):
            sc = Scatter(2, j)

            @pl.when(inner)
            def _():
                for q in quarters:
                    m = m_all[u, q_rows(q), :]
                    inv = rms_inverse(m)
                    normed = m * inv
                    dn = sc.total(q)
                    gb8[...] += fold(dn * normed)
                    dn = dn * gain_b
                    dm = d_all[u, rows_of(near + q), :].astype(F32) + inv * (
                        dn - normed * jnp.mean(dn * normed, axis=-1, keepdims=True))
                    m_all[u, q_rows(q), :] = dm
                    dmbuf[gslot(j), rows_of(near + q), :] = dm.astype(BF16)
                    gather_dm(j).send(q)

        def b_relay_dm(j, u):
            gather_dm(j).relay()

        def b_collect_dm(j, u):
            gather_dm(j).collect()

        def b_attention(j, u):
            s = sslot(j)
            p = lax.rem(u, per_seq)
            @pl.when(j >= n_send)
            def _():
                save_dqkv(j, u).wait()

            save_dm(j, u).start()

            @pl.when(is_first)
            def _():
                x_again(j, u).start()

            @pl.when(p == per_seq - 1)
            def _():
                dkacc[...] = jnp.zeros_like(dkacc)
                dvacc[...] = jnp.zeros_like(dvacc)

            datt[...] = dot_nt(dmbuf[gslot(j)], wout[...]).astype(BF16)
            p_rows = pl.ds(pl.multiple_of(p * tok, tok), tok)
            for h in range(n_head):
                cols = pl.ds(h * head_dim, head_dim)
                q, k, v, pr = softmax_of(u, p, h)
                da = datt[:, cols]
                dp = dot_nt(da, v)
                ds = (pr * (dp - jnp.sum(pr * dp, axis=-1, keepdims=True)) * scale).astype(BF16)
                dvacc[:, cols] += dot_tn(pr.astype(BF16), da)
                dkacc[:, cols] += dot_tn(ds, q)
                dqkvst[s, :, cols] = dot_nn(ds, k).astype(BF16)
            dqkvst[s, :, pl.ds(att_w, att_w)] = dkacc[p_rows, :].astype(BF16)
            dqkvst[s, :, pl.ds(2 * att_w, att_w)] = dvacc[p_rows, :].astype(BF16)
            save_dqkv(j, u).start()
            part[3, s] = dot_nt(dqkvst[s], wqkv[...])

            @pl.when(st > 0)
            def _():
                Scatter(3, j).start(j)

        def b_relay_h(j, u):
            @pl.when(st > 0)
            def _():
                Scatter(3, j).relay(j)

        def b_leave(j, u):
            s = lax.rem(j, n_hand)

            @pl.when(st > 0)
            def _():
                sc = Scatter(3, j)

                @pl.when(inner)
                def _():
                    @pl.when(j >= n_hand)
                    def _():
                        hand_sent(True, u, j)

                    for q in quarters:
                        h32 = hslot[u, q_rows(q), :].astype(F32)
                        inv = rms_inverse(h32)
                        normed = h32 * inv
                        dn = sc.total(q)
                        ga8[...] += fold(dn * normed)
                        dg = dn * gain_a
                        dout[s, q_rows(q), :] = (m_all[u, q_rows(q), :] + inv * (
                            dg - normed * jnp.mean(dg * normed, axis=-1, keepdims=True))).astype(BF16)
                        hand_quarter(True, u, j, q)

            @pl.when(is_first)
            def _():
                x_again(j, u).wait()
                for k in range(n_block):
                    rs = pl.ds(k * row, row)
                    h32 = xtmp[sslot(j), rs, :].astype(F32)
                    ga8[...] += fold(part[3, sslot(j), rs, :] * (h32 * rms_inverse(h32)))

        backward = (b_enter, b_relay_d, b_collect_d, b_mlp, scatter_relay(2), b_middle, b_relay_dm, b_collect_dm,
                    b_attention, b_relay_h, b_leave)
        f_lag, b_lag = lags(False), lags(True)
        back_from = BACK_START + BACK_STEP * (last_s - st)

        def hand_finish(back):
            @pl.when(inner)
            def _():
                for j in range(n_unit - n_hand, n_unit):
                    hand_sent(back, j, j)

        def finish_forward():
            for j in range(n_unit - n_gath, n_unit):
                save_a(j).wait()
                save_b(j).wait()
                gather_b(j).drain()
                gather_b(j).drain_own()

                @pl.when(st > 0)
                def _():
                    gather_a(j).drain()

            for j in range(n_unit - n_send, n_unit):
                save_o(j).wait()
                save_z(j).wait()
                Scatter(0, j).drain()
                Scatter(1, j).drain()

            @pl.when(st < last_s)
            def _():
                hand_finish(False)

        def finish_backward():
            for j in range(n_unit - n_gath, n_unit):
                save_d(j, j).wait()
                save_dm(j, j).wait()
                gather_dm(j).drain()
                gather_dm(j).drain_own()
                gather_d(j, j).drain()

                @pl.when(is_last)
                def _():
                    gather_d(j, j).drain_own()

            for j in range(n_unit - n_send, n_unit):
                save_du(j, j).wait()
                save_dqkv(j, j).wait()
                Scatter(2, j).drain()

                @pl.when(st > 0)
                def _():
                    Scatter(3, j).drain()

            @pl.when(st > 0)
            def _():
                hand_finish(True)
                gain_send().wait_send()

        def turn(i, carry):
            @pl.when(i == n_unit + f_lag[-1])
            def _():
                finish_forward()

            for back, phase in ORDER:
                j = (i - back_from - b_lag[phase]) if back else (i - f_lag[phase])

                @pl.when((j >= 0) & (j < n_unit))
                def _():
                    if back:
                        seq = lax.div(j, per_seq)
                        backward[phase](j, 2 * seq * per_seq + (per_seq - 1) - j)
                    else:
                        forward[phase](j, j)
            return carry

        lax.fori_loop(0, n_unit + back_from + b_lag[-1], turn, 0)

        def loss_send():
            return rdma(lossacc, lossacc, loss_sem.at[0], loss_sem.at[1], stage=st - 1)

        @pl.when(is_last)
        def _():
            loss_send().start()

        @pl.when(st < last_s)
        def _():
            loss_send().wait_recv()

            @pl.when(st > 0)
            def _():
                loss_send().start()

        loss_row = jnp.sum(jnp.sum(lossacc[...], axis=0, keepdims=True), axis=1, keepdims=True)
        gx[z, 0:1, :] = jnp.sum(ga8[...], axis=0, keepdims=True)
        gx[z, 1:2, :] = jnp.sum(gb8[...], axis=0, keepdims=True)
        gx[z, 2:8, :] = jnp.broadcast_to(loss_row, (6, d_model))

        def gx_send(dz):
            return rdma(gx.at[z], gx.at[z], gx_s.at[dz], gx_r.at[z], model=lax.rem(z + dz, nz))

        def gx_recv(dz):
            k = lax.rem(z + dz, nz)
            return rdma(gx.at[k], gx.at[k], gx_s.at[dz], gx_r.at[k], model=k)

        for dz in range(1, nz):
            gx_send(dz).start()
        finish_backward()

        @pl.when(st > 0)
        def _():
            loss_send().wait_send()

        for dz in range(1, nz):
            gx_recv(dz).wait_recv()
        red_out[...] = gx[0] + gx[1] + gx[2] + gx[3]
        for dz in range(1, nz):
            gx_send(dz).wait_send()

    any_spec = pl.BlockSpec(memory_space=pl.ANY)
    vmem_spec = pl.BlockSpec(memory_space=pltpu.VMEM)

    def out(width):
        return jax.ShapeDtypeStruct((n_unit, tok, width), BF16)

    dma = pltpu.SemaphoreType.DMA
    vmem = pltpu.VMEM
    return pl.pallas_call(
        kernel,
        out_shape=(out(d_model), out(d_model), out(d_model), out(d_model), out(qkv_w), out(att_w), out(ff_w), out(ff_w),
                   jax.ShapeDtypeStruct((8, d_model), F32)),
        in_specs=[any_spec] * 6 + [vmem_spec],
        out_specs=(any_spec,) * 8 + (vmem_spec,),
        scratch_shapes=[
            vmem((d_model, qkv_w), BF16), vmem((att_w, d_model), BF16), vmem((d_model, ff_w), BF16), vmem((ff_w, d_model), BF16),
            vmem((n_unit, half, d_model), BF16), vmem((n_hand, half, d_model), BF16),
            vmem((n_unit, tok, d_model), BF16), vmem((n_unit, tok, d_model), BF16),
            vmem((n_gath, tok, d_model), BF16), vmem((n_gath, tok, d_model), BF16), vmem((n_send, tok, d_model), BF16),
            vmem((n_unit, tok, qkv_w), BF16), vmem((n_unit, tok, ff_w), F32), vmem((n_unit, half, d_model), F32),
            vmem((n_send, tok, att_w), BF16), vmem((n_send, tok, ff_w), BF16), vmem((n_send, tok, ff_w), BF16),
            vmem((n_send, tok, qkv_w), BF16), vmem((tok, att_w), BF16), vmem((4, n_send, tok, d_model), F32),
            vmem((4, n_recv, n_block, row, d_model), BF16), vmem((4, n_recv, n_part, row, d_model), BF16),
            vmem((4, n_send, n_block, row, d_model), BF16),
            vmem((n_hand, half, d_model), BF16), vmem((n_hand, half, d_model), BF16), vmem((n_hand, half, d_model), BF16),
            vmem((seq_len, att_w), F32), vmem((seq_len, att_w), F32),
            vmem((2, d_model), F32), vmem((2, d_model), F32),
            vmem((8, d_model), F32), vmem((8, d_model), F32), vmem((8, d_model), F32), vmem((nz, 8, d_model), F32),
            dma((n_slab + 3,)), dma((n_unit,)), dma((n_hand,)), dma((n_send,)), dma((2,)), dma((n_hand, 2)), dma((n_hand, 2)),
            dma((8, n_gath)),
            dma((n_unit, n_block + 1)), dma((n_unit, n_block + 1)), dma((n_gath,)), dma((n_gath,)), dma((n_gath,)), dma((n_gath,)),
            dma((n_gath, n_block + 1)), dma((n_gath, n_block + 1)),
            dma((n_gath,)), dma((n_gath,)), dma((n_gath,)), dma((n_gath,)),
            dma((4, n_recv, n_part + 1)), dma((4, n_recv, n_part)), dma((4, n_send)),
            dma((2,)), dma((nz,)), dma((nz,)),
        ],
        compiler_params=pltpu.CompilerParams(collective_id=0, has_side_effects=True, vmem_limit_bytes=67_043_328),
        name="layer_step",
    )(x_in, y_target, w_qkv, w_out, w_up, w_down, gain)


def weight_grads(o, dm, a, dqkv, b, du, zz, d, red, head_dim, loss_scale):
    n_tok = o.shape[0] * o.shape[1]
    rows = 256

    def flat(v):
        return v.reshape(n_tok, v.shape[2])

    acts = [flat(v) for v in (o, dm, a, dqkv, b, du, zz, d)]
    att_w, d_model = acts[0].shape[1], acts[1].shape[1]
    qkv_w, ff_w = acts[3].shape[1], acts[5].shape[1]
    n_slab = qkv_w // head_dim

    def kernel(*refs):
        src, red_ref, outs = refs[:8], refs[8], refs[9:13]
        gain_out, loss_out = refs[13:15]
        held, tiles = refs[15:23], refs[23:27]
        in_sem, out_sem = refs[27:]
        loads = [pltpu.make_async_copy(src[i], held[i], in_sem.at[i]) for i in range(8)]
        for cp in loads:
            cp.start()

        def stores(pair, i, slot):
            n = tiles[pair].shape[1]
            at = pl.ds(pl.multiple_of(i * n, n), n)
            sem = out_sem.at[pair, slot]
            if pair == 1:
                return [pltpu.make_async_copy(tiles[1].at[slot, :, pl.ds(k * head_dim, head_dim)], outs[1].at[k, at, :], sem)
                        for k in range(n_slab)]
            return [pltpu.make_async_copy(tiles[pair].at[slot], outs[pair].at[at, :], sem)]

        def finish(cps):
            for cp in cps:
                cp.wait()

        gain_out[...] = red_ref[0:2, :]
        loss_out[...] = red_ref[2:3, 0:1] * loss_scale
        counts = []
        for pair in range(4):
            loads[2 * pair].wait()
            loads[2 * pair + 1].wait()
            left, right, tile = held[2 * pair], held[2 * pair + 1], tiles[pair]
            n = tile.shape[1]
            count = left.shape[1] // n
            counts.append(count)

            def body(i, carry):
                slot = lax.rem(i, 2)

                @pl.when(i >= 2)
                def _():
                    finish(stores(pair, i - 2, slot))

                tile[slot] = dot_tn(left[:, pl.ds(pl.multiple_of(i * n, n), n)], right[...])
                for cp in stores(pair, i, slot):
                    cp.start()
                return carry

            lax.fori_loop(0, count, body, 0)
        for pair in range(4):
            for i in range(max(0, counts[pair] - 2), counts[pair]):
                finish(stores(pair, i, i % 2))

    any_spec = pl.BlockSpec(memory_space=pl.ANY)
    vmem_spec = pl.BlockSpec(memory_space=pltpu.VMEM)
    return pl.pallas_call(
        kernel,
        out_shape=(jax.ShapeDtypeStruct((att_w, d_model), F32), jax.ShapeDtypeStruct((n_slab, d_model, head_dim), F32),
                   jax.ShapeDtypeStruct((d_model, ff_w), F32), jax.ShapeDtypeStruct((ff_w, d_model), F32),
                   jax.ShapeDtypeStruct((2, d_model), F32), jax.ShapeDtypeStruct((1, 1), F32)),
        in_specs=[any_spec] * 8 + [vmem_spec],
        out_specs=(any_spec,) * 4 + (vmem_spec,) * 2,
        scratch_shapes=[pltpu.VMEM(v.shape, BF16) for v in acts] + [
            pltpu.VMEM((1, att_w, d_model), F32), pltpu.VMEM((2, rows, qkv_w), F32),
            pltpu.VMEM((2, rows, ff_w), F32), pltpu.VMEM((2, rows, d_model), F32),
            pltpu.SemaphoreType.DMA((8,)), pltpu.SemaphoreType.DMA((4, 2))],
        compiler_params=pltpu.CompilerParams(vmem_limit_bytes=67_043_328),
        name="weight_grads",
    )(*acts, red)


def solution(mesh):
    dims = dict(mesh.shape)

    def device_fn(x_in, y_target, w_qkv, w_out, w_up, w_down, norm_gain):
        n_batch, seq_len, d_model = x_in.shape
        heads, head_dim = w_qkv.shape[3], w_qkv.shape[4]
        a, b, d, dm, dqkv, o, zz, du, red = layer_step(
            dims, x_in, y_target,
            w_qkv[0].transpose(1, 2, 0, 3).reshape(3 * heads, d_model, head_dim),
            w_out[0].reshape(heads * head_dim, d_model), w_up[0], w_down[0], norm_gain[0])
        g_out, g_qkv, g_up, g_down, g_gain, loss = weight_grads(
            o, dm, a, dqkv, b, du, zz, d, red, head_dim, 0.5 / (n_batch * seq_len * d_model))
        grad_qkv = g_qkv.reshape(3, heads, d_model, head_dim).transpose(2, 0, 1, 3)[None]
        grad_out = g_out.reshape(1, heads, head_dim, d_model)
        grad_up = g_up[None]
        grad_down = g_down[None]
        return loss.reshape(1), grad_qkv, grad_out, grad_up, grad_down, g_gain[None]

    act_spec = P("data", None, None)
    weight_specs = (
        P("stage", None, None, "model", None),
        P("stage", "model", None, None),
        P("stage", None, "model"),
        P("stage", "model", None),
        P("stage", None, None),
    )
    grad_specs = (
        P(("data", "stage"), None, None, "model", None),
        P(("data", "stage"), "model", None, None),
        P(("data", "stage"), None, "model"),
        P(("data", "stage"), "model", None),
        P(("data", "stage"), None, None),
    )
    return jax.shard_map(
        device_fn,
        mesh=mesh,
        in_specs=(act_spec, act_spec) + weight_specs,
        out_specs=(P("data"),) + grad_specs,
        check_vma=False,
    )
```

```python
import jax
import jax.numpy as jnp
from jax import lax
from jax.experimental import pallas as pl
from jax.experimental.pallas import tpu as pltpu
from jax.sharding import PartitionSpec as P

NORM_EPS = 1e-6
NEG_BIG = -1e30
MESH = pl.DeviceIdType.MESH
GELU_K = 0.7978845608028654
GELU_C = 0.044715
F32 = jnp.float32
BF16 = jnp.bfloat16


def dot_nn(a, b):
    return lax.dot_general(a, b, (((1,), (0,)), ((), ())), preferred_element_type=F32)


def dot_nt(a, b):
    return lax.dot_general(a, b, (((1,), (1,)), ((), ())), preferred_element_type=F32)


def dot_tn(a, b):
    return lax.dot_general(a, b, (((0,), (0,)), ((), ())), preferred_element_type=F32)


def rms_inverse(v32):
    return lax.rsqrt(jnp.mean(v32 * v32, axis=-1, keepdims=True) + NORM_EPS)


ORDER = (
    (1, 6), (0, 3), (1, 2), (0, 7), (0, 9), (0, 5), (1, 3), (0, 8), (1, 9), (0, 1), (1, 1), (1, 7), (0, 0), (0,
    2), (1, 5), (1, 8), (0, 4), (0, 6), (1, 0), (0, 10), (1, 4), (1, 10),
)
BACK_START, BACK_STEP = 13, 10


def lags(back):
    place = {phase: i for i, (is_back, phase) in enumerate(ORDER) if is_back == int(back)}
    lag = [0]
    for phase in range(1, len(place)):
        lag.append(lag[-1] + (1 if place[phase] < place[phase - 1] else 0))
    return lag


def layer_step(dims, x_in, y_target, w_qkv, w_out, w_up, w_down, gain):
    nz, ns = dims["model"], dims["stage"]
    n_seq, seq_len, d_model = x_in.shape
    n_slab, _, head_dim = w_qkv.shape
    qkv_w = n_slab * head_dim
    att_w = w_out.shape[0]
    ff_w = w_up.shape[1]
    n_head = att_w // head_dim
    tok = 64
    n_part = 2
    row = tok // (2 * n_part)
    n_block = 2 * n_part
    per_seq = seq_len // tok
    n_unit = n_seq * per_seq
    scale = head_dim ** -0.5
    inv_count = 1.0 / (n_seq * seq_len * d_model)
    last_z, last_s = nz - 1, ns - 1
    sub_rows = 16
    half = tok // 2
    n_send, n_recv, n_gath, n_hand = 2, 3, 4, 2
    quarters = range(n_part)

    def kernel(x_ref, y_ref, wqkv_h, wout_h, wup_h, wdown_h, gain_ref,
               a_out, b_out, d_out, dm_out, dqkv_out, o_out, z_out, du_out, red_out,
               wqkv, wout, wup, wdown, hslot, yslot, a_all, d_all, bbuf, dmbuf, xtmp,
               qkv_all, u_all, m_all, ost, zst, dust, dqkvst, datt, part,
               recv_o, recv_i, send_p, hout, aout, dout, dkacc, dvacc,
               gains, gain_next, lossacc, ga8, gb8, gx,
               w_sem, hsem, ysem, x_sem, gain_sem, hand_sem, back_sem, save_sem,
               a_rs, d_rs, a_si, a_so, d_si, d_so, b_rs, dm_rs, b_si, b_so, dm_si, dm_so,
               rs_ro, rs_ri, rs_s, loss_sem, gx_s, gx_r):
        z = lax.axis_index("model")
        st = lax.axis_index("stage")
        is_first = st == 0
        is_last = st == last_s
        inner = (z > 0) & (z < last_z)
        outer = (z == 0) | (z == last_z)
        side = lax.div(z, 2)
        near = n_part * side
        far = n_part - near
        inner_peer = 1 + lax.rem(z, 2)
        outer_peer = last_z * side
        my_half = pl.ds(pl.multiple_of(side * half, half), half)

        def rdma(src, dst, ssem, rsem, **dev):
            return pltpu.make_async_remote_copy(src_ref=src, dst_ref=dst, send_sem=ssem, recv_sem=rsem,
                                                device_id=dev, device_id_type=MESH)

        def rows_of(k):
            return pl.ds(pl.multiple_of(k * row, row), row)

        qkv_copies = [pltpu.make_async_copy(wqkv_h.at[i], wqkv.at[:, pl.ds(i * head_dim, head_dim)], w_sem.at[i])
                      for i in range(n_slab)]
        w_copies = [pltpu.make_async_copy(src, dst, w_sem.at[n_slab + i])
                    for i, (src, dst) in enumerate(((wout_h, wout), (wup_h, wup), (wdown_h, wdown)))]

        def tokens_of(u):
            return lax.div(u, per_seq), pl.multiple_of(lax.rem(u, per_seq) * tok, tok)

        def x_copy(u):
            q, first = tokens_of(u)
            return pltpu.make_async_copy(x_ref.at[q, pl.ds(first, tok), :], a_all.at[u], hsem.at[u])

        def x_again(j, u):
            q, first = tokens_of(u)
            slot = lax.rem(j, n_send)
            return pltpu.make_async_copy(x_ref.at[q, pl.ds(first, tok), :], xtmp.at[slot], x_sem.at[slot])

        def y_copy(u):
            q, first = tokens_of(u)
            rs = pl.ds(pl.multiple_of(first + side * half, half), half)
            slot = lax.rem(u, n_hand)
            return pltpu.make_async_copy(y_ref.at[q, rs, :], yslot.at[slot], ysem.at[slot])

        @pl.when(is_first)
        def _():
            @pl.loop(0, n_unit)
            def _(u):
                x_copy(u).start()

        for cp in qkv_copies + w_copies:
            cp.start()

        barrier = pltpu.get_barrier_semaphore()
        for i in range(1, nz * ns):
            dz, dst = i % nz, i // nz
            pl.semaphore_signal(barrier, inc=1, device_id_type=MESH,
                                device_id={"model": lax.rem(z + dz, nz), "stage": lax.rem(st + dst, ns)})
        qkv_all[...] = jnp.zeros_like(qkv_all)
        dkacc[...] = jnp.zeros_like(dkacc)
        dvacc[...] = jnp.zeros_like(dvacc)
        lossacc[...] = jnp.zeros_like(lossacc)
        ga8[...] = jnp.zeros_like(ga8)
        gb8[...] = jnp.zeros_like(gb8)
        gains[...] = gain_ref[...].astype(F32)
        pl.semaphore_wait(barrier, nz * ns - 1)

        def gain_send():
            return rdma(gains, gain_next, gain_sem.at[0], gain_sem.at[1], stage=st - 1)

        @pl.when(st > 0)
        def _():
            gain_send().start()

        class Gather:
            def __init__(self, buf, slot, rsem, own_sem, far_sem, sslot):
                self.buf, self.slot, self.rsem = buf, slot, rsem
                self.own_sem, self.far_sem = own_sem.at[sslot], far_sem.at[sslot]

            def block(self, k):
                return self.buf.at[self.slot, rows_of(k), :]

            def inward(self, k):
                return rdma(self.block(k), self.block(k), self.own_sem, self.rsem.at[self.slot, k], model=inner_peer)

            def outward(self, k, sem):
                return rdma(self.block(k), self.block(k), sem, self.rsem.at[self.slot, n_block], model=outer_peer)

            def unit(self):
                ref = self.buf.at[self.slot]
                return rdma(ref, ref, self.own_sem, self.rsem.at[self.slot, n_block], model=outer_peer)

            def half_unit(self):
                ref = self.buf.at[self.slot, my_half, :]
                return rdma(ref, ref, self.far_sem, self.rsem.at[self.slot, n_block], model=outer_peer)

            def send(self, q):
                self.inward(near + q).start()
                self.outward(near + q, self.own_sem).start()

            def relay(self):
                @pl.when(inner)
                def _():
                    for q in quarters:
                        self.inward(far + q).wait_recv()
                        self.outward(far + q, self.far_sem).start()

            def collect(self):
                @pl.when(outer)
                def _():
                    self.unit().wait_recv()

            def own(self):
                @pl.when(inner)
                def _():
                    self.half_unit().wait_recv()

            def drain(self):
                @pl.when(inner)
                def _():
                    self.half_unit().wait_send()

            def drain_own(self):
                @pl.when(inner)
                def _():
                    self.unit().wait_send()

        def gather_a(u):
            return Gather(a_all, u, a_rs, a_si, a_so, lax.rem(u, n_gath))

        def gather_d(j, u):
            return Gather(d_all, u, d_rs, d_si, d_so, lax.rem(j, n_gath))

        def gather_b(u):
            return Gather(bbuf, lax.rem(u, n_gath), b_rs, b_si, b_so, lax.rem(u, n_gath))

        def gather_dm(j):
            return Gather(dmbuf, lax.rem(j, n_gath), dm_rs, dm_si, dm_so, lax.rem(j, n_gath))

        class Scatter:
            def __init__(self, op, u):
                self.op, self.ss, self.rs = op, lax.rem(u, n_send), lax.rem(u, n_recv)

            def in_copy(self, k, q):
                return rdma(send_p.at[self.op, self.ss, k], recv_o.at[self.op, self.rs, k],
                            rs_s.at[self.op, self.ss], rs_ro.at[self.op, self.rs, q], model=inner_peer)

            def cross_copy(self, k, q):
                return rdma(send_p.at[self.op, self.ss, k], recv_i.at[self.op, self.rs, q],
                            rs_s.at[self.op, self.ss], rs_ri.at[self.op, self.rs, q], model=inner_peer)

            def near_copies(self):
                return rdma(send_p.at[self.op, self.ss, pl.ds(near, n_part)], recv_o.at[self.op, self.rs, pl.ds(near, n_part)],
                            rs_s.at[self.op, self.ss], rs_ro.at[self.op, self.rs, n_part], model=inner_peer)

            def mine(self, k):
                return part[self.op, self.ss, rows_of(k), :]

            def start(self, j):
                @pl.when(outer)
                def _():
                    @pl.when(j >= n_send)
                    def _():
                        self.drain_outer()

                    for k, q in [(far + q, q) for q in quarters] + [(near + q, n_part) for q in quarters]:
                        send_p[self.op, self.ss, k] = self.mine(k).astype(BF16)
                        self.in_copy(k, q).start()

            def relay(self, j):
                @pl.when(inner)
                def _():
                    @pl.when(j >= n_send)
                    def _():
                        self.drain_inner()

                    for q in quarters:
                        k = far + q
                        self.in_copy(k, q).wait_recv()
                        send_p[self.op, self.ss, k] = (
                            self.mine(k) + recv_o[self.op, self.rs, k].astype(F32)).astype(BF16)
                        self.cross_copy(k, q).start()

            def total(self, q):
                k = near + q
                if q == 0:
                    self.near_copies().wait_recv()
                self.cross_copy(k, q).wait_recv()
                return (self.mine(k) + recv_o[self.op, self.rs, k].astype(F32)) + recv_i[self.op, self.rs, q].astype(F32)

            def drain_outer(self):
                ref = send_p.at[self.op, self.ss]
                rdma(ref, ref, rs_s.at[self.op, self.ss], rs_ro.at[self.op, self.rs, 0], model=inner_peer).wait_send()

            def drain_inner(self):
                self.near_copies().wait_send()

            def drain(self):
                @pl.when(outer)
                def _():
                    self.drain_outer()

                @pl.when(inner)
                def _():
                    self.drain_inner()

        def save(kind, src, src_slot, dst, j, u):
            return pltpu.make_async_copy(src.at[src_slot], dst.at[u],
                                         save_sem.at[kind, lax.rem(j, n_send if kind % 2 else n_gath)])

        def sslot(u):
            return lax.rem(u, n_send)

        def gslot(u):
            return lax.rem(u, n_gath)

        def q_rows(q):
            return pl.ds(q * row, row)

        def save_a(u):
            return save(0, a_all, u, a_out, u, u)

        def save_o(u):
            return save(1, ost, sslot(u), o_out, u, u)

        def save_b(u):
            return save(2, bbuf, gslot(u), b_out, u, u)

        def save_z(u):
            return save(3, zst, sslot(u), z_out, u, u)

        def save_d(j, u):
            return save(4, d_all, u, d_out, j, u)

        def save_du(j, u):
            return save(5, dust, sslot(j), du_out, j, u)

        def save_dm(j, u):
            return save(6, dmbuf, gslot(j), dm_out, j, u)

        def save_dqkv(j, u):
            return save(7, dqkvst, sslot(j), dqkv_out, j, u)

        gain_a = gains[0:1, :]
        gain_b = gains[1:2, :]

        def hand_h(u, j):
            s = lax.rem(j, n_hand)
            return rdma(hout.at[s], hslot.at[u], hand_sem.at[s, 1], hsem.at[u], stage=st + 1)

        def hand_quarter(back, u, j, q):
            s = lax.rem(j, n_hand)
            k = near + q
            src, buf, sems, own = (dout, d_all, d_rs, back_sem) if back else (aout, a_all, a_rs, hand_sem)
            for peer, side_sem, to in ((inner_peer, 0, k), (outer_peer, 0, n_block), (z, 1, n_block)):
                rdma(src.at[s, q_rows(q), :], buf.at[u, rows_of(k), :], own.at[s, side_sem], sems.at[u, to],
                     model=peer, stage=(st - 1) if back else (st + 1)).start()

        def hand_sent(back, u, j):
            s = lax.rem(j, n_hand)
            own = back_sem if back else hand_sem
            whole, part_of = d_all.at[u], hslot.at[u]
            rdma(whole, whole, own.at[s, 0], d_rs.at[u, 0], model=z).wait_send()
            last = part_of if back else whole
            rdma(last, last, own.at[s, 1], d_rs.at[u, 0], model=z).wait_send()

        def softmax_of(u, p, i):
            first = u - p
            cols = pl.ds(i * head_dim, head_dim)
            q = qkv_all[u, :, cols]
            k = qkv_all[pl.ds(first, per_seq), :, pl.ds(att_w + i * head_dim, head_dim)].reshape(seq_len, head_dim)
            v = qkv_all[pl.ds(first, per_seq), :, pl.ds(2 * att_w + i * head_dim, head_dim)].reshape(seq_len, head_dim)
            sc = dot_nt(q, k) * scale
            q_pos = p * tok + lax.broadcasted_iota(jnp.int32, sc.shape, 0)
            k_pos = lax.broadcasted_iota(jnp.int32, sc.shape, 1)
            sc = jnp.where(k_pos <= q_pos, sc, NEG_BIG)
            e = jnp.exp(sc - jnp.max(sc, axis=-1, keepdims=True))
            pr = e * (1.0 / jnp.sum(e, axis=-1, keepdims=True))
            return q, k, v, pr

        def fold(v):
            return jnp.sum(v.reshape(v.shape[0] // 8, 8, d_model), axis=0)

        def f_enter(j, u):
            @pl.when(is_first)
            def _():
                x_copy(u).wait()
                hslot[u] = a_all[u, my_half, :]
                for k in range(n_block):
                    rs = pl.ds(k * row, row)
                    h32 = a_all[u, rs, :].astype(F32)
                    a_all[u, rs, :] = (h32 * rms_inverse(h32) * gain_a).astype(BF16)

        def f_relay_a(j, u):
            @pl.when(st > 0)
            def _():
                @pl.when(j >= n_gath)
                def _():
                    gather_a(u).drain()

                gather_a(u).relay()

        def f_collect_a(j, u):
            @pl.when(st > 0)
            def _():
                gather_a(u).collect()
                gather_a(u).own()

        def f_attention(j, u):
            @pl.when(j == 0)
            def _():
                for cp in qkv_copies:
                    cp.wait()
                w_copies[0].wait()

            @pl.when(j >= n_gath)
            def _():
                save_a(u).wait()
                save_b(u).wait()
                gather_b(u).drain()
                gather_b(u).drain_own()

            @pl.when(j >= n_send)
            def _():
                save_o(u).wait()

            s = sslot(u)
            p = lax.rem(u, per_seq)
            save_a(u).start()
            qkv_all[u] = dot_nn(a_all[u], wqkv[...]).astype(BF16)
            for i in range(n_head):
                _, _, v, pr = softmax_of(u, p, i)
                ost[s, :, pl.ds(i * head_dim, head_dim)] = dot_nn(pr.astype(BF16), v).astype(BF16)
            save_o(u).start()
            part[0, s] = dot_nn(ost[s], wout[...])
            Scatter(0, u).start(j)

        def scatter_relay(op):
            def run(j, u):
                Scatter(op, j).relay(j)
            return run

        def f_middle(j, u):
            sc = Scatter(0, u)

            @pl.when(inner)
            def _():
                @pl.when(st > 0)
                def _():
                    rdma(hout.at[0], hslot.at[u], hand_sem.at[0, 1], hsem.at[u], stage=st).wait_recv()

                for q in quarters:
                    m = hslot[u, q_rows(q), :].astype(F32) + sc.total(q)
                    m_all[u, q_rows(q), :] = m
                    bbuf[gslot(u), rows_of(near + q), :] = (m * rms_inverse(m) * gain_b).astype(BF16)
                    gather_b(u).send(q)

        def f_relay_b(j, u):
            gather_b(u).relay()

        def f_collect_b(j, u):
            gather_b(u).collect()

        def f_mlp(j, u):
            @pl.when(j == 0)
            def _():
                w_copies[1].wait()
                w_copies[2].wait()

            s = sslot(u)
            @pl.when(j >= n_send)
            def _():
                save_z(u).wait()

            save_b(u).start()

            @pl.when(is_last & inner)
            def _():
                y_copy(u).start()

            u_all[u] = dot_nn(bbuf[gslot(u)], wup[...])

            for r in range(tok // sub_rows):
                rr = pl.ds(r * sub_rows, sub_rows)
                v = u_all[u, rr, :]
                th = jnp.tanh(GELU_K * (v + GELU_C * (v * v * v)))
                zst[s, rr, :] = (0.5 * v * (1.0 + th)).astype(BF16)

            save_z(u).start()
            part[1, s] = dot_nn(zst[s], wdown[...])
            Scatter(1, u).start(j)

        def f_leave(j, u):
            sc = Scatter(1, u)
            s = lax.rem(j, n_hand)

            @pl.when((j == 0) & (st < last_s))
            def _():
                gain_send().wait_recv()

            @pl.when(inner)
            def _():
                @pl.when(st < last_s)
                def _():
                    @pl.when(j >= n_hand)
                    def _():
                        hand_sent(False, u, j)

                @pl.when(is_last)
                def _():
                    y_copy(u).wait()

                for q in quarters:
                    h_new = (m_all[u, q_rows(q), :] + sc.total(q)).astype(BF16)
                    h32 = h_new.astype(F32)

                    @pl.when(st < last_s)
                    def _():
                        aout[s, q_rows(q), :] = (h32 * rms_inverse(h32) * gain_next[0:1, :]).astype(BF16)
                        hand_quarter(False, u, j, q)
                        hout[s, q_rows(q), :] = h_new

                    @pl.when(is_last)
                    def _():
                        diff = h32 - yslot[lax.rem(u, n_hand), q_rows(q), :].astype(F32)
                        d_all[u, rows_of(near + q), :] = (diff * inv_count).astype(BF16)
                        lossacc[...] += fold(diff * diff)

                @pl.when(st < last_s)
                def _():
                    hand_h(u, j).start()

        forward = (f_enter, f_relay_a, f_collect_a, f_attention, scatter_relay(0), f_middle, f_relay_b, f_collect_b, f_mlp,
                   scatter_relay(1), f_leave)

        def b_enter(j, u):
            @pl.when(is_last & inner)
            def _():
                @pl.when(j >= n_gath)
                def _():
                    gather_d(j, u).drain_own()

                for q in quarters:
                    gather_d(j, u).send(q)

        def b_relay_d(j, u):
            @pl.when(j >= n_gath)
            def _():
                gather_d(j, u).drain()

            gather_d(j, u).relay()

        def b_collect_d(j, u):
            gather_d(j, u).collect()

            @pl.when(st < last_s)
            def _():
                gather_d(j, u).own()

        def b_mlp(j, u):
            @pl.when(j >= n_gath)
            def _():
                save_d(j, u).wait()
                save_dm(j, u).wait()
                gather_dm(j).drain()
                gather_dm(j).drain_own()

            @pl.when(j >= n_send)
            def _():
                save_du(j, u).wait()

            s = sslot(j)
            save_d(j, u).start()
            part[2, s] = dot_nt(d_all[u], wdown[...])

            for r in range(tok // sub_rows):
                rr = pl.ds(r * sub_rows, sub_rows)
                v = u_all[u, rr, :]
                v2 = v * v
                th = jnp.tanh(GELU_K * (v + GELU_C * (v2 * v)))
                slope = 0.5 * (1.0 + th) + 0.5 * v * (1.0 - th * th) * (GELU_K * (1.0 + 3.0 * GELU_C * v2))
                dust[s, rr, :] = (part[2, s, rr, :] * slope).astype(BF16)

            save_du(j, u).start()
            part[2, s] = dot_nt(dust[s], wup[...])
            Scatter(2, j).start(j)

        def b_middle(j, u):
            sc = Scatter(2, j)

            @pl.when(inner)
            def _():
                for q in quarters:
                    m = m_all[u, q_rows(q), :]
                    inv = rms_inverse(m)
                    normed = m * inv
                    dn = sc.total(q)
                    gb8[...] += fold(dn * normed)
                    dn = dn * gain_b
                    dm = d_all[u, rows_of(near + q), :].astype(F32) + inv * (
                        dn - normed * jnp.mean(dn * normed, axis=-1, keepdims=True))
                    m_all[u, q_rows(q), :] = dm
                    dmbuf[gslot(j), rows_of(near + q), :] = dm.astype(BF16)
                    gather_dm(j).send(q)

        def b_relay_dm(j, u):
            gather_dm(j).relay()

        def b_collect_dm(j, u):
            gather_dm(j).collect()

        def b_attention(j, u):
            s = sslot(j)
            p = lax.rem(u, per_seq)
            @pl.when(j >= n_send)
            def _():
                save_dqkv(j, u).wait()

            save_dm(j, u).start()

            @pl.when(is_first)
            def _():
                x_again(j, u).start()

            datt[...] = dot_nt(dmbuf[gslot(j)], wout[...]).astype(BF16)
            p_rows = pl.ds(pl.multiple_of(p * tok, tok), tok)
            for h in range(n_head):
                cols = pl.ds(h * head_dim, head_dim)
                q, k, v, pr = softmax_of(u, p, h)
                da = datt[:, cols]
                dp = dot_nt(da, v)
                ds = (pr * (dp - jnp.sum(pr * dp, axis=-1, keepdims=True)) * scale).astype(BF16)
                dvacc[:, cols] += dot_tn(pr.astype(BF16), da)
                dkacc[:, cols] += dot_tn(ds, q)
                dqkvst[s, :, cols] = dot_nn(ds, k).astype(BF16)
            dqkvst[s, :, pl.ds(att_w, att_w)] = dkacc[p_rows, :].astype(BF16)
            dqkvst[s, :, pl.ds(2 * att_w, att_w)] = dvacc[p_rows, :].astype(BF16)
            dkacc[p_rows, :] = jnp.zeros((tok, att_w), F32)
            dvacc[p_rows, :] = jnp.zeros((tok, att_w), F32)
            save_dqkv(j, u).start()
            part[3, s] = dot_nt(dqkvst[s], wqkv[...])

            @pl.when(st > 0)
            def _():
                Scatter(3, j).start(j)

        def b_relay_h(j, u):
            @pl.when(st > 0)
            def _():
                Scatter(3, j).relay(j)

        def b_leave(j, u):
            s = lax.rem(j, n_hand)

            @pl.when(st > 0)
            def _():
                sc = Scatter(3, j)

                @pl.when(inner)
                def _():
                    @pl.when(j >= n_hand)
                    def _():
                        hand_sent(True, u, j)

                    for q in quarters:
                        h32 = hslot[u, q_rows(q), :].astype(F32)
                        inv = rms_inverse(h32)
                        normed = h32 * inv
                        dn = sc.total(q)
                        ga8[...] += fold(dn * normed)
                        dg = dn * gain_a
                        dout[s, q_rows(q), :] = (m_all[u, q_rows(q), :] + inv * (
                            dg - normed * jnp.mean(dg * normed, axis=-1, keepdims=True))).astype(BF16)
                        hand_quarter(True, u, j, q)

            @pl.when(is_first)
            def _():
                x_again(j, u).wait()
                for k in range(n_block):
                    rs = pl.ds(k * row, row)
                    h32 = xtmp[sslot(j), rs, :].astype(F32)
                    ga8[...] += fold(part[3, sslot(j), rs, :] * (h32 * rms_inverse(h32)))

        backward = (b_enter, b_relay_d, b_collect_d, b_mlp, scatter_relay(2), b_middle, b_relay_dm, b_collect_dm,
                    b_attention, b_relay_h, b_leave)
        f_lag, b_lag = lags(False), lags(True)
        back_from = BACK_START + BACK_STEP * (last_s - st)

        def hand_finish(back):
            @pl.when(inner)
            def _():
                for j in range(n_unit - n_hand, n_unit):
                    hand_sent(back, j, j)

        def finish_forward():
            for j in range(n_unit - n_gath, n_unit):
                save_a(j).wait()
                save_b(j).wait()
                gather_b(j).drain()
                gather_b(j).drain_own()

                @pl.when(st > 0)
                def _():
                    gather_a(j).drain()

            for j in range(n_unit - n_send, n_unit):
                save_o(j).wait()
                save_z(j).wait()
                Scatter(0, j).drain()
                Scatter(1, j).drain()

            @pl.when(st < last_s)
            def _():
                hand_finish(False)

        def finish_backward():
            for j in range(n_unit - n_gath, n_unit):
                save_d(j, j).wait()
                save_dm(j, j).wait()
                gather_dm(j).drain()
                gather_dm(j).drain_own()
                gather_d(j, j).drain()

                @pl.when(is_last)
                def _():
                    gather_d(j, j).drain_own()

            for j in range(n_unit - n_send, n_unit):
                save_du(j, j).wait()
                save_dqkv(j, j).wait()
                Scatter(2, j).drain()

                @pl.when(st > 0)
                def _():
                    Scatter(3, j).drain()

            @pl.when(st > 0)
            def _():
                hand_finish(True)
                gain_send().wait_send()

        def turn(i, carry):
            @pl.when(i == n_unit + f_lag[-1])
            def _():
                finish_forward()

            for back, phase in ORDER:
                j = (i - back_from - b_lag[phase]) if back else (i - f_lag[phase])

                @pl.when((j >= 0) & (j < n_unit))
                def _():
                    if back:
                        seq = lax.div(j, per_seq)
                        backward[phase](j, 2 * seq * per_seq + (per_seq - 1) - j)
                    else:
                        forward[phase](j, j)
            return carry

        lax.fori_loop(0, n_unit + back_from + b_lag[-1], turn, 0)

        def loss_send():
            return rdma(lossacc, lossacc, loss_sem.at[0], loss_sem.at[1], stage=st - 1)

        @pl.when(is_last)
        def _():
            loss_send().start()

        @pl.when(st < last_s)
        def _():
            loss_send().wait_recv()

            @pl.when(st > 0)
            def _():
                loss_send().start()

        loss_row = jnp.sum(jnp.sum(lossacc[...], axis=0, keepdims=True), axis=1, keepdims=True)
        gx[z, 0:1, :] = jnp.sum(ga8[...], axis=0, keepdims=True)
        gx[z, 1:2, :] = jnp.sum(gb8[...], axis=0, keepdims=True)
        gx[z, 2:8, :] = jnp.broadcast_to(loss_row, (6, d_model))

        def gx_send(dz):
            return rdma(gx.at[z], gx.at[z], gx_s.at[dz], gx_r.at[z], model=lax.rem(z + dz, nz))

        def gx_recv(dz):
            k = lax.rem(z + dz, nz)
            return rdma(gx.at[k], gx.at[k], gx_s.at[dz], gx_r.at[k], model=k)

        for dz in range(1, nz):
            gx_send(dz).start()
        finish_backward()

        @pl.when(st > 0)
        def _():
            loss_send().wait_send()

        for dz in range(1, nz):
            gx_recv(dz).wait_recv()
        red_out[...] = gx[0] + gx[1] + gx[2] + gx[3]
        for dz in range(1, nz):
            gx_send(dz).wait_send()

    any_spec = pl.BlockSpec(memory_space=pl.ANY)
    vmem_spec = pl.BlockSpec(memory_space=pltpu.VMEM)

    def out(width):
        return jax.ShapeDtypeStruct((n_unit, tok, width), BF16)

    dma = pltpu.SemaphoreType.DMA
    vmem = pltpu.VMEM
    return pl.pallas_call(
        kernel,
        out_shape=(out(d_model), out(d_model), out(d_model), out(d_model), out(qkv_w), out(att_w), out(ff_w), out(ff_w),
                   jax.ShapeDtypeStruct((8, d_model), F32)),
        in_specs=[any_spec] * 6 + [vmem_spec],
        out_specs=(any_spec,) * 8 + (vmem_spec,),
        scratch_shapes=[
            vmem((d_model, qkv_w), BF16), vmem((att_w, d_model), BF16), vmem((d_model, ff_w), BF16), vmem((ff_w, d_model), BF16),
            vmem((n_unit, half, d_model), BF16), vmem((n_hand, half, d_model), BF16),
            vmem((n_unit, tok, d_model), BF16), vmem((n_unit, tok, d_model), BF16),
            vmem((n_gath, tok, d_model), BF16), vmem((n_gath, tok, d_model), BF16), vmem((n_send, tok, d_model), BF16),
            vmem((n_unit, tok, qkv_w), BF16), vmem((n_unit, tok, ff_w), F32), vmem((n_unit, half, d_model), F32),
            vmem((n_send, tok, att_w), BF16), vmem((n_send, tok, ff_w), BF16), vmem((n_send, tok, ff_w), BF16),
            vmem((n_send, tok, qkv_w), BF16), vmem((tok, att_w), BF16), vmem((4, n_send, tok, d_model), F32),
            vmem((4, n_recv, n_block, row, d_model), BF16), vmem((4, n_recv, n_part, row, d_model), BF16),
            vmem((4, n_send, n_block, row, d_model), BF16),
            vmem((n_hand, half, d_model), BF16), vmem((n_hand, half, d_model), BF16), vmem((n_hand, half, d_model), BF16),
            vmem((seq_len, att_w), F32), vmem((seq_len, att_w), F32),
            vmem((2, d_model), F32), vmem((2, d_model), F32),
            vmem((8, d_model), F32), vmem((8, d_model), F32), vmem((8, d_model), F32), vmem((nz, 8, d_model), F32),
            dma((n_slab + 3,)), dma((n_unit,)), dma((n_hand,)), dma((n_send,)), dma((2,)), dma((n_hand, 2)), dma((n_hand, 2)),
            dma((8, n_gath)),
            dma((n_unit, n_block + 1)), dma((n_unit, n_block + 1)), dma((n_gath,)), dma((n_gath,)), dma((n_gath,)), dma((n_gath,)),
            dma((n_gath, n_block + 1)), dma((n_gath, n_block + 1)),
            dma((n_gath,)), dma((n_gath,)), dma((n_gath,)), dma((n_gath,)),
            dma((4, n_recv, n_part + 1)), dma((4, n_recv, n_part)), dma((4, n_send)),
            dma((2,)), dma((nz,)), dma((nz,)),
        ],
        compiler_params=pltpu.CompilerParams(collective_id=0, has_side_effects=True, vmem_limit_bytes=67_043_328),
        name="layer_step",
    )(x_in, y_target, w_qkv, w_out, w_up, w_down, gain)


def weight_grads(o, dm, a, dqkv, b, du, zz, d, red, head_dim, loss_scale):
    n_tok = o.shape[0] * o.shape[1]
    rows = 256

    def flat(v):
        return v.reshape(n_tok, v.shape[2])

    acts = [flat(v) for v in (o, dm, a, dqkv, b, du, zz, d)]
    att_w, d_model = acts[0].shape[1], acts[1].shape[1]
    qkv_w, ff_w = acts[3].shape[1], acts[5].shape[1]
    n_slab = qkv_w // head_dim

    def kernel(*refs):
        src, red_ref, outs = refs[:8], refs[8], refs[9:13]
        gain_out, loss_out = refs[13:15]
        held, tiles = refs[15:23], refs[23:27]
        in_sem, out_sem = refs[27:]
        loads = [pltpu.make_async_copy(src[i], held[i], in_sem.at[i]) for i in range(8)]
        for cp in loads:
            cp.start()

        def stores(pair, i, slot):
            n = tiles[pair].shape[1]
            at = pl.ds(pl.multiple_of(i * n, n), n)
            sem = out_sem.at[pair, slot]
            if pair == 1:
                return [pltpu.make_async_copy(tiles[1].at[slot, :, pl.ds(k * head_dim, head_dim)], outs[1].at[k, at, :], sem)
                        for k in range(n_slab)]
            return [pltpu.make_async_copy(tiles[pair].at[slot], outs[pair].at[at, :], sem)]

        def finish(cps):
            for cp in cps:
                cp.wait()

        gain_out[...] = red_ref[0:2, :]
        loss_out[...] = red_ref[2:3, 0:1] * loss_scale
        counts = []
        for pair in range(4):
            loads[2 * pair].wait()
            loads[2 * pair + 1].wait()
            left, right, tile = held[2 * pair], held[2 * pair + 1], tiles[pair]
            n = tile.shape[1]
            count = left.shape[1] // n
            counts.append(count)

            def body(i, carry):
                slot = lax.rem(i, 2)

                @pl.when(i >= 2)
                def _():
                    finish(stores(pair, i - 2, slot))

                tile[slot] = dot_tn(left[:, pl.ds(pl.multiple_of(i * n, n), n)], right[...])
                for cp in stores(pair, i, slot):
                    cp.start()
                return carry

            lax.fori_loop(0, count, body, 0)
        for pair in range(4):
            for i in range(max(0, counts[pair] - 2), counts[pair]):
                finish(stores(pair, i, i % 2))

    any_spec = pl.BlockSpec(memory_space=pl.ANY)
    vmem_spec = pl.BlockSpec(memory_space=pltpu.VMEM)
    return pl.pallas_call(
        kernel,
        out_shape=(jax.ShapeDtypeStruct((att_w, d_model), F32), jax.ShapeDtypeStruct((n_slab, d_model, head_dim), F32),
                   jax.ShapeDtypeStruct((d_model, ff_w), F32), jax.ShapeDtypeStruct((ff_w, d_model), F32),
                   jax.ShapeDtypeStruct((2, d_model), F32), jax.ShapeDtypeStruct((1, 1), F32)),
        in_specs=[any_spec] * 8 + [vmem_spec],
        out_specs=(any_spec,) * 4 + (vmem_spec,) * 2,
        scratch_shapes=[pltpu.VMEM(v.shape, BF16) for v in acts] + [
            pltpu.VMEM((1, att_w, d_model), F32), pltpu.VMEM((2, rows, qkv_w), F32),
            pltpu.VMEM((2, rows, ff_w), F32), pltpu.VMEM((2, rows, d_model), F32),
            pltpu.SemaphoreType.DMA((8,)), pltpu.SemaphoreType.DMA((4, 2))],
        compiler_params=pltpu.CompilerParams(vmem_limit_bytes=67_043_328),
        name="weight_grads",
    )(*acts, red)


def solution(mesh):
    dims = dict(mesh.shape)

    def device_fn(x_in, y_target, w_qkv, w_out, w_up, w_down, norm_gain):
        n_batch, seq_len, d_model = x_in.shape
        heads, head_dim = w_qkv.shape[3], w_qkv.shape[4]
        a, b, d, dm, dqkv, o, zz, du, red = layer_step(
            dims, x_in, y_target,
            w_qkv[0].transpose(1, 2, 0, 3).reshape(3 * heads, d_model, head_dim),
            w_out[0].reshape(heads * head_dim, d_model), w_up[0], w_down[0], norm_gain[0])
        g_out, g_qkv, g_up, g_down, g_gain, loss = weight_grads(
            o, dm, a, dqkv, b, du, zz, d, red, head_dim, 0.5 / (n_batch * seq_len * d_model))
        grad_qkv = g_qkv.reshape(3, heads, d_model, head_dim).transpose(2, 0, 1, 3)[None]
        grad_out = g_out.reshape(1, heads, head_dim, d_model)
        grad_up = g_up[None]
        grad_down = g_down[None]
        return loss.reshape(1), grad_qkv, grad_out, grad_up, grad_down, g_gain[None]

    act_spec = P("data", None, None)
    weight_specs = (
        P("stage", None, None, "model", None),
        P("stage", "model", None, None),
        P("stage", None, "model"),
        P("stage", "model", None),
        P("stage", None, None),
    )
    grad_specs = (
        P(("data", "stage"), None, None, "model", None),
        P(("data", "stage"), "model", None, None),
        P(("data", "stage"), None, "model"),
        P(("data", "stage"), "model", None),
        P(("data", "stage"), None, None),
    )
    return jax.shard_map(
        device_fn,
        mesh=mesh,
        in_specs=(act_spec, act_spec) + weight_specs,
        out_specs=(P("data"),) + grad_specs,
        check_vma=False,
    )
```
